32 devices in a mesh: seq: 8 (over y, x, core), head: 4 (over z).
Axes of the slice: x: 2, y: 2, z: 4, core: 2. Of those that a mesh axis runs over, the one named last changes fastest.
Arguments:
- hidden_in: bfloat16 [4096, 1536], P('seq', 'head'), may hold values from -6 to 6
- seq_lengths: int32 [8], replicated, may hold values from 1 to 1536, 4096 in all
- norm_gain: float32 [1536], P('head'), may hold values from 0.5 to 1.5
- w_z: bfloat16 [1536, 3072], P(None, 'head'), may hold values from -0.15625 to 0.15625
- w_x: bfloat16 [1536, 3072], P(None, 'head'), may hold values from -0.15625 to 0.15625
- w_bc: bfloat16 [1536, 256], P('head'), may hold values from -0.15625 to 0.15625
- w_dt: bfloat16 [1536, 48], P(None, 'head'), may hold values from -0.15625 to 0.15625
- conv_x_w: float32 [4, 3072], P(None, 'head'), may hold values from -3 to 3
- conv_x_b: float32 [3072], P('head'), may hold values from -3 to 3
- conv_bc_w: float32 [4, 256], replicated, may hold values from -3 to 3
- conv_bc_b: float32 [256], replicated, may hold values from -3 to 3
- dt_bias: float32 [48], P('head'), may hold values from -2 to 0.5
- a_log: float32 [48], P('head'), may hold values from -9 to -3
- d_skip: float32 [48], P('head'), may hold values from 0.5 to 2
- gate_gain: float32 [3072], P('head'), may hold values from 0.5 to 1.5
- w_out: bfloat16 [3072, 1536], P('head'), may hold values from -0.109375 to 0.109375
- cotangent: bfloat16 [4096, 1536], P('seq', 'head'), may hold values from -6 to 6
Outputs:
- layer_out: bfloat16 [4096, 1536], P('seq', 'head')
- grad_in: float32 [4096, 1536], P('seq', 'head')
- grad_norm_gain: float32 [1536], P('head')
- grad_w_z: float32 [1536, 3072], P(None, 'head')
- grad_w_x: float32 [1536, 3072], P(None, 'head')
- grad_w_bc: float32 [1536, 256], P('head')
- grad_w_dt: float32 [1536, 48], P(None, 'head')
- grad_conv_x_w: float32 [4, 3072], P(None, 'head')
- grad_conv_x_b: float32 [3072], P('head')
- grad_conv_bc_w: float32 [4, 256], replicated
- grad_conv_bc_b: float32 [256], replicated
- grad_dt_bias: float32 [48], P('head')
- grad_a_log: float32 [48], P('head')
- grad_d_skip: float32 [48], P('head')
- grad_gate_gain: float32 [3072], P('head')
- grad_w_out: float32 [3072, 1536], P('head')
The draws below stay inside these ranges and needn't reach their ends.
Inputs may be any that keep to these rules, and one draw needn't show every extreme that they name: `seq_lengths`: the lengths add up to 4096; the largest is exactly 1536.
All inputs are finite; a program needn't handle non-finite values.
Results may differ from the reference program's by a relative error of at most 0.007.
The reference program's roundings to bfloat16 on the way count: a program that leaves them out, or rounds other values in their place, can miss the bound.
Values may be sent and summed in bfloat16 or wider, within the bound.
A program may use at most 128 MiB of HBM per device.

```python
import math
import jax
import jax.numpy as jnp
import numpy as np
from jax import lax

D = 1536
HEADS = 48
HEAD_DIM = 64
STATE = 128
CONV = 4
SPAN = 256
SEQS = 8
INNER = 3072
TOKENS = 4096
MOST_LEN = 1536


def steps_of(stream_key, shape, split, least, largest):
    def one(axis_at, blocks):
        steps = jax.random.uniform(jax.random.fold_in(jax.random.fold_in(stream_key, 6), axis_at), (blocks,), jnp.float32, least / len(split), largest / len(split))
        return jnp.repeat(jnp.exp(steps), shape[axis_at] // blocks).reshape((-1,) + (1,) * (len(shape) - axis_at - 1))

    level = one(*split[0])
    for cut in split[1:]:
        level = level * one(*cut)
    return level


def split_up(number_of, total, limit, slope):
    portions = [(1 << 20) // math.isqrt(grade ** slope) + 1 for grade in range(2, number_of + 1)]
    surplus, given = total - limit - (number_of - 1), [1] * (number_of - 1)
    while surplus > 0:
        movable = [i for i in range(number_of - 1) if given[i] < limit]
        whole, remaining = sum([portions[i] for i in movable]), surplus
        for i in movable:
            addition = min(limit - given[i], max(1, remaining * portions[i] // whole), surplus)
            given[i] = given[i] + addition
            surplus = surplus - addition
    return np.array([limit] + given)


def uneven(own_key, amount, total, bound, slope):
    if amount == 2:
        one = jax.random.randint(own_key, (), max(1, total - bound), min(bound, total - 1) + 1)
        return jnp.stack([one, total - one])
    tallies = jnp.asarray(split_up(amount, total, bound, slope), jnp.int32)
    couples = (amount - 1) // 2
    source_of, receiver = tallies[1:1 + 2 * couples:2], tallies[2:2 + 2 * couples:2]
    slack = jnp.minimum(source_of - 1, bound - receiver)
    passed = jax.random.randint(jax.random.fold_in(own_key, 1), (couples,), 0, 1 << 20) % (slack + 1)
    tallies = tallies.at[1:1 + 2 * couples:2].set(source_of - passed).at[2:2 + 2 * couples:2].set(receiver + passed)
    return tallies[jax.random.permutation(jax.random.fold_in(own_key, 2), amount)]


def gaussian(stream_key, shape, scale, bound, pieces=(), held_as=jnp.bfloat16):
    values = jax.random.normal(stream_key, shape, jnp.float32) * scale
    if len(pieces) > 0:
        values = steps_of(stream_key, shape, pieces, -0.22, 0.18) * values
    return jnp.clip(values, min=-bound, max=bound).astype(held_as)


def setup_inputs(seed: int = 0) -> dict:
    streams_of = jax.random.split(jax.random.key(seed), 18)
    hidden_in = gaussian(streams_of[0], (TOKENS, D), 1.0, 6.0, ((0, 8), (1, 4)))
    seq_lengths = uneven(streams_of[1], SEQS, TOKENS, MOST_LEN, 2).astype(jnp.int32)
    norm_gain = jnp.clip(1.0 + 0.1 * jax.random.normal(streams_of[2], (D,), jnp.float32), 0.5, 1.5)
    w_z = gaussian(streams_of[3], (D, INNER), D ** -0.5, 0.15625, ((1, 4),))
    w_x = gaussian(streams_of[4], (D, INNER), D ** -0.5, 0.15625, ((1, 4),))
    w_bc = gaussian(streams_of[5], (D, 2 * STATE), D ** -0.5, 0.15625, ((0, 4),))
    w_dt = gaussian(streams_of[6], (D, HEADS), D ** -0.5, 0.15625, ((1, 4),))
    conv_x_w = gaussian(streams_of[7], (CONV, INNER), CONV ** -0.5, 3.0, ((1, 4),), jnp.float32)
    conv_x_b = gaussian(streams_of[8], (INNER,), 0.5, 3.0, ((0, 4),), jnp.float32)
    conv_bc_w = gaussian(streams_of[9], (CONV, 2 * STATE), CONV ** -0.5, 3.0, (), jnp.float32)
    conv_bc_b = gaussian(streams_of[10], (2 * STATE,), 0.5, 3.0, (), jnp.float32)
    dt_bias = jnp.clip(-2.0 + 2.5 * jax.random.uniform(streams_of[11], (HEADS,), jnp.float32) ** steps_of(streams_of[11], (HEADS,), ((0, 4),), -0.2, 0.2), -2.0, 0.5)
    a_log = jnp.clip(-9.0 + 6.0 * jax.random.uniform(streams_of[12], (HEADS,), jnp.float32) ** steps_of(streams_of[12], (HEADS,), ((0, 4),), -0.2, 0.2), -9.0, -3.0)
    d_skip = jnp.clip(0.5 + 1.5 * jax.random.uniform(streams_of[13], (HEADS,), jnp.float32) ** steps_of(streams_of[13], (HEADS,), ((0, 4),), -0.2, 0.2), 0.5, 2.0)
    gate_gain = jnp.clip(1.0 + 0.1 * jax.random.normal(streams_of[14], (INNER,), jnp.float32), 0.5, 1.5)
    w_out = gaussian(streams_of[15], (INNER, D), INNER ** -0.5, 0.109375, ((0, 4),))
    cotangent = gaussian(streams_of[16], (TOKENS, D), 1.0, 6.0, ((0, 8), (1, 4)))
    return {"hidden_in": hidden_in, "seq_lengths": seq_lengths, "norm_gain": norm_gain, "w_z": w_z, "w_x": w_x, "w_bc": w_bc, "w_dt": w_dt, "conv_x_w": conv_x_w, "conv_x_b": conv_x_b, "conv_bc_w": conv_bc_w, "conv_bc_b": conv_bc_b, "dt_bias": dt_bias, "a_log": a_log, "d_skip": d_skip, "gate_gain": gate_gain, "w_out": w_out, "cotangent": cotangent}


epsilon = 1e-05
highest = lax.Precision.HIGHEST

@jax.custom_vjp
def low(v):
    return lax.optimization_barrier(v.astype(jnp.bfloat16)).astype(jnp.float32)

@jax.custom_vjp
def low_back(v):
    return v

def low_keep(v):
    return (low(v), None)

def low_pass(kept, grad):
    return (grad,)

def back_keep(v):
    return (v, None)

def back_low(kept, grad):
    return (low(grad),)
low.defvjp(low_keep, low_pass)
low_back.defvjp(back_keep, back_low)

def rms_scale(values, gain_vec):
    return values * lax.rsqrt(lax.optimization_barrier(jnp.mean(values * values, axis=-1, keepdims=True)) + epsilon) * gain_vec

def segment_of(positions, starts):
    return lax.optimization_barrier(jnp.sum((positions[:, None] >= starts[None, :]).astype(jnp.int32), axis=1)) - 1

def span_step(state_carry, span_item):
    inner_c, b_rows, c_rows, step_c, decay_c, seg_rows, seg_prev = span_item
    row_ids = jnp.arange(SPAN)
    lower_tri = row_ids[:, None] >= row_ids[None, :]
    cumul = jnp.dot(lower_tri.astype(jnp.float32), decay_c, precision=highest)
    last_cum = cumul[SPAN - 1]
    same_seq = ((seg_rows[:, None] == seg_rows[None, :]) & lower_tri)[:, :, None]
    spread = cumul[:, None, :] - cumul[None, :, :]
    decay_mat = jnp.where(same_seq, jnp.exp(jnp.where(same_seq, spread, 0.0)), 0.0)
    scores = jnp.dot(c_rows, b_rows.T, precision=highest)
    mixing = low(scores[:, :, None] * decay_mat * step_c[None, :, :])
    y_inside = jnp.einsum('ijh,jhp->ihp', mixing, inner_c, precision=highest)
    tail_weight = jnp.exp(last_cum[None, :] - cumul) * (seg_rows == seg_rows[SPAN - 1]).astype(jnp.float32)[:, None]
    loaded = low(b_rows[:, None, :] * (tail_weight * step_c)[:, :, None])
    local_state = low_back(jnp.einsum('jhn,jhp->hnp', loaded, inner_c, precision=highest))
    head_weight = jnp.exp(cumul) * (seg_rows == seg_prev).astype(jnp.float32)[:, None]
    c_weighted = low(c_rows[:, None, :] * head_weight[:, :, None])
    y_outside = jnp.einsum('ihn,hnp->ihp', c_weighted, low(state_carry), precision=highest)
    carry_decay = jnp.exp(last_cum) * (seg_rows[SPAN - 1] == seg_prev).astype(jnp.float32)
    new_state = carry_decay[:, None, None] * state_carry + local_state
    return (new_state, y_inside + y_outside)

def reference(hidden_in, seq_lengths, norm_gain, w_z, w_x, w_bc, w_dt, conv_x_w, conv_x_b, conv_bc_w, conv_bc_b, dt_bias, a_log, d_skip, gate_gain, w_out, cotangent):
    starts = (jnp.cumsum(seq_lengths) - seq_lengths).astype(jnp.int32)
    segment = segment_of(jnp.arange(TOKENS, dtype=jnp.int32), starts)
    spans = TOKENS // SPAN
    span_prev = segment_of((jnp.arange(spans, dtype=jnp.int32) * SPAN - 1).astype(jnp.int32), starts)

    def forward(x_in, gain_in, weight_z, weight_x, weight_bc, weight_dt, taps_x, bias_x, taps_bc, bias_bc, step_bias, log_rate, skip_weight, gain_gate, weight_out):
        normed = low(rms_scale(x_in, gain_in))
        gate_pre = low_back(jnp.dot(normed, weight_z, precision=highest))
        x_pre = low_back(low(jnp.dot(normed, weight_x, precision=highest)))
        bc_pre = low_back(low(jnp.dot(normed, weight_bc, precision=highest)))
        step_raw = low_back(jnp.dot(normed, weight_dt, precision=highest))
        conv_in = jnp.concatenate([x_pre, bc_pre], axis=1)
        channels = conv_in.shape[1]
        padded = jnp.concatenate([jnp.zeros((CONV - 1, channels), jnp.float32), conv_in], axis=0)
        seg_padded = jnp.concatenate([jnp.full((CONV - 1,), -1, jnp.int32), segment])
        conv_weight = jnp.concatenate([taps_x, taps_bc], axis=1)
        conv_out = jnp.zeros((TOKENS, channels), jnp.float32) + jnp.concatenate([bias_x, bias_bc])[None, :]
        for offset in range(CONV):
            mask_col = (seg_padded[offset:offset + TOKENS] == segment).astype(jnp.float32)[:, None]
            conv_out = conv_out + conv_weight[offset] * padded[offset:offset + TOKENS] * mask_col
        activated = jax.nn.silu(conv_out)
        inner_vals = low(activated[:, :INNER])
        b_vals = low(activated[:, INNER:INNER + STATE])
        c_vals = low(activated[:, INNER + STATE:])
        step_size = jax.nn.softplus(step_raw + step_bias)
        log_decay = -jnp.exp(log_rate) * step_size
        span_items = (inner_vals.reshape(spans, SPAN, HEADS, HEAD_DIM), b_vals.reshape(spans, SPAN, STATE), c_vals.reshape(spans, SPAN, STATE), step_size.reshape(spans, SPAN, HEADS), log_decay.reshape(spans, SPAN, HEADS), segment.reshape(spans, SPAN), span_prev)
        initial = jnp.zeros((HEADS, STATE, HEAD_DIM), jnp.float32)
        final_state, outputs = lax.scan(jax.checkpoint(span_step), initial, span_items)
        mixed_out = low_back(outputs.reshape(TOKENS, INNER) + inner_vals * jnp.repeat(skip_weight, HEAD_DIM))
        gate_normed = low(rms_scale(mixed_out * jax.nn.silu(gate_pre), gain_gate))
        return x_in + jnp.dot(gate_normed, weight_out, precision=highest)
    float_args = (hidden_in.astype(jnp.float32), norm_gain, w_z.astype(jnp.float32), w_x.astype(jnp.float32), w_bc.astype(jnp.float32), w_dt.astype(jnp.float32), conv_x_w, conv_x_b, conv_bc_w, conv_bc_b, dt_bias, a_log, d_skip, gate_gain, w_out.astype(jnp.float32))
    result_out, pullback = jax.vjp(forward, *float_args)
    grads = pullback(cotangent.astype(jnp.float32))
    return (result_out.astype(jnp.bfloat16), grads[0], grads[1], grads[2], grads[3], grads[4], grads[5], grads[6], grads[7], grads[8], grads[9], grads[10], grads[11], grads[12], grads[13], grads[14])
```

```python
import jax
import jax.numpy as jnp
from jax import lax
from jax.experimental import pallas as pl
from jax.experimental.pallas import tpu as pltpu
from jax.sharding import PartitionSpec as P

D = 1536
HEAD_DIM = 64
STATE = 128
CONV = 4
SPAN = 256
INNER = 3072


epsilon = 1e-05
highest = lax.Precision.HIGHEST


def prefix(part, axis, combine, identity, reverse):
    count = lax.axis_size(axis)
    place = lax.axis_index(axis)
    ahead = count - 1 - place if reverse else place
    gathered = jax.tree.map(lambda a: lax.all_gather(a, axis), part)
    state = jax.tree.map(lambda a, e: jnp.zeros_like(a) + jnp.asarray(e, a.dtype), part, identity)

    def one(hop, state):
        source = count - 1 - hop if reverse else hop
        return combine(
            state, jax.tree.map(lambda a: lax.dynamic_index_in_dim(a, source, 0, False), gathered)
        )

    return lax.fori_loop(0, ahead, one, state)


def passed_along(block, axis, distance):
    devices = range(lax.axis_size(axis))
    route = [(i - distance, i) for i in devices if i - distance in devices]
    return lax.ppermute(block, axis, route)


def segment_of(positions, starts):
    return jnp.sum((positions[:, None] >= starts[None, :]).astype(jnp.int32), axis=1) - 1


def silu_slope(values):
    sigmoid_val = jax.nn.sigmoid(values)
    return sigmoid_val * (1.0 + values * (1.0 - sigmoid_val))


def chain_join(earlier, later):
    return (earlier[0] * later[0], earlier[1] * later[0][:, None, None] + later[1])


def state_prefix(decay, summary, backwards):
    identity = (jnp.ones_like(decay), jnp.zeros_like(summary))
    result = prefix((decay, summary), "seq", chain_join, identity, backwards)
    return result[1]


def span_terms(span_item, lower_tri):
    inner_c, b_rows, c_rows, step_c, cumul_c, seg_rows, seg_prev = span_item
    same_seq = ((seg_rows[:, None] == seg_rows[None, :]) & (lower_tri > 0.5))[None, :, :]
    spread = cumul_c[:, :, None] - cumul_c[:, None, :]
    decay_mat = jnp.where(same_seq, jnp.exp(jnp.where(same_seq, spread, 0.0)), 0.0)
    scores = lax.dot_general(
        c_rows, b_rows, (((1,), (1,)), ((), ())), preferred_element_type=jnp.float32
    )
    mixing = scores[None, :, :] * decay_mat * step_c[:, None, :]
    last_cum = cumul_c[:, SPAN - 1]
    tail_weight = (
        jnp.exp(last_cum[:, None] - cumul_c)
        * (seg_rows == seg_rows[SPAN - 1]).astype(jnp.float32)[None, :]
    )
    head_weight = jnp.exp(cumul_c) * (seg_rows == seg_prev).astype(jnp.float32)[None, :]
    carry_decay = jnp.exp(last_cum) * (seg_rows[SPAN - 1] == seg_prev).astype(jnp.float32)
    return (decay_mat, scores, mixing, tail_weight, head_weight, carry_decay)


def on_device(
    hidden_in,
    seq_lengths,
    norm_gain,
    w_z,
    w_x,
    w_bc,
    w_dt,
    conv_x_w,
    conv_x_b,
    conv_bc_w,
    conv_bc_b,
    dt_bias,
    a_log,
    d_skip,
    gate_gain,
    w_out,
    cotangent,
):
    tokens_here = hidden_in.shape[0]
    heads_here = dt_bias.shape[0]
    inner_here = w_z.shape[1]
    spans = tokens_here // SPAN
    first_pos = lax.axis_index("seq") * tokens_here
    starts = jnp.cumsum(seq_lengths) - seq_lengths
    segment = segment_of(first_pos + jnp.arange(tokens_here, dtype=jnp.int32), starts)
    edge_segment = segment_of(
        first_pos - (CONV - 1) + jnp.arange(CONV - 1, dtype=jnp.int32), starts
    )
    span_prev = segment_of(first_pos - 1 + jnp.arange(spans, dtype=jnp.int32) * SPAN, starts)
    row_ids = jnp.arange(SPAN)
    lower_tri = (row_ids[:, None] >= row_ids[None, :]).astype(jnp.float32)
    inputs = hidden_in.astype(jnp.float32)
    squares = lax.psum(jnp.sum(inputs * inputs, axis=1), "head")
    scale_in = lax.rsqrt(squares / D + epsilon)
    normed = (inputs * scale_in[:, None] * norm_gain).astype(jnp.bfloat16)
    gathered, bc_weight = (
        lax.all_gather(normed, "head", axis=1, tiled=True),
        lax.all_gather(w_bc, "head", axis=0, tiled=True),
    )
    gate_pre = jnp.dot(gathered, w_z, preferred_element_type=jnp.float32)
    x_part = jnp.dot(gathered, w_x, preferred_element_type=jnp.float32)
    bc_part = jnp.dot(gathered, bc_weight, preferred_element_type=jnp.float32)
    conv_in = jnp.concatenate([x_part, bc_part], axis=1).astype(jnp.bfloat16)
    step_raw = jnp.dot(gathered, w_dt, preferred_element_type=jnp.float32)
    edge_rows = passed_along(conv_in[tokens_here - (CONV - 1) :], "seq", 1)
    padded = jnp.concatenate([edge_rows, conv_in], axis=0).astype(jnp.float32)
    seg_padded = jnp.concatenate([edge_segment, segment])
    conv_weight = jnp.concatenate([conv_x_w, conv_bc_w], axis=1)
    conv_bias = jnp.concatenate([conv_x_b, conv_bc_b])
    tap_masks = [
        (seg_padded[offset : offset + tokens_here] == segment).astype(jnp.float32)[:, None]
        for offset in range(CONV)
    ]
    conv_out = jnp.zeros(conv_in.shape, jnp.float32) + conv_bias[None, :]
    for offset in range(CONV):
        conv_out = (
            conv_out
            + conv_weight[offset] * padded[offset : offset + tokens_here] * tap_masks[offset]
        )
    activated = jax.nn.silu(conv_out)
    inner_vals = activated[:, :inner_here].astype(jnp.bfloat16)
    b_vals = activated[:, inner_here : inner_here + STATE].astype(jnp.bfloat16)
    c_vals = activated[:, inner_here + STATE :].astype(jnp.bfloat16)
    step_pre = step_raw + dt_bias
    step_size = jax.nn.softplus(step_pre)
    rates = jnp.exp(a_log)
    log_decay = -rates * step_size
    decay_heads = log_decay.reshape(spans, SPAN, heads_here).transpose(0, 2, 1)
    step_heads = step_size.reshape(spans, SPAN, heads_here).transpose(0, 2, 1)
    cumul = jnp.einsum("ij,chj->chi", lower_tri, decay_heads, precision=highest)
    inner_spans = inner_vals.reshape(spans, SPAN, heads_here, HEAD_DIM).transpose(0, 2, 1, 3)
    c_spans = c_vals.reshape(spans, SPAN, STATE)
    per_span = (
        inner_spans,
        b_vals.reshape(spans, SPAN, STATE),
        c_spans,
        step_heads,
        cumul,
        segment.reshape(spans, SPAN),
        span_prev,
    )

    def forward_span(span_item):
        decay_mat, scores, mixing, tail_weight, head_weight, carry_decay = span_terms(
            span_item, lower_tri
        )
        inner_c = span_item[0]
        y_inside = jnp.einsum(
            "hij,hjp->hip", mixing.astype(jnp.bfloat16), inner_c, preferred_element_type=jnp.float32
        )
        loaded = (
            span_item[1].astype(jnp.float32)[None, :, :] * (tail_weight * span_item[3])[:, :, None]
        ).astype(jnp.bfloat16)
        local_state = jnp.einsum(
            "hjn,hjp->hnp", loaded, inner_c, preferred_element_type=jnp.float32
        )
        return (y_inside, local_state, carry_decay, head_weight)

    y_inside, local_states, carry_decay, head_weight = lax.map(forward_span, per_span)

    def advance(state_carry, span_item):
        running, factor = state_carry
        local_c, decay_c = span_item
        return ((decay_c[:, None, None] * running + local_c, decay_c * factor), (running, factor))

    zero_state = jnp.zeros((heads_here, STATE, HEAD_DIM), jnp.float32)
    unit_decay = jnp.ones((heads_here,), jnp.float32)
    (device_state, device_decay), (local_in, local_factor) = lax.scan(
        advance, (zero_state, unit_decay), (local_states, carry_decay)
    )
    incoming = state_prefix(device_decay, device_state, False)
    state_in = local_in + local_factor[:, :, None, None] * incoming
    state_low = state_in.astype(jnp.bfloat16)
    c_weighted = (c_spans.astype(jnp.float32)[:, None, :, :] * head_weight[:, :, :, None]).astype(
        jnp.bfloat16
    )
    y_outside = jnp.einsum(
        "chin,chnp->chip", c_weighted, state_low, preferred_element_type=jnp.float32
    )
    skip_rep = jnp.repeat(d_skip, HEAD_DIM)
    mixed_out = (y_inside + y_outside).transpose(0, 2, 1, 3).reshape(
        tokens_here, inner_here
    ) + inner_vals.astype(jnp.float32) * skip_rep
    gate_act = jax.nn.silu(gate_pre)
    gated = mixed_out * gate_act
    gate_squares = lax.psum(jnp.sum(gated * gated, axis=1), "head")
    scale_gate = lax.rsqrt(gate_squares / INNER + epsilon)
    gate_normed = (gated * scale_gate[:, None] * gate_gain).astype(jnp.bfloat16)
    partial_value = jnp.dot(gate_normed, w_out, preferred_element_type=jnp.float32)
    mixed_sum = lax.psum_scatter(partial_value, "head", scatter_dimension=1, tiled=True)
    layer_out = (inputs + mixed_sum).astype(jnp.bfloat16)
    grad_full = lax.all_gather(cotangent, "head", axis=1, tiled=True)
    grad_gate_normed = lax.dot_general(
        grad_full, w_out, (((1,), (1,)), ((), ())), preferred_element_type=jnp.float32
    )
    grad_w_out = lax.dot_general(
        gate_normed, grad_full, (((0,), (0,)), ((), ())), preferred_element_type=jnp.float32
    )
    grad_gate_gain = jnp.sum(grad_gate_normed * gated * scale_gate[:, None], axis=0)
    grad_scaled = grad_gate_normed * gate_gain
    gate_inner = lax.psum(jnp.sum(grad_scaled * gated, axis=1), "head")
    grad_gated = (
        scale_gate[:, None] * grad_scaled - gated * (scale_gate**3 * gate_inner / INNER)[:, None]
    )
    grad_mixed = (grad_gated * gate_act).astype(jnp.bfloat16)
    grad_gate_pre = (grad_gated * mixed_out * silu_slope(gate_pre)).astype(jnp.bfloat16)
    grad_d_skip = jnp.sum(
        (grad_mixed.astype(jnp.float32) * inner_vals.astype(jnp.float32)).reshape(
            tokens_here, heads_here, HEAD_DIM
        ),
        axis=(0, 2),
    )
    grad_spans = grad_mixed.reshape(spans, SPAN, heads_here, HEAD_DIM).transpose(0, 2, 1, 3)
    from_inter = jnp.einsum(
        "chin,chip->chnp", c_weighted, grad_spans, preferred_element_type=jnp.float32
    )

    def retreat(state_carry, span_item):
        running, factor = state_carry
        local_c, decay_c = span_item
        current = local_c + decay_c[:, None, None] * running
        product = decay_c * factor
        return ((current, product), (current, product))

    (device_grad, device_reach), (local_grad, local_reach) = lax.scan(
        retreat, (zero_state, unit_decay), (from_inter, carry_decay), reverse=True
    )
    beyond = state_prefix(device_reach, device_grad, True)
    grad_state_in = local_grad + local_reach[:, :, None, None] * beyond
    grad_local_states = jnp.concatenate([grad_state_in[1:], beyond[None]], axis=0)
    grad_carry_decay = jnp.sum(grad_local_states * state_in, axis=(2, 3))

    def backward_span(span_item):
        span_base = span_item[:7]
        inner_c, b_rows, c_rows, step_c = (span_base[0], span_base[1], span_base[2], span_base[3])
        grad_y, grad_state, state_c, grad_decay = (
            span_item[7],
            span_item[8],
            span_item[9],
            span_item[10],
        )
        decay_mat, scores, mixing, tail_weight, head_weight, carry_decay = span_terms(
            span_base, lower_tri
        )
        grad_mixing = jnp.einsum(
            "hip,hjp->hij", grad_y, inner_c, preferred_element_type=jnp.float32
        )
        grad_inner = jnp.einsum(
            "hij,hip->hjp", mixing.astype(jnp.bfloat16), grad_y, preferred_element_type=jnp.float32
        )
        related = grad_mixing * mixing
        grad_cum = jnp.sum(related, axis=2) - jnp.sum(related, axis=1)
        grad_scores = jnp.sum(grad_mixing * decay_mat * step_c[:, None, :], axis=0)
        grad_step = jnp.sum(grad_mixing * decay_mat * scores[None, :, :], axis=1)
        b_float = b_rows.astype(jnp.float32)
        c_float = c_rows.astype(jnp.float32)
        grad_c = jnp.dot(grad_scores, b_float, precision=highest)
        grad_b = lax.dot_general(grad_scores, c_float, (((0,), (0,)), ((), ())), precision=highest)
        loading = tail_weight * step_c
        loaded = (b_float[None, :, :] * loading[:, :, None]).astype(jnp.bfloat16)
        grad_loaded = jnp.einsum(
            "hjp,hnp->hjn", inner_c, grad_state, preferred_element_type=jnp.float32
        )
        grad_inner = grad_inner + jnp.einsum(
            "hjn,hnp->hjp", loaded, grad_state, preferred_element_type=jnp.float32
        )
        grad_loading = jnp.sum(grad_loaded * b_float[None, :, :], axis=2)
        grad_b = grad_b + jnp.einsum("hjn,hj->jn", grad_loaded, loading, precision=highest)
        tail_term = grad_loading * loading
        grad_cum = grad_cum - tail_term
        grad_last = jnp.sum(tail_term, axis=1) + grad_decay * carry_decay
        grad_step = grad_step + grad_loading * tail_weight
        grad_weighted = jnp.einsum(
            "hip,hnp->hin", grad_y, state_c, preferred_element_type=jnp.float32
        )
        grad_head = jnp.sum(grad_weighted * c_float[None, :, :], axis=2)
        grad_c = grad_c + jnp.einsum("hin,hi->in", grad_weighted, head_weight, precision=highest)
        grad_cum = grad_cum + grad_head * head_weight
        grad_cum = grad_cum.at[:, SPAN - 1].add(grad_last)
        grad_log = jnp.einsum("ij,hi->hj", lower_tri, grad_cum, precision=highest)
        return (grad_inner, grad_b, grad_c, grad_step, grad_log)

    back_items = per_span + (
        grad_spans,
        grad_local_states.astype(jnp.bfloat16),
        state_low,
        grad_carry_decay,
    )
    grad_inner_s, grad_b_s, grad_c_s, grad_step_s, grad_log_s = lax.map(backward_span, back_items)
    grad_inner = (
        grad_inner_s.transpose(0, 2, 1, 3).reshape(tokens_here, inner_here)
        + grad_mixed.astype(jnp.float32) * skip_rep
    )
    grad_log_decay = grad_log_s.transpose(0, 2, 1).reshape(tokens_here, heads_here)
    grad_step_total = (
        grad_step_s.transpose(0, 2, 1).reshape(tokens_here, heads_here) - grad_log_decay * rates
    )
    grad_a_log = jnp.sum(grad_log_decay * log_decay, axis=0)
    grad_step_pre = grad_step_total * jax.nn.sigmoid(step_pre)
    grad_dt_bias = jnp.sum(grad_step_pre, axis=0)
    grad_step_raw = grad_step_pre.astype(jnp.bfloat16)
    grad_bc = lax.psum(
        jnp.concatenate(
            [grad_b_s.reshape(tokens_here, STATE), grad_c_s.reshape(tokens_here, STATE)], axis=1
        ),
        "head",
    )
    grad_conv = jnp.concatenate([grad_inner, grad_bc], axis=1) * silu_slope(conv_out)
    grad_conv_bias = jnp.sum(grad_conv, axis=0)
    grad_conv_weight = jnp.stack(
        [
            jnp.sum(grad_conv * padded[offset : offset + tokens_here] * tap_masks[offset], axis=0)
            for offset in range(CONV)
        ]
    )
    grad_padded = jnp.zeros(padded.shape, jnp.float32)
    for offset in range(CONV):
        grad_padded = grad_padded + jnp.pad(
            conv_weight[offset] * grad_conv * tap_masks[offset],
            ((offset, CONV - 1 - offset), (0, 0)),
        )
    returned = passed_along(grad_padded[: CONV - 1], "seq", -1)
    grad_conv_in = (
        grad_padded[CONV - 1 :] + jnp.pad(returned, ((tokens_here - (CONV - 1), 0), (0, 0)))
    ).astype(jnp.bfloat16)
    grad_x_pre = grad_conv_in[:, :inner_here]
    grad_bc_pre = grad_conv_in[:, inner_here:]
    contract_rows = (((0,), (0,)), ((), ()))
    contract_cols = (((1,), (1,)), ((), ()))
    grad_w_z = lax.dot_general(
        gathered, grad_gate_pre, contract_rows, preferred_element_type=jnp.float32
    )
    grad_w_x = lax.dot_general(
        gathered, grad_x_pre, contract_rows, preferred_element_type=jnp.float32
    )
    grad_w_dt = lax.dot_general(
        gathered, grad_step_raw, contract_rows, preferred_element_type=jnp.float32
    )
    grad_w_bc = lax.dot_general(
        normed, grad_bc_pre, contract_rows, preferred_element_type=jnp.float32
    )
    partial_back = lax.dot_general(
        grad_gate_pre, w_z, contract_cols, preferred_element_type=jnp.float32
    )
    partial_back = partial_back + lax.dot_general(
        grad_x_pre, w_x, contract_cols, preferred_element_type=jnp.float32
    )
    partial_back = partial_back + lax.dot_general(
        grad_step_raw, w_dt, contract_cols, preferred_element_type=jnp.float32
    )
    grad_normed = lax.psum_scatter(partial_back, "head", scatter_dimension=1, tiled=True)
    grad_normed = grad_normed + lax.dot_general(
        grad_bc_pre, w_bc, contract_cols, preferred_element_type=jnp.float32
    )
    grad_scaled_in = grad_normed * norm_gain
    grad_norm_gain = jnp.sum(grad_normed * inputs * scale_in[:, None], axis=0)
    norm_inner = lax.psum(jnp.sum(grad_scaled_in * inputs, axis=1), "head")
    grad_in = (
        cotangent.astype(jnp.float32)
        + scale_in[:, None] * grad_scaled_in
        - inputs * (scale_in**3 * norm_inner / D)[:, None]
    )
    summed = lax.psum(
        (
            grad_norm_gain,
            grad_w_z,
            grad_w_x,
            grad_w_bc,
            grad_w_dt,
            grad_conv_weight[:, :inner_here],
            grad_conv_bias[:inner_here],
            grad_conv_weight[:, inner_here:],
            grad_conv_bias[inner_here:],
            grad_dt_bias,
            grad_a_log,
            grad_d_skip,
            grad_gate_gain,
            grad_w_out,
        ),
        "seq",
    )
    return (
        layer_out,
        grad_in,
        summed[0],
        summed[1],
        summed[2],
        summed[3],
        summed[4],
        summed[5],
        summed[6],
        summed[7],
        summed[8],
        summed[9],
        summed[10],
        summed[11],
        summed[12],
        summed[13],
    )


BF = jnp.bfloat16
F32 = jnp.float32
MESH = pl.DeviceIdType.MESH
ROWS = 512
BLOCK = 384
CHANNELS = 768
WIDE = 1024
HALO = 16
HOPS = 3
SEQ = 8
LINE = 4
ALONG = "seq"
ACROSS = "head"
NN = (((1,), (0,)), ((), ()))
NT = (((1,), (1,)), ((), ()))
TN = (((0,), (0,)), ((), ()))


def mul(a, b, dims=NN):
    return lax.dot_general(a, b, dims, preferred_element_type=F32)


def cut(start, size, mult):
    return pl.ds(pl.multiple_of(start, mult), size)


def parts(v, n):
    out = []
    for _ in range(n):
        p = v.astype(BF)
        out.append(p)
        v = v - p.astype(F32)
    return out


def lanes_sum(v):
    total = v[:, 0:128]
    for i in range(1, v.shape[1] // 128):
        total = total + v[:, 128 * i : 128 * i + 128]
    return total


def rows_sum(v):
    return jnp.sum(v.reshape(v.shape[0] // 8, 8, v.shape[1]), axis=0)


def wide_of(v, n):
    return jnp.concatenate([v] * n, axis=1)


def to_row(part):
    return jnp.sum(part.T, axis=0, keepdims=True)


def to_col(row):
    return jnp.broadcast_to(row, (128, row.shape[1])).T


def loop(n, body):
    def run(i, carry):
        body(i)
        return carry

    lax.fori_loop(0, n, run, 0)


def remote(src, dst, send, recv, peer):
    return pltpu.make_async_remote_copy(
        src_ref=src, dst_ref=dst, send_sem=send, recv_sem=recv, device_id=peer, device_id_type=MESH
    )


class Total:
    def __init__(self, whole, bufs, send, recv, freed, base, me):
        self.w = whole
        self.freed, self.slot = freed, 3 * (base // 10)
        self.r0, self.ra, self.rb, self.qa, self.qb = bufs
        self.send, self.recv, self.base = send, recv, base
        self.c, self.x, self.y, self.s = me
        self.rows, self.cols = whole.shape
        self.live, self.left = {}, set()

    def peer(self, bit):
        return {ALONG: self.s + bit - 2 * bit * {1: self.c, 2: self.x, 4: self.y}[bit]}

    def free(self, k, n, bit):
        self.sent(k)
        pl.semaphore_signal(
            self.freed.at[self.slot + n], inc=1, device_id=self.peer(bit), device_id_type=MESH
        )

    def copy(self, k, src, dst, bit):
        d = remote(src, dst, self.send.at[self.base + k], self.recv.at[self.base + k], self.peer(bit))
        d.start()
        self.live[k] = d
        self.left.add(k)

    def wait(self, k):
        self.live[k].wait_recv()

    def sent(self, k):
        self.left.remove(k)
        self.live[k].wait_send()

    def add(self, start, got, rows, col, cols, step):
        def body(i):
            at = (cut(start + i * step, step, 16), pl.ds(col, cols))
            new = self.w[at].astype(F32) + got[cut(i * step, step, 16), :].astype(F32)
            self.w[at] = new.astype(self.w.dtype)

        loop(rows // step, body)

    def s0(self):
        h = self.rows // 2
        self.copy(0, self.w.at[cut((1 - self.c) * h, h, 16)], self.r0, 1)

    def s1(self):
        h, q, m = self.rows // 2, self.rows // 4, self.cols // 2
        base = self.c * h
        self.free(0, 0, 1)
        self.wait(0)
        self.add(base, self.r0, h, 0, self.cols, 32)
        self.copy(1, self.w.at[cut(base + (1 - self.x) * q, q, 16), pl.ds(0, m)], self.ra, 2)
        self.copy(2, self.w.at[cut(base + (1 - self.y) * q, q, 16), pl.ds(m, m)], self.rb, 4)

    def s2(self):
        h, q, e, m = self.rows // 2, self.rows // 4, self.rows // 8, self.cols // 2
        ba = self.c * h + self.x * q
        bb = self.c * h + self.y * q
        self.wait(1)
        self.add(ba, self.ra, q, 0, m, 32)
        self.sent(2)
        self.copy(3, self.w.at[cut(ba + (1 - self.y) * e, e, 16), pl.ds(0, m)], self.qa, 4)
        self.wait(2)
        self.add(bb, self.rb, q, m, m, 32)
        self.sent(1)
        self.copy(4, self.w.at[cut(bb + (1 - self.x) * e, e, 16), pl.ds(m, m)], self.qb, 2)

    def s3(self):
        h, q, e, m = self.rows // 2, self.rows // 4, self.rows // 8, self.cols // 2
        ba = self.c * h + self.x * q + self.y * e
        bb = self.c * h + self.y * q + self.x * e
        self.free(3, 1, 4)
        self.free(4, 2, 2)
        self.wait(3)
        self.add(ba, self.qa, e, 0, m, 16)
        pl.semaphore_wait(self.freed.at[self.slot + 1], 1)
        p = self.w.at[cut(ba, e, 16), pl.ds(0, m)]
        self.copy(5, p, p, 4)
        self.wait(4)
        self.add(bb, self.qb, e, m, m, 16)
        pl.semaphore_wait(self.freed.at[self.slot + 2], 1)
        p = self.w.at[cut(bb, e, 16), pl.ds(m, m)]
        self.copy(6, p, p, 2)

    def s4(self):
        h, q, m = self.rows // 2, self.rows // 4, self.cols // 2
        self.wait(5)
        p = self.w.at[cut(self.c * h + self.x * q, q, 16), pl.ds(0, m)]
        self.copy(7, p, p, 2)
        self.wait(6)
        p = self.w.at[cut(self.c * h + self.y * q, q, 16), pl.ds(m, m)]
        self.copy(8, p, p, 4)

    def s5(self):
        h = self.rows // 2
        self.wait(7)
        self.wait(8)
        pl.semaphore_wait(self.freed.at[self.slot], 1)
        p = self.w.at[cut(self.c * h, h, 16)]
        self.copy(9, p, p, 1)

    def s6(self):
        self.wait(9)
        for k in sorted(self.left):
            self.sent(k)


def total_bufs(rows, cols, kind):
    sizes = [(2, 1), (4, 2), (4, 2), (8, 2), (8, 2)]
    return [pltpu.VMEM((rows // a, cols // b), kind) for a, b in sizes]


class Refs:
    def __init__(self, named):
        self.__dict__.update(named)


def layer_kernel(named, sum_bufs):
    g = Refs(named)
    g.ggn = g.acc.at[:, pl.ds(0, CHANNELS)]
    g.z = g.ggn
    g.gn = g.xg.at[:, pl.ds(0, CHANNELS)]
    g.gz = g.xg.at[:, pl.ds(CHANNELS, CHANNELS)]
    g.gconv = g.slope
    g.gx = g.gm
    g.sblk2 = g.sblk
    g.own = g.gated.at[:, pl.ds(0, BLOCK)]
    g.gb = g.gated.at[:, pl.ds(BLOCK, 128)]
    g.gc = g.gated.at[:, pl.ds(BLOCK + 128, 128)]
    s = lax.axis_index(ALONG)
    z = lax.axis_index(ACROSS)
    me = (lax.rem(s, 2), lax.rem(s // 2, 2), s // 4, s)
    zpeers = [{ACROSS: lax.rem(z + d, LINE)} for d in range(1, LINE)]
    speers = [{ALONG: lax.rem(s + d, SEQ)} for d in range(1, SEQ)]

    loads = []
    for i, (src, dst) in enumerate(
        [(g.x_hbm, g.x), (g.w_x, g.wx), (g.w_z, g.wz), (g.cot_hbm, g.cotg.at[:, cut(z * BLOCK, BLOCK, 128)]), (g.w_out, g.wo)]
    ):
        d = pltpu.make_async_copy(src, dst, g.load_sem.at[i])
        d.start()
        loads.append(d)

    sem = pltpu.get_barrier_semaphore()
    for p in zpeers + speers:
        pl.semaphore_signal(sem, inc=1, device_id=p, device_id_type=MESH)
    pl.semaphore_wait(sem, len(zpeers) + len(speers))

    pending = []

    def send(src, dst, sems, i, peer):
        d = remote(src, dst, sems[0].at[i], sems[1].at[i], peer)
        d.start()
        pending.append(d)
        return d

    loads[0].wait()
    loads[3].wait()
    gain = g.params[0:1, 0:BLOCK]
    xv = g.x[...].astype(F32)
    g.ssq[z] = jnp.broadcast_to(to_row(lanes_sum(xv * xv)), (8, ROWS))
    g.gains[z] = jnp.broadcast_to(gain, (8, BLOCK))
    piece = cut(48 * s, 48, 16)
    own = cut(z * BLOCK, BLOCK, 128)
    g.wbc[z, piece, :] = g.w_bc[piece, :]
    small = []
    for i, p in enumerate(zpeers):
        small.append(send(g.ssq.at[z], g.ssq.at[z], g.small, i, p))
        small.append(send(g.gains.at[z], g.gains.at[z], g.small, 3 + i, p))
        small.append(send(g.w_bc.at[piece], g.wbc.at[z, piece], g.small, 6 + i, p))
    xin = [send(g.x, g.xg.at[:, own], g.gather, i, p) for i, p in enumerate(zpeers)]
    cin = [send(g.cotg.at[:, own], g.cotg.at[:, own], g.gather, 3 + i, p) for i, p in enumerate(zpeers)]

    g.wd[...] = jnp.zeros(g.wd.shape, BF)
    g.wd[:, 0:12] = g.w_dt[...]
    g.taps[...] = jnp.zeros(g.taps.shape, F32)
    g.taps[0:4, 0:CHANNELS] = g.conv_x_w[...]
    g.taps[0:4, CHANNELS:WIDE] = g.conv_bc_w[...]
    g.taps[4:5, 0:CHANNELS] = g.params[1:2, :]
    g.taps[4:5, CHANNELS:WIDE] = g.params[2:3, 0:256]
    expand_row = lax.broadcasted_iota(jnp.int32, (256, CHANNELS), 0)
    expand_col = lax.broadcasted_iota(jnp.int32, (256, CHANNELS), 1)
    g.spread[...] = jnp.where((expand_col >> 6) == (expand_row & 127), 1.0, 0.0).astype(BF)
    starts = [jnp.int32(0)]
    for k in range(7):
        starts.append(starts[-1] + g.lengths[k])

    def segment(pos):
        total = jnp.full(pos.shape, -1, jnp.int32)
        for k in range(8):
            total = total + jnp.where(pos >= starts[k], 1, 0)
        return total.astype(F32)

    g.segc[...] = segment(
        lax.broadcasted_iota(jnp.int32, (ROWS + HALO, 128), 0) + (s * ROWS - HALO)
    )
    g.segr[...] = segment(lax.broadcasted_iota(jnp.int32, (8, ROWS), 1) + s * ROWS)
    tri_i = lax.broadcasted_iota(jnp.int32, (SPAN, SPAN), 0)
    tri_j = lax.broadcasted_iota(jnp.int32, (SPAN, SPAN), 1)
    g.tri[...] = jnp.where(tri_i >= tri_j, 1.0, 0.0).astype(BF)
    lane = lax.broadcasted_iota(jnp.int32, (1, 128), 1)
    left = lane < 64

    def spread(v):
        hi, lo = parts(v, 2)
        return mul(jnp.concatenate([hi, lo], axis=1), g.spread[...])

    def head_sum(v):
        hi, lo = parts(v, 2)
        e = g.spread[0:128, :]
        return mul(hi, e, NT) + mul(lo, e, NT)

    g.skipe[...] = spread(jnp.broadcast_to(g.params[5:6, 0:128], (8, 128)))
    rates = jnp.exp(g.params[4:5, 0:128])

    for d in small:
        d.wait_recv()
    wide = [
        send(g.wbc.at[:, piece], g.wbc.at[:, piece], g.wide, i, p) for i, p in enumerate(speers)
    ]
    total = g.ssq[0] + g.ssq[1] + g.ssq[2] + g.ssq[3]
    g.xscale[...] = to_col(lax.rsqrt(total[0:1] / D + epsilon))

    def normalise(k, src):
        gk = g.gains[k][0:1]
        cols = cut(k * BLOCK, BLOCK, 128)

        def body(i):
            at = cut(i * 64, 64, 16)
            v = src(at, cols).astype(F32)
            g.xn[at, cols] = (v * wide_of(g.xscale[at, :], 3) * gk).astype(BF)

        loop(ROWS // 64, body)

    def project(k, w, cols, base, first, width=256):
        at = cut(k * BLOCK, BLOCK, 128)

        def body(n):
            p = mul(g.xn[:, at], w[cut(k * BLOCK, BLOCK, 16), cut(n * width, width, 128)])
            dst = cut(base + n * width, width, 128)
            if first:
                g.acc[:, dst] = p
            else:
                g.acc[:, dst] += p

        loop(cols // width, body)

    def project_bc(k, first):
        p = mul(g.xn[:, cut(k * BLOCK, BLOCK, 128)], g.wbc[k])
        if first:
            g.acc[:, CHANNELS:WIDE] = p
        else:
            g.acc[:, CHANNELS:WIDE] += p

    normalise(z, lambda at, cols: g.x[at, :])
    loads[1].wait()
    loads[2].wait()
    project(z, g.wx, CHANNELS, 0, True)
    project(z, g.wz, CHANNELS, WIDE, True)
    project(z, g.wd, 128, WIDE + CHANNELS, True, 128)
    for d in wide:
        d.wait_recv()
    project_bc(z, True)
    ks = [lax.rem(z + LINE - d, LINE) for d in range(1, LINE)]
    for i, k in enumerate(ks):
        xin[i].wait_recv()
        normalise(k, lambda at, cols: g.xg[at, cols])
        project(k, g.wx, CHANNELS, 0, False)
        project_bc(k, False)
        if i < 2:
            project(k, g.wz, CHANNELS, WIDE, False)
            project(k, g.wd, 128, WIDE + CHANNELS, False, 128)

    g.edge[...] = g.acc[ROWS - HALO : ROWS, 0:WIDE].astype(BF)
    edge = remote(g.edge, g.halo, g.edge_sem.at[0], g.edge_sem.at[1], {ALONG: s + 1})

    @pl.when(s < SEQ - 1)
    def _():
        edge.start()

    @pl.when(s == 0)
    def _():
        g.halo[...] = jnp.zeros(g.halo.shape, BF)

    def put(i):
        g.cf[cut(HALO + i * 64, 64, 8), :] = (
            g.acc[cut(i * 64, 64, 8), 0:WIDE].astype(BF).astype(F32)
        )

    loop(ROWS // 64, put)
    project(ks[2], g.wz, CHANNELS, WIDE, False)
    project(ks[2], g.wd, 128, WIDE + CHANNELS, False, 128)

    step_pre = g.acc[:, WIDE + CHANNELS :] + g.params[3:4, 0:128]
    g.spre[...] = step_pre
    g.step[...] = jnp.where(lane < 12, jax.nn.softplus(step_pre), 0.0)
    for q in range(2):
        rows = pl.ds(q * SPAN, SPAN)
        log_decay = -rates * g.step[rows, :]
        cum = sum(mul(g.tri[...], p) for p in parts(log_decay, 3))
        g.cum[rows, :] = cum
        g.cumt[q] = cum.T[0:16, :]
        last = cum[SPAN - 1 : SPAN, :]
        seg = g.segc[pl.ds(HALO + q * SPAN, SPAN), :]
        seg_last = g.segc[HALO + q * SPAN + SPAN - 1 : HALO + q * SPAN + SPAN, :]
        seg_prev = g.segc[HALO + q * SPAN - 1 : HALO + q * SPAN, :]
        tail = jnp.where(seg == seg_last, jnp.exp(last - cum), 0.0)
        load = tail * g.step[rows, :]
        lead = jnp.where(seg == seg_prev, jnp.exp(cum), 0.0)
        g.tail[rows, :] = tail
        g.load[rows, :] = load
        g.lead[rows, :] = lead
        g.loadt[q] = load.T[0:16, :]
        g.leadt[q] = lead.T[0:16, :]
        g.stept[q] = g.step[rows, :].T[0:16, :]
        carry = jnp.where(seg_last == seg_prev, jnp.exp(last), 0.0)
        g.carry[q] = jnp.broadcast_to(carry, (8, 128))
        g.carrye[q] = spread(jnp.broadcast_to(carry, (8, 128)))
    g.decay[0] = g.carrye[0] * g.carrye[1]

    @pl.when(s > 0)
    def _():
        edge.wait_recv()

    g.cf[0:HALO, :] = g.halo[...].astype(F32)

    def taps_of(first, cols):
        v = g.cf[cut(first + 8, 72, 8), cols]
        sv = g.segc[cut(first + 8, 72, 8), :]
        width = v.shape[1] // 128
        out = []
        for k in range(3):
            same = pltpu.roll(sv, 67 - k, 0)[0:64] == sv[8:72]
            out.append(jnp.where(wide_of(same, width), pltpu.roll(v, 67 - k, 0)[0:64], 0.0))
        out.append(v[8:72])
        return out

    def convolve(i):
        first = i * 64
        at = cut(first, 64, 16)
        for n in range(4):
            cols = pl.ds(n * 256, 256)
            v = jnp.broadcast_to(g.taps[4:5, cols], (64, 256))
            for k, t in enumerate(taps_of(first, cols)):
                v = v + g.taps[k : k + 1, cols] * t
            sig = jax.nn.sigmoid(v)
            act = (v * sig).astype(BF)
            g.slope[at, cols] = sig * (1.0 + v * (1.0 - sig))
            if n < 3:
                g.inner[at, cols] = act
            else:
                g.b[at, :] = act[:, 0:128]
                g.c[at, :] = act[:, 128:256]

    loop(ROWS // 64, convolve)

    g.bt[...] = g.b[...].astype(F32).T
    g.ct[...] = g.c[...].astype(F32).T

    def outer(maps, weights, vals):
        def body(t):
            q, p = t // 6, lax.rem(t, 6)
            at = cut(p * 128, 128, 128)
            v = vals[cut(q * SPAN, SPAN, 256), at]
            m = maps[:, cut(q * SPAN, SPAN, 256)]
            o = [mul((m * weights[q, pl.ds(2 * p + e, 1), :]).astype(BF), v) for e in range(2)]
            g.local[q, :, at] = jnp.where(left, o[0], o[1])

        loop(12, body)

    outer(g.bt, g.loadt, g.inner)
    c0, c1 = g.carrye[0][0:1], g.carrye[1][0:1]
    g.state_out[...] = (c1 * g.local[0] + g.local[1])
    for j in range(1, HOPS + 1):
        ahead = s + j < SEQ
        behind = s - j >= 0
        d = remote(g.state_out, g.states.at[j - 1], g.st_send.at[j - 1], g.st_recv.at[j - 1], {ALONG: s + j})

        @pl.when(ahead)
        def _():
            d.start()

        @pl.when(jnp.logical_not(behind))
        def _():
            g.states[j - 1] = jnp.zeros((STATE, CHANNELS), F32)

    for j in range(1, HOPS):
        up = remote(g.decay.at[0], g.decay.at[j], g.st_send.at[2 + j], g.st_recv.at[2 + j], {ALONG: s + j})
        down = remote(g.decay.at[0], g.decay.at[2 + j], g.st_send.at[4 + j], g.st_recv.at[4 + j], {ALONG: s - j})

        @pl.when(s + j < SEQ)
        def _():
            up.start()

        @pl.when(s - j >= 0)
        def _():
            down.start()

        @pl.when(s - j < 0)
        def _():
            g.decay[j] = jnp.zeros((8, CHANNELS), F32)

        @pl.when(s + j >= SEQ)
        def _():
            g.decay[2 + j] = jnp.zeros((8, CHANNELS), F32)

    def head_cols(ref, rows, p):
        moved = pltpu.roll(ref[rows, :], lax.rem(128 - 2 * p, 128), 1)
        return moved[:, 0:1], moved[:, 1:2]

    def inside(q):
        rows = cut(q * SPAN, SPAN, 256)
        seg = g.segc[cut(HALO + q * SPAN, SPAN, 16), 0:1]
        segr = g.segr[0:1, cut(q * SPAN, SPAN, 256)]
        scores = mul(g.c[rows, :], g.b[rows, :], NT)
        g.scores[...] = jnp.where((tri_i >= tri_j) & (seg == segr), scores, 0.0)

        def pair(p):
            cols = head_cols(g.cum, rows, p)
            at = cut(p * 128, 128, 128)
            outs = []
            for e in range(2):
                row = g.cumt[q, pl.ds(2 * p + e, 1), :]
                step = g.stept[q, pl.ds(2 * p + e, 1), :]
                fall = jnp.exp(jnp.minimum(cols[e] - row, 0.0))
                outs.append(mul((g.scores[...] * fall * step).astype(BF), g.inner[rows, at]))
            g.out[rows, at] = jnp.where(left, outs[0], outs[1])

        loop(6, pair)

    loop(2, inside)

    for j in range(1, HOPS + 1):
        d = remote(g.state_out, g.states.at[j - 1], g.st_send.at[j - 1], g.st_recv.at[j - 1], {ALONG: s + j})

        @pl.when(s - j >= 0)
        def _():
            d.wait_recv()

    for j in range(1, HOPS):
        up = remote(g.decay.at[0], g.decay.at[j], g.st_send.at[2 + j], g.st_recv.at[2 + j], {ALONG: s + j})

        @pl.when(s - j >= 0)
        def _():
            up.wait_recv()

    got = [g.states[j].astype(F32) for j in range(HOPS)]
    incoming = got[0] + g.decay[1][0:1] * (got[1] + g.decay[2][0:1] * got[2])
    g.sin[0] = incoming
    g.sin[1] = g.local[0] + c0 * incoming
    for q in range(2):
        g.slow[q] = g.sin[q].astype(BF)

    def outside(t):
        q, p = t // 6, lax.rem(t, 6)
        rows, at = cut(q * SPAN, SPAN, 256), cut(p * 128, 128, 128)
        cols = head_cols(g.lead, rows, p)
        cv = g.c[rows, :].astype(F32)
        o = [mul((cv * cols[e]).astype(BF), g.slow[q, :, at]) for e in range(2)]
        g.out[rows, at] += jnp.where(left, o[0], o[1])

    loop(12, outside)

    gate_cols = pl.ds(WIDE, CHANNELS)
    skip = g.skipe[0:1]

    def gate(i):
        at = cut(i * 64, 64, 16)
        pre = g.acc[at, gate_cols]
        mixed = g.out[at, :] + g.inner[at, :].astype(F32) * skip
        gated = mixed * (pre * jax.nn.sigmoid(pre))
        g.gated[at, :] = gated
        g.part[0, at, :] = lanes_sum(gated * gated)

    loop(ROWS // 64, gate)

    for d in cin:
        d.wait_recv()
    loads[4].wait()
    gate_gain = g.params[6:7, :]

    def down(n):
        g.ggn[:, cut(n * 256, 256, 256)] = mul(g.cotg[...], g.wo[cut(n * 256, 256, 256), :], NT)

    loop(3, down)

    def inner_part(i):
        at = cut(i * 64, 64, 16)
        g.part[1, at, :] = lanes_sum(g.ggn[at, :] * gate_gain * g.gated[at, :])

    loop(ROWS // 64, inner_part)
    g.stats[z, 0:8, :] = jnp.broadcast_to(to_row(g.part[0]), (8, ROWS))
    g.stats[z, 8:16, :] = jnp.broadcast_to(to_row(g.part[1]), (8, ROWS))
    stat = [send(g.stats.at[z], g.stats.at[z], g.stat, i, p) for i, p in enumerate(zpeers)]
    for d in stat:
        d.wait_recv()
    sums = g.stats[0] + g.stats[1] + g.stats[2] + g.stats[3]
    gscale = lax.rsqrt(sums[0:1] / INNER + epsilon)
    g.part[0] = to_col(gscale)
    g.part[1] = to_col(gscale * gscale * gscale * sums[8:9] / INNER)
    g.vacc[...] = jnp.zeros(g.vacc.shape, F32)

    def ungate(i):
        at = cut(i * 64, 64, 16)
        a = wide_of(g.part[0, at, :], 6)
        pre = g.acc[at, gate_cols]
        vals = g.inner[at, :].astype(F32)
        mixed = g.out[at, :] + vals * skip
        gated, ggn = g.gated[at, :], g.ggn[at, :]
        g.gn[at, :] = (gated * a * gate_gain).astype(BF)
        gg = a * (ggn * gate_gain) - gated * wide_of(g.part[1, at, :], 6)
        sig = jax.nn.sigmoid(pre)
        gm = (gg * (pre * sig)).astype(BF)
        g.gm[at, :] = gm
        g.gz[at, :] = (gg * mixed * (sig * (1.0 + pre * (1.0 - sig)))).astype(BF)
        g.vacc[0] += rows_sum(ggn * gated * a)
        g.vacc[1] += rows_sum(gm.astype(F32) * vals)

    loop(ROWS // 64, ungate)

    outer(g.ct, g.leadt, g.gm)
    g.sent_grad[...] = (g.local[0] + c0 * g.local[1])
    back = []
    for j in range(1, HOPS + 1):
        d = remote(g.sent_grad, g.gstates.at[j - 1], g.gs_send.at[j - 1], g.gs_recv.at[j - 1], {ALONG: s - j})
        back.append(d)

        @pl.when(s - j >= 0)
        def _():
            d.start()

        @pl.when(s + j >= SEQ)
        def _():
            g.gstates[j - 1] = jnp.zeros((STATE, CHANNELS), F32)

    def total_of(i, ref, n):
        return Total(ref, sum_bufs[5 * i : 5 * i + 5], g.tot_send, g.tot_recv, g.freed, 10 * i, me)

    t_out = total_of(0, g.p_out, 0)
    t_z = total_of(1, g.p_z, 0)
    t_x = total_of(2, g.p_x, 0)
    t_bc = total_of(3, g.p_bc, 0)

    def grad_out(n):
        at = cut(n * 256, 256, 256)
        g.p_out[at, :] = mul(g.gn[:, at], g.cotg[...], TN).astype(BF)

    loop(3, grad_out)
    t_out.s0()

    def grad_z(n):
        at = cut(n * 256, 256, 256)
        g.p_z[at, :] = mul(g.xn[:, at], g.gz[...], TN).astype(BF)

    loop(6, grad_z)
    t_z.s0()
    t_out.s1()

    outs = []
    for i, p in enumerate(zpeers):
        k = lax.rem(z + 1 + i, LINE)
        g.sblk[i] = mul(g.gn[...], g.wo[:, cut(k * BLOCK, BLOCK, 128)]).astype(BF)
        outs.append(send(g.sblk.at[i], g.rblk.at[i], g.block, i, p))
    g.own[...] = mul(g.gn[...], g.wo[:, own])
    t_z.s1()

    def inside_back(q):
        rows = cut(q * SPAN, SPAN, 256)
        seg = g.segc[cut(HALO + q * SPAN, SPAN, 16), 0:1]
        segr = g.segr[0:1, cut(q * SPAN, SPAN, 256)]
        scores = mul(g.b[rows, :], g.c[rows, :], NT)
        mask = (tri_i <= tri_j) & (seg == segr)
        g.scores[...] = jnp.where(mask, scores, 0.0)
        g.gscores[...] = jnp.zeros((SPAN, SPAN), F32)

        def pair(p):
            cols = head_cols(g.cum, rows, p)
            at = cut(p * 128, 128, 128)
            steps = head_cols(g.step, rows, p)
            gm = g.gm[rows, at]
            outs = []
            for e in range(2):
                row = g.cumt[q, pl.ds(2 * p + e, 1), :]
                fall = jnp.exp(jnp.minimum(row - cols[e], 0.0)) * steps[e]
                outs.append(mul((g.scores[...] * fall).astype(BF), gm))
                keep = left if e == 0 else jnp.logical_not(left)
                vals = jnp.where(keep, g.inner[rows, at].astype(F32), 0.0).astype(BF)
                g.gscores[...] += mul(vals, gm, NT) * fall
            g.z[rows, at] = jnp.where(left, outs[0], outs[1])

        loop(6, pair)
        gs = jnp.where(mask, g.gscores[...], 0.0)
        hi, lo = parts(gs, 2)
        g.gb[rows, :] = mul(hi, g.c[rows, :]) + mul(lo, g.c[rows, :])
        g.gc[rows, :] = mul(hi, g.b[rows, :], TN) + mul(lo, g.b[rows, :], TN)

    inside_back(1)
    t_out.s2()
    inside_back(0)
    t_z.s2()

    for j in range(1, HOPS + 1):
        @pl.when(s + j < SEQ)
        def _():
            back[j - 1].wait_recv()

    for j in range(1, HOPS):
        d = remote(g.decay.at[0], g.decay.at[2 + j], g.st_send.at[4 + j], g.st_recv.at[4 + j], {ALONG: s - j})

        @pl.when(s + j < SEQ)
        def _():
            d.wait_recv()

    got = [g.gstates[j].astype(F32) for j in range(HOPS)]
    beyond = got[0] + g.decay[3][0:1] * (got[1] + g.decay[4][0:1] * got[2])
    g.gloc[1] = beyond
    g.gloc[0] = g.local[1] + c1 * beyond
    t_out.s3()
    ends = []
    for q in range(2):
        rows = pl.ds(q * SPAN, SPAN)
        glow = g.gloc[q].astype(BF)
        vals = g.inner[rows, :].astype(F32)
        gm = g.gm[rows, :].astype(F32)
        loade = spread(g.load[rows, :])
        bg = mul(g.b[rows, :], glow)
        zed = g.z[rows, :]
        carry_sum = jnp.sum(g.gloc[q] * g.sin[q], axis=0, keepdims=True)
        grad_carry = head_sum(jnp.broadcast_to(carry_sum, (8, CHANNELS)))[0:1]
        t1 = head_sum(gm * g.out[rows, :])
        q1 = head_sum(vals * zed)
        q2 = head_sum(vals * bg)
        step, load = g.step[rows, :], g.load[rows, :]
        tail_term = q2 * load
        gcum = t1 - q1 - tail_term
        end = jnp.sum(tail_term, axis=0, keepdims=True) + grad_carry * g.carry[q][0:1]
        is_last = lax.broadcasted_iota(jnp.int32, (SPAN, 128), 0) == SPAN - 1
        gcum = gcum + jnp.where(is_last, end, 0.0)
        glog = sum(mul(g.tri[...], p, TN) for p in parts(gcum, 3))
        gstep = jnp.where(step > 1e-30, q1 / jnp.maximum(step, 1e-30), 0.0) + q2 * g.tail[rows, :]
        gpre = (gstep - rates * glog) * jax.nn.sigmoid(g.spre[rows, :])
        g.gsr[rows, :] = gpre.astype(BF)
        ends.append((rows_sum(gpre), rows_sum(glog * (-rates * step))))
        g.z[rows, :] = zed + loade * bg + skip * gm
        g.gb[rows, :] += sum(mul(p, glow, NT) for p in parts(vals * loade, 2))
        g.gc[rows, :] += sum(mul(p, g.slow[q], NT) for p in parts(gm * spread(g.lead[rows, :]), 2))
    g.pack[16:24, 0:128] = jnp.broadcast_to(
        jnp.sum(ends[0][0] + ends[1][0], axis=0, keepdims=True), (8, 128)
    )
    g.pack[16:24, 128:256] = jnp.broadcast_to(
        jnp.sum(ends[0][1] + ends[1][1], axis=0, keepdims=True), (8, 128)
    )
    t_z.s3()

    def grads_of(at, n):
        cols = pl.ds(n * 256, 256)
        if n < 3:
            v = g.z[at, cols]
        else:
            v = jnp.concatenate([g.gb[at, :], g.gc[at, :]], axis=1)
        return v * g.slope[at, cols]

    def slopes(i):
        at = cut(i * 64, 64, 16)
        for n in range(4):
            g.gconv[cut(i * 64, 64, 8), pl.ds(n * 256, 256)] = grads_of(at, n)

    g.gconv[ROWS : ROWS + 16, :] = jnp.zeros((16, WIDE), F32)
    loop(ROWS // 64, slopes)

    def same_ahead(first, count, shift):
        sv = g.segc[cut(first + HALO, count + 8, 8), :] if count else None
        return sv

    v = g.gconv[0:8, :]
    sv = g.segc[HALO - 8 : HALO + 8, :]
    back_rows = jnp.zeros((8, WIDE), F32)
    for k in range(3):
        shift = 3 - k
        full = jnp.concatenate([jnp.zeros((8, WIDE), F32), v], axis=0)
        src = pltpu.roll(full, 16 - shift, 0)[0:8]
        same = pltpu.roll(sv, 16 - shift, 0)[0:8] == sv[0:8]
        back_rows = back_rows + jnp.where(wide_of(same, 8), g.taps[k : k + 1, :] * src, 0.0)
    g.ret_out[...] = back_rows
    ret = remote(g.ret_out, g.ret_in, g.edge_sem.at[2], g.edge_sem.at[3], {ALONG: s - 1})

    @pl.when(s > 0)
    def _():
        ret.start()

    @pl.when(s == SEQ - 1)
    def _():
        g.ret_in[...] = jnp.zeros((8, WIDE), F32)

    g.wacc[...] = jnp.zeros(g.wacc.shape, F32)

    def convolve_back(i):
        first = i * 64
        at = cut(first, 64, 16)
        sv = g.segc[cut(first + HALO, 64, 8), :]
        ahead = jnp.where(i < ROWS // 64 - 1, 1.0, 0.0)
        for n in range(4):
            cols = pl.ds(n * 256, 256)
            v = g.gconv[cut(first, 72, 8), cols]
            here = v[0:64]
            total = g.taps[3:4, cols] * here
            nxt = g.segc[cut(jnp.minimum(first + HALO + 64, ROWS + HALO - 8), 8, 8), :]
            sfull = jnp.concatenate([sv, nxt], axis=0)
            for k in range(3):
                shift = 3 - k
                same = pltpu.roll(sfull, 72 - shift, 0)[0:64] == sv
                src = pltpu.roll(v, 72 - shift, 0)[0:64]
                total = total + jnp.where(wide_of(same, 2), g.taps[k : k + 1, cols] * src, 0.0)
            if n < 3:
                g.gx[at, cols] = total.astype(BF)
            else:
                for k, v in enumerate(parts(total, 2)):
                    g.gbc[k, at, :] = v

            @pl.when(i == ROWS // 64 - 1)
            def _():
                g.tail_rows[:, cols] = total[48:64]

            for k, t in enumerate(taps_of(first, cols)):
                g.wacc[k, :, cols] += rows_sum(here * t)
            g.wacc[4, :, cols] += rows_sum(here)

    loop(ROWS // 64, convolve_back)
    t_out.s4()

    @pl.when(s < SEQ - 1)
    def _():
        ret.wait_recv()

    last_rows = g.tail_rows[...] + jnp.concatenate([jnp.zeros((8, WIDE), F32), g.ret_in[...]], axis=0)
    g.gx[ROWS - 16 : ROWS, :] = last_rows[:, 0:CHANNELS].astype(BF)
    for k, v in enumerate(parts(last_rows[:, CHANNELS:WIDE], 2)):
        g.gbc[k, ROWS - 16 : ROWS, :] = v

    def bc_block(at):
        return sum(mul(g.xn[:, at], g.gbc[k], TN) for k in range(2))

    bcs = []
    for i, p in enumerate(zpeers):
        k = lax.rem(z + 1 + i, LINE)
        g.sbc[i] = bc_block(cut(k * BLOCK, BLOCK, 128)).astype(BF)
        bcs.append(send(g.sbc.at[i], g.rbc.at[i], g.bcsem, i, p))

    def grad_x(n):
        at = cut(n * 256, 256, 256)
        g.p_x[at, :] = mul(g.xn[:, at], g.gx[...], TN).astype(BF)

    loop(6, grad_x)
    t_x.s0()
    t_z.s4()

    def back_block(k):
        at = cut(k * BLOCK, BLOCK, 16)
        v = mul(g.gx[...], g.wx[at, :], NT) + mul(g.gz[...], g.wz[at, :], NT)
        return v + mul(g.gsr[...], g.wd[at, :], NT) + mul(g.gbc[0], g.wbc[k], NT) + mul(g.gbc[1], g.wbc[k], NT)

    for d in outs:
        d.wait_recv()
        d.wait_send()
        pending[:] = [q for q in pending if q is not d]
    out_sum = g.own[...]
    for i in range(3):
        out_sum = out_sum + g.rblk[i].astype(F32)
    g.layer_out[...] = (g.x[...].astype(F32) + out_sum).astype(BF)
    ins = []
    for i, p in enumerate(zpeers):
        k = lax.rem(z + 1 + i, LINE)
        g.sblk2[i] = back_block(k).astype(BF)
        ins.append(send(g.sblk2.at[i], g.rblk2.at[i], g.block, 3 + i, p))
        if i == 0:
            t_x.s1()
            t_out.s5()
    g.own[...] = back_block(z)

    for k in range(5):
        row = jnp.sum(g.wacc[k], axis=0, keepdims=True)
        g.pack[k : k + 1, :] = row[:, 0:CHANNELS]
        g.pack[8 + k : 9 + k, 0:256] = row[:, CHANNELS:WIDE]
    g.pack[5:6, :] = jnp.sum(g.vacc[0], axis=0, keepdims=True)
    g.pack[6:7, :] = jnp.sum(g.vacc[1], axis=0, keepdims=True)
    g.dt_out[...] = mul(g.gsr[...], g.xn[...], TN)[0:16].astype(BF)
    packs = []
    for i, p in enumerate(speers):
        packs.append(send(g.pack, g.packs.at[i], g.packsem, i, p))
        packs.append(send(g.dt_out, g.dts.at[i], g.packsem, 7 + i, p))
    bc = bc_block(own)
    for d in bcs:
        d.wait_recv()
    for i in range(3):
        bc = bc + g.rbc[i].astype(F32)
    g.p_bc[...] = bc
    t_bc.s0()
    t_z.s5()
    t_out.s6()
    store = [pltpu.make_async_copy(g.p_out, g.grad_out, g.load_sem.at[5])]
    store[0].start()
    t_x.s2()
    t_bc.s1()
    t_z.s6()
    store.append(pltpu.make_async_copy(g.p_z, g.grad_z, g.load_sem.at[6]))
    store[1].start()
    for d in packs:
        d.wait_recv()
    vec = g.pack[...]
    dts = g.dt_out[...].astype(F32)
    for i in range(7):
        vec = vec + g.packs[i]
        dts = dts + g.dts[i].astype(F32)
    g.vec[...] = vec
    g.grad_dt[...] = dts
    g.bcv[z] = vec[8:16, 0:256]
    bcv = [send(g.bcv.at[z], g.bcv.at[z], g.bcvsem, i, p) for i, p in enumerate(zpeers)]
    t_x.s3()
    t_bc.s2()
    t_bc.s3()
    t_x.s4()
    t_bc.s4()

    for d in ins:
        d.wait_recv()
    g.nacc[...] = jnp.zeros(g.nacc.shape, F32)

    def finish(i):
        at = cut(i * 64, 64, 16)
        v = g.own[at, :]
        for k in range(3):
            v = v + g.rblk2[k, at, :].astype(F32)
        g.own[at, :] = v
        x = g.x[at, :].astype(F32)
        g.part[0, at, :] = lanes_sum(v * gain * x)
        g.nacc[...] += rows_sum(v * x * wide_of(g.xscale[at, :], 3))

    loop(ROWS // 64, finish)
    g.nstat[z] = jnp.broadcast_to(to_row(g.part[0]), (8, ROWS))
    nst = [send(g.nstat.at[z], g.nstat.at[z], g.nsem, i, p) for i, p in enumerate(zpeers)]
    g.ngain[0] = jnp.broadcast_to(jnp.sum(g.nacc[...], axis=0, keepdims=True), (8, BLOCK))
    ngs = [send(g.ngain.at[0], g.ngain.at[1 + i], g.nsem, 3 + i, p) for i, p in enumerate(speers)]
    t_x.s5()
    t_bc.s5()
    for d in nst:
        d.wait_recv()
    rows = (g.nstat[0] + g.nstat[1] + g.nstat[2] + g.nstat[3])[0:1]
    g.part[0] = to_col(rows / D)

    def last(i):
        at = cut(i * 64, 64, 16)
        sc = wide_of(g.xscale[at, :], 3)
        x = g.x[at, :].astype(F32)
        g.grad_in[at, :] = (
            g.cotg[at, own].astype(F32)
            + sc * (g.own[at, :] * gain)
            - x * (sc * sc * sc * wide_of(g.part[0, at, :], 3))
        )

    loop(ROWS // 64, last)
    for d in ngs:
        d.wait_recv()
    total = g.ngain[0]
    for i in range(7):
        total = total + g.ngain[1 + i]
    g.grad_gain[...] = total
    for d in bcv:
        d.wait_recv()
    g.vec[8:16, 0:256] = g.bcv[0] + g.bcv[1] + g.bcv[2] + g.bcv[3]
    t_bc.s6()
    g.grad_bc[...] = g.p_bc[...]
    t_x.s6()
    store.append(pltpu.make_async_copy(g.p_x, g.grad_x, g.load_sem.at[7]))
    store[2].start()
    for d in pending:
        d.wait_send()

    @pl.when(s < SEQ - 1)
    def _():
        edge.wait_send()

    @pl.when(s > 0)
    def _():
        ret.wait_send()

    for j in range(1, HOPS + 1):
        d = remote(g.state_out, g.states.at[j - 1], g.st_send.at[j - 1], g.st_recv.at[j - 1], {ALONG: s + j})

        @pl.when(s + j < SEQ)
        def _():
            d.wait_send()

        @pl.when(s - j >= 0)
        def _():
            back[j - 1].wait_send()

    for j in range(1, HOPS):
        up = remote(g.decay.at[0], g.decay.at[j], g.st_send.at[2 + j], g.st_recv.at[2 + j], {ALONG: s + j})
        down_copy = remote(g.decay.at[0], g.decay.at[2 + j], g.st_send.at[4 + j], g.st_recv.at[4 + j], {ALONG: s - j})

        @pl.when(s + j < SEQ)
        def _():
            up.wait_send()

        @pl.when(s - j >= 0)
        def _():
            down_copy.wait_send()

    for d in store:
        d.wait()


def fast_layer(
    hidden_in, seq_lengths, norm_gain, w_z, w_x, w_bc, w_dt, conv_x_w, conv_x_b, conv_bc_w,
    conv_bc_b, dt_bias, a_log, d_skip, gate_gain, w_out, cotangent,
):
    vectors = (norm_gain, conv_x_b, conv_bc_b, dt_bias, a_log, d_skip, gate_gain)
    params = jnp.stack([jnp.pad(v, (0, CHANNELS - v.shape[0])) for v in vectors] + [jnp.zeros((CHANNELS,), F32)])
    vm = pl.BlockSpec(memory_space=pltpu.VMEM)
    hbm = pl.BlockSpec(memory_space=pl.ANY)
    sm = pl.BlockSpec(memory_space=pltpu.SMEM)
    ins = dict(
        x_hbm=(hidden_in, hbm), cot_hbm=(cotangent, hbm), w_x=(w_x, hbm), w_z=(w_z, hbm), w_out=(w_out, hbm),
        lengths=(seq_lengths, sm), params=(params, vm), w_bc=(w_bc, vm), w_dt=(w_dt, vm),
        conv_x_w=(conv_x_w, vm), conv_bc_w=(conv_bc_w, vm),
    )
    outs = dict(
        layer_out=((ROWS, BLOCK), BF, vm),
        grad_in=((ROWS, BLOCK), F32, vm),
        grad_out=((CHANNELS, D), BF, hbm),
        grad_z=((D, CHANNELS), BF, hbm),
        grad_x=((D, CHANNELS), BF, hbm),
        grad_bc=((BLOCK, 256), F32, vm),
        grad_dt=((16, D), F32, vm),
        vec=((24, CHANNELS), F32, vm),
        grad_gain=((8, BLOCK), F32, vm),
    )
    V = pltpu.VMEM
    S = pltpu.SemaphoreType.DMA
    scr = dict(
        x=V((ROWS, BLOCK), BF),
        wx=V((D, CHANNELS), BF),
        wz=V((D, CHANNELS), BF),
        wo=V((CHANNELS, D), BF),
        xg=V((ROWS, D), BF),
        xn=V((ROWS, D), BF),
        cotg=V((ROWS, D), BF),
        ssq=V((LINE, 8, ROWS), F32),
        gains=V((LINE, 8, BLOCK), F32),
        wbc=V((LINE, BLOCK, 256), BF),
        wd=V((D, 128), BF),
        taps=V((8, WIDE), F32),
        spread=V((256, CHANNELS), BF),
        segc=V((ROWS + HALO, 128), F32),
        segr=V((8, ROWS), F32),
        tri=V((SPAN, SPAN), BF),
        skipe=V((8, CHANNELS), F32),
        xscale=V((ROWS, 128), F32),
        acc=V((ROWS, WIDE + CHANNELS + 128), F32),
        edge=V((HALO, WIDE), BF),
        halo=V((HALO, WIDE), BF),
        cf=V((ROWS + HALO, WIDE), F32),
        spre=V((ROWS, 128), F32),
        step=V((ROWS, 128), F32),
        cum=V((ROWS, 128), F32),
        cumt=V((2, 16, SPAN), F32),
        tail=V((ROWS, 128), F32),
        load=V((ROWS, 128), F32),
        lead=V((ROWS, 128), F32),
        carry=V((2, 8, 128), F32),
        carrye=V((2, 8, CHANNELS), F32),
        decay=V((5, 8, CHANNELS), F32),
        slope=V((ROWS + 16, WIDE), F32),
        inner=V((ROWS, CHANNELS), BF),
        b=V((ROWS, 128), BF),
        c=V((ROWS, 128), BF),
        bt=V((STATE, ROWS), F32),
        ct=V((STATE, ROWS), F32),
        loadt=V((2, 16, SPAN), F32),
        leadt=V((2, 16, SPAN), F32),
        stept=V((2, 16, SPAN), F32),
        local=V((2, STATE, CHANNELS), F32),
        state_out=V((STATE, CHANNELS), F32),
        states=V((HOPS, STATE, CHANNELS), F32),
        scores=V((SPAN, SPAN), F32),
        gscores=V((SPAN, SPAN), F32),
        out=V((ROWS, CHANNELS), F32),
        sin=V((2, STATE, CHANNELS), F32),
        slow=V((2, STATE, CHANNELS), BF),
        gated=V((ROWS, CHANNELS), F32),
        part=V((2, ROWS, 128), F32),
        stats=V((LINE, 16, ROWS), F32),
        vacc=V((2, 8, CHANNELS), F32),
        gm=V((ROWS, CHANNELS), BF),
        sent_grad=V((STATE, CHANNELS), F32),
        gstates=V((HOPS, STATE, CHANNELS), F32),
        gloc=V((2, STATE, CHANNELS), F32),
        sblk=V((3, ROWS, BLOCK), BF),
        rblk=V((3, ROWS, BLOCK), BF),
        rblk2=V((3, ROWS, BLOCK), BF),
        gsr=V((ROWS, 128), BF),
        pack=V((24, CHANNELS), F32),
        packs=V((7, 24, CHANNELS), F32),
        ret_out=V((8, WIDE), F32),
        ret_in=V((8, WIDE), F32),
        wacc=V((5, 8, WIDE), F32),
        gbc=V((2, ROWS, 256), BF),
        tail_rows=V((16, WIDE), F32),
        sbc=V((3, BLOCK, 256), BF),
        rbc=V((3, BLOCK, 256), BF),
        dt_out=V((16, D), BF),
        dts=V((7, 16, D), BF),
        bcv=V((LINE, 8, 256), F32),
        nacc=V((8, BLOCK), F32),
        nstat=V((LINE, 8, ROWS), F32),
        ngain=V((8, 8, BLOCK), F32),
        p_out=V((CHANNELS, D), BF),
        p_z=V((D, CHANNELS), BF),
        p_x=V((D, CHANNELS), BF),
        p_bc=V((BLOCK, 256), F32),
        load_sem=S((8,)),
        edge_sem=S((4,)),
        st_send=S((7,)),
        st_recv=S((7,)),
        gs_send=S((3,)),
        gs_recv=S((3,)),
        tot_send=S((40,)),
        tot_recv=S((40,)),
        freed=pltpu.SemaphoreType.REGULAR((12,)),
    )
    pairs = dict(
        small=9,
        gather=6,
        wide=7,
        stat=3,
        block=6,
        bcsem=3,
        packsem=14,
        bcvsem=3,
        nsem=10,
    )
    sums = [(CHANNELS, D, BF), (D, CHANNELS, BF), (D, CHANNELS, BF), (BLOCK, 256, F32)]
    bufs = [b for spec in sums for b in total_bufs(*spec)]
    sems = [S((k,)) for k in pairs.values() for _ in range(2)]
    names = [*ins, *outs, *scr]

    def kernel(*refs):
        n, m = len(names), len(names) + len(bufs)
        d = dict(zip(names, refs[:n]))
        rest = refs[m:]
        for i, name in enumerate(pairs):
            d[name] = (rest[2 * i], rest[2 * i + 1])
        layer_kernel(d, refs[n:m])

    res = pl.pallas_call(
        kernel,
        out_shape=[jax.ShapeDtypeStruct(sh, dt) for sh, dt, _ in outs.values()],
        in_specs=[sp for _, sp in ins.values()],
        out_specs=[sp for _, _, sp in outs.values()],
        scratch_shapes=[*scr.values(), *bufs, *sems],
        compiler_params=pltpu.CompilerParams(collective_id=0, has_side_effects=True, vmem_limit_bytes=66 * 2**20 - 2**21),
        name="layer",
    )(*[a for a, _ in ins.values()])
    layer_out, grad_in, grad_out, grad_z, grad_x, grad_bc, grad_dt, vec, grad_gain = res
    return (
        layer_out, grad_in, grad_gain[0], grad_z.astype(F32), grad_x.astype(F32), grad_bc,
        grad_dt[0:12].T, vec[0:4], vec[4], vec[8:12, 0:256], vec[12, 0:256], vec[16, 0:12], vec[16, 128:140],
        jnp.sum(vec[6].reshape(12, HEAD_DIM), axis=1), vec[5], grad_out.astype(F32),
    )


def solution(mesh):
    placed = (
        P("seq", "head"),
        P(),
        P("head"),
        P(None, "head"),
        P(None, "head"),
        P("head", None),
        P(None, "head"),
        P(None, "head"),
        P("head"),
        P(),
        P(),
        P("head"),
        P("head"),
        P("head"),
        P("head"),
        P("head", None),
        P("seq", "head"),
    )
    fits = mesh.shape["seq"] == SEQ and mesh.shape["head"] == LINE
    return jax.shard_map(
        fast_layer if fits else on_device,
        mesh=mesh,
        in_specs=placed,
        out_specs=(
            P("seq", "head"),
            P("seq", "head"),
            P("head"),
            P(None, "head"),
            P(None, "head"),
            P("head", None),
            P(None, "head"),
            P(None, "head"),
            P("head"),
            P(),
            P(),
            P("head"),
            P("head"),
            P("head"),
            P("head"),
            P("head", None),
        ),
        check_vma=False,
    )
```

```python
import jax
import jax.numpy as jnp
from jax import lax
from jax.experimental import pallas as pl
from jax.experimental.pallas import tpu as pltpu
from jax.sharding import PartitionSpec as P

D = 1536
HEAD_DIM = 64
STATE = 128
CONV = 4
SPAN = 256
INNER = 3072


epsilon = 1e-05
highest = lax.Precision.HIGHEST


def prefix(part, axis, combine, identity, reverse):
    count = lax.axis_size(axis)
    place = lax.axis_index(axis)
    ahead = count - 1 - place if reverse else place
    gathered = jax.tree.map(lambda a: lax.all_gather(a, axis), part)
    state = jax.tree.map(lambda a, e: jnp.zeros_like(a) + jnp.asarray(e, a.dtype), part, identity)

    def one(hop, state):
        source = count - 1 - hop if reverse else hop
        return combine(
            state, jax.tree.map(lambda a: lax.dynamic_index_in_dim(a, source, 0, False), gathered)
        )

    return lax.fori_loop(0, ahead, one, state)


def passed_along(block, axis, distance):
    devices = range(lax.axis_size(axis))
    route = [(i - distance, i) for i in devices if i - distance in devices]
    return lax.ppermute(block, axis, route)


def segment_of(positions, starts):
    return jnp.sum((positions[:, None] >= starts[None, :]).astype(jnp.int32), axis=1) - 1


def silu_slope(values):
    sigmoid_val = jax.nn.sigmoid(values)
    return sigmoid_val * (1.0 + values * (1.0 - sigmoid_val))


def chain_join(earlier, later):
    return (earlier[0] * later[0], earlier[1] * later[0][:, None, None] + later[1])


def state_prefix(decay, summary, backwards):
    identity = (jnp.ones_like(decay), jnp.zeros_like(summary))
    result = prefix((decay, summary), "seq", chain_join, identity, backwards)
    return result[1]


def span_terms(span_item, lower_tri):
    inner_c, b_rows, c_rows, step_c, cumul_c, seg_rows, seg_prev = span_item
    same_seq = ((seg_rows[:, None] == seg_rows[None, :]) & (lower_tri > 0.5))[None, :, :]
    spread = cumul_c[:, :, None] - cumul_c[:, None, :]
    decay_mat = jnp.where(same_seq, jnp.exp(jnp.where(same_seq, spread, 0.0)), 0.0)
    scores = lax.dot_general(
        c_rows, b_rows, (((1,), (1,)), ((), ())), preferred_element_type=jnp.float32
    )
    mixing = scores[None, :, :] * decay_mat * step_c[:, None, :]
    last_cum = cumul_c[:, SPAN - 1]
    tail_weight = (
        jnp.exp(last_cum[:, None] - cumul_c)
        * (seg_rows == seg_rows[SPAN - 1]).astype(jnp.float32)[None, :]
    )
    head_weight = jnp.exp(cumul_c) * (seg_rows == seg_prev).astype(jnp.float32)[None, :]
    carry_decay = jnp.exp(last_cum) * (seg_rows[SPAN - 1] == seg_prev).astype(jnp.float32)
    return (decay_mat, scores, mixing, tail_weight, head_weight, carry_decay)


def on_device(
    hidden_in,
    seq_lengths,
    norm_gain,
    w_z,
    w_x,
    w_bc,
    w_dt,
    conv_x_w,
    conv_x_b,
    conv_bc_w,
    conv_bc_b,
    dt_bias,
    a_log,
    d_skip,
    gate_gain,
    w_out,
    cotangent,
):
    tokens_here = hidden_in.shape[0]
    heads_here = dt_bias.shape[0]
    inner_here = w_z.shape[1]
    spans = tokens_here // SPAN
    first_pos = lax.axis_index("seq") * tokens_here
    starts = jnp.cumsum(seq_lengths) - seq_lengths
    segment = segment_of(first_pos + jnp.arange(tokens_here, dtype=jnp.int32), starts)
    edge_segment = segment_of(
        first_pos - (CONV - 1) + jnp.arange(CONV - 1, dtype=jnp.int32), starts
    )
    span_prev = segment_of(first_pos - 1 + jnp.arange(spans, dtype=jnp.int32) * SPAN, starts)
    row_ids = jnp.arange(SPAN)
    lower_tri = (row_ids[:, None] >= row_ids[None, :]).astype(jnp.float32)
    inputs = hidden_in.astype(jnp.float32)
    squares = lax.psum(jnp.sum(inputs * inputs, axis=1), "head")
    scale_in = lax.rsqrt(squares / D + epsilon)
    normed = (inputs * scale_in[:, None] * norm_gain).astype(jnp.bfloat16)
    gathered, bc_weight = (
        lax.all_gather(normed, "head", axis=1, tiled=True),
        lax.all_gather(w_bc, "head", axis=0, tiled=True),
    )
    gate_pre = jnp.dot(gathered, w_z, preferred_element_type=jnp.float32)
    x_part = jnp.dot(gathered, w_x, preferred_element_type=jnp.float32)
    bc_part = jnp.dot(gathered, bc_weight, preferred_element_type=jnp.float32)
    conv_in = jnp.concatenate([x_part, bc_part], axis=1).astype(jnp.bfloat16)
    step_raw = jnp.dot(gathered, w_dt, preferred_element_type=jnp.float32)
    edge_rows = passed_along(conv_in[tokens_here - (CONV - 1) :], "seq", 1)
    padded = jnp.concatenate([edge_rows, conv_in], axis=0).astype(jnp.float32)
    seg_padded = jnp.concatenate([edge_segment, segment])
    conv_weight = jnp.concatenate([conv_x_w, conv_bc_w], axis=1)
    conv_bias = jnp.concatenate([conv_x_b, conv_bc_b])
    tap_masks = [
        (seg_padded[offset : offset + tokens_here] == segment).astype(jnp.float32)[:, None]
        for offset in range(CONV)
    ]
    conv_out = jnp.zeros(conv_in.shape, jnp.float32) + conv_bias[None, :]
    for offset in range(CONV):
        conv_out = (
            conv_out
            + conv_weight[offset] * padded[offset : offset + tokens_here] * tap_masks[offset]
        )
    activated = jax.nn.silu(conv_out)
    inner_vals = activated[:, :inner_here].astype(jnp.bfloat16)
    b_vals = activated[:, inner_here : inner_here + STATE].astype(jnp.bfloat16)
    c_vals = activated[:, inner_here + STATE :].astype(jnp.bfloat16)
    step_pre = step_raw + dt_bias
    step_size = jax.nn.softplus(step_pre)
    rates = jnp.exp(a_log)
    log_decay = -rates * step_size
    decay_heads = log_decay.reshape(spans, SPAN, heads_here).transpose(0, 2, 1)
    step_heads = step_size.reshape(spans, SPAN, heads_here).transpose(0, 2, 1)
    cumul = jnp.einsum("ij,chj->chi", lower_tri, decay_heads, precision=highest)
    inner_spans = inner_vals.reshape(spans, SPAN, heads_here, HEAD_DIM).transpose(0, 2, 1, 3)
    c_spans = c_vals.reshape(spans, SPAN, STATE)
    per_span = (
        inner_spans,
        b_vals.reshape(spans, SPAN, STATE),
        c_spans,
        step_heads,
        cumul,
        segment.reshape(spans, SPAN),
        span_prev,
    )

    def forward_span(span_item):
        decay_mat, scores, mixing, tail_weight, head_weight, carry_decay = span_terms(
            span_item, lower_tri
        )
        inner_c = span_item[0]
        y_inside = jnp.einsum(
            "hij,hjp->hip", mixing.astype(jnp.bfloat16), inner_c, preferred_element_type=jnp.float32
        )
        loaded = (
            span_item[1].astype(jnp.float32)[None, :, :] * (tail_weight * span_item[3])[:, :, None]
        ).astype(jnp.bfloat16)
        local_state = jnp.einsum(
            "hjn,hjp->hnp", loaded, inner_c, preferred_element_type=jnp.float32
        )
        return (y_inside, local_state, carry_decay, head_weight)

    y_inside, local_states, carry_decay, head_weight = lax.map(forward_span, per_span)

    def advance(state_carry, span_item):
        running, factor = state_carry
        local_c, decay_c = span_item
        return ((decay_c[:, None, None] * running + local_c, decay_c * factor), (running, factor))

    zero_state = jnp.zeros((heads_here, STATE, HEAD_DIM), jnp.float32)
    unit_decay = jnp.ones((heads_here,), jnp.float32)
    (device_state, device_decay), (local_in, local_factor) = lax.scan(
        advance, (zero_state, unit_decay), (local_states, carry_decay)
    )
    incoming = state_prefix(device_decay, device_state, False)
    state_in = local_in + local_factor[:, :, None, None] * incoming
    state_low = state_in.astype(jnp.bfloat16)
    c_weighted = (c_spans.astype(jnp.float32)[:, None, :, :] * head_weight[:, :, :, None]).astype(
        jnp.bfloat16
    )
    y_outside = jnp.einsum(
        "chin,chnp->chip", c_weighted, state_low, preferred_element_type=jnp.float32
    )
    skip_rep = jnp.repeat(d_skip, HEAD_DIM)
    mixed_out = (y_inside + y_outside).transpose(0, 2, 1, 3).reshape(
        tokens_here, inner_here
    ) + inner_vals.astype(jnp.float32) * skip_rep
    gate_act = jax.nn.silu(gate_pre)
    gated = mixed_out * gate_act
    gate_squares = lax.psum(jnp.sum(gated * gated, axis=1), "head")
    scale_gate = lax.rsqrt(gate_squares / INNER + epsilon)
    gate_normed = (gated * scale_gate[:, None] * gate_gain).astype(jnp.bfloat16)
    partial_value = jnp.dot(gate_normed, w_out, preferred_element_type=jnp.float32)
    mixed_sum = lax.psum_scatter(partial_value, "head", scatter_dimension=1, tiled=True)
    layer_out = (inputs + mixed_sum).astype(jnp.bfloat16)
    grad_full = lax.all_gather(cotangent, "head", axis=1, tiled=True)
    grad_gate_normed = lax.dot_general(
        grad_full, w_out, (((1,), (1,)), ((), ())), preferred_element_type=jnp.float32
    )
    grad_w_out = lax.dot_general(
        gate_normed, grad_full, (((0,), (0,)), ((), ())), preferred_element_type=jnp.float32
    )
    grad_gate_gain = jnp.sum(grad_gate_normed * gated * scale_gate[:, None], axis=0)
    grad_scaled = grad_gate_normed * gate_gain
    gate_inner = lax.psum(jnp.sum(grad_scaled * gated, axis=1), "head")
    grad_gated = (
        scale_gate[:, None] * grad_scaled - gated * (scale_gate**3 * gate_inner / INNER)[:, None]
    )
    grad_mixed = (grad_gated * gate_act).astype(jnp.bfloat16)
    grad_gate_pre = (grad_gated * mixed_out * silu_slope(gate_pre)).astype(jnp.bfloat16)
    grad_d_skip = jnp.sum(
        (grad_mixed.astype(jnp.float32) * inner_vals.astype(jnp.float32)).reshape(
            tokens_here, heads_here, HEAD_DIM
        ),
        axis=(0, 2),
    )
    grad_spans = grad_mixed.reshape(spans, SPAN, heads_here, HEAD_DIM).transpose(0, 2, 1, 3)
    from_inter = jnp.einsum(
        "chin,chip->chnp", c_weighted, grad_spans, preferred_element_type=jnp.float32
    )

    def retreat(state_carry, span_item):
        running, factor = state_carry
        local_c, decay_c = span_item
        current = local_c + decay_c[:, None, None] * running
        product = decay_c * factor
        return ((current, product), (current, product))

    (device_grad, device_reach), (local_grad, local_reach) = lax.scan(
        retreat, (zero_state, unit_decay), (from_inter, carry_decay), reverse=True
    )
    beyond = state_prefix(device_reach, device_grad, True)
    grad_state_in = local_grad + local_reach[:, :, None, None] * beyond
    grad_local_states = jnp.concatenate([grad_state_in[1:], beyond[None]], axis=0)
    grad_carry_decay = jnp.sum(grad_local_states * state_in, axis=(2, 3))

    def backward_span(span_item):
        span_base = span_item[:7]
        inner_c, b_rows, c_rows, step_c = (span_base[0], span_base[1], span_base[2], span_base[3])
        grad_y, grad_state, state_c, grad_decay = (
            span_item[7],
            span_item[8],
            span_item[9],
            span_item[10],
        )
        decay_mat, scores, mixing, tail_weight, head_weight, carry_decay = span_terms(
            span_base, lower_tri
        )
        grad_mixing = jnp.einsum(
            "hip,hjp->hij", grad_y, inner_c, preferred_element_type=jnp.float32
        )
        grad_inner = jnp.einsum(
            "hij,hip->hjp", mixing.astype(jnp.bfloat16), grad_y, preferred_element_type=jnp.float32
        )
        related = grad_mixing * mixing
        grad_cum = jnp.sum(related, axis=2) - jnp.sum(related, axis=1)
        grad_scores = jnp.sum(grad_mixing * decay_mat * step_c[:, None, :], axis=0)
        grad_step = jnp.sum(grad_mixing * decay_mat * scores[None, :, :], axis=1)
        b_float = b_rows.astype(jnp.float32)
        c_float = c_rows.astype(jnp.float32)
        grad_c = jnp.dot(grad_scores, b_float, precision=highest)
        grad_b = lax.dot_general(grad_scores, c_float, (((0,), (0,)), ((), ())), precision=highest)
        loading = tail_weight * step_c
        loaded = (b_float[None, :, :] * loading[:, :, None]).astype(jnp.bfloat16)
        grad_loaded = jnp.einsum(
            "hjp,hnp->hjn", inner_c, grad_state, preferred_element_type=jnp.float32
        )
        grad_inner = grad_inner + jnp.einsum(
            "hjn,hnp->hjp", loaded, grad_state, preferred_element_type=jnp.float32
        )
        grad_loading = jnp.sum(grad_loaded * b_float[None, :, :], axis=2)
        grad_b = grad_b + jnp.einsum("hjn,hj->jn", grad_loaded, loading, precision=highest)
        tail_term = grad_loading * loading
        grad_cum = grad_cum - tail_term
        grad_last = jnp.sum(tail_term, axis=1) + grad_decay * carry_decay
        grad_step = grad_step + grad_loading * tail_weight
        grad_weighted = jnp.einsum(
            "hip,hnp->hin", grad_y, state_c, preferred_element_type=jnp.float32
        )
        grad_head = jnp.sum(grad_weighted * c_float[None, :, :], axis=2)
        grad_c = grad_c + jnp.einsum("hin,hi->in", grad_weighted, head_weight, precision=highest)
        grad_cum = grad_cum + grad_head * head_weight
        grad_cum = grad_cum.at[:, SPAN - 1].add(grad_last)
        grad_log = jnp.einsum("ij,hi->hj", lower_tri, grad_cum, precision=highest)
        return (grad_inner, grad_b, grad_c, grad_step, grad_log)

    back_items = per_span + (
        grad_spans,
        grad_local_states.astype(jnp.bfloat16),
        state_low,
        grad_carry_decay,
    )
    grad_inner_s, grad_b_s, grad_c_s, grad_step_s, grad_log_s = lax.map(backward_span, back_items)
    grad_inner = (
        grad_inner_s.transpose(0, 2, 1, 3).reshape(tokens_here, inner_here)
        + grad_mixed.astype(jnp.float32) * skip_rep
    )
    grad_log_decay = grad_log_s.transpose(0, 2, 1).reshape(tokens_here, heads_here)
    grad_step_total = (
        grad_step_s.transpose(0, 2, 1).reshape(tokens_here, heads_here) - grad_log_decay * rates
    )
    grad_a_log = jnp.sum(grad_log_decay * log_decay, axis=0)
    grad_step_pre = grad_step_total * jax.nn.sigmoid(step_pre)
    grad_dt_bias = jnp.sum(grad_step_pre, axis=0)
    grad_step_raw = grad_step_pre.astype(jnp.bfloat16)
    grad_bc = lax.psum(
        jnp.concatenate(
            [grad_b_s.reshape(tokens_here, STATE), grad_c_s.reshape(tokens_here, STATE)], axis=1
        ),
        "head",
    )
    grad_conv = jnp.concatenate([grad_inner, grad_bc], axis=1) * silu_slope(conv_out)
    grad_conv_bias = jnp.sum(grad_conv, axis=0)
    grad_conv_weight = jnp.stack(
        [
            jnp.sum(grad_conv * padded[offset : offset + tokens_here] * tap_masks[offset], axis=0)
            for offset in range(CONV)
        ]
    )
    grad_padded = jnp.zeros(padded.shape, jnp.float32)
    for offset in range(CONV):
        grad_padded = grad_padded + jnp.pad(
            conv_weight[offset] * grad_conv * tap_masks[offset],
            ((offset, CONV - 1 - offset), (0, 0)),
        )
    returned = passed_along(grad_padded[: CONV - 1], "seq", -1)
    grad_conv_in = (
        grad_padded[CONV - 1 :] + jnp.pad(returned, ((tokens_here - (CONV - 1), 0), (0, 0)))
    ).astype(jnp.bfloat16)
    grad_x_pre = grad_conv_in[:, :inner_here]
    grad_bc_pre = grad_conv_in[:, inner_here:]
    contract_rows = (((0,), (0,)), ((), ()))
    contract_cols = (((1,), (1,)), ((), ()))
    grad_w_z = lax.dot_general(
        gathered, grad_gate_pre, contract_rows, preferred_element_type=jnp.float32
    )
    grad_w_x = lax.dot_general(
        gathered, grad_x_pre, contract_rows, preferred_element_type=jnp.float32
    )
    grad_w_dt = lax.dot_general(
        gathered, grad_step_raw, contract_rows, preferred_element_type=jnp.float32
    )
    grad_w_bc = lax.dot_general(
        normed, grad_bc_pre, contract_rows, preferred_element_type=jnp.float32
    )
    partial_back = lax.dot_general(
        grad_gate_pre, w_z, contract_cols, preferred_element_type=jnp.float32
    )
    partial_back = partial_back + lax.dot_general(
        grad_x_pre, w_x, contract_cols, preferred_element_type=jnp.float32
    )
    partial_back = partial_back + lax.dot_general(
        grad_step_raw, w_dt, contract_cols, preferred_element_type=jnp.float32
    )
    grad_normed = lax.psum_scatter(partial_back, "head", scatter_dimension=1, tiled=True)
    grad_normed = grad_normed + lax.dot_general(
        grad_bc_pre, w_bc, contract_cols, preferred_element_type=jnp.float32
    )
    grad_scaled_in = grad_normed * norm_gain
    grad_norm_gain = jnp.sum(grad_normed * inputs * scale_in[:, None], axis=0)
    norm_inner = lax.psum(jnp.sum(grad_scaled_in * inputs, axis=1), "head")
    grad_in = (
        cotangent.astype(jnp.float32)
        + scale_in[:, None] * grad_scaled_in
        - inputs * (scale_in**3 * norm_inner / D)[:, None]
    )
    summed = lax.psum(
        (
            grad_norm_gain,
            grad_w_z,
            grad_w_x,
            grad_w_bc,
            grad_w_dt,
            grad_conv_weight[:, :inner_here],
            grad_conv_bias[:inner_here],
            grad_conv_weight[:, inner_here:],
            grad_conv_bias[inner_here:],
            grad_dt_bias,
            grad_a_log,
            grad_d_skip,
            grad_gate_gain,
            grad_w_out,
        ),
        "seq",
    )
    return (
        layer_out,
        grad_in,
        summed[0],
        summed[1],
        summed[2],
        summed[3],
        summed[4],
        summed[5],
        summed[6],
        summed[7],
        summed[8],
        summed[9],
        summed[10],
        summed[11],
        summed[12],
        summed[13],
    )


BF = jnp.bfloat16
F32 = jnp.float32
MESH = pl.DeviceIdType.MESH
ROWS = 512
BLOCK = 384
CHANNELS = 768
WIDE = 1024
HALO = 16
SEQ = 8
LINE = 4
ALONG = "seq"
ACROSS = "head"
NN = (((1,), (0,)), ((), ()))
NT = (((1,), (1,)), ((), ()))
TN = (((0,), (0,)), ((), ()))


def mul(a, b, dims=NN):
    return lax.dot_general(a, b, dims, preferred_element_type=F32)


def cut(start, size, mult):
    return pl.ds(pl.multiple_of(start, mult), size)


def parts(v, n):
    out = []
    for _ in range(n):
        p = v.astype(BF)
        out.append(p)
        v = v - p.astype(F32)
    return out


def along_line(z, ends, middles):
    k = jnp.where(lax.rem(z, 3) == 0, ends, middles)
    return jnp.where(z >= 2, 3 - k, k)


def lanes_sum(v):
    total = v[:, 0:128]
    for i in range(1, v.shape[1] // 128):
        total = total + v[:, 128 * i : 128 * i + 128]
    return total


def rows_sum(v):
    return jnp.sum(v.reshape(v.shape[0] // 8, 8, v.shape[1]), axis=0)


def wide_of(v, n):
    return jnp.concatenate([v] * n, axis=1)


def to_row(part):
    return jnp.sum(part.T, axis=0, keepdims=True)


def to_col(row):
    return jnp.broadcast_to(row, (128, row.shape[1])).T


def loop(n, body):
    def run(i, carry):
        body(i)
        return carry

    lax.fori_loop(0, n, run, 0)


def remote(src, dst, send, recv, peer):
    return pltpu.make_async_remote_copy(
        src_ref=src, dst_ref=dst, send_sem=send, recv_sem=recv, device_id=peer, device_id_type=MESH
    )


class Total:
    def __init__(self, whole, bufs, send, recv, freed, base, me):
        self.w = whole
        self.freed, self.slot = freed, 3 * (base // 10)
        self.r0, self.ra, self.rb, self.qa, self.qb = bufs
        self.send, self.recv, self.base = send, recv, base
        self.c, self.x, self.y, self.s = me
        self.rows, self.cols = whole.shape
        self.live, self.left = {}, set()

    def peer(self, bit):
        return {ALONG: self.s + bit - 2 * bit * {1: self.c, 2: self.x, 4: self.y}[bit]}

    def free(self, k, n, bit):
        self.sent(k)
        pl.semaphore_signal(
            self.freed.at[self.slot + n], inc=1, device_id=self.peer(bit), device_id_type=MESH
        )

    def copy(self, k, src, dst, bit):
        d = remote(src, dst, self.send.at[self.base + k], self.recv.at[self.base + k], self.peer(bit))
        d.start()
        self.live[k] = d
        self.left.add(k)

    def wait(self, k):
        self.live[k].wait_recv()

    def sent(self, k):
        self.left.remove(k)
        self.live[k].wait_send()

    def add(self, start, got, rows, col, cols, step):
        def body(i):
            at = (cut(start + i * step, step, 16), pl.ds(col, cols))
            new = self.w[at].astype(F32) + got[cut(i * step, step, 16), :].astype(F32)
            self.w[at] = new.astype(self.w.dtype)

        loop(rows // step, body)

    def s0(self):
        h = self.rows // 2
        self.copy(0, self.w.at[cut((1 - self.c) * h, h, 16)], self.r0, 1)

    def s1(self):
        h, q, m = self.rows // 2, self.rows // 4, self.cols // 2
        base = self.c * h
        self.free(0, 0, 1)
        self.wait(0)
        self.add(base, self.r0, h, 0, self.cols, 32)
        self.copy(1, self.w.at[cut(base + (1 - self.x) * q, q, 16), pl.ds(0, m)], self.ra, 2)
        self.copy(2, self.w.at[cut(base + (1 - self.y) * q, q, 16), pl.ds(m, m)], self.rb, 4)

    def s2(self):
        h, q, e, m = self.rows // 2, self.rows // 4, self.rows // 8, self.cols // 2
        ba = self.c * h + self.x * q
        bb = self.c * h + self.y * q
        self.wait(1)
        self.add(ba, self.ra, q, 0, m, 32)
        self.sent(2)
        self.copy(3, self.w.at[cut(ba + (1 - self.y) * e, e, 16), pl.ds(0, m)], self.qa, 4)
        self.wait(2)
        self.add(bb, self.rb, q, m, m, 32)
        self.sent(1)
        self.copy(4, self.w.at[cut(bb + (1 - self.x) * e, e, 16), pl.ds(m, m)], self.qb, 2)

    def s3(self):
        h, q, e, m = self.rows // 2, self.rows // 4, self.rows // 8, self.cols // 2
        ba = self.c * h + self.x * q + self.y * e
        bb = self.c * h + self.y * q + self.x * e
        self.free(3, 1, 4)
        self.free(4, 2, 2)
        self.wait(3)
        self.add(ba, self.qa, e, 0, m, 16)
        pl.semaphore_wait(self.freed.at[self.slot + 1], 1)
        p = self.w.at[cut(ba, e, 16), pl.ds(0, m)]
        self.copy(5, p, p, 4)
        self.wait(4)
        self.add(bb, self.qb, e, m, m, 16)
        pl.semaphore_wait(self.freed.at[self.slot + 2], 1)
        p = self.w.at[cut(bb, e, 16), pl.ds(m, m)]
        self.copy(6, p, p, 2)

    def s4(self):
        h, q, m = self.rows // 2, self.rows // 4, self.cols // 2
        self.wait(5)
        p = self.w.at[cut(self.c * h + self.x * q, q, 16), pl.ds(0, m)]
        self.copy(7, p, p, 2)
        self.wait(6)
        p = self.w.at[cut(self.c * h + self.y * q, q, 16), pl.ds(m, m)]
        self.copy(8, p, p, 4)

    def s5(self):
        h = self.rows // 2
        self.wait(7)
        self.wait(8)
        pl.semaphore_wait(self.freed.at[self.slot], 1)
        p = self.w.at[cut(self.c * h, h, 16)]
        self.copy(9, p, p, 1)

    def s6(self):
        self.wait(9)
        for k in sorted(self.left):
            self.sent(k)


def total_bufs(rows, cols, kind):
    sizes = [(2, 1), (4, 2), (4, 2), (8, 2), (8, 2)]
    return [pltpu.VMEM((rows // a, cols // b), kind) for a, b in sizes]


class Refs:
    def __init__(self, named):
        self.__dict__.update(named)


def layer_kernel(named, sum_bufs):
    g = Refs(named)
    g.ggn = g.acc.at[:, pl.ds(0, CHANNELS)]
    g.z = g.ggn
    g.gn = g.xg.at[:, pl.ds(0, CHANNELS)]
    g.gz = g.xg.at[:, pl.ds(CHANNELS, CHANNELS)]
    g.gconv = g.slope
    g.gx = g.gm
    g.sblk2 = g.sblk
    g.own = g.gated.at[:, pl.ds(0, BLOCK)]
    g.gb = g.gated.at[:, pl.ds(BLOCK, 128)]
    g.gc = g.gated.at[:, pl.ds(BLOCK + 128, 128)]
    s = lax.axis_index(ALONG)
    z = lax.axis_index(ACROSS)
    me = (lax.rem(s, 2), lax.rem(s // 2, 2), s // 4, s)
    zpeers = [{ACROSS: lax.rem(z + d, LINE)} for d in range(1, LINE)]
    speers = [{ALONG: lax.rem(s + d, SEQ)} for d in range(1, SEQ)]

    loads = []
    for i, (src, dst) in enumerate(
        [(g.x_hbm, g.x), (g.w_x, g.wx), (g.w_z, g.wz), (g.cot_hbm, g.cotg.at[:, cut(z * BLOCK, BLOCK, 128)]), (g.w_out, g.wo)]
    ):
        d = pltpu.make_async_copy(src, dst, g.load_sem.at[i])
        d.start()
        loads.append(d)

    g.params[...] = jnp.zeros(g.params.shape, F32)
    vectors = (g.norm_gain, g.conv_x_b, g.conv_bc_b, g.dt_bias, g.a_log, g.d_skip, g.gate_gain)
    for i, v in enumerate(vectors):
        for n in range(v.shape[0]):
            g.params[i : i + 1, 128 * n : 128 * n + v.shape[1]] = v[n : n + 1, :]

    sem = pltpu.get_barrier_semaphore()
    for p in zpeers + speers:
        pl.semaphore_signal(sem, inc=1, device_id=p, device_id_type=MESH)
    pl.semaphore_wait(sem, len(zpeers) + len(speers))

    pending = []

    def send(src, dst, sems, i, peer):
        d = remote(src, dst, sems[0].at[i], sems[1].at[i], peer)
        d.start()
        pending.append(d)
        return d

    loads[0].wait()
    loads[3].wait()
    gain = g.params[0:1, 0:BLOCK]
    xv = g.x[...].astype(F32)
    g.ssq[z] = jnp.broadcast_to(to_row(lanes_sum(xv * xv)), (8, ROWS))
    g.gains[z] = jnp.broadcast_to(gain, (8, BLOCK))
    piece = cut(48 * s, 48, 16)
    own = cut(z * BLOCK, BLOCK, 128)
    g.wbc[z, piece, :] = g.w_bc[piece, :]
    small = []
    for i, p in enumerate(zpeers):
        small.append(send(g.ssq.at[z], g.ssq.at[z], g.small, i, p))
        small.append(send(g.gains.at[z], g.gains.at[z], g.small, 3 + i, p))
        small.append(send(g.w_bc.at[piece], g.wbc.at[z, piece], g.small, 6 + i, p))
    middle = lax.rem(z, 3) != 0
    near = [along_line(z, a, b) for a, b in ((1, 2), (2, 0), (3, 3))]

    def block_copy(src, whole, base, slot, k, to):
        cols = cut(k * BLOCK, BLOCK, 128)
        return remote(src, whole.at[:, cols], g.gather_s.at[base + slot], g.gather_r.at[base + k], {ACROSS: to})

    def gather(src, whole, base):
        for j in range(2):
            pending.append(block_copy(src, whole, base, j, z, near[j]))
            pending[-1].start()
        third = block_copy(src, whole, base, 2, z, near[2])

        @pl.when(jnp.logical_not(middle))
        def _():
            third.start()

        return third

    def gathered(src, whole, base, j):
        block_copy(src, whole, base, 0, near[j], z).wait_recv()

    def relay(whole, base):
        part = whole.at[:, cut(near[0] * BLOCK, BLOCK, 128)]

        @pl.when(middle)
        def _():
            block_copy(part, whole, base, 2, near[0], near[1]).start()

    x_third = gather(g.x, g.xg, 0)

    g.wd[...] = jnp.zeros(g.wd.shape, BF)
    g.wd[0:12, :] = g.w_dt[...]
    g.taps[...] = jnp.zeros(g.taps.shape, F32)
    g.taps[0:4, 0:CHANNELS] = g.conv_x_w[...]
    g.taps[0:4, CHANNELS:WIDE] = g.conv_bc_w[...]
    g.taps[4:5, 0:CHANNELS] = g.params[1:2, :]
    g.taps[4:5, CHANNELS:WIDE] = g.params[2:3, 0:256]
    expand_row = lax.broadcasted_iota(jnp.int32, (256, CHANNELS), 0)
    expand_col = lax.broadcasted_iota(jnp.int32, (256, CHANNELS), 1)
    g.spread[...] = jnp.where((expand_col >> 6) == (expand_row & 127), 1.0, 0.0).astype(BF)
    starts = [jnp.int32(0)]
    for k in range(7):
        starts.append(starts[-1] + g.lengths[k])

    def segment(pos):
        total = jnp.full(pos.shape, -1, jnp.int32)
        for k in range(8):
            total = total + jnp.where(pos >= starts[k], 1, 0)
        return total.astype(F32)

    g.segc[...] = segment(
        lax.broadcasted_iota(jnp.int32, (ROWS + HALO, 128), 0) + (s * ROWS - HALO)
    )
    g.segr[...] = segment(lax.broadcasted_iota(jnp.int32, (8, ROWS), 1) + s * ROWS)
    tri_i = lax.broadcasted_iota(jnp.int32, (SPAN, SPAN), 0)
    tri_j = lax.broadcasted_iota(jnp.int32, (SPAN, SPAN), 1)
    g.tri[...] = jnp.where(tri_i >= tri_j, 1.0, 0.0).astype(BF)
    lane = lax.broadcasted_iota(jnp.int32, (1, 128), 1)
    left = lane < 64

    def spread(v):
        hi, lo = parts(v, 2)
        return mul(jnp.concatenate([hi, lo], axis=1), g.spread[...])

    def head_sum(v):
        hi, lo = parts(v, 2)
        e = g.spread[0:128, :]
        return mul(hi, e, NT) + mul(lo, e, NT)

    g.skipe[...] = spread(jnp.broadcast_to(g.params[5:6, 0:128], (8, 128)))
    rates = jnp.exp(g.params[4:5, 0:128])

    for d in small:
        d.wait_recv()
    wide = [
        send(g.wbc.at[:, piece], g.wbc.at[:, piece], g.wide, i, p) for i, p in enumerate(speers)
    ]
    total = g.ssq[0] + g.ssq[1] + g.ssq[2] + g.ssq[3]
    g.xscale[...] = to_col(lax.rsqrt(total[0:1] / D + epsilon))

    def normalise(k, src):
        gk = g.gains[k][0:1]
        cols = cut(k * BLOCK, BLOCK, 128)

        def body(i):
            at = cut(i * 64, 64, 16)
            v = src(at, cols).astype(F32)
            g.xn[at, cols] = (v * wide_of(g.xscale[at, :], 3) * gk).astype(BF)

        loop(ROWS // 64, body)

    def project(k, w, cols, base, first, width=256):
        at = cut(k * BLOCK, BLOCK, 128)

        def body(n):
            p = mul(g.xn[:, at], w[cut(k * BLOCK, BLOCK, 16), cut(n * width, width, 128)])
            dst = cut(base + n * width, width, 128)
            if first:
                g.acc[:, dst] = p
            else:
                g.acc[:, dst] += p

        loop(cols // width, body)

    def project_dt(k, first):
        at = cut(k * BLOCK, BLOCK, 128)
        p = mul(g.xn[:, at], g.wd[:, at], NT)
        if first:
            g.acc[:, WIDE + CHANNELS :] = p
        else:
            g.acc[:, WIDE + CHANNELS :] += p

    normalise(z, lambda at, cols: g.x[at, :])
    loads[1].wait()
    loads[2].wait()
    project(z, g.wx, CHANNELS, 0, True)
    project(z, g.wz, CHANNELS, WIDE, True)
    project_dt(z, True)
    for i, k in enumerate(near):
        gathered(g.x, g.xg, 0, i)
        if i == 0:
            relay(g.xg, 0)
        if i == 2:
            pending.append(gather(g.cotg.at[:, own], g.cotg, 4))
        normalise(k, lambda at, cols: g.xg[at, cols])
        project(k, g.wx, CHANNELS, 0, False)
        if i < 2:
            project(k, g.wz, CHANNELS, WIDE, False)
            project_dt(k, False)
    for d in wide:
        d.wait_recv()
    g.acc[:, CHANNELS:WIDE] = sum(
        mul(g.xn[:, BLOCK * k : BLOCK * k + BLOCK], g.wbc[k]) for k in range(LINE)
    )

    g.edge[...] = g.acc[ROWS - HALO : ROWS, 0:WIDE].astype(BF)
    edge = remote(g.edge, g.halo, g.edge_sem.at[0], g.edge_sem.at[1], {ALONG: s + 1})

    @pl.when(s < SEQ - 1)
    def _():
        edge.start()

    @pl.when(s == 0)
    def _():
        g.halo[...] = jnp.zeros(g.halo.shape, BF)

    def put(i):
        g.cf[cut(HALO + i * 64, 64, 8), :] = (
            g.acc[cut(i * 64, 64, 8), 0:WIDE].astype(BF).astype(F32)
        )

    loop(ROWS // 64, put)
    project(near[2], g.wz, CHANNELS, WIDE, False)
    project_dt(near[2], False)

    step_pre = g.acc[:, WIDE + CHANNELS :] + g.params[3:4, 0:128]
    g.step[...] = jnp.where(lane < 12, jax.nn.softplus(step_pre), 0.0)
    for q in range(2):
        rows = pl.ds(q * SPAN, SPAN)
        log_decay = -rates * g.step[rows, :]
        cum = sum(mul(g.tri[...], p) for p in parts(log_decay, 3))
        g.cum[rows, :] = cum
        g.cumt[q] = cum.T[0:16, :]
        last = cum[SPAN - 1 : SPAN, :]
        seg = g.segc[pl.ds(HALO + q * SPAN, SPAN), :]
        seg_last = g.segc[HALO + q * SPAN + SPAN - 1 : HALO + q * SPAN + SPAN, :]
        seg_prev = g.segc[HALO + q * SPAN - 1 : HALO + q * SPAN, :]
        tail = jnp.where(seg == seg_last, jnp.exp(last - cum), 0.0)
        load = tail * g.step[rows, :]
        lead = jnp.where(seg == seg_prev, jnp.exp(cum), 0.0)
        g.tail[rows, :] = tail
        g.load[rows, :] = load
        g.lead[rows, :] = lead
        g.loadt[q] = load.T[0:16, :]
        g.leadt[q] = lead.T[0:16, :]
        g.stept[q] = g.step[rows, :].T[0:16, :]
        carry = jnp.where(seg_last == seg_prev, jnp.exp(last), 0.0)
        g.carry[q] = jnp.broadcast_to(carry, (8, 128))
        g.carrye[q] = spread(jnp.broadcast_to(carry, (8, 128)))
    g.decay[0] = g.carrye[0] * g.carrye[1]

    def taps_of(first, cols):
        v = g.cf[cut(first + 8, 72, 8), cols]
        sv = g.segc[cut(first + 8, 72, 8), :]
        width = v.shape[1] // 128
        out = []
        for k in range(3):
            same = pltpu.roll(sv, 67 - k, 0)[0:64] == sv[8:72]
            out.append(jnp.where(wide_of(same, width), pltpu.roll(v, 67 - k, 0)[0:64], 0.0))
        out.append(v[8:72])
        return out

    def convolve(i):
        first = i * 64
        at = cut(first, 64, 16)
        for n in range(4):
            cols = pl.ds(n * 256, 256)
            v = jnp.broadcast_to(g.taps[4:5, cols], (64, 256))
            for k, t in enumerate(taps_of(first, cols)):
                v = v + g.taps[k : k + 1, cols] * t
            sig = jax.nn.sigmoid(v)
            act = (v * sig).astype(BF)
            g.slope[at, cols] = sig * (1.0 + v * (1.0 - sig))
            if n < 3:
                g.inner[at, cols] = act
            else:
                g.b[at, :] = act[:, 0:128]
                g.c[at, :] = act[:, 128:256]

    loop(ROWS // 64 - 1, lambda i: convolve(i + 1))

    @pl.when(s > 0)
    def _():
        edge.wait_recv()

    g.cf[0:HALO, :] = g.halo[...].astype(F32)
    convolve(0)

    g.bt[...] = g.b[...].astype(F32).T
    g.ct[...] = g.c[...].astype(F32).T

    def outer(maps, weights, vals):
        def body(t):
            q, p = t // 6, lax.rem(t, 6)
            at = cut(p * 128, 128, 128)
            v = vals[cut(q * SPAN, SPAN, 256), at]
            m = maps[:, cut(q * SPAN, SPAN, 256)]
            o = [mul((m * weights[q, pl.ds(2 * p + e, 1), :]).astype(BF), v) for e in range(2)]
            g.local[q, :, at] = jnp.where(left, o[0], o[1])

        loop(12, body)

    outer(g.bt, g.loadt, g.inner)
    c0, c1 = g.carrye[0][0:1], g.carrye[1][0:1]
    core, chip = me[0], s // 2
    half, rest = cut(core * BLOCK, BLOCK, 128), cut((1 - core) * BLOCK, BLOCK, 128)
    partner = {ALONG: s + 1 - 2 * core}
    later = []

    class Chain:
        def __init__(self, mine, other, joined, got, result, base, way):
            self.mine, self.other, self.joined, self.got, self.result = mine, other, joined, got, result
            self.base, self.way = base, way
            self.near = self.link(joined, got.at[0], 1, way)
            self.far = self.link(joined, got.at[1], 2, 2 * way)

        def link(self, src, dst, i, hop):
            to = {ALONG: s + 2 * hop}
            return remote(src, dst, g.st_send.at[self.base + i], g.st_recv.at[self.base + i], to)

        def share(self):
            self.first = send(self.mine, self.other, (g.st_send, g.st_recv), self.base, partner)

        def join(self):
            self.first.wait_recv()
            own, other = self.mine[:, half], self.other[:, half]
            even, odd = jnp.where(core == 0, own, other), jnp.where(core == 0, other, own)
            if self.way > 0:
                self.joined[...] = odd_decay() * even + odd
            else:
                self.joined[...] = even + even_decay() * odd
            for d, hop in ((self.near, 1), (self.far, 2)):
                pass_on(d, hop * self.way)
            for i, hop in ((0, 1), (1, 2)):
                outside = chip - hop * self.way

                @pl.when((outside < 0) | (outside > 3))
                def _():
                    self.got[i] = jnp.zeros((STATE, BLOCK), F32)

        def meet(self, decay):
            for d, hop in ((self.near, 1), (self.far, 2)):
                arrive(d, hop * self.way)
            self.result[:, half] = self.got[0] + decay * self.got[1]
            p = self.result.at[:, half]
            self.last = send(p, p, (g.st_send, g.st_recv), self.base + 3, partner)

        def end(self):
            self.last.wait_recv()

    def pass_on(d, hop):
        inside = (chip + hop >= 0) & (chip + hop <= 3)

        @pl.when(inside)
        def _():
            d.start()

        later.append((inside, d))

    def arrive(d, hop):
        @pl.when((chip - hop >= 0) & (chip - hop <= 3))
        def _():
            d.wait_recv()

    def odd_decay():
        return jnp.where(core == 0, g.decay[1, 0:1, half], g.decay[0, 0:1, half])

    def even_decay():
        return jnp.where(core == 0, g.decay[0, 0:1, half], g.decay[1, 0:1, half])

    g.mine[...] = c1 * g.local[0] + g.local[1]
    ahead = Chain(g.mine, g.other, g.joined, g.got, g.chain, 0, 1)
    ahead.share()
    dec = send(g.decay.at[0], g.decay.at[1], (g.st_send, g.st_recv), 8, partner)
    both_up = remote(g.both, g.boths.at[0], g.st_send.at[9], g.st_recv.at[9], {ALONG: s + 2})
    both_down = remote(g.both, g.boths.at[1], g.st_send.at[10], g.st_recv.at[10], {ALONG: s - 2})

    def head_cols(ref, rows, p):
        moved = pltpu.roll(ref[rows, :], lax.rem(128 - 2 * p, 128), 1)
        return moved[:, 0:1], moved[:, 1:2]

    def inside(q, first, count):
        rows = cut(q * SPAN, SPAN, 256)
        seg = g.segc[cut(HALO + q * SPAN, SPAN, 16), 0:1]
        segr = g.segr[0:1, cut(q * SPAN, SPAN, 256)]
        scores = mul(g.c[rows, :], g.b[rows, :], NT)
        g.scores[...] = jnp.where((tri_i >= tri_j) & (seg == segr), scores, 0.0)

        def pair(t):
            p = first + t
            cols = head_cols(g.cum, rows, p)
            at = cut(p * 128, 128, 128)
            outs = []
            for e in range(2):
                row = g.cumt[q, pl.ds(2 * p + e, 1), :]
                step = g.stept[q, pl.ds(2 * p + e, 1), :]
                fall = jnp.exp(jnp.minimum(cols[e] - row, 0.0))
                outs.append(mul((g.scores[...] * fall * step).astype(BF), g.inner[rows, at]))
            g.out[rows, at] = jnp.where(left, outs[0], outs[1])

        loop(count, pair)

    inside(0, 0, 3)
    dec.wait_recv()
    g.both[...] = g.decay[0, :, half] * g.decay[1, :, half]
    ahead.join()
    pass_on(both_up, 1)
    pass_on(both_down, -1)
    for i, hop in ((0, 1), (1, -1)):
        @pl.when((chip - hop < 0) | (chip - hop > 3))
        def _():
            g.boths[i] = jnp.zeros((8, BLOCK), F32)

    inside(0, 3, 3)
    gathered(g.cotg.at[:, own], g.cotg, 4, 0)
    relay(g.cotg, 4)
    inside(1, 0, 6)

    arrive(both_up, 1)
    ahead.meet(g.boths[0, 0:1, :])

    def act(i):
        at = cut(i * 64, 64, 16)
        pre = g.acc[at, gate_cols]
        g.gated[at, :] = pre * jax.nn.sigmoid(pre)

    gate_cols = pl.ds(WIDE, CHANNELS)
    loop(ROWS // 64, act)
    ahead.end()
    from_chips = g.chain[...]
    incoming = jnp.where(core == 0, from_chips, g.other[...] + g.decay[1, 0:1] * from_chips)
    g.sin[0] = incoming
    g.sin[1] = g.local[0] + c0 * incoming
    for q in range(2):
        g.slow[q] = g.sin[q].astype(BF)

    def outside(t):
        q, p = t // 6, lax.rem(t, 6)
        rows, at = cut(q * SPAN, SPAN, 256), cut(p * 128, 128, 128)
        cols = head_cols(g.lead, rows, p)
        cv = g.c[rows, :].astype(F32)
        o = [mul((cv * cols[e]).astype(BF), g.slow[q, :, at]) for e in range(2)]
        g.out[rows, at] += jnp.where(left, o[0], o[1])

    loop(12, outside)

    skip = g.skipe[0:1]

    def gate(i):
        at = cut(i * 64, 64, 16)
        mixed = g.out[at, :] + g.inner[at, :].astype(F32) * skip
        gated = mixed * g.gated[at, :]
        g.gated[at, :] = gated
        g.part[0, at, :] = lanes_sum(gated * gated)

    loop(ROWS // 64, gate)

    loads[4].wait()
    gate_gain = g.params[6:7, :]

    def down(k, first):
        at = cut(k * BLOCK, BLOCK, 128)

        def body(n):
            cols = cut(n * 256, 256, 256)
            p = mul(g.cotg[:, at], g.wo[cols, at], NT)
            if first:
                g.ggn[:, cols] = p
            else:
                g.ggn[:, cols] += p

        loop(3, body)

    down(z, True)
    for i, k in enumerate(near):
        if i > 0:
            gathered(g.cotg.at[:, own], g.cotg, 4, i)
        down(k, False)

    def inner_part(i):
        at = cut(i * 64, 64, 16)
        g.part[1, at, :] = lanes_sum(g.ggn[at, :] * gate_gain * g.gated[at, :])

    loop(ROWS // 64, inner_part)
    which = lax.broadcasted_iota(jnp.int32, (8, ROWS), 0)
    g.stats[z] = jnp.where(which == 0, to_row(g.part[0]), to_row(g.part[1]))
    stat = [send(g.stats.at[z], g.stats.at[z], g.stat, i, p) for i, p in enumerate(zpeers)]
    for d in stat:
        d.wait_recv()
    sums = g.stats[0] + g.stats[1] + g.stats[2] + g.stats[3]
    gscale = lax.rsqrt(sums[0:1] / INNER + epsilon)
    g.part[0] = to_col(gscale)
    g.part[1] = to_col(gscale * gscale * gscale * sums[1:2] / INNER)
    x_third.wait_send()
    g.vacc[...] = jnp.zeros(g.vacc.shape, F32)
    g.pack[...] = jnp.zeros(g.pack.shape, F32)
    g.bcv[z] = jnp.zeros((8, 256), F32)

    def ungate(i):
        at = cut(i * 64, 64, 16)
        a = wide_of(g.part[0, at, :], 6)
        pre = g.acc[at, gate_cols]
        vals = g.inner[at, :].astype(F32)
        mixed = g.out[at, :] + vals * skip
        gated, ggn = g.gated[at, :], g.ggn[at, :]
        g.gn[at, :] = (gated * a * gate_gain).astype(BF)
        gg = a * (ggn * gate_gain) - gated * wide_of(g.part[1, at, :], 6)
        sig = jax.nn.sigmoid(pre)
        gm = (gg * (pre * sig)).astype(BF)
        g.gm[at, :] = gm
        g.gz[at, :] = (gg * mixed * (sig * (1.0 + pre * (1.0 - sig)))).astype(BF)
        g.vacc[0] += rows_sum(ggn * gated * a)
        g.vacc[1] += rows_sum(gm.astype(F32) * vals)

    loop(ROWS // 64, ungate)

    outer(g.ct, g.leadt, g.gm)
    g.mine_b[...] = g.local[0] + c0 * g.local[1]
    behind = Chain(g.mine_b, g.other_b, g.joined_b, g.got_b, g.chain_b, 4, -1)
    behind.share()

    t_out, t_z, t_x, t_rest = [
        Total(ref, sum_bufs[5 * i : 5 * i + 5], g.tot_send, g.tot_recv, g.freed, 10 * i, me)
        for i, ref in enumerate((g.p_out, g.p_z, g.p_x, g.p_rest))
    ]

    def grad_out(n):
        at = cut(n * 256, 256, 256)
        g.p_out[at, :] = mul(g.gn[:, at], g.cotg[...], TN).astype(BF)

    loop(3, grad_out)
    behind.join()
    t_out.s0()

    def grad_z(n):
        at = cut(n * 256, 256, 256)
        g.p_z[at, :] = mul(g.xn[:, at], g.gz[...], TN).astype(BF)

    loop(6, grad_z)
    t_z.s0()
    t_out.s1()

    dests = [along_line(z, a, b) for a, b in ((2, 3), (3, 0), (1, 2))]

    class Scatter:
        def __init__(self, sent, got, via, base):
            self.sent, self.got, self.via, self.base = sent, got, via, base

        def copy(self, j, dst, i, to):
            return remote(self.sent.at[j], dst, g.block_s.at[self.base + j], g.block_r.at[self.base + i], {ACROSS: to})

        def direct(self, j):
            slot = lax.rem(z - dests[j] + 7, 4)
            return self.copy(j, self.got.at[slot], slot, dests[j])

        def block(self, j, value):
            v = value
            if j == 2:
                @pl.when(middle)
                def _():
                    self.copy(0, self.via, 3, z).wait_recv()

                v = v + self.via[...].astype(F32)
            self.sent[j] = v.astype(BF)
            if j == 0:
                @pl.when(middle)
                def _():
                    self.direct(0).start()

                @pl.when(jnp.logical_not(middle))
                def _():
                    self.copy(0, self.via, 3, dests[2]).start()
            else:
                self.direct(j).start()

        def arrived(self):
            for i in (0, 2):
                self.copy(0, self.got.at[i], i, z).wait_recv()

            @pl.when(jnp.logical_not(middle))
            def _():
                self.copy(0, self.got.at[1], 1, z).wait_recv()

        def left(self):
            for j in range(3):
                self.copy(j, self.via, 3, z).wait_send()

    out_blocks = Scatter(g.sblk, g.rblk, g.via, 0)
    in_blocks = Scatter(g.sblk2, g.rblk2, g.via2, 4)

    @pl.when(middle)
    def _():
        g.rblk[1] = jnp.zeros((ROWS, BLOCK), BF)
        g.rblk2[1] = jnp.zeros((ROWS, BLOCK), BF)

    @pl.when(jnp.logical_not(middle))
    def _():
        g.via[...] = jnp.zeros((ROWS, BLOCK), BF)
        g.via2[...] = jnp.zeros((ROWS, BLOCK), BF)

    def out_block(k):
        return mul(g.gn[...], g.wo[:, cut(k * BLOCK, BLOCK, 128)])

    out_blocks.block(0, out_block(dests[0]))
    out_blocks.block(1, out_block(dests[1]))
    t_z.s1()
    g.own[...] = mul(g.gn[...], g.wo[:, own])

    def inside_back(q, first, count):
        rows = cut(q * SPAN, SPAN, 256)
        seg = g.segc[cut(HALO + q * SPAN, SPAN, 16), 0:1]
        segr = g.segr[0:1, cut(q * SPAN, SPAN, 256)]
        mask = (tri_i <= tri_j) & (seg == segr)
        if first == 0:
            g.scores[...] = jnp.where(mask, mul(g.b[rows, :], g.c[rows, :], NT), 0.0)
            g.gscores[...] = jnp.zeros((SPAN, SPAN), F32)

        def pair(t):
            p = first + t
            cols = head_cols(g.cum, rows, p)
            at = cut(p * 128, 128, 128)
            steps = head_cols(g.step, rows, p)
            gm = g.gm[rows, at]
            outs = []
            for e in range(2):
                row = g.cumt[q, pl.ds(2 * p + e, 1), :]
                fall = jnp.exp(jnp.minimum(row - cols[e], 0.0)) * steps[e]
                outs.append(mul((g.scores[...] * fall).astype(BF), gm))
                keep = left if e == 0 else jnp.logical_not(left)
                vals = jnp.where(keep, g.inner[rows, at].astype(F32), 0.0).astype(BF)
                g.gscores[...] += mul(vals, gm, NT) * fall
            g.z[rows, at] = jnp.where(left, outs[0], outs[1])

        loop(count, pair)
        if first + count < 6:
            return
        gs = jnp.where(mask, g.gscores[...], 0.0)
        hi, lo = parts(gs, 2)
        g.gb[rows, :] = mul(hi, g.c[rows, :]) + mul(lo, g.c[rows, :])
        g.gc[rows, :] = mul(hi, g.b[rows, :], TN) + mul(lo, g.b[rows, :], TN)

    inside_back(1, 0, 6)
    arrive(both_down, -1)
    behind.meet(g.boths[1, 0:1, :])
    out_blocks.block(2, out_block(dests[2]))
    inside_back(0, 0, 3)
    t_out.s2()
    inside_back(0, 3, 3)

    behind.end()
    from_chips = g.chain_b[...]
    beyond = jnp.where(core == 1, from_chips, g.other_b[...] + g.decay[1, 0:1] * from_chips)
    g.gloc[1] = beyond
    g.gloc[0] = g.local[1] + c1 * beyond
    ends = []
    for q in range(2):
        rows = pl.ds(q * SPAN, SPAN)
        glow = g.gloc[q].astype(BF)
        vals = g.inner[rows, :].astype(F32)
        gm = g.gm[rows, :].astype(F32)
        loade = spread(g.load[rows, :])
        bg = mul(g.b[rows, :], glow)
        zed = g.z[rows, :]
        carry_sum = jnp.sum(g.gloc[q] * g.sin[q], axis=0, keepdims=True)
        grad_carry = head_sum(jnp.broadcast_to(carry_sum, (8, CHANNELS)))[0:1]
        t1 = head_sum(gm * g.out[rows, :])
        q1 = head_sum(vals * zed)
        q2 = head_sum(vals * bg)
        step, load = g.step[rows, :], g.load[rows, :]
        tail_term = q2 * load
        gcum = t1 - q1 - tail_term
        end = jnp.sum(tail_term, axis=0, keepdims=True) + grad_carry * g.carry[q][0:1]
        is_last = lax.broadcasted_iota(jnp.int32, (SPAN, 128), 0) == SPAN - 1
        gcum = gcum + jnp.where(is_last, end, 0.0)
        glog = sum(mul(g.tri[...], p, TN) for p in parts(gcum, 3))
        gstep = jnp.where(step > 1e-30, q1 / jnp.maximum(step, 1e-30), 0.0) + q2 * g.tail[rows, :]
        gpre = (gstep - rates * glog) * jax.nn.sigmoid(
            g.acc[rows, WIDE + CHANNELS :] + g.params[3:4, 0:128]
        )
        g.gsr[rows, :] = gpre.astype(BF)
        ends.append((rows_sum(gpre), rows_sum(glog * (-rates * step))))
        g.z[rows, :] = zed + loade * bg + skip * gm
        g.gb[rows, :] += sum(mul(p, glow, NT) for p in parts(vals * loade, 2))
        g.gc[rows, :] += sum(mul(p, g.slow[q], NT) for p in parts(gm * spread(g.lead[rows, :]), 2))
        if q == 0:
            t_z.s2()
    g.pack[16:24, 0:128] = jnp.broadcast_to(
        jnp.sum(ends[0][0] + ends[1][0], axis=0, keepdims=True), (8, 128)
    )
    g.pack[16:24, 128:256] = jnp.broadcast_to(
        jnp.sum(ends[0][1] + ends[1][1], axis=0, keepdims=True), (8, 128)
    )
    def grads_of(at, n):
        cols = pl.ds(n * 256, 256)
        if n < 3:
            v = g.z[at, cols]
        else:
            v = jnp.concatenate([g.gb[at, :], g.gc[at, :]], axis=1)
        return v * g.slope[at, cols]

    def slopes(i):
        at = cut(i * 64, 64, 16)
        for n in range(4):
            g.gconv[cut(i * 64, 64, 8), pl.ds(n * 256, 256)] = grads_of(at, n)

    g.gconv[ROWS : ROWS + 16, :] = jnp.zeros((16, WIDE), F32)
    loop(ROWS // 64, slopes)

    v = g.gconv[0:8, :]
    sv = g.segc[HALO - 8 : HALO + 8, :]
    back_rows = jnp.zeros((8, WIDE), F32)
    for k in range(3):
        shift = 3 - k
        full = jnp.concatenate([jnp.zeros((8, WIDE), F32), v], axis=0)
        src = pltpu.roll(full, 16 - shift, 0)[0:8]
        same = pltpu.roll(sv, 16 - shift, 0)[0:8] == sv[0:8]
        back_rows = back_rows + jnp.where(wide_of(same, 8), g.taps[k : k + 1, :] * src, 0.0)
    g.ret_out[...] = back_rows
    ret = remote(g.ret_out, g.ret_in, g.edge_sem.at[2], g.edge_sem.at[3], {ALONG: s - 1})

    @pl.when(s > 0)
    def _():
        ret.start()

    @pl.when(s == SEQ - 1)
    def _():
        g.ret_in[...] = jnp.zeros((8, WIDE), F32)

    g.wacc[...] = jnp.zeros(g.wacc.shape, F32)
    t_out.s3()

    def convolve_back(i):
        first = i * 64
        at = cut(first, 64, 16)
        sv = g.segc[cut(first + HALO, 64, 8), :]
        ahead = jnp.where(i < ROWS // 64 - 1, 1.0, 0.0)
        for n in range(4):
            cols = pl.ds(n * 256, 256)
            v = g.gconv[cut(first, 72, 8), cols]
            here = v[0:64]
            total = g.taps[3:4, cols] * here
            nxt = g.segc[cut(jnp.minimum(first + HALO + 64, ROWS + HALO - 8), 8, 8), :]
            sfull = jnp.concatenate([sv, nxt], axis=0)
            for k in range(3):
                shift = 3 - k
                same = pltpu.roll(sfull, 72 - shift, 0)[0:64] == sv
                src = pltpu.roll(v, 72 - shift, 0)[0:64]
                total = total + jnp.where(wide_of(same, 2), g.taps[k : k + 1, cols] * src, 0.0)
            if n < 3:
                g.gx[at, cols] = total.astype(BF)
            else:
                for k, v in enumerate(parts(total, 2)):
                    g.gbc[k, at, :] = v

            @pl.when(i == ROWS // 64 - 1)
            def _():
                g.tail_rows[:, cols] = total[48:64]

            for k, t in enumerate(taps_of(first, cols)):
                g.wacc[k, :, cols] += rows_sum(here * t)
            g.wacc[4, :, cols] += rows_sum(here)

    loop(ROWS // 64, convolve_back)
    t_z.s3()

    @pl.when(s < SEQ - 1)
    def _():
        ret.wait_recv()

    last_rows = g.tail_rows[...] + jnp.concatenate([jnp.zeros((8, WIDE), F32), g.ret_in[...]], axis=0)
    g.gx[ROWS - 16 : ROWS, :] = last_rows[:, 0:CHANNELS].astype(BF)
    for k, v in enumerate(parts(last_rows[:, CHANNELS:WIDE], 2)):
        g.gbc[k, ROWS - 16 : ROWS, :] = v

    def bc_block(at):
        return sum(mul(g.xn[:, at], g.gbc[k], TN) for k in range(2))

    for k in range(5):
        row = jnp.sum(g.wacc[k], axis=0, keepdims=True)
        g.pack[k : k + 1, :] = row[:, 0:CHANNELS]
        g.bcv[z, k : k + 1, :] = row[:, CHANNELS:WIDE]
    bcv = [send(g.bcv.at[z], g.bcv.at[z], g.bcvsem, i, p) for i, p in enumerate(zpeers)]
    bcs = []
    for k in range(LINE):
        g.sbc[k] = bc_block(pl.ds(BLOCK * k, BLOCK)).astype(BF)
    mine, other = cut(core * 192, 192, 16), cut((1 - core) * 192, 192, 16)
    halves = send(g.sbc.at[:, other], g.hbc, g.bcsem, 3, partner)

    def grad_x(n):
        at = cut(n * 256, 256, 256)
        g.p_x[at, :] = mul(g.xn[:, at], g.gx[...], TN).astype(BF)

    loop(6, grad_x)
    t_x.s0()
    halves.wait_recv()
    bc_rows = cut(core * 320, 192, 16)
    g.p_rest[bc_rows, :] = g.sbc[z, mine, :].astype(F32) + g.hbc[z].astype(F32)
    for i, p in enumerate(zpeers):
        k = lax.rem(z + 1 + i, LINE)
        g.sbc[k, mine, :] = (g.sbc[k, mine, :].astype(F32) + g.hbc[k].astype(F32)).astype(BF)
        bcs.append(send(g.sbc.at[k, mine], g.rbc.at[i], g.bcsem, i, p))

    def back_block(k):
        at = cut(k * BLOCK, BLOCK, 16)
        v = mul(g.gx[...], g.wx[at, :], NT) + mul(g.gz[...], g.wz[at, :], NT)
        return v + mul(g.gsr[...], g.wd[:, cut(k * BLOCK, BLOCK, 128)]) + mul(g.gbc[0], g.wbc[k], NT) + mul(g.gbc[1], g.wbc[k], NT)

    out_blocks.arrived()
    out_blocks.left()
    out_sum = g.own[...]
    for i in range(3):
        out_sum = out_sum + g.rblk[i].astype(F32)
    g.layer_out[...] = (g.x[...].astype(F32) + out_sum).astype(BF)
    in_blocks.block(0, back_block(dests[0]))
    t_x.s1()
    t_out.s4()
    in_blocks.block(1, back_block(dests[1]))
    g.own[...] = back_block(z)
    in_blocks.block(2, back_block(dests[2]))
    t_x.s2()
    t_z.s4()

    for d in bcs + bcv:
        d.wait_recv()
    g.pack[8:16, 0:256] = g.bcv[0] + g.bcv[1] + g.bcv[2] + g.bcv[3]
    g.pack[5:6, :] = jnp.sum(g.vacc[0], axis=0, keepdims=True)
    skips = head_sum(jnp.broadcast_to(jnp.sum(g.vacc[1], axis=0, keepdims=True), (8, CHANNELS)))
    g.pack[16:24, 256:384] = skips
    bc = g.p_rest[bc_rows, :]
    for i in range(3):
        bc = bc + g.rbc[i].astype(F32)
    g.p_rest[bc_rows, :] = bc
    g.p_rest[cut((1 - core) * 320, 192, 16), :] = jnp.zeros((192, 256), F32)
    for n in range(6):
        cols = pl.ds(256 * n, 256)
        g.p_rest[192 + 16 * n : 208 + 16 * n, :] = mul(g.gsr[...], g.xn[:, cols], TN)[0:16]
    g.p_rest[288:320, :] = jnp.zeros((32, 256), F32)
    for n in range(3):
        g.p_rest[512 + 24 * n : 536 + 24 * n, :] = g.pack[:, 256 * n : 256 * n + 256]
    g.p_rest[584:640, :] = jnp.zeros((56, 256), F32)
    t_rest.s0()
    t_x.s3()
    t_rest.s1()
    t_out.s5()
    t_rest.s2()
    t_x.s4()
    t_z.s5()
    t_rest.s3()
    t_out.s6()
    store = [pltpu.make_async_copy(g.p_out, g.grad_out, g.load_sem.at[5])]
    store[0].start()
    t_rest.s4()
    t_z.s6()
    store.append(pltpu.make_async_copy(g.p_z, g.grad_z, g.load_sem.at[6]))
    store[1].start()

    in_blocks.arrived()
    g.nacc[...] = jnp.zeros(g.nacc.shape, F32)

    def finish(i):
        at = cut(i * 64, 64, 16)
        v = g.own[at, :]
        for k in range(3):
            v = v + g.rblk2[k, at, :].astype(F32)
        g.own[at, :] = v
        x = g.x[at, :].astype(F32)
        g.part[0, at, :] = lanes_sum(v * gain * x)
        g.nacc[...] += rows_sum(v * x * wide_of(g.xscale[at, :], 3))

    loop(ROWS // 64, finish)
    g.nstat[z] = jnp.broadcast_to(to_row(g.part[0]), (8, ROWS))
    nst = [send(g.nstat.at[z], g.nstat.at[z], g.nsem, i, p) for i, p in enumerate(zpeers)]
    g.ngain[0] = jnp.broadcast_to(jnp.sum(g.nacc[...], axis=0, keepdims=True), (8, BLOCK))
    ngs = [send(g.ngain.at[0], g.ngain.at[1 + i], g.nsem, 3 + i, p) for i, p in enumerate(speers)]
    t_x.s5()
    t_rest.s5()
    for d in nst:
        d.wait_recv()
    rows = (g.nstat[0] + g.nstat[1] + g.nstat[2] + g.nstat[3])[0:1]
    g.part[0] = to_col(rows / D)

    def last(i):
        at = cut(i * 64, 64, 16)
        sc = wide_of(g.xscale[at, :], 3)
        x = g.x[at, :].astype(F32)
        g.grad_in[at, :] = (
            g.cotg[at, own].astype(F32)
            + sc * (g.own[at, :] * gain)
            - x * (sc * sc * sc * wide_of(g.part[0, at, :], 3))
        )

    loop(ROWS // 64, last)
    for d in ngs:
        d.wait_recv()
    total = g.ngain[0]
    for i in range(7):
        total = total + g.ngain[1 + i]
    g.grad_gain[...] = total
    t_rest.s6()
    g.rest[...] = g.p_rest[...]
    t_x.s6()
    store.append(pltpu.make_async_copy(g.p_x, g.grad_x, g.load_sem.at[7]))
    store[2].start()
    for d in pending:
        d.wait_send()

    @pl.when(s < SEQ - 1)
    def _():
        edge.wait_send()

    @pl.when(s > 0)
    def _():
        ret.wait_send()

    for inside_it, d in later:
        @pl.when(inside_it)
        def _():
            d.wait_send()

    in_blocks.left()
    for d in store:
        d.wait()


def unpack_kernel(
    layer_hbm, in_hbm, out_low, z_low, x_low, rest, gain_sum,
    layer_out, grad_in, gain, w_z, w_x, w_bc, w_dt, conv_x_w, conv_x_b, conv_bc_w, conv_bc_b, dt_bias, a_log, d_skip, gate_gain, w_out,
    low_a, low_b, low_c, full_a, full_b, full_c, keep_a, keep_b, in_sem, out_sem,
):
    steps = 6
    mats = [(out_low, low_a, full_a, w_out), (z_low, low_b, full_b, w_z), (x_low, low_c, full_c, w_x)]
    loads, stores = [], []
    for m, (src, low, _, _) in enumerate(mats):
        n = low.shape[0] // steps
        for i in range(steps):
            at = pl.ds(i * n, n)
            loads.append(pltpu.make_async_copy(src.at[at], low.at[at], in_sem.at[steps * m + i]))
    for i, (src, dst) in enumerate([(layer_hbm, keep_a), (in_hbm, keep_b)]):
        loads.append(pltpu.make_async_copy(src, dst, in_sem.at[18 + i]))
    for d in loads:
        d.start()
    for n in range(3):
        gain[n : n + 1, :] = gain_sum[0:1, 128 * n : 128 * n + 128]
    w_bc[0:192, :] = rest[0:192, :]
    w_bc[192:BLOCK, :] = rest[320:512, :]
    for n in range(6):
        w_dt[:, 256 * n : 256 * n + 256] = rest[192 + 16 * n : 204 + 16 * n, :]
    for n in range(3):
        at, base = pl.ds(256 * n, 256), 512 + 24 * n
        conv_x_w[:, at] = rest[base : base + 4, :]
        for e in range(2):
            lanes, to = pl.ds(128 * e, 128), pl.ds(2 * n + e, 1)
            conv_x_b[to, :] = rest[base + 4 : base + 5, lanes]
            gate_gain[to, :] = rest[base + 5 : base + 6, lanes]
    conv_bc_w[...] = rest[520:524, :]
    for e in range(2):
        conv_bc_b[e : e + 1, :] = rest[524:525, 128 * e : 128 * e + 128]
    dt_bias[...] = rest[528:529, 0:12]
    a_log[...] = rest[528:529, 128:140]
    d_skip[...] = rest[552:553, 0:12]
    for m, (_, low, full, dst) in enumerate(mats):
        n = low.shape[0] // steps
        for i in range(steps):
            loads[steps * m + i].wait()
            at = pl.ds(i * n, n)
            full[at, :] = low[at, :].astype(F32)
            stores.append(pltpu.make_async_copy(full.at[at], dst.at[at], out_sem.at[steps * m + i]))
            stores[-1].start()
    for i, (src, dst) in enumerate([(keep_a, layer_out), (keep_b, grad_in)]):
        loads[18 + i].wait()
        stores.append(pltpu.make_async_copy(src, dst, out_sem.at[18 + i]))
        stores[-1].start()
    for d in stores:
        d.wait()


def fast_layer(
    hidden_in, seq_lengths, norm_gain, w_z, w_x, w_bc, w_dt, conv_x_w, conv_x_b, conv_bc_w,
    conv_bc_b, dt_bias, a_log, d_skip, gate_gain, w_out, cotangent,
):
    row = lambda v: v.reshape(-1, min(128, v.shape[0]))
    vm = pl.BlockSpec(memory_space=pltpu.VMEM)
    hbm = pl.BlockSpec(memory_space=pltpu.HBM)
    sm = pl.BlockSpec(memory_space=pltpu.SMEM)
    ins = dict(
        x_hbm=(hidden_in, hbm), cot_hbm=(cotangent, hbm), w_x=(w_x, hbm), w_z=(w_z, hbm), w_out=(w_out, hbm),
        lengths=(seq_lengths, sm), norm_gain=(row(norm_gain), vm), conv_x_b=(row(conv_x_b), vm),
        conv_bc_b=(row(conv_bc_b), vm), dt_bias=(row(dt_bias), vm), a_log=(row(a_log), vm), d_skip=(row(d_skip), vm),
        gate_gain=(row(gate_gain), vm), w_bc=(w_bc, vm), w_dt=(w_dt.T, vm),
        conv_x_w=(conv_x_w, vm), conv_bc_w=(conv_bc_w, vm),
    )
    outs = dict(
        layer_out=((ROWS, BLOCK), BF, vm),
        grad_in=((ROWS, BLOCK), F32, vm),
        grad_out=((CHANNELS, D), BF, hbm),
        grad_z=((D, CHANNELS), BF, hbm),
        grad_x=((D, CHANNELS), BF, hbm),
        rest=((640, 256), F32, vm),
        grad_gain=((8, BLOCK), F32, vm),
    )
    V = pltpu.VMEM
    S = pltpu.SemaphoreType.DMA
    scr = dict(
        x=V((ROWS, BLOCK), BF),
        wx=V((D, CHANNELS), BF),
        wz=V((D, CHANNELS), BF),
        wo=V((CHANNELS, D), BF),
        xg=V((ROWS, D), BF),
        xn=V((ROWS, D), BF),
        cotg=V((ROWS, D), BF),
        ssq=V((LINE, 8, ROWS), F32),
        gains=V((LINE, 8, BLOCK), F32),
        wbc=V((LINE, BLOCK, 256), BF),
        wd=V((128, D), BF),
        params=V((8, CHANNELS), F32),
        taps=V((8, WIDE), F32),
        spread=V((256, CHANNELS), BF),
        segc=V((ROWS + HALO, 128), F32),
        segr=V((8, ROWS), F32),
        tri=V((SPAN, SPAN), BF),
        skipe=V((8, CHANNELS), F32),
        xscale=V((ROWS, 128), F32),
        acc=V((ROWS, WIDE + CHANNELS + 128), F32),
        edge=V((HALO, WIDE), BF),
        halo=V((HALO, WIDE), BF),
        cf=V((ROWS + HALO, WIDE), F32),
        step=V((ROWS, 128), F32),
        cum=V((ROWS, 128), F32),
        cumt=V((2, 16, SPAN), F32),
        tail=V((ROWS, 128), F32),
        load=V((ROWS, 128), F32),
        lead=V((ROWS, 128), F32),
        carry=V((2, 8, 128), F32),
        carrye=V((2, 8, CHANNELS), F32),
        decay=V((2, 8, CHANNELS), F32),
        slope=V((ROWS + 16, WIDE), F32),
        inner=V((ROWS, CHANNELS), BF),
        b=V((ROWS, 128), BF),
        c=V((ROWS, 128), BF),
        bt=V((STATE, ROWS), F32),
        ct=V((STATE, ROWS), F32),
        loadt=V((2, 16, SPAN), F32),
        leadt=V((2, 16, SPAN), F32),
        stept=V((2, 16, SPAN), F32),
        local=V((2, STATE, CHANNELS), F32),
        mine=V((STATE, CHANNELS), F32),
        other=V((STATE, CHANNELS), F32),
        joined=V((STATE, BLOCK), F32),
        got=V((2, STATE, BLOCK), F32),
        chain=V((STATE, CHANNELS), F32),
        mine_b=V((STATE, CHANNELS), F32),
        other_b=V((STATE, CHANNELS), F32),
        joined_b=V((STATE, BLOCK), F32),
        got_b=V((2, STATE, BLOCK), F32),
        chain_b=V((STATE, CHANNELS), F32),
        both=V((8, BLOCK), F32),
        boths=V((2, 8, BLOCK), F32),
        scores=V((SPAN, SPAN), F32),
        gscores=V((SPAN, SPAN), F32),
        out=V((ROWS, CHANNELS), F32),
        sin=V((2, STATE, CHANNELS), F32),
        slow=V((2, STATE, CHANNELS), BF),
        gated=V((ROWS, CHANNELS), F32),
        part=V((2, ROWS, 128), F32),
        stats=V((LINE, 8, ROWS), F32),
        vacc=V((2, 8, CHANNELS), F32),
        gm=V((ROWS, CHANNELS), BF),
        gloc=V((2, STATE, CHANNELS), F32),
        sblk=V((3, ROWS, BLOCK), BF),
        rblk=V((3, ROWS, BLOCK), BF),
        rblk2=V((3, ROWS, BLOCK), BF),
        gsr=V((ROWS, 128), BF),
        pack=V((24, CHANNELS), F32),
        ret_out=V((8, WIDE), F32),
        ret_in=V((8, WIDE), F32),
        wacc=V((5, 8, WIDE), F32),
        gbc=V((2, ROWS, 256), BF),
        tail_rows=V((16, WIDE), F32),
        sbc=V((LINE, BLOCK, 256), BF),
        hbc=V((LINE, 192, 256), BF),
        rbc=V((3, 192, 256), BF),
        via=V((ROWS, BLOCK), BF),
        via2=V((ROWS, BLOCK), BF),
        bcv=V((LINE, 8, 256), F32),
        nacc=V((8, BLOCK), F32),
        nstat=V((LINE, 8, ROWS), F32),
        ngain=V((8, 8, BLOCK), F32),
        p_out=V((CHANNELS, D), BF),
        p_z=V((D, CHANNELS), BF),
        p_x=V((D, CHANNELS), BF),
        p_rest=V((640, 256), F32),
        load_sem=S((8,)),
        edge_sem=S((4,)),
        gather_s=S((8,)),
        gather_r=S((8,)),
        block_s=S((8,)),
        block_r=S((8,)),
        st_send=S((11,)),
        st_recv=S((11,)),
        tot_send=S((40,)),
        tot_recv=S((40,)),
        freed=pltpu.SemaphoreType.REGULAR((12,)),
    )
    pairs = dict(
        small=9,
        wide=7,
        stat=3,
        bcsem=4,
        bcvsem=3,
        nsem=10,
    )
    sums = [(CHANNELS, D, BF), (D, CHANNELS, BF), (D, CHANNELS, BF), (640, 256, F32)]
    bufs = [b for spec in sums for b in total_bufs(*spec)]
    sems = [S((k,)) for k in pairs.values() for _ in range(2)]
    names = [*ins, *outs, *scr]

    def kernel(*refs):
        n, m = len(names), len(names) + len(bufs)
        d = dict(zip(names, refs[:n]))
        rest = refs[m:]
        for i, name in enumerate(pairs):
            d[name] = (rest[2 * i], rest[2 * i + 1])
        layer_kernel(d, refs[n:m])

    res = pl.pallas_call(
        kernel,
        out_shape=[jax.ShapeDtypeStruct(sh, dt) for sh, dt, _ in outs.values()],
        in_specs=[sp for _, sp in ins.values()],
        out_specs=[sp for _, _, sp in outs.values()],
        scratch_shapes=[*scr.values(), *bufs, *sems],
        compiler_params=pltpu.CompilerParams(collective_id=0, has_side_effects=True, vmem_limit_bytes=66 * 2**20 - 2**21),
        name="layer",
    )(*[a for a, _ in ins.values()])
    layer_out, grad_in, grad_out, grad_z, grad_x, rest, grad_gain = res
    shapes = dict(
        layer_out=((ROWS, BLOCK), BF, hbm), grad_in=((ROWS, BLOCK), F32, hbm), gain=((3, 128), F32, vm), w_z=((D, CHANNELS), F32, hbm),
        w_x=((D, CHANNELS), F32, hbm), w_bc=((BLOCK, 256), F32, vm), w_dt=((12, D), F32, vm), conv_x_w=((4, CHANNELS), F32, vm),
        conv_x_b=((6, 128), F32, vm), conv_bc_w=((4, 256), F32, vm), conv_bc_b=((2, 128), F32, vm), dt_bias=((1, 12), F32, vm),
        a_log=((1, 12), F32, vm), d_skip=((1, 12), F32, vm), gate_gain=((6, 128), F32, vm), w_out=((CHANNELS, D), F32, hbm),
    )
    final = pl.pallas_call(
        unpack_kernel,
        out_shape=[jax.ShapeDtypeStruct(sh, dt) for sh, dt, _ in shapes.values()],
        in_specs=[hbm] * 5 + [vm] * 2,
        out_specs=[sp for _, _, sp in shapes.values()],
        scratch_shapes=[
            V((CHANNELS, D), BF), V((D, CHANNELS), BF), V((D, CHANNELS), BF),
            V((CHANNELS, D), F32), V((D, CHANNELS), F32), V((D, CHANNELS), F32),
            V((ROWS, BLOCK), BF), V((ROWS, BLOCK), F32), S((20,)), S((20,)),
        ],
        compiler_params=pltpu.CompilerParams(vmem_limit_bytes=63 * 2**20),
    )(layer_out, grad_in, grad_out, grad_z, grad_x, rest, grad_gain)
    flat = [v.reshape(v.size) if v.shape[1] <= 128 else v for v in final]
    flat[6] = flat[6].T
    return tuple(flat)


def solution(mesh):
    placed = (
        P("seq", "head"),
        P(),
        P("head"),
        P(None, "head"),
        P(None, "head"),
        P("head", None),
        P(None, "head"),
        P(None, "head"),
        P("head"),
        P(),
        P(),
        P("head"),
        P("head"),
        P("head"),
        P("head"),
        P("head", None),
        P("seq", "head"),
    )
    fits = mesh.shape["seq"] == SEQ and mesh.shape["head"] == LINE
    return jax.shard_map(
        fast_layer if fits else on_device,
        mesh=mesh,
        in_specs=placed,
        out_specs=(
            P("seq", "head"),
            P("seq", "head"),
            P("head"),
            P(None, "head"),
            P(None, "head"),
            P("head", None),
            P(None, "head"),
            P(None, "head"),
            P("head"),
            P(),
            P(),
            P("head"),
            P("head"),
            P("head"),
            P("head"),
            P("head", None),
        ),
        check_vma=False,
    )
```

```python
import jax
import jax.numpy as jnp
from jax import lax
from jax.experimental import pallas as pl
from jax.experimental.pallas import tpu as pltpu
from jax.sharding import PartitionSpec as P

D = 1536
HEAD_DIM = 64
STATE = 128
CONV = 4
SPAN = 256
INNER = 3072


epsilon = 1e-05
highest = lax.Precision.HIGHEST


def prefix(part, axis, combine, identity, reverse):
    count = lax.axis_size(axis)
    place = lax.axis_index(axis)
    ahead = count - 1 - place if reverse else place
    gathered = jax.tree.map(lambda a: lax.all_gather(a, axis), part)
    state = jax.tree.map(lambda a, e: jnp.zeros_like(a) + jnp.asarray(e, a.dtype), part, identity)

    def one(hop, state):
        source = count - 1 - hop if reverse else hop
        return combine(
            state, jax.tree.map(lambda a: lax.dynamic_index_in_dim(a, source, 0, False), gathered)
        )

    return lax.fori_loop(0, ahead, one, state)


def passed_along(block, axis, distance):
    devices = range(lax.axis_size(axis))
    route = [(i - distance, i) for i in devices if i - distance in devices]
    return lax.ppermute(block, axis, route)


def segment_of(positions, starts):
    return jnp.sum((positions[:, None] >= starts[None, :]).astype(jnp.int32), axis=1) - 1


def silu_slope(values):
    sigmoid_val = jax.nn.sigmoid(values)
    return sigmoid_val * (1.0 + values * (1.0 - sigmoid_val))


def chain_join(earlier, later):
    return (earlier[0] * later[0], earlier[1] * later[0][:, None, None] + later[1])


def state_prefix(decay, summary, backwards):
    identity = (jnp.ones_like(decay), jnp.zeros_like(summary))
    result = prefix((decay, summary), "seq", chain_join, identity, backwards)
    return result[1]


def span_terms(span_item, lower_tri):
    inner_c, b_rows, c_rows, step_c, cumul_c, seg_rows, seg_prev = span_item
    same_seq = ((seg_rows[:, None] == seg_rows[None, :]) & (lower_tri > 0.5))[None, :, :]
    spread = cumul_c[:, :, None] - cumul_c[:, None, :]
    decay_mat = jnp.where(same_seq, jnp.exp(jnp.where(same_seq, spread, 0.0)), 0.0)
    scores = lax.dot_general(
        c_rows, b_rows, (((1,), (1,)), ((), ())), preferred_element_type=jnp.float32
    )
    mixing = scores[None, :, :] * decay_mat * step_c[:, None, :]
    last_cum = cumul_c[:, SPAN - 1]
    tail_weight = (
        jnp.exp(last_cum[:, None] - cumul_c)
        * (seg_rows == seg_rows[SPAN - 1]).astype(jnp.float32)[None, :]
    )
    head_weight = jnp.exp(cumul_c) * (seg_rows == seg_prev).astype(jnp.float32)[None, :]
    carry_decay = jnp.exp(last_cum) * (seg_rows[SPAN - 1] == seg_prev).astype(jnp.float32)
    return (decay_mat, scores, mixing, tail_weight, head_weight, carry_decay)


def on_device(
    hidden_in,
    seq_lengths,
    norm_gain,
    w_z,
    w_x,
    w_bc,
    w_dt,
    conv_x_w,
    conv_x_b,
    conv_bc_w,
    conv_bc_b,
    dt_bias,
    a_log,
    d_skip,
    gate_gain,
    w_out,
    cotangent,
):
    tokens_here = hidden_in.shape[0]
    heads_here = dt_bias.shape[0]
    inner_here = w_z.shape[1]
    spans = tokens_here // SPAN
    first_pos = lax.axis_index("seq") * tokens_here
    starts = jnp.cumsum(seq_lengths) - seq_lengths
    segment = segment_of(first_pos + jnp.arange(tokens_here, dtype=jnp.int32), starts)
    edge_segment = segment_of(
        first_pos - (CONV - 1) + jnp.arange(CONV - 1, dtype=jnp.int32), starts
    )
    span_prev = segment_of(first_pos - 1 + jnp.arange(spans, dtype=jnp.int32) * SPAN, starts)
    row_ids = jnp.arange(SPAN)
    lower_tri = (row_ids[:, None] >= row_ids[None, :]).astype(jnp.float32)
    inputs = hidden_in.astype(jnp.float32)
    squares = lax.psum(jnp.sum(inputs * inputs, axis=1), "head")
    scale_in = lax.rsqrt(squares / D + epsilon)
    normed = (inputs * scale_in[:, None] * norm_gain).astype(jnp.bfloat16)
    gathered, bc_weight = (
        lax.all_gather(normed, "head", axis=1, tiled=True),
        lax.all_gather(w_bc, "head", axis=0, tiled=True),
    )
    gate_pre = jnp.dot(gathered, w_z, preferred_element_type=jnp.float32)
    x_part = jnp.dot(gathered, w_x, preferred_element_type=jnp.float32)
    bc_part = jnp.dot(gathered, bc_weight, preferred_element_type=jnp.float32)
    conv_in = jnp.concatenate([x_part, bc_part], axis=1).astype(jnp.bfloat16)
    step_raw = jnp.dot(gathered, w_dt, preferred_element_type=jnp.float32)
    edge_rows = passed_along(conv_in[tokens_here - (CONV - 1) :], "seq", 1)
    padded = jnp.concatenate([edge_rows, conv_in], axis=0).astype(jnp.float32)
    seg_padded = jnp.concatenate([edge_segment, segment])
    conv_weight = jnp.concatenate([conv_x_w, conv_bc_w], axis=1)
    conv_bias = jnp.concatenate([conv_x_b, conv_bc_b])
    tap_masks = [
        (seg_padded[offset : offset + tokens_here] == segment).astype(jnp.float32)[:, None]
        for offset in range(CONV)
    ]
    conv_out = jnp.zeros(conv_in.shape, jnp.float32) + conv_bias[None, :]
    for offset in range(CONV):
        conv_out = (
            conv_out
            + conv_weight[offset] * padded[offset : offset + tokens_here] * tap_masks[offset]
        )
    activated = jax.nn.silu(conv_out)
    inner_vals = activated[:, :inner_here].astype(jnp.bfloat16)
    b_vals = activated[:, inner_here : inner_here + STATE].astype(jnp.bfloat16)
    c_vals = activated[:, inner_here + STATE :].astype(jnp.bfloat16)
    step_pre = step_raw + dt_bias
    step_size = jax.nn.softplus(step_pre)
    rates = jnp.exp(a_log)
    log_decay = -rates * step_size
    decay_heads = log_decay.reshape(spans, SPAN, heads_here).transpose(0, 2, 1)
    step_heads = step_size.reshape(spans, SPAN, heads_here).transpose(0, 2, 1)
    cumul = jnp.einsum("ij,chj->chi", lower_tri, decay_heads, precision=highest)
    inner_spans = inner_vals.reshape(spans, SPAN, heads_here, HEAD_DIM).transpose(0, 2, 1, 3)
    c_spans = c_vals.reshape(spans, SPAN, STATE)
    per_span = (
        inner_spans,
        b_vals.reshape(spans, SPAN, STATE),
        c_spans,
        step_heads,
        cumul,
        segment.reshape(spans, SPAN),
        span_prev,
    )

    def forward_span(span_item):
        decay_mat, scores, mixing, tail_weight, head_weight, carry_decay = span_terms(
            span_item, lower_tri
        )
        inner_c = span_item[0]
        y_inside = jnp.einsum(
            "hij,hjp->hip", mixing.astype(jnp.bfloat16), inner_c, preferred_element_type=jnp.float32
        )
        loaded = (
            span_item[1].astype(jnp.float32)[None, :, :] * (tail_weight * span_item[3])[:, :, None]
        ).astype(jnp.bfloat16)
        local_state = jnp.einsum(
            "hjn,hjp->hnp", loaded, inner_c, preferred_element_type=jnp.float32
        )
        return (y_inside, local_state, carry_decay, head_weight)

    y_inside, local_states, carry_decay, head_weight = lax.map(forward_span, per_span)

    def advance(state_carry, span_item):
        running, factor = state_carry
        local_c, decay_c = span_item
        return ((decay_c[:, None, None] * running + local_c, decay_c * factor), (running, factor))

    zero_state = jnp.zeros((heads_here, STATE, HEAD_DIM), jnp.float32)
    unit_decay = jnp.ones((heads_here,), jnp.float32)
    (device_state, device_decay), (local_in, local_factor) = lax.scan(
        advance, (zero_state, unit_decay), (local_states, carry_decay)
    )
    incoming = state_prefix(device_decay, device_state, False)
    state_in = local_in + local_factor[:, :, None, None] * incoming
    state_low = state_in.astype(jnp.bfloat16)
    c_weighted = (c_spans.astype(jnp.float32)[:, None, :, :] * head_weight[:, :, :, None]).astype(
        jnp.bfloat16
    )
    y_outside = jnp.einsum(
        "chin,chnp->chip", c_weighted, state_low, preferred_element_type=jnp.float32
    )
    skip_rep = jnp.repeat(d_skip, HEAD_DIM)
    mixed_out = (y_inside + y_outside).transpose(0, 2, 1, 3).reshape(
        tokens_here, inner_here
    ) + inner_vals.astype(jnp.float32) * skip_rep
    gate_act = jax.nn.silu(gate_pre)
    gated = mixed_out * gate_act
    gate_squares = lax.psum(jnp.sum(gated * gated, axis=1), "head")
    scale_gate = lax.rsqrt(gate_squares / INNER + epsilon)
    gate_normed = (gated * scale_gate[:, None] * gate_gain).astype(jnp.bfloat16)
    partial_value = jnp.dot(gate_normed, w_out, preferred_element_type=jnp.float32)
    mixed_sum = lax.psum_scatter(partial_value, "head", scatter_dimension=1, tiled=True)
    layer_out = (inputs + mixed_sum).astype(jnp.bfloat16)
    grad_full = lax.all_gather(cotangent, "head", axis=1, tiled=True)
    grad_gate_normed = lax.dot_general(
        grad_full, w_out, (((1,), (1,)), ((), ())), preferred_element_type=jnp.float32
    )
    grad_w_out = lax.dot_general(
        gate_normed, grad_full, (((0,), (0,)), ((), ())), preferred_element_type=jnp.float32
    )
    grad_gate_gain = jnp.sum(grad_gate_normed * gated * scale_gate[:, None], axis=0)
    grad_scaled = grad_gate_normed * gate_gain
    gate_inner = lax.psum(jnp.sum(grad_scaled * gated, axis=1), "head")
    grad_gated = (
        scale_gate[:, None] * grad_scaled - gated * (scale_gate**3 * gate_inner / INNER)[:, None]
    )
    grad_mixed = (grad_gated * gate_act).astype(jnp.bfloat16)
    grad_gate_pre = (grad_gated * mixed_out * silu_slope(gate_pre)).astype(jnp.bfloat16)
    grad_d_skip = jnp.sum(
        (grad_mixed.astype(jnp.float32) * inner_vals.astype(jnp.float32)).reshape(
            tokens_here, heads_here, HEAD_DIM
        ),
        axis=(0, 2),
    )
    grad_spans = grad_mixed.reshape(spans, SPAN, heads_here, HEAD_DIM).transpose(0, 2, 1, 3)
    from_inter = jnp.einsum(
        "chin,chip->chnp", c_weighted, grad_spans, preferred_element_type=jnp.float32
    )

    def retreat(state_carry, span_item):
        running, factor = state_carry
        local_c, decay_c = span_item
        current = local_c + decay_c[:, None, None] * running
        product = decay_c * factor
        return ((current, product), (current, product))

    (device_grad, device_reach), (local_grad, local_reach) = lax.scan(
        retreat, (zero_state, unit_decay), (from_inter, carry_decay), reverse=True
    )
    beyond = state_prefix(device_reach, device_grad, True)
    grad_state_in = local_grad + local_reach[:, :, None, None] * beyond
    grad_local_states = jnp.concatenate([grad_state_in[1:], beyond[None]], axis=0)
    grad_carry_decay = jnp.sum(grad_local_states * state_in, axis=(2, 3))

    def backward_span(span_item):
        span_base = span_item[:7]
        inner_c, b_rows, c_rows, step_c = (span_base[0], span_base[1], span_base[2], span_base[3])
        grad_y, grad_state, state_c, grad_decay = (
            span_item[7],
            span_item[8],
            span_item[9],
            span_item[10],
        )
        decay_mat, scores, mixing, tail_weight, head_weight, carry_decay = span_terms(
            span_base, lower_tri
        )
        grad_mixing = jnp.einsum(
            "hip,hjp->hij", grad_y, inner_c, preferred_element_type=jnp.float32
        )
        grad_inner = jnp.einsum(
            "hij,hip->hjp", mixing.astype(jnp.bfloat16), grad_y, preferred_element_type=jnp.float32
        )
        related = grad_mixing * mixing
        grad_cum = jnp.sum(related, axis=2) - jnp.sum(related, axis=1)
        grad_scores = jnp.sum(grad_mixing * decay_mat * step_c[:, None, :], axis=0)
        grad_step = jnp.sum(grad_mixing * decay_mat * scores[None, :, :], axis=1)
        b_float = b_rows.astype(jnp.float32)
        c_float = c_rows.astype(jnp.float32)
        grad_c = jnp.dot(grad_scores, b_float, precision=highest)
        grad_b = lax.dot_general(grad_scores, c_float, (((0,), (0,)), ((), ())), precision=highest)
        loading = tail_weight * step_c
        loaded = (b_float[None, :, :] * loading[:, :, None]).astype(jnp.bfloat16)
        grad_loaded = jnp.einsum(
            "hjp,hnp->hjn", inner_c, grad_state, preferred_element_type=jnp.float32
        )
        grad_inner = grad_inner + jnp.einsum(
            "hjn,hnp->hjp", loaded, grad_state, preferred_element_type=jnp.float32
        )
        grad_loading = jnp.sum(grad_loaded * b_float[None, :, :], axis=2)
        grad_b = grad_b + jnp.einsum("hjn,hj->jn", grad_loaded, loading, precision=highest)
        tail_term = grad_loading * loading
        grad_cum = grad_cum - tail_term
        grad_last = jnp.sum(tail_term, axis=1) + grad_decay * carry_decay
        grad_step = grad_step + grad_loading * tail_weight
        grad_weighted = jnp.einsum(
            "hip,hnp->hin", grad_y, state_c, preferred_element_type=jnp.float32
        )
        grad_head = jnp.sum(grad_weighted * c_float[None, :, :], axis=2)
        grad_c = grad_c + jnp.einsum("hin,hi->in", grad_weighted, head_weight, precision=highest)
        grad_cum = grad_cum + grad_head * head_weight
        grad_cum = grad_cum.at[:, SPAN - 1].add(grad_last)
        grad_log = jnp.einsum("ij,hi->hj", lower_tri, grad_cum, precision=highest)
        return (grad_inner, grad_b, grad_c, grad_step, grad_log)

    back_items = per_span + (
        grad_spans,
        grad_local_states.astype(jnp.bfloat16),
        state_low,
        grad_carry_decay,
    )
    grad_inner_s, grad_b_s, grad_c_s, grad_step_s, grad_log_s = lax.map(backward_span, back_items)
    grad_inner = (
        grad_inner_s.transpose(0, 2, 1, 3).reshape(tokens_here, inner_here)
        + grad_mixed.astype(jnp.float32) * skip_rep
    )
    grad_log_decay = grad_log_s.transpose(0, 2, 1).reshape(tokens_here, heads_here)
    grad_step_total = (
        grad_step_s.transpose(0, 2, 1).reshape(tokens_here, heads_here) - grad_log_decay * rates
    )
    grad_a_log = jnp.sum(grad_log_decay * log_decay, axis=0)
    grad_step_pre = grad_step_total * jax.nn.sigmoid(step_pre)
    grad_dt_bias = jnp.sum(grad_step_pre, axis=0)
    grad_step_raw = grad_step_pre.astype(jnp.bfloat16)
    grad_bc = lax.psum(
        jnp.concatenate(
            [grad_b_s.reshape(tokens_here, STATE), grad_c_s.reshape(tokens_here, STATE)], axis=1
        ),
        "head",
    )
    grad_conv = jnp.concatenate([grad_inner, grad_bc], axis=1) * silu_slope(conv_out)
    grad_conv_bias = jnp.sum(grad_conv, axis=0)
    grad_conv_weight = jnp.stack(
        [
            jnp.sum(grad_conv * padded[offset : offset + tokens_here] * tap_masks[offset], axis=0)
            for offset in range(CONV)
        ]
    )
    grad_padded = jnp.zeros(padded.shape, jnp.float32)
    for offset in range(CONV):
        grad_padded = grad_padded + jnp.pad(
            conv_weight[offset] * grad_conv * tap_masks[offset],
            ((offset, CONV - 1 - offset), (0, 0)),
        )
    returned = passed_along(grad_padded[: CONV - 1], "seq", -1)
    grad_conv_in = (
        grad_padded[CONV - 1 :] + jnp.pad(returned, ((tokens_here - (CONV - 1), 0), (0, 0)))
    ).astype(jnp.bfloat16)
    grad_x_pre = grad_conv_in[:, :inner_here]
    grad_bc_pre = grad_conv_in[:, inner_here:]
    contract_rows = (((0,), (0,)), ((), ()))
    contract_cols = (((1,), (1,)), ((), ()))
    grad_w_z = lax.dot_general(
        gathered, grad_gate_pre, contract_rows, preferred_element_type=jnp.float32
    )
    grad_w_x = lax.dot_general(
        gathered, grad_x_pre, contract_rows, preferred_element_type=jnp.float32
    )
    grad_w_dt = lax.dot_general(
        gathered, grad_step_raw, contract_rows, preferred_element_type=jnp.float32
    )
    grad_w_bc = lax.dot_general(
        normed, grad_bc_pre, contract_rows, preferred_element_type=jnp.float32
    )
    partial_back = lax.dot_general(
        grad_gate_pre, w_z, contract_cols, preferred_element_type=jnp.float32
    )
    partial_back = partial_back + lax.dot_general(
        grad_x_pre, w_x, contract_cols, preferred_element_type=jnp.float32
    )
    partial_back = partial_back + lax.dot_general(
        grad_step_raw, w_dt, contract_cols, preferred_element_type=jnp.float32
    )
    grad_normed = lax.psum_scatter(partial_back, "head", scatter_dimension=1, tiled=True)
    grad_normed = grad_normed + lax.dot_general(
        grad_bc_pre, w_bc, contract_cols, preferred_element_type=jnp.float32
    )
    grad_scaled_in = grad_normed * norm_gain
    grad_norm_gain = jnp.sum(grad_normed * inputs * scale_in[:, None], axis=0)
    norm_inner = lax.psum(jnp.sum(grad_scaled_in * inputs, axis=1), "head")
    grad_in = (
        cotangent.astype(jnp.float32)
        + scale_in[:, None] * grad_scaled_in
        - inputs * (scale_in**3 * norm_inner / D)[:, None]
    )
    summed = lax.psum(
        (
            grad_norm_gain,
            grad_w_z,
            grad_w_x,
            grad_w_bc,
            grad_w_dt,
            grad_conv_weight[:, :inner_here],
            grad_conv_bias[:inner_here],
            grad_conv_weight[:, inner_here:],
            grad_conv_bias[inner_here:],
            grad_dt_bias,
            grad_a_log,
            grad_d_skip,
            grad_gate_gain,
            grad_w_out,
        ),
        "seq",
    )
    return (
        layer_out,
        grad_in,
        summed[0],
        summed[1],
        summed[2],
        summed[3],
        summed[4],
        summed[5],
        summed[6],
        summed[7],
        summed[8],
        summed[9],
        summed[10],
        summed[11],
        summed[12],
        summed[13],
    )


BF = jnp.bfloat16
F32 = jnp.float32
MESH = pl.DeviceIdType.MESH
ROWS = 512
BLOCK = 384
CHANNELS = 768
WIDE = 1024
HALO = 16
SEQ = 8
LINE = 4
ALONG = "seq"
ACROSS = "head"
NN = (((1,), (0,)), ((), ()))
NT = (((1,), (1,)), ((), ()))
TN = (((0,), (0,)), ((), ()))


def mul(a, b, dims=NN):
    return lax.dot_general(a, b, dims, preferred_element_type=F32)


def cut(start, size, mult):
    return pl.ds(pl.multiple_of(start, mult), size)


def parts(v, n):
    out = []
    for _ in range(n):
        p = v.astype(BF)
        out.append(p)
        v = v - p.astype(F32)
    return out


def along_line(z, ends, middles):
    k = jnp.where(lax.rem(z, 3) == 0, ends, middles)
    return jnp.where(z >= 2, 3 - k, k)


def lanes_sum(v):
    total = v[:, 0:128]
    for i in range(1, v.shape[1] // 128):
        total = total + v[:, 128 * i : 128 * i + 128]
    return total


def rows_sum(v):
    return jnp.sum(v.reshape(v.shape[0] // 8, 8, v.shape[1]), axis=0)


def wide_of(v, n):
    return jnp.concatenate([v] * n, axis=1)


def to_row(part):
    return jnp.sum(part.T, axis=0, keepdims=True)


def to_col(row):
    return jnp.broadcast_to(row, (128, row.shape[1])).T


def loop(n, body):
    def run(i, carry):
        body(i)
        return carry

    lax.fori_loop(0, n, run, 0)


def remote(src, dst, send, recv, peer):
    return pltpu.make_async_remote_copy(
        src_ref=src, dst_ref=dst, send_sem=send, recv_sem=recv, device_id=peer, device_id_type=MESH
    )


class Total:
    def __init__(self, whole, bufs, send, recv, freed, base, me):
        self.w = whole
        self.freed, self.slot = freed, 3 * (base // 10)
        self.r0, self.ra, self.rb, self.qa, self.qb = bufs
        self.send, self.recv, self.base = send, recv, base
        self.c, self.x, self.y, self.s = me
        self.rows, self.cols = whole.shape
        self.live, self.left = {}, set()

    def peer(self, bit):
        return {ALONG: self.s + bit - 2 * bit * {1: self.c, 2: self.x, 4: self.y}[bit]}

    def free(self, k, n, bit):
        self.sent(k)
        pl.semaphore_signal(
            self.freed.at[self.slot + n], inc=1, device_id=self.peer(bit), device_id_type=MESH
        )

    def copy(self, k, src, dst, bit):
        d = remote(src, dst, self.send.at[self.base + k], self.recv.at[self.base + k], self.peer(bit))
        d.start()
        self.live[k] = d
        self.left.add(k)

    def wait(self, k):
        self.live[k].wait_recv()

    def sent(self, k):
        self.left.remove(k)
        self.live[k].wait_send()

    def add(self, start, got, rows, col, cols, step):
        def body(i):
            at = (cut(start + i * step, step, 16), pl.ds(col, cols))
            new = self.w[at].astype(F32) + got[cut(i * step, step, 16), :].astype(F32)
            self.w[at] = new.astype(self.w.dtype)

        loop(rows // step, body)

    def s0(self):
        h = self.rows // 2
        self.copy(0, self.w.at[cut((1 - self.c) * h, h, 16)], self.r0, 1)

    def s1(self):
        h, q, m = self.rows // 2, self.rows // 4, self.cols // 2
        base = self.c * h
        self.free(0, 0, 1)
        self.wait(0)
        self.add(base, self.r0, h, 0, self.cols, 32)
        self.copy(1, self.w.at[cut(base + (1 - self.x) * q, q, 16), pl.ds(0, m)], self.ra, 2)
        self.copy(2, self.w.at[cut(base + (1 - self.y) * q, q, 16), pl.ds(m, m)], self.rb, 4)

    def s2(self):
        h, q, e, m = self.rows // 2, self.rows // 4, self.rows // 8, self.cols // 2
        ba = self.c * h + self.x * q
        bb = self.c * h + self.y * q
        self.wait(1)
        self.add(ba, self.ra, q, 0, m, 32)
        self.sent(2)
        self.copy(3, self.w.at[cut(ba + (1 - self.y) * e, e, 16), pl.ds(0, m)], self.qa, 4)
        self.wait(2)
        self.add(bb, self.rb, q, m, m, 32)
        self.sent(1)
        self.copy(4, self.w.at[cut(bb + (1 - self.x) * e, e, 16), pl.ds(m, m)], self.qb, 2)

    def s3(self):
        h, q, e, m = self.rows // 2, self.rows // 4, self.rows // 8, self.cols // 2
        ba = self.c * h + self.x * q + self.y * e
        bb = self.c * h + self.y * q + self.x * e
        self.free(3, 1, 4)
        self.free(4, 2, 2)
        self.wait(3)
        self.add(ba, self.qa, e, 0, m, 16)
        pl.semaphore_wait(self.freed.at[self.slot + 1], 1)
        p = self.w.at[cut(ba, e, 16), pl.ds(0, m)]
        self.copy(5, p, p, 4)
        self.wait(4)
        self.add(bb, self.qb, e, m, m, 16)
        pl.semaphore_wait(self.freed.at[self.slot + 2], 1)
        p = self.w.at[cut(bb, e, 16), pl.ds(m, m)]
        self.copy(6, p, p, 2)

    def s4(self):
        h, q, m = self.rows // 2, self.rows // 4, self.cols // 2
        self.wait(5)
        p = self.w.at[cut(self.c * h + self.x * q, q, 16), pl.ds(0, m)]
        self.copy(7, p, p, 2)
        self.wait(6)
        p = self.w.at[cut(self.c * h + self.y * q, q, 16), pl.ds(m, m)]
        self.copy(8, p, p, 4)

    def s5(self):
        h = self.rows // 2
        self.wait(7)
        self.wait(8)
        pl.semaphore_wait(self.freed.at[self.slot], 1)
        p = self.w.at[cut(self.c * h, h, 16)]
        self.copy(9, p, p, 1)

    def s6(self):
        self.wait(9)
        for k in sorted(self.left):
            self.sent(k)


def total_bufs(rows, cols, kind):
    sizes = [(2, 1), (4, 2), (4, 2), (8, 2), (8, 2)]
    return [pltpu.VMEM((rows // a, cols // b), kind) for a, b in sizes]


class Refs:
    def __init__(self, named):
        self.__dict__.update(named)


def layer_kernel(named, sum_bufs):
    g = Refs(named)
    g.ggn = g.acc.at[:, pl.ds(0, CHANNELS)]
    g.z = g.ggn
    g.gn = g.xg.at[:, pl.ds(0, CHANNELS)]
    g.gz = g.xg.at[:, pl.ds(CHANNELS, CHANNELS)]
    g.gconv = g.slope
    g.gx = g.gm
    g.own_in = g.acc.at[:, pl.ds(0, BLOCK)]
    g.own = g.gated.at[:, pl.ds(0, BLOCK)]
    g.gb = g.gated.at[:, pl.ds(BLOCK, 128)]
    g.gc = g.gated.at[:, pl.ds(BLOCK + 128, 128)]
    s = lax.axis_index(ALONG)
    z = lax.axis_index(ACROSS)
    me = (lax.rem(s, 2), lax.rem(s // 2, 2), s // 4, s)
    zpeers = [{ACROSS: lax.rem(z + d, LINE)} for d in range(1, LINE)]
    speers = [{ALONG: lax.rem(s + d, SEQ)} for d in range(1, SEQ)]

    loads = []
    for i, (src, dst) in enumerate(
        [(g.x_hbm, g.x), (g.w_x, g.wx), (g.w_z, g.wz), (g.cot_hbm, g.cotg.at[:, cut(z * BLOCK, BLOCK, 128)]), (g.w_out, g.wo)]
    ):
        d = pltpu.make_async_copy(src, dst, g.load_sem.at[i])
        d.start()
        loads.append(d)

    g.params[...] = jnp.zeros(g.params.shape, F32)
    vectors = (g.norm_gain, g.conv_x_b, g.conv_bc_b, g.dt_bias, g.a_log, g.d_skip, g.gate_gain)
    for i, v in enumerate(vectors):
        for n in range(v.shape[0]):
            g.params[i : i + 1, 128 * n : 128 * n + v.shape[1]] = v[n : n + 1, :]

    sem = pltpu.get_barrier_semaphore()
    for p in zpeers + speers:
        pl.semaphore_signal(sem, inc=1, device_id=p, device_id_type=MESH)
    pl.semaphore_wait(sem, len(zpeers) + len(speers))

    pending = []

    def send(src, dst, sems, i, peer):
        d = remote(src, dst, sems[0].at[i], sems[1].at[i], peer)
        d.start()
        pending.append(d)
        return d

    loads[0].wait()
    loads[3].wait()
    gain = g.params[0:1, 0:BLOCK]
    xv = g.x[...].astype(F32)
    g.ssq[z] = to_row(lanes_sum(xv * xv))
    g.gains[z] = gain
    core, chip = me[0], s // 2
    partner = {ALONG: s + 1 - 2 * core}
    chips = [{ALONG: lax.rem(s + 2 * d, SEQ)} for d in range(1, 4)]
    piece = cut(48 * (4 * core + chip), 48, 16)
    own = cut(z * BLOCK, BLOCK, 128)
    g.wbc[z, piece, :] = g.w_bc[piece, :]
    small = []
    for i, p in enumerate(zpeers):
        small.append(send(g.ssq.at[z], g.ssq.at[z], g.small, i, p))
        small.append(send(g.gains.at[z], g.gains.at[z], g.small, 3 + i, p))
        small.append(send(g.w_bc.at[piece], g.wbc.at[z, piece], g.small, 6 + i, p))
    middle = lax.rem(z, 3) != 0
    near = [along_line(z, a, b) for a, b in ((1, 2), (2, 0), (3, 3))]

    def block_copy(src, whole, base, slot, k, to):
        cols = cut(k * BLOCK, BLOCK, 128)
        return remote(src, whole.at[:, cols], g.gather_s.at[base + slot], g.gather_r.at[base + k], {ACROSS: to})

    def gather(src, whole, base):
        for j in range(2):
            pending.append(block_copy(src, whole, base, j, z, near[j]))
            pending[-1].start()
        third = block_copy(src, whole, base, 2, z, near[2])

        @pl.when(jnp.logical_not(middle))
        def _():
            third.start()

        return third

    def gathered(src, whole, base, j):
        block_copy(src, whole, base, 0, near[j], z).wait_recv()

    def relay(whole, base):
        part = whole.at[:, cut(near[0] * BLOCK, BLOCK, 128)]

        @pl.when(middle)
        def _():
            block_copy(part, whole, base, 2, near[0], near[1]).start()

    x_own = [block_copy(g.x, g.xg, 0, j, z, near[j]) for j in range(2)]
    x_on = [block_copy(g.xg.at[:, cut(near[j] * BLOCK, BLOCK, 128)], g.xg, 0, 2 + j, near[j], near[1 - j % 2]) for j in range(2)]
    x_on.append(block_copy(g.xg.at[:, cut(near[2] * BLOCK, BLOCK, 128)], g.xg, 0, 4, near[2], near[1]))
    x_own[0].start()

    @pl.when(middle)
    def _():
        x_own[1].start()


    g.wd[...] = jnp.zeros(g.wd.shape, BF)
    g.wd[0:12, :] = g.w_dt[...]
    g.taps[...] = jnp.zeros(g.taps.shape, F32)
    g.taps[0:4, 0:CHANNELS] = g.conv_x_w[...]
    g.taps[0:4, CHANNELS:WIDE] = g.conv_bc_w[...]
    g.taps[4:5, 0:CHANNELS] = g.params[1:2, :]
    g.taps[4:5, CHANNELS:WIDE] = g.params[2:3, 0:256]
    expand_row = lax.broadcasted_iota(jnp.int32, (256, CHANNELS), 0)
    expand_col = lax.broadcasted_iota(jnp.int32, (256, CHANNELS), 1)
    g.spread[...] = jnp.where((expand_col >> 6) == (expand_row & 127), 1.0, 0.0).astype(BF)
    starts = [jnp.int32(0)]
    for k in range(7):
        starts.append(starts[-1] + g.lengths[k])

    def segment(pos):
        total = jnp.full(pos.shape, -1, jnp.int32)
        for k in range(8):
            total = total + jnp.where(pos >= starts[k], 1, 0)
        return total.astype(F32)

    g.segc[...] = segment(
        lax.broadcasted_iota(jnp.int32, (ROWS + HALO, 128), 0) + (s * ROWS - HALO)
    )
    g.segr[...] = segment(lax.broadcasted_iota(jnp.int32, (8, ROWS), 1) + s * ROWS)
    tri_i = lax.broadcasted_iota(jnp.int32, (SPAN, SPAN), 0)
    tri_j = lax.broadcasted_iota(jnp.int32, (SPAN, SPAN), 1)
    g.tri[...] = jnp.where(tri_i >= tri_j, 1.0, 0.0).astype(BF)
    lane = lax.broadcasted_iota(jnp.int32, (1, 128), 1)
    left = lane < 64

    def spread(v):
        hi, lo = parts(v, 2)
        return mul(jnp.concatenate([hi, lo], axis=1), g.spread[...])

    def head_sum(v):
        hi, lo = parts(v, 2)
        e = g.spread[0:128, :]
        return mul(hi, e, NT) + mul(lo, e, NT)

    g.skipe[...] = spread(jnp.broadcast_to(g.params[5:6, 0:128], (8, 128)))
    rates = jnp.exp(g.params[4:5, 0:128])

    for d in small:
        d.wait_recv()
    wide = [
        send(g.wbc.at[:, piece], g.wbc.at[:, piece], g.wide, i, p) for i, p in enumerate(chips)
    ]
    total = g.ssq[0] + g.ssq[1] + g.ssq[2] + g.ssq[3]
    g.xscale[...] = to_col(lax.rsqrt(total / D + epsilon))

    def normalise(k, src):
        gk = g.gains[k]
        cols = cut(k * BLOCK, BLOCK, 128)

        def body(i):
            at = cut(i * 64, 64, 16)
            v = src(at, cols).astype(F32)
            g.xn[at, cols] = (v * wide_of(g.xscale[at, :], 3) * gk).astype(BF)

        loop(ROWS // 64, body)

    def project(k, w, cols, base, first, width=256):
        at = cut(k * BLOCK, BLOCK, 128)

        def body(n):
            p = mul(g.xn[:, at], w[cut(k * BLOCK, BLOCK, 16), cut(n * width, width, 128)])
            dst = cut(base + n * width, width, 128)
            if first:
                g.acc[:, dst] = p
            else:
                g.acc[:, dst] += p

        loop(cols // width, body)

    def project_dt(k, first):
        at = cut(k * BLOCK, BLOCK, 128)
        p = mul(g.xn[:, at], g.wd[:, at], NT)
        if first:
            g.acc[:, WIDE + CHANNELS :] = p
        else:
            g.acc[:, WIDE + CHANNELS :] += p

    normalise(z, lambda at, cols: g.x[at, :])
    loads[1].wait()
    loads[2].wait()
    project(z, g.wx, CHANNELS, 0, True)
    project(z, g.wz, CHANNELS, WIDE, True)
    project_dt(z, True)
    for i, k in enumerate(near):
        if i != 1:
            gathered(g.x, g.xg, 0, i)
        else:
            @pl.when(jnp.logical_not(middle))
            def _():
                gathered(g.x, g.xg, 0, 1)

        if i == 2:
            @pl.when(middle)
            def _():
                x_on[2].start()

        if i == 0:
            @pl.when(middle)
            def _():
                x_on[0].start()
                gathered(g.x, g.xg, 0, 1)
                x_on[1].start()

            for d in wide:
                d.wait_recv()
            share = g.wbc.at[:, cut(192 * core, 192, 16)]
            wide = [send(share, share, g.wide, 3, partner)]
        if i == 2:
            pending.append(gather(g.cotg.at[:, own], g.cotg, 5))
        normalise(k, lambda at, cols: g.xg[at, cols])
        project(k, g.wx, CHANNELS, 0, False)
        if i < 2:
            project(k, g.wz, CHANNELS, WIDE, False)
            project_dt(k, False)
    for d in wide:
        d.wait_recv()
    g.acc[:, CHANNELS:WIDE] = sum(
        mul(g.xn[:, BLOCK * k : BLOCK * k + BLOCK], g.wbc[k]) for k in range(LINE)
    )

    g.edge[...] = g.acc[ROWS - HALO : ROWS, 0:WIDE].astype(BF)
    edge = remote(g.edge, g.halo, g.edge_sem.at[0], g.edge_sem.at[1], {ALONG: s + 1})

    @pl.when(s < SEQ - 1)
    def _():
        edge.start()

    @pl.when(s == 0)
    def _():
        g.halo[...] = jnp.zeros(g.halo.shape, BF)

    def put(i):
        g.cf[cut(HALO + i * 64, 64, 8), :] = (
            g.acc[cut(i * 64, 64, 8), 0:WIDE].astype(BF).astype(F32)
        )

    loop(ROWS // 64, put)
    project(near[2], g.wz, CHANNELS, WIDE, False)
    project_dt(near[2], False)

    step_pre = g.acc[:, WIDE + CHANNELS :] + g.params[3:4, 0:128]
    g.step[...] = jnp.where(lane < 12, jax.nn.softplus(step_pre), 0.0)
    for q in range(2):
        rows = pl.ds(q * SPAN, SPAN)
        log_decay = -rates * g.step[rows, :]
        cum = sum(mul(g.tri[...], p) for p in parts(log_decay, 3))
        g.cum[rows, :] = cum
        g.cumt[q] = cum.T[0:16, :]
        last = cum[SPAN - 1 : SPAN, :]
        seg = g.segc[pl.ds(HALO + q * SPAN, SPAN), :]
        seg_last = g.segc[HALO + q * SPAN + SPAN - 1 : HALO + q * SPAN + SPAN, :]
        seg_prev = g.segc[HALO + q * SPAN - 1 : HALO + q * SPAN, :]
        tail = jnp.where(seg == seg_last, jnp.exp(last - cum), 0.0)
        load = tail * g.step[rows, :]
        lead = jnp.where(seg == seg_prev, jnp.exp(cum), 0.0)
        g.tail[rows, :] = tail
        g.load[rows, :] = load
        g.lead[rows, :] = lead
        g.loadt[q] = load.T[0:16, :]
        g.leadt[q] = lead.T[0:16, :]
        g.stept[q] = g.step[rows, :].T[0:16, :]
        carry = jnp.where(seg_last == seg_prev, jnp.exp(last), 0.0)
        g.carry[q] = jnp.broadcast_to(carry, (8, 128))
        g.carrye[q] = spread(jnp.broadcast_to(carry, (8, 128)))
    g.decay[0] = g.carrye[0] * g.carrye[1]

    def taps_of(first, cols):
        v = g.cf[cut(first + 8, 72, 8), cols]
        sv = g.segc[cut(first + 8, 72, 8), :]
        width = v.shape[1] // 128
        out = []
        for k in range(3):
            same = pltpu.roll(sv, 67 - k, 0)[0:64] == sv[8:72]
            out.append(jnp.where(wide_of(same, width), pltpu.roll(v, 67 - k, 0)[0:64], 0.0))
        out.append(v[8:72])
        return out

    def convolve(i):
        first = i * 64
        at = cut(first, 64, 16)
        for n in range(4):
            cols = pl.ds(n * 256, 256)
            v = jnp.broadcast_to(g.taps[4:5, cols], (64, 256))
            for k, t in enumerate(taps_of(first, cols)):
                v = v + g.taps[k : k + 1, cols] * t
            sig = jax.nn.sigmoid(v)
            act = (v * sig).astype(BF)
            g.slope[at, cols] = sig * (1.0 + v * (1.0 - sig))
            if n < 3:
                g.inner[at, cols] = act
            else:
                g.b[at, :] = act[:, 0:128]
                g.c[at, :] = act[:, 128:256]

    loop(ROWS // 64 - 1, lambda i: convolve(i + 1))

    @pl.when(s > 0)
    def _():
        edge.wait_recv()

    g.cf[0:HALO, :] = g.halo[...].astype(F32)
    convolve(0)

    g.bt[...] = g.b[...].astype(F32).T
    g.ct[...] = g.c[...].astype(F32).T

    def outer(maps, weights, vals):
        def body(t):
            q, p = t // 6, lax.rem(t, 6)
            at = cut(p * 128, 128, 128)
            v = vals[cut(q * SPAN, SPAN, 256), at]
            m = maps[:, cut(q * SPAN, SPAN, 256)]
            o = [mul((m * weights[q, pl.ds(2 * p + e, 1), :]).astype(BF), v) for e in range(2)]
            g.local[q, :, at] = jnp.where(left, o[0], o[1])

        loop(12, body)

    outer(g.bt, g.loadt, g.inner)
    c0, c1 = g.carrye[0][0:1], g.carrye[1][0:1]
    half, rest = cut(core * BLOCK, BLOCK, 128), cut((1 - core) * BLOCK, BLOCK, 128)
    later = []

    class Chain:
        def __init__(self, mine, other, joined, got, result, base, way):
            self.mine, self.other, self.joined, self.got, self.result = mine, other, joined, got, result
            self.base, self.way = base, way
            self.near = self.link(joined, got.at[0], 1, way)
            self.far = self.link(joined, got.at[1], 2, 2 * way)

        def link(self, src, dst, i, hop):
            to = {ALONG: s + 2 * hop}
            return remote(src, dst, g.st_send.at[self.base + i], g.st_recv.at[self.base + i], to)

        def share(self):
            self.first = send(self.mine, self.other, (g.st_send, g.st_recv), self.base, partner)

        def join(self):
            self.first.wait_recv()
            own, other = self.mine[:, half], self.other[:, half]
            even, odd = jnp.where(core == 0, own, other), jnp.where(core == 0, other, own)
            if self.way > 0:
                self.joined[...] = odd_decay() * even + odd
            else:
                self.joined[...] = even + even_decay() * odd
            for d, hop in ((self.near, 1), (self.far, 2)):
                pass_on(d, hop * self.way)
            for i, hop in ((0, 1), (1, 2)):
                outside = chip - hop * self.way

                @pl.when((outside < 0) | (outside > 3))
                def _():
                    self.got[i] = jnp.zeros((STATE, BLOCK), F32)

        def meet(self, decay):
            for d, hop in ((self.near, 1), (self.far, 2)):
                arrive(d, hop * self.way)
            self.result[:, half] = self.got[0] + decay * self.got[1]
            p = self.result.at[:, half]
            self.last = send(p, p, (g.st_send, g.st_recv), self.base + 3, partner)

        def end(self):
            self.last.wait_recv()

    def pass_on(d, hop):
        inside = (chip + hop >= 0) & (chip + hop <= 3)

        @pl.when(inside)
        def _():
            d.start()

        later.append((inside, d))

    def arrive(d, hop):
        @pl.when((chip - hop >= 0) & (chip - hop <= 3))
        def _():
            d.wait_recv()

    def odd_decay():
        return jnp.where(core == 0, g.decay[1, 0:1, half], g.decay[0, 0:1, half])

    def even_decay():
        return jnp.where(core == 0, g.decay[0, 0:1, half], g.decay[1, 0:1, half])

    g.mine[...] = c1 * g.local[0] + g.local[1]
    ahead = Chain(g.mine, g.other, g.joined, g.got, g.chain, 0, 1)
    ahead.share()
    dec = send(g.decay.at[0], g.decay.at[1], (g.st_send, g.st_recv), 8, partner)
    both_up = remote(g.both, g.boths.at[0], g.st_send.at[9], g.st_recv.at[9], {ALONG: s + 2})
    both_down = remote(g.both, g.boths.at[1], g.st_send.at[10], g.st_recv.at[10], {ALONG: s - 2})

    def head_cols(ref, rows, p):
        moved = pltpu.roll(ref[rows, :], lax.rem(128 - 2 * p, 128), 1)
        return moved[:, 0:1], moved[:, 1:2]

    def inside(q, first, count):
        rows = cut(q * SPAN, SPAN, 256)
        seg = g.segc[cut(HALO + q * SPAN, SPAN, 16), 0:1]
        segr = g.segr[0:1, cut(q * SPAN, SPAN, 256)]
        scores = mul(g.c[rows, :], g.b[rows, :], NT)
        g.scores[...] = jnp.where((tri_i >= tri_j) & (seg == segr), scores, 0.0)

        def pair(t):
            p = first + t
            cols = head_cols(g.cum, rows, p)
            at = cut(p * 128, 128, 128)
            outs = []
            for e in range(2):
                row = g.cumt[q, pl.ds(2 * p + e, 1), :]
                step = g.stept[q, pl.ds(2 * p + e, 1), :]
                fall = jnp.exp(jnp.minimum(cols[e] - row, 0.0))
                outs.append(mul((g.scores[...] * fall * step).astype(BF), g.inner[rows, at]))
            g.out[rows, at] = jnp.where(left, outs[0], outs[1])

        loop(count, pair)

    inside(0, 0, 3)
    dec.wait_recv()
    g.both[...] = g.decay[0, :, half] * g.decay[1, :, half]
    ahead.join()
    pass_on(both_up, 1)
    pass_on(both_down, -1)
    for i, hop in ((0, 1), (1, -1)):
        @pl.when((chip - hop < 0) | (chip - hop > 3))
        def _():
            g.boths[i] = jnp.zeros((8, BLOCK), F32)

    inside(0, 3, 3)
    gathered(g.cotg.at[:, own], g.cotg, 5, 0)
    relay(g.cotg, 5)
    inside(1, 0, 6)

    arrive(both_up, 1)
    loads[4].wait()
    gate_gain = g.params[6:7, :]

    def down(k, first):
        at = cut(k * BLOCK, BLOCK, 128)

        def body(n):
            cols = cut(n * 256, 256, 256)
            p = mul(g.cotg[:, at], g.wo[cols, at], NT)
            if first:
                g.ggn[:, cols] = p
            else:
                g.ggn[:, cols] += p

        loop(3, body)

    down(z, True)
    down(near[0], False)
    ahead.meet(g.boths[0, 0:1, :])

    def act(i):
        at = cut(i * 64, 64, 16)
        pre = g.acc[at, gate_cols]
        g.gated[at, :] = pre * jax.nn.sigmoid(pre)

    gate_cols = pl.ds(WIDE, CHANNELS)
    loop(ROWS // 64, act)
    ahead.end()
    from_chips = g.chain[...]
    incoming = jnp.where(core == 0, from_chips, g.other[...] + g.decay[1, 0:1] * from_chips)
    g.sin[0] = incoming
    g.sin[1] = g.local[0] + c0 * incoming
    for q in range(2):
        g.slow[q] = g.sin[q].astype(BF)

    def outside(t):
        q, p = t // 6, lax.rem(t, 6)
        rows, at = cut(q * SPAN, SPAN, 256), cut(p * 128, 128, 128)
        cols = head_cols(g.lead, rows, p)
        cv = g.c[rows, :].astype(F32)
        o = [mul((cv * cols[e]).astype(BF), g.slow[q, :, at]) for e in range(2)]
        g.out[rows, at] += jnp.where(left, o[0], o[1])

    loop(12, outside)

    skip = g.skipe[0:1]

    def gate(i):
        at = cut(i * 64, 64, 16)
        mixed = g.out[at, :] + g.inner[at, :].astype(F32) * skip
        gated = mixed * g.gated[at, :]
        g.gated[at, :] = gated
        g.part[0, at, :] = lanes_sum(gated * gated)

    loop(ROWS // 64, gate)
    g.stats[z, 0:1, :] = to_row(g.part[0])

    for i in (1, 2):
        gathered(g.cotg.at[:, own], g.cotg, 5, i)
        down(near[i], False)

    def inner_part(i):
        at = cut(i * 64, 64, 16)
        g.part[1, at, :] = lanes_sum(g.ggn[at, :] * gate_gain * g.gated[at, :])

    loop(ROWS // 64, inner_part)
    g.stats[z, 1:2, :] = to_row(g.part[1])
    stat = [send(g.stats.at[z], g.stats.at[z], g.stat, i, p) for i, p in enumerate(zpeers)]
    for d in stat:
        d.wait_recv()
    sums = g.stats[0] + g.stats[1] + g.stats[2] + g.stats[3]
    gscale = lax.rsqrt(sums[0:1] / INNER + epsilon)
    g.part[0] = to_col(gscale)
    g.part[1] = to_col(gscale * gscale * gscale * sums[1:2] / INNER)
    @pl.when(middle)
    def _():
        for d in x_on:
            d.wait_send()

    g.vacc[...] = jnp.zeros(g.vacc.shape, F32)
    g.pack[...] = jnp.zeros(g.pack.shape, F32)
    g.bcv[z] = jnp.zeros((8, 256), F32)

    def ungate(i):
        at = cut(i * 64, 64, 16)
        a = wide_of(g.part[0, at, :], 6)
        pre = g.acc[at, gate_cols]
        vals = g.inner[at, :].astype(F32)
        mixed = g.out[at, :] + vals * skip
        gated, ggn = g.gated[at, :], g.ggn[at, :]
        g.gn[at, :] = (gated * a * gate_gain).astype(BF)
        gg = a * (ggn * gate_gain) - gated * wide_of(g.part[1, at, :], 6)
        sig = jax.nn.sigmoid(pre)
        gm = (gg * (pre * sig)).astype(BF)
        g.gm[at, :] = gm
        g.gz[at, :] = (gg * mixed * (sig * (1.0 + pre * (1.0 - sig)))).astype(BF)
        g.vacc[0] += rows_sum(ggn * gated * a)
        g.vacc[1] += rows_sum(gm.astype(F32) * vals)

    loop(ROWS // 64, ungate)

    outer(g.ct, g.leadt, g.gm)
    g.mine_b[...] = g.local[0] + c0 * g.local[1]
    behind = Chain(g.mine_b, g.other_b, g.joined_b, g.got_b, g.chain_b, 4, -1)
    behind.share()

    t_out, t_z, t_xa, t_xb = [
        Total(ref, sum_bufs[5 * i : 5 * i + 5], g.tot_send, g.tot_recv, g.freed, 10 * i, me)
        for i, ref in enumerate((g.p_out, g.p_z, g.p_xa, g.p_xb))
    ]

    def grad_out(n):
        at = cut(n * 256, 256, 256)
        g.p_out[at, :] = mul(g.gn[:, at], g.cotg[...], TN).astype(BF)

    loop(3, grad_out)
    behind.join()
    t_out.s0()

    def grad_z(n):
        at = cut(n * 256, 256, 256)
        g.p_z[at, :] = mul(g.xn[:, at], g.gz[...], TN).astype(BF)

    loop(6, grad_z)
    t_z.s0()
    t_out.s1()

    dests = [along_line(z, a, b) for a, b in ((2, 3), (3, 0), (1, 2))]

    class Scatter:
        def __init__(self, sent, got, via, base):
            self.sent, self.got, self.via, self.base = sent, got, via, base

        def copy(self, j, dst, i, to):
            return remote(self.sent[j], dst, g.block_s.at[self.base + j], g.block_r.at[self.base + i], {ACROSS: to})

        def direct(self, j):
            slot = lax.rem(z - dests[j] + 7, 4)
            return self.copy(j, self.got.at[slot], slot, dests[j])

        def block(self, j, value):
            v = value
            if j == 2:
                @pl.when(middle)
                def _():
                    self.copy(0, self.via, 3, z).wait_recv()

                v = v + self.via[...].astype(F32)
            self.sent[j][...] = v.astype(BF)
            if j == 0:
                @pl.when(middle)
                def _():
                    self.direct(0).start()

                @pl.when(jnp.logical_not(middle))
                def _():
                    self.copy(0, self.via, 3, dests[2]).start()
            else:
                self.direct(j).start()

        def arrived(self):
            for i in (0, 2):
                self.copy(0, self.got.at[i], i, z).wait_recv()

            @pl.when(jnp.logical_not(middle))
            def _():
                self.copy(0, self.got.at[1], 1, z).wait_recv()

        def left(self):
            for j in range(3):
                self.copy(j, self.via, 3, z).wait_send()

    blocks = [pl.ds(0, BLOCK), pl.ds(BLOCK, BLOCK)]
    out_blocks = Scatter([g.sblk.at[j] for j in range(3)], g.rblk, g.via, 0)
    in_blocks = Scatter(
        [g.gn.at[:, blocks[0]], g.gn.at[:, blocks[1]], g.inner.at[:, blocks[0]]], g.rblk2, g.via2, 4
    )

    @pl.when(middle)
    def _():
        g.rblk[1] = jnp.zeros((ROWS, BLOCK), BF)
        g.rblk2[1] = jnp.zeros((ROWS, BLOCK), BF)

    @pl.when(jnp.logical_not(middle))
    def _():
        g.via[...] = jnp.zeros((ROWS, BLOCK), BF)
        g.via2[...] = jnp.zeros((ROWS, BLOCK), BF)

    def out_block(k):
        return mul(g.gn[...], g.wo[:, cut(k * BLOCK, BLOCK, 128)])

    out_blocks.block(0, out_block(dests[0]))
    out_blocks.block(1, out_block(dests[1]))
    t_z.s1()
    g.own[...] = mul(g.gn[...], g.wo[:, own])

    def inside_back(q, first, count):
        rows = cut(q * SPAN, SPAN, 256)
        seg = g.segc[cut(HALO + q * SPAN, SPAN, 16), 0:1]
        segr = g.segr[0:1, cut(q * SPAN, SPAN, 256)]
        mask = (tri_i <= tri_j) & (seg == segr)
        if first == 0:
            g.scores[...] = jnp.where(mask, mul(g.b[rows, :], g.c[rows, :], NT), 0.0)
            g.gscores[...] = jnp.zeros((SPAN, SPAN), F32)

        def pair(t):
            p = first + t
            cols = head_cols(g.cum, rows, p)
            at = cut(p * 128, 128, 128)
            steps = head_cols(g.step, rows, p)
            gm = g.gm[rows, at]
            outs = []
            for e in range(2):
                row = g.cumt[q, pl.ds(2 * p + e, 1), :]
                fall = jnp.exp(jnp.minimum(row - cols[e], 0.0)) * steps[e]
                outs.append(mul((g.scores[...] * fall).astype(BF), gm))
                keep = left if e == 0 else jnp.logical_not(left)
                vals = jnp.where(keep, g.inner[rows, at].astype(F32), 0.0).astype(BF)
                g.gscores[...] += mul(vals, gm, NT) * fall
            g.z[rows, at] = jnp.where(left, outs[0], outs[1])

        loop(count, pair)
        if first + count < 6:
            return
        gs = jnp.where(mask, g.gscores[...], 0.0)
        hi, lo = parts(gs, 2)
        g.gb[rows, :] = mul(hi, g.c[rows, :]) + mul(lo, g.c[rows, :])
        g.gc[rows, :] = mul(hi, g.b[rows, :], TN) + mul(lo, g.b[rows, :], TN)

    inside_back(1, 0, 6)
    arrive(both_down, -1)
    behind.meet(g.boths[1, 0:1, :])
    inside_back(0, 0, 3)
    inside_back(0, 3, 3)

    behind.end()
    from_chips = g.chain_b[...]
    beyond = jnp.where(core == 1, from_chips, g.other_b[...] + g.decay[1, 0:1] * from_chips)
    g.gloc[1] = beyond
    g.gloc[0] = g.local[1] + c1 * beyond
    ends = []
    for q in range(2):
        rows = pl.ds(q * SPAN, SPAN)
        glow = g.gloc[q].astype(BF)
        vals = g.inner[rows, :].astype(F32)
        gm = g.gm[rows, :].astype(F32)
        loade = spread(g.load[rows, :])
        bg = mul(g.b[rows, :], glow)
        zed = g.z[rows, :]
        carry_sum = jnp.sum(g.gloc[q] * g.sin[q], axis=0, keepdims=True)
        grad_carry = head_sum(jnp.broadcast_to(carry_sum, (8, CHANNELS)))[0:1]
        t1 = head_sum(gm * g.out[rows, :])
        q1 = head_sum(vals * zed)
        q2 = head_sum(vals * bg)
        step, load = g.step[rows, :], g.load[rows, :]
        tail_term = q2 * load
        gcum = t1 - q1 - tail_term
        end = jnp.sum(tail_term, axis=0, keepdims=True) + grad_carry * g.carry[q][0:1]
        is_last = lax.broadcasted_iota(jnp.int32, (SPAN, 128), 0) == SPAN - 1
        gcum = gcum + jnp.where(is_last, end, 0.0)
        glog = sum(mul(g.tri[...], p, TN) for p in parts(gcum, 3))
        gstep = jnp.where(step > 1e-30, q1 / jnp.maximum(step, 1e-30), 0.0) + q2 * g.tail[rows, :]
        gpre = (gstep - rates * glog) * jax.nn.sigmoid(
            g.acc[rows, WIDE + CHANNELS :] + g.params[3:4, 0:128]
        )
        g.gsr[rows, :] = gpre.astype(BF)
        ends.append((rows_sum(gpre), rows_sum(glog * (-rates * step))))
        g.z[rows, :] = zed + loade * bg + skip * gm
        g.gb[rows, :] += sum(mul(p, glow, NT) for p in parts(vals * loade, 2))
        g.gc[rows, :] += sum(mul(p, g.slow[q], NT) for p in parts(gm * spread(g.lead[rows, :]), 2))
        if q == 0:
            t_out.s2()
            out_blocks.block(2, out_block(dests[2]))
    g.pack[16:24, 0:128] = jnp.broadcast_to(
        jnp.sum(ends[0][0] + ends[1][0], axis=0, keepdims=True), (8, 128)
    )
    g.pack[16:24, 128:256] = jnp.broadcast_to(
        jnp.sum(ends[0][1] + ends[1][1], axis=0, keepdims=True), (8, 128)
    )
    def grads_of(at, n):
        cols = pl.ds(n * 256, 256)
        if n < 3:
            v = g.z[at, cols]
        else:
            v = jnp.concatenate([g.gb[at, :], g.gc[at, :]], axis=1)
        return v * g.slope[at, cols]

    def slopes(i):
        at = cut(i * 64, 64, 16)
        for n in range(4):
            g.gconv[cut(i * 64, 64, 8), pl.ds(n * 256, 256)] = grads_of(at, n)

    g.gconv[ROWS : ROWS + 16, :] = jnp.zeros((16, WIDE), F32)
    loop(ROWS // 64, slopes)

    v = g.gconv[0:8, :]
    sv = g.segc[HALO - 8 : HALO + 8, :]
    back_rows = jnp.zeros((8, WIDE), F32)
    for k in range(3):
        shift = 3 - k
        full = jnp.concatenate([jnp.zeros((8, WIDE), F32), v], axis=0)
        src = pltpu.roll(full, 16 - shift, 0)[0:8]
        same = pltpu.roll(sv, 16 - shift, 0)[0:8] == sv[0:8]
        back_rows = back_rows + jnp.where(wide_of(same, 8), g.taps[k : k + 1, :] * src, 0.0)
    g.ret_out[...] = back_rows
    ret = remote(g.ret_out, g.ret_in, g.edge_sem.at[2], g.edge_sem.at[3], {ALONG: s - 1})

    @pl.when(s > 0)
    def _():
        ret.start()

    @pl.when(s == SEQ - 1)
    def _():
        g.ret_in[...] = jnp.zeros((8, WIDE), F32)

    g.wacc[...] = jnp.zeros(g.wacc.shape, F32)
    t_z.s2()

    def convolve_back(i):
        first = i * 64
        at = cut(first, 64, 16)
        sv = g.segc[cut(first + HALO, 64, 8), :]
        ahead = jnp.where(i < ROWS // 64 - 1, 1.0, 0.0)
        for n in range(4):
            cols = pl.ds(n * 256, 256)
            v = g.gconv[cut(first, 72, 8), cols]
            here = v[0:64]
            total = g.taps[3:4, cols] * here
            nxt = g.segc[cut(jnp.minimum(first + HALO + 64, ROWS + HALO - 8), 8, 8), :]
            sfull = jnp.concatenate([sv, nxt], axis=0)
            for k in range(3):
                shift = 3 - k
                same = pltpu.roll(sfull, 72 - shift, 0)[0:64] == sv
                src = pltpu.roll(v, 72 - shift, 0)[0:64]
                total = total + jnp.where(wide_of(same, 2), g.taps[k : k + 1, cols] * src, 0.0)
            if n < 3:
                g.gx[at, cols] = total.astype(BF)
            else:
                for k, v in enumerate(parts(total, 2)):
                    g.gbc[k, at, :] = v

            @pl.when(i == ROWS // 64 - 1)
            def _():
                g.tail_rows[:, cols] = total[48:64]

            for k, t in enumerate(taps_of(first, cols)):
                g.wacc[k, :, cols] += rows_sum(here * t)
            g.wacc[4, :, cols] += rows_sum(here)

    loop(ROWS // 64, convolve_back)
    t_out.s3()

    @pl.when(s < SEQ - 1)
    def _():
        ret.wait_recv()

    last_rows = g.tail_rows[...] + jnp.concatenate([jnp.zeros((8, WIDE), F32), g.ret_in[...]], axis=0)
    g.gx[ROWS - 16 : ROWS, :] = last_rows[:, 0:CHANNELS].astype(BF)
    for k, v in enumerate(parts(last_rows[:, CHANNELS:WIDE], 2)):
        g.gbc[k, ROWS - 16 : ROWS, :] = v

    def bc_block(at):
        return sum(mul(g.xn[:, at], g.gbc[k], TN) for k in range(2))

    for k in range(5):
        row = jnp.sum(g.wacc[k], axis=0, keepdims=True)
        g.pack[k : k + 1, :] = row[:, 0:CHANNELS]
        g.bcv[z, k : k + 1, :] = row[:, CHANNELS:WIDE]
    bcv = [send(g.bcv.at[z], g.bcv.at[z], g.bcvsem, i, p) for i, p in enumerate(zpeers)]
    bcs = []
    for k in range(LINE):
        g.sbc[k] = bc_block(pl.ds(BLOCK * k, BLOCK)).astype(BF)
    mine, other = cut(core * 192, 192, 16), cut((1 - core) * 192, 192, 16)
    halves = send(g.sbc.at[:, other], g.hbc, g.bcsem, 3, partner)

    def grad_x(ref, first):
        def body(n):
            at = cut(n * 256, 256, 256)
            ref[at, :] = mul(g.xn[:, cut(first + n * 256, 256, 256)], g.gx[...], TN).astype(BF)

        loop(3, body)

    grad_x(g.p_xa, 0)
    t_xa.s0()
    grad_x(g.p_xb, CHANNELS)
    t_xb.s0()
    halves.wait_recv()
    g.bcsum[...] = g.sbc[z, mine, :].astype(F32) + g.hbc[z].astype(F32)
    for i, p in enumerate(zpeers):
        k = lax.rem(z + 1 + i, LINE)
        g.sbc[k, mine, :] = (g.sbc[k, mine, :].astype(F32) + g.hbc[k].astype(F32)).astype(BF)
        bcs.append(send(g.sbc.at[k, mine], g.rbc.at[i], g.bcsem, i, p))

    def back_block(k):
        at = cut(k * BLOCK, BLOCK, 16)
        v = mul(g.gx[...], g.wx[at, :], NT) + mul(g.gz[...], g.wz[at, :], NT)
        return v + mul(g.gsr[...], g.wd[:, cut(k * BLOCK, BLOCK, 128)]) + mul(g.gbc[0], g.wbc[k], NT) + mul(g.gbc[1], g.wbc[k], NT)

    in_blocks.block(0, back_block(dests[0]))
    t_xa.s1()
    t_xb.s1()
    in_blocks.block(1, back_block(dests[1]))
    g.own_in[...] = back_block(z)
    t_z.s3()
    t_xa.s2()
    t_xb.s2()

    for d in bcs + bcv:
        d.wait_recv()
    g.pack[8:16, 0:256] = g.bcv[0] + g.bcv[1] + g.bcv[2] + g.bcv[3]
    g.pack[5:6, :] = jnp.sum(g.vacc[0], axis=0, keepdims=True)
    skips = head_sum(jnp.broadcast_to(jnp.sum(g.vacc[1], axis=0, keepdims=True), (8, CHANNELS)))
    g.pack[16:24, 256:384] = skips
    bc = g.bcsum[...]
    for i in range(3):
        bc = bc + g.rbc[i].astype(F32)
    g.q_out[0:192, :] = bc.astype(BF)
    for n in range(6):
        cols = pl.ds(256 * n, 256)
        g.few[16 * n : 16 * n + 16, :] = mul(g.gsr[...], g.xn[:, cols], TN)[0:16]
    for n in range(3):
        g.few[96 + 24 * n : 120 + 24 * n, :] = g.pack[:, 256 * n : 256 * n + 256]
    g.few[168:192, :] = jnp.zeros((24, 256), F32)
    few = send(g.few, g.few_in, g.restsem, 0, partner)
    in_blocks.block(2, back_block(dests[2]))
    t_out.s4()
    t_xa.s3()
    few.wait_recv()
    few_half = cut(96 * core, 96, 8)
    g.q_out[192:288, :] = (g.few[few_half, :] + g.few_in[few_half, :]).astype(BF)
    across_x = send(g.q_out, g.q_in.at[0], g.restsem, 1, {ALONG: s + 2 - 4 * me[1]})
    t_xb.s3()
    t_z.s4()
    out_blocks.arrived()
    out_sum = g.own[...]
    for i in range(3):
        out_sum = out_sum + g.rblk[i].astype(F32)
    g.layer_out[...] = (g.x[...].astype(F32) + out_sum).astype(BF)

    in_blocks.arrived()
    g.nacc[...] = jnp.zeros(g.nacc.shape, F32)

    def finish(i):
        at = cut(i * 64, 64, 16)
        v = g.own_in[at, :]
        for k in range(3):
            v = v + g.rblk2[k, at, :].astype(F32)
        g.own_in[at, :] = v
        x = g.x[at, :].astype(F32)
        g.part[0, at, :] = lanes_sum(v * gain * x)
        g.nacc[...] += rows_sum(v * x * wide_of(g.xscale[at, :], 3))

    loop(ROWS // 64, finish)
    g.nstat[z] = to_row(g.part[0])
    nst = [send(g.nstat.at[z], g.nstat.at[z], g.nsem, i, p) for i, p in enumerate(zpeers)]
    g.ngain[0] = jnp.sum(g.nacc[...], axis=0, keepdims=True)
    ngs = [send(g.ngain.at[0], g.ngain.at[1 + i], g.nsem, 3 + i, p) for i, p in enumerate(speers)]
    t_xa.s4()
    across_x.wait_recv()
    g.q_mid[...] = (g.q_out[...].astype(F32) + g.q_in[0].astype(F32)).astype(BF)
    across_y = send(g.q_mid, g.q_in.at[1], g.restsem, 2, {ALONG: s + 4 - 8 * me[2]})
    t_xb.s4()
    t_out.s5()
    t_xa.s5()
    t_z.s5()
    t_xb.s5()
    across_y.wait_recv()
    g.rest[core] = g.q_mid[...].astype(F32) + g.q_in[1].astype(F32)
    q_last = send(g.rest.at[core], g.rest.at[core], g.restsem, 3, partner)
    t_out.s6()
    store = [pltpu.make_async_copy(g.p_out, g.grad_out, g.load_sem.at[5])]
    store[0].start()
    t_z.s6()
    store.append(pltpu.make_async_copy(g.p_z, g.grad_z, g.load_sem.at[6]))
    store[1].start()
    for d in nst:
        d.wait_recv()
    rows = g.nstat[0] + g.nstat[1] + g.nstat[2] + g.nstat[3]
    g.part[0] = to_col(rows / D)

    def last(i):
        at = cut(i * 64, 64, 16)
        sc = wide_of(g.xscale[at, :], 3)
        x = g.x[at, :].astype(F32)
        g.grad_in[at, :] = (
            g.cotg[at, own].astype(F32)
            + sc * (g.own_in[at, :] * gain)
            - x * (sc * sc * sc * wide_of(g.part[0, at, :], 3))
        )

    loop(ROWS // 64, last)
    for d in ngs:
        d.wait_recv()
    total = g.ngain[0]
    for i in range(7):
        total = total + g.ngain[1 + i]
    g.grad_gain[...] = jnp.broadcast_to(total, (8, BLOCK))
    q_last.wait_recv()
    for i, (t, ref) in enumerate(((t_xa, g.p_xa), (t_xb, g.p_xb))):
        t.s6()
        rows_of = pl.ds(CHANNELS * i, CHANNELS)
        store.append(pltpu.make_async_copy(ref, g.grad_x.at[rows_of], g.load_sem.at[7 + i]))
        store[-1].start()
    for d in pending:
        d.wait_send()

    @pl.when(s < SEQ - 1)
    def _():
        edge.wait_send()

    @pl.when(s > 0)
    def _():
        ret.wait_send()

    x_own[0].wait_send()

    @pl.when(middle)
    def _():
        x_own[1].wait_send()

    for inside_it, d in later:
        @pl.when(inside_it)
        def _():
            d.wait_send()

    out_blocks.left()
    in_blocks.left()
    for d in store:
        d.wait()


def unpack_kernel(
    layer_hbm, in_hbm, out_low, z_low, x_low, rest, gain_sum,
    layer_out, grad_in, gain, w_z, w_x, w_bc, w_dt, conv_x_w, conv_x_b, conv_bc_w, conv_bc_b, dt_bias, a_log, d_skip, gate_gain, w_out,
    low_a, low_b, low_c, full_a, full_b, full_c, keep_a, keep_b, in_sem, out_sem,
):
    steps = 6
    mats = [(out_low, low_a, full_a, w_out), (z_low, low_b, full_b, w_z), (x_low, low_c, full_c, w_x)]
    loads, stores = [], []
    for m, (src, low, _, _) in enumerate(mats):
        n = low.shape[0] // steps
        for i in range(steps):
            at = pl.ds(i * n, n)
            loads.append(pltpu.make_async_copy(src.at[at], low.at[at], in_sem.at[steps * m + i]))
    for i, (src, dst) in enumerate([(layer_hbm, keep_a), (in_hbm, keep_b)]):
        loads.append(pltpu.make_async_copy(src, dst, in_sem.at[18 + i]))
    for d in loads:
        d.start()
    for n in range(3):
        gain[n : n + 1, :] = gain_sum[0:1, 128 * n : 128 * n + 128]
    w_bc[0:192, :] = rest[0, 0:192, :]
    w_bc[192:BLOCK, :] = rest[1, 0:192, :]
    for n in range(6):
        w_dt[:, 256 * n : 256 * n + 256] = rest[0, 192 + 16 * n : 204 + 16 * n, :]
    for n in range(3):
        at, base = pl.ds(256 * n, 256), 192 + 24 * n
        conv_x_w[:, at] = rest[1, base : base + 4, :]
        for e in range(2):
            lanes, to = pl.ds(128 * e, 128), pl.ds(2 * n + e, 1)
            conv_x_b[to, :] = rest[1, base + 4 : base + 5, lanes]
            gate_gain[to, :] = rest[1, base + 5 : base + 6, lanes]
    conv_bc_w[...] = rest[1, 200:204, :]
    for e in range(2):
        conv_bc_b[e : e + 1, :] = rest[1, 204:205, 128 * e : 128 * e + 128]
    dt_bias[...] = rest[1, 208:209, 0:12]
    a_log[...] = rest[1, 208:209, 128:140]
    d_skip[...] = rest[1, 232:233, 0:12]
    for m, (_, low, full, dst) in enumerate(mats):
        n = low.shape[0] // steps
        for i in range(steps):
            loads[steps * m + i].wait()
            at = pl.ds(i * n, n)
            full[at, :] = low[at, :].astype(F32)
            stores.append(pltpu.make_async_copy(full.at[at], dst.at[at], out_sem.at[steps * m + i]))
            stores[-1].start()
    for i, (src, dst) in enumerate([(keep_a, layer_out), (keep_b, grad_in)]):
        loads[18 + i].wait()
        stores.append(pltpu.make_async_copy(src, dst, out_sem.at[18 + i]))
        stores[-1].start()
    for d in stores:
        d.wait()


def fast_layer(
    hidden_in, seq_lengths, norm_gain, w_z, w_x, w_bc, w_dt, conv_x_w, conv_x_b, conv_bc_w,
    conv_bc_b, dt_bias, a_log, d_skip, gate_gain, w_out, cotangent,
):
    row = lambda v: v.reshape(-1, min(128, v.shape[0]))
    vm = pl.BlockSpec(memory_space=pltpu.VMEM)
    hbm = pl.BlockSpec(memory_space=pltpu.HBM)
    sm = pl.BlockSpec(memory_space=pltpu.SMEM)
    ins = dict(
        x_hbm=(hidden_in, hbm), cot_hbm=(cotangent, hbm), w_x=(w_x, hbm), w_z=(w_z, hbm), w_out=(w_out, hbm),
        lengths=(seq_lengths, sm), norm_gain=(row(norm_gain), vm), conv_x_b=(row(conv_x_b), vm),
        conv_bc_b=(row(conv_bc_b), vm), dt_bias=(row(dt_bias), vm), a_log=(row(a_log), vm), d_skip=(row(d_skip), vm),
        gate_gain=(row(gate_gain), vm), w_bc=(w_bc, vm), w_dt=(w_dt.T, vm),
        conv_x_w=(conv_x_w, vm), conv_bc_w=(conv_bc_w, vm),
    )
    outs = dict(
        layer_out=((ROWS, BLOCK), BF, vm),
        grad_in=((ROWS, BLOCK), F32, vm),
        grad_out=((CHANNELS, D), BF, hbm),
        grad_z=((D, CHANNELS), BF, hbm),
        grad_x=((D, CHANNELS), BF, hbm),
        rest=((2, 288, 256), F32, vm),
        grad_gain=((8, BLOCK), F32, vm),
    )
    V = pltpu.VMEM
    S = pltpu.SemaphoreType.DMA
    scr = dict(
        x=V((ROWS, BLOCK), BF),
        wx=V((D, CHANNELS), BF),
        wz=V((D, CHANNELS), BF),
        wo=V((CHANNELS, D), BF),
        xg=V((ROWS, D), BF),
        xn=V((ROWS, D), BF),
        cotg=V((ROWS, D), BF),
        ssq=V((LINE, 1, ROWS), F32),
        gains=V((LINE, 1, BLOCK), F32),
        wbc=V((LINE, BLOCK, 256), BF),
        wd=V((128, D), BF),
        params=V((8, CHANNELS), F32),
        taps=V((8, WIDE), F32),
        spread=V((256, CHANNELS), BF),
        segc=V((ROWS + HALO, 128), F32),
        segr=V((8, ROWS), F32),
        tri=V((SPAN, SPAN), BF),
        skipe=V((8, CHANNELS), F32),
        xscale=V((ROWS, 128), F32),
        acc=V((ROWS, WIDE + CHANNELS + 128), F32),
        edge=V((HALO, WIDE), BF),
        halo=V((HALO, WIDE), BF),
        cf=V((ROWS + HALO, WIDE), F32),
        step=V((ROWS, 128), F32),
        cum=V((ROWS, 128), F32),
        cumt=V((2, 16, SPAN), F32),
        tail=V((ROWS, 128), F32),
        load=V((ROWS, 128), F32),
        lead=V((ROWS, 128), F32),
        carry=V((2, 8, 128), F32),
        carrye=V((2, 8, CHANNELS), F32),
        decay=V((2, 8, CHANNELS), F32),
        slope=V((ROWS + 16, WIDE), F32),
        inner=V((ROWS, CHANNELS), BF),
        b=V((ROWS, 128), BF),
        c=V((ROWS, 128), BF),
        bt=V((STATE, ROWS), F32),
        ct=V((STATE, ROWS), F32),
        loadt=V((2, 16, SPAN), F32),
        leadt=V((2, 16, SPAN), F32),
        stept=V((2, 16, SPAN), F32),
        local=V((2, STATE, CHANNELS), F32),
        mine=V((STATE, CHANNELS), F32),
        other=V((STATE, CHANNELS), F32),
        joined=V((STATE, BLOCK), F32),
        got=V((2, STATE, BLOCK), F32),
        chain=V((STATE, CHANNELS), F32),
        mine_b=V((STATE, CHANNELS), F32),
        other_b=V((STATE, CHANNELS), F32),
        joined_b=V((STATE, BLOCK), F32),
        got_b=V((2, STATE, BLOCK), F32),
        chain_b=V((STATE, CHANNELS), F32),
        both=V((8, BLOCK), F32),
        boths=V((2, 8, BLOCK), F32),
        scores=V((SPAN, SPAN), F32),
        gscores=V((SPAN, SPAN), F32),
        out=V((ROWS, CHANNELS), F32),
        sin=V((2, STATE, CHANNELS), F32),
        slow=V((2, STATE, CHANNELS), BF),
        gated=V((ROWS, CHANNELS), F32),
        part=V((2, ROWS, 128), F32),
        stats=V((LINE, 2, ROWS), F32),
        vacc=V((2, 8, CHANNELS), F32),
        gm=V((ROWS, CHANNELS), BF),
        gloc=V((2, STATE, CHANNELS), F32),
        sblk=V((3, ROWS, BLOCK), BF),
        rblk=V((3, ROWS, BLOCK), BF),
        rblk2=V((3, ROWS, BLOCK), BF),
        gsr=V((ROWS, 128), BF),
        pack=V((24, CHANNELS), F32),
        ret_out=V((8, WIDE), F32),
        ret_in=V((8, WIDE), F32),
        wacc=V((5, 8, WIDE), F32),
        gbc=V((2, ROWS, 256), BF),
        tail_rows=V((16, WIDE), F32),
        sbc=V((LINE, BLOCK, 256), BF),
        hbc=V((LINE, 192, 256), BF),
        rbc=V((3, 192, 256), BF),
        via=V((ROWS, BLOCK), BF),
        via2=V((ROWS, BLOCK), BF),
        bcv=V((LINE, 8, 256), F32),
        nacc=V((8, BLOCK), F32),
        nstat=V((LINE, 1, ROWS), F32),
        ngain=V((8, 1, BLOCK), F32),
        p_out=V((CHANNELS, D), BF),
        p_z=V((D, CHANNELS), BF),
        p_xa=V((CHANNELS, CHANNELS), BF),
        p_xb=V((CHANNELS, CHANNELS), BF),
        bcsum=V((192, 256), F32),
        few=V((192, 256), F32),
        few_in=V((192, 256), F32),
        q_out=V((288, 256), BF),
        q_mid=V((288, 256), BF),
        q_in=V((2, 288, 256), BF),
        load_sem=S((9,)),
        edge_sem=S((4,)),
        gather_s=S((8,)),
        gather_r=S((9,)),
        block_s=S((8,)),
        block_r=S((8,)),
        st_send=S((11,)),
        st_recv=S((11,)),
        tot_send=S((40,)),
        tot_recv=S((40,)),
        freed=pltpu.SemaphoreType.REGULAR((12,)),
    )
    pairs = dict(
        small=9,
        wide=4,
        stat=3,
        bcsem=4,
        restsem=4,
        bcvsem=3,
        nsem=10,
    )
    sums = [(CHANNELS, D, BF), (D, CHANNELS, BF), (CHANNELS, CHANNELS, BF), (CHANNELS, CHANNELS, BF)]
    bufs = [b for spec in sums for b in total_bufs(*spec)]
    sems = [S((k,)) for k in pairs.values() for _ in range(2)]
    names = [*ins, *outs, *scr]

    def kernel(*refs):
        n, m = len(names), len(names) + len(bufs)
        d = dict(zip(names, refs[:n]))
        rest = refs[m:]
        for i, name in enumerate(pairs):
            d[name] = (rest[2 * i], rest[2 * i + 1])
        layer_kernel(d, refs[n:m])

    res = pl.pallas_call(
        kernel,
        out_shape=[jax.ShapeDtypeStruct(sh, dt) for sh, dt, _ in outs.values()],
        in_specs=[sp for _, sp in ins.values()],
        out_specs=[sp for _, _, sp in outs.values()],
        scratch_shapes=[*scr.values(), *bufs, *sems],
        compiler_params=pltpu.CompilerParams(collective_id=0, has_side_effects=True, vmem_limit_bytes=66 * 2**20 - 2**21),
        name="layer",
    )(*[a for a, _ in ins.values()])
    layer_out, grad_in, grad_out, grad_z, grad_x, rest, grad_gain = res
    shapes = dict(
        layer_out=((ROWS, BLOCK), BF, hbm), grad_in=((ROWS, BLOCK), F32, hbm), gain=((3, 128), F32, vm), w_z=((D, CHANNELS), F32, hbm),
        w_x=((D, CHANNELS), F32, hbm), w_bc=((BLOCK, 256), F32, vm), w_dt=((12, D), F32, vm), conv_x_w=((4, CHANNELS), F32, vm),
        conv_x_b=((6, 128), F32, vm), conv_bc_w=((4, 256), F32, vm), conv_bc_b=((2, 128), F32, vm), dt_bias=((1, 12), F32, vm),
        a_log=((1, 12), F32, vm), d_skip=((1, 12), F32, vm), gate_gain=((6, 128), F32, vm), w_out=((CHANNELS, D), F32, hbm),
    )
    final = pl.pallas_call(
        unpack_kernel,
        out_shape=[jax.ShapeDtypeStruct(sh, dt) for sh, dt, _ in shapes.values()],
        in_specs=[hbm] * 5 + [vm] * 2,
        out_specs=[sp for _, _, sp in shapes.values()],
        scratch_shapes=[
            V((CHANNELS, D), BF), V((D, CHANNELS), BF), V((D, CHANNELS), BF),
            V((CHANNELS, D), F32), V((D, CHANNELS), F32), V((D, CHANNELS), F32),
            V((ROWS, BLOCK), BF), V((ROWS, BLOCK), F32), S((20,)), S((20,)),
        ],
        compiler_params=pltpu.CompilerParams(vmem_limit_bytes=63 * 2**20),
    )(layer_out, grad_in, grad_out, grad_z, grad_x, rest, grad_gain)
    flat = [v.reshape(v.size) if v.shape[1] <= 128 else v for v in final]
    flat[6] = flat[6].T
    return tuple(flat)


def solution(mesh):
    placed = (
        P("seq", "head"),
        P(),
        P("head"),
        P(None, "head"),
        P(None, "head"),
        P("head", None),
        P(None, "head"),
        P(None, "head"),
        P("head"),
        P(),
        P(),
        P("head"),
        P("head"),
        P("head"),
        P("head"),
        P("head", None),
        P("seq", "head"),
    )
    fits = mesh.shape["seq"] == SEQ and mesh.shape["head"] == LINE
    return jax.shard_map(
        fast_layer if fits else on_device,
        mesh=mesh,
        in_specs=placed,
        out_specs=(
            P("seq", "head"),
            P("seq", "head"),
            P("head"),
            P(None, "head"),
            P(None, "head"),
            P("head", None),
            P(None, "head"),
            P(None, "head"),
            P("head"),
            P(),
            P(),
            P("head"),
            P("head"),
            P("head"),
            P("head"),
            P("head", None),
        ),
        check_vma=False,
    )
```

```python
import jax
import jax.numpy as jnp
from jax import lax
from jax.experimental import pallas as pl
from jax.experimental.pallas import tpu as pltpu
from jax.sharding import PartitionSpec as P

D = 1536
HEAD_DIM = 64
STATE = 128
CONV = 4
SPAN = 256
INNER = 3072


epsilon = 1e-05
highest = lax.Precision.HIGHEST


def prefix(part, axis, combine, identity, reverse):
    count = lax.axis_size(axis)
    place = lax.axis_index(axis)
    ahead = count - 1 - place if reverse else place
    gathered = jax.tree.map(lambda a: lax.all_gather(a, axis), part)
    state = jax.tree.map(lambda a, e: jnp.zeros_like(a) + jnp.asarray(e, a.dtype), part, identity)

    def one(hop, state):
        source = count - 1 - hop if reverse else hop
        return combine(
            state, jax.tree.map(lambda a: lax.dynamic_index_in_dim(a, source, 0, False), gathered)
        )

    return lax.fori_loop(0, ahead, one, state)


def passed_along(block, axis, distance):
    devices = range(lax.axis_size(axis))
    route = [(i - distance, i) for i in devices if i - distance in devices]
    return lax.ppermute(block, axis, route)


def segment_of(positions, starts):
    return jnp.sum((positions[:, None] >= starts[None, :]).astype(jnp.int32), axis=1) - 1


def silu_slope(values):
    sigmoid_val = jax.nn.sigmoid(values)
    return sigmoid_val * (1.0 + values * (1.0 - sigmoid_val))


def chain_join(earlier, later):
    return (earlier[0] * later[0], earlier[1] * later[0][:, None, None] + later[1])


def state_prefix(decay, summary, backwards):
    identity = (jnp.ones_like(decay), jnp.zeros_like(summary))
    result = prefix((decay, summary), "seq", chain_join, identity, backwards)
    return result[1]


def span_terms(span_item, lower_tri):
    inner_c, b_rows, c_rows, step_c, cumul_c, seg_rows, seg_prev = span_item
    same_seq = ((seg_rows[:, None] == seg_rows[None, :]) & (lower_tri > 0.5))[None, :, :]
    spread = cumul_c[:, :, None] - cumul_c[:, None, :]
    decay_mat = jnp.where(same_seq, jnp.exp(jnp.where(same_seq, spread, 0.0)), 0.0)
    scores = lax.dot_general(
        c_rows, b_rows, (((1,), (1,)), ((), ())), preferred_element_type=jnp.float32
    )
    mixing = scores[None, :, :] * decay_mat * step_c[:, None, :]
    last_cum = cumul_c[:, SPAN - 1]
    tail_weight = (
        jnp.exp(last_cum[:, None] - cumul_c)
        * (seg_rows == seg_rows[SPAN - 1]).astype(jnp.float32)[None, :]
    )
    head_weight = jnp.exp(cumul_c) * (seg_rows == seg_prev).astype(jnp.float32)[None, :]
    carry_decay = jnp.exp(last_cum) * (seg_rows[SPAN - 1] == seg_prev).astype(jnp.float32)
    return (decay_mat, scores, mixing, tail_weight, head_weight, carry_decay)


def on_device(
    hidden_in,
    seq_lengths,
    norm_gain,
    w_z,
    w_x,
    w_bc,
    w_dt,
    conv_x_w,
    conv_x_b,
    conv_bc_w,
    conv_bc_b,
    dt_bias,
    a_log,
    d_skip,
    gate_gain,
    w_out,
    cotangent,
):
    tokens_here = hidden_in.shape[0]
    heads_here = dt_bias.shape[0]
    inner_here = w_z.shape[1]
    spans = tokens_here // SPAN
    first_pos = lax.axis_index("seq") * tokens_here
    starts = jnp.cumsum(seq_lengths) - seq_lengths
    segment = segment_of(first_pos + jnp.arange(tokens_here, dtype=jnp.int32), starts)
    edge_segment = segment_of(
        first_pos - (CONV - 1) + jnp.arange(CONV - 1, dtype=jnp.int32), starts
    )
    span_prev = segment_of(first_pos - 1 + jnp.arange(spans, dtype=jnp.int32) * SPAN, starts)
    row_ids = jnp.arange(SPAN)
    lower_tri = (row_ids[:, None] >= row_ids[None, :]).astype(jnp.float32)
    inputs = hidden_in.astype(jnp.float32)
    squares = lax.psum(jnp.sum(inputs * inputs, axis=1), "head")
    scale_in = lax.rsqrt(squares / D + epsilon)
    normed = (inputs * scale_in[:, None] * norm_gain).astype(jnp.bfloat16)
    gathered, bc_weight = (
        lax.all_gather(normed, "head", axis=1, tiled=True),
        lax.all_gather(w_bc, "head", axis=0, tiled=True),
    )
    gate_pre = jnp.dot(gathered, w_z, preferred_element_type=jnp.float32)
    x_part = jnp.dot(gathered, w_x, preferred_element_type=jnp.float32)
    bc_part = jnp.dot(gathered, bc_weight, preferred_element_type=jnp.float32)
    conv_in = jnp.concatenate([x_part, bc_part], axis=1).astype(jnp.bfloat16)
    step_raw = jnp.dot(gathered, w_dt, preferred_element_type=jnp.float32)
    edge_rows = passed_along(conv_in[tokens_here - (CONV - 1) :], "seq", 1)
    padded = jnp.concatenate([edge_rows, conv_in], axis=0).astype(jnp.float32)
    seg_padded = jnp.concatenate([edge_segment, segment])
    conv_weight = jnp.concatenate([conv_x_w, conv_bc_w], axis=1)
    conv_bias = jnp.concatenate([conv_x_b, conv_bc_b])
    tap_masks = [
        (seg_padded[offset : offset + tokens_here] == segment).astype(jnp.float32)[:, None]
        for offset in range(CONV)
    ]
    conv_out = jnp.zeros(conv_in.shape, jnp.float32) + conv_bias[None, :]
    for offset in range(CONV):
        conv_out = (
            conv_out
            + conv_weight[offset] * padded[offset : offset + tokens_here] * tap_masks[offset]
        )
    activated = jax.nn.silu(conv_out)
    inner_vals = activated[:, :inner_here].astype(jnp.bfloat16)
    b_vals = activated[:, inner_here : inner_here + STATE].astype(jnp.bfloat16)
    c_vals = activated[:, inner_here + STATE :].astype(jnp.bfloat16)
    step_pre = step_raw + dt_bias
    step_size = jax.nn.softplus(step_pre)
    rates = jnp.exp(a_log)
    log_decay = -rates * step_size
    decay_heads = log_decay.reshape(spans, SPAN, heads_here).transpose(0, 2, 1)
    step_heads = step_size.reshape(spans, SPAN, heads_here).transpose(0, 2, 1)
    cumul = jnp.einsum("ij,chj->chi", lower_tri, decay_heads, precision=highest)
    inner_spans = inner_vals.reshape(spans, SPAN, heads_here, HEAD_DIM).transpose(0, 2, 1, 3)
    c_spans = c_vals.reshape(spans, SPAN, STATE)
    per_span = (
        inner_spans,
        b_vals.reshape(spans, SPAN, STATE),
        c_spans,
        step_heads,
        cumul,
        segment.reshape(spans, SPAN),
        span_prev,
    )

    def forward_span(span_item):
        decay_mat, scores, mixing, tail_weight, head_weight, carry_decay = span_terms(
            span_item, lower_tri
        )
        inner_c = span_item[0]
        y_inside = jnp.einsum(
            "hij,hjp->hip", mixing.astype(jnp.bfloat16), inner_c, preferred_element_type=jnp.float32
        )
        loaded = (
            span_item[1].astype(jnp.float32)[None, :, :] * (tail_weight * span_item[3])[:, :, None]
        ).astype(jnp.bfloat16)
        local_state = jnp.einsum(
            "hjn,hjp->hnp", loaded, inner_c, preferred_element_type=jnp.float32
        )
        return (y_inside, local_state, carry_decay, head_weight)

    y_inside, local_states, carry_decay, head_weight = lax.map(forward_span, per_span)

    def advance(state_carry, span_item):
        running, factor = state_carry
        local_c, decay_c = span_item
        return ((decay_c[:, None, None] * running + local_c, decay_c * factor), (running, factor))

    zero_state = jnp.zeros((heads_here, STATE, HEAD_DIM), jnp.float32)
    unit_decay = jnp.ones((heads_here,), jnp.float32)
    (device_state, device_decay), (local_in, local_factor) = lax.scan(
        advance, (zero_state, unit_decay), (local_states, carry_decay)
    )
    incoming = state_prefix(device_decay, device_state, False)
    state_in = local_in + local_factor[:, :, None, None] * incoming
    state_low = state_in.astype(jnp.bfloat16)
    c_weighted = (c_spans.astype(jnp.float32)[:, None, :, :] * head_weight[:, :, :, None]).astype(
        jnp.bfloat16
    )
    y_outside = jnp.einsum(
        "chin,chnp->chip", c_weighted, state_low, preferred_element_type=jnp.float32
    )
    skip_rep = jnp.repeat(d_skip, HEAD_DIM)
    mixed_out = (y_inside + y_outside).transpose(0, 2, 1, 3).reshape(
        tokens_here, inner_here
    ) + inner_vals.astype(jnp.float32) * skip_rep
    gate_act = jax.nn.silu(gate_pre)
    gated = mixed_out * gate_act
    gate_squares = lax.psum(jnp.sum(gated * gated, axis=1), "head")
    scale_gate = lax.rsqrt(gate_squares / INNER + epsilon)
    gate_normed = (gated * scale_gate[:, None] * gate_gain).astype(jnp.bfloat16)
    partial_value = jnp.dot(gate_normed, w_out, preferred_element_type=jnp.float32)
    mixed_sum = lax.psum_scatter(partial_value, "head", scatter_dimension=1, tiled=True)
    layer_out = (inputs + mixed_sum).astype(jnp.bfloat16)
    grad_full = lax.all_gather(cotangent, "head", axis=1, tiled=True)
    grad_gate_normed = lax.dot_general(
        grad_full, w_out, (((1,), (1,)), ((), ())), preferred_element_type=jnp.float32
    )
    grad_w_out = lax.dot_general(
        gate_normed, grad_full, (((0,), (0,)), ((), ())), preferred_element_type=jnp.float32
    )
    grad_gate_gain = jnp.sum(grad_gate_normed * gated * scale_gate[:, None], axis=0)
    grad_scaled = grad_gate_normed * gate_gain
    gate_inner = lax.psum(jnp.sum(grad_scaled * gated, axis=1), "head")
    grad_gated = (
        scale_gate[:, None] * grad_scaled - gated * (scale_gate**3 * gate_inner / INNER)[:, None]
    )
    grad_mixed = (grad_gated * gate_act).astype(jnp.bfloat16)
    grad_gate_pre = (grad_gated * mixed_out * silu_slope(gate_pre)).astype(jnp.bfloat16)
    grad_d_skip = jnp.sum(
        (grad_mixed.astype(jnp.float32) * inner_vals.astype(jnp.float32)).reshape(
            tokens_here, heads_here, HEAD_DIM
        ),
        axis=(0, 2),
    )
    grad_spans = grad_mixed.reshape(spans, SPAN, heads_here, HEAD_DIM).transpose(0, 2, 1, 3)
    from_inter = jnp.einsum(
        "chin,chip->chnp", c_weighted, grad_spans, preferred_element_type=jnp.float32
    )

    def retreat(state_carry, span_item):
        running, factor = state_carry
        local_c, decay_c = span_item
        current = local_c + decay_c[:, None, None] * running
        product = decay_c * factor
        return ((current, product), (current, product))

    (device_grad, device_reach), (local_grad, local_reach) = lax.scan(
        retreat, (zero_state, unit_decay), (from_inter, carry_decay), reverse=True
    )
    beyond = state_prefix(device_reach, device_grad, True)
    grad_state_in = local_grad + local_reach[:, :, None, None] * beyond
    grad_local_states = jnp.concatenate([grad_state_in[1:], beyond[None]], axis=0)
    grad_carry_decay = jnp.sum(grad_local_states * state_in, axis=(2, 3))

    def backward_span(span_item):
        span_base = span_item[:7]
        inner_c, b_rows, c_rows, step_c = (span_base[0], span_base[1], span_base[2], span_base[3])
        grad_y, grad_state, state_c, grad_decay = (
            span_item[7],
            span_item[8],
            span_item[9],
            span_item[10],
        )
        decay_mat, scores, mixing, tail_weight, head_weight, carry_decay = span_terms(
            span_base, lower_tri
        )
        grad_mixing = jnp.einsum(
            "hip,hjp->hij", grad_y, inner_c, preferred_element_type=jnp.float32
        )
        grad_inner = jnp.einsum(
            "hij,hip->hjp", mixing.astype(jnp.bfloat16), grad_y, preferred_element_type=jnp.float32
        )
        related = grad_mixing * mixing
        grad_cum = jnp.sum(related, axis=2) - jnp.sum(related, axis=1)
        grad_scores = jnp.sum(grad_mixing * decay_mat * step_c[:, None, :], axis=0)
        grad_step = jnp.sum(grad_mixing * decay_mat * scores[None, :, :], axis=1)
        b_float = b_rows.astype(jnp.float32)
        c_float = c_rows.astype(jnp.float32)
        grad_c = jnp.dot(grad_scores, b_float, precision=highest)
        grad_b = lax.dot_general(grad_scores, c_float, (((0,), (0,)), ((), ())), precision=highest)
        loading = tail_weight * step_c
        loaded = (b_float[None, :, :] * loading[:, :, None]).astype(jnp.bfloat16)
        grad_loaded = jnp.einsum(
            "hjp,hnp->hjn", inner_c, grad_state, preferred_element_type=jnp.float32
        )
        grad_inner = grad_inner + jnp.einsum(
            "hjn,hnp->hjp", loaded, grad_state, preferred_element_type=jnp.float32
        )
        grad_loading = jnp.sum(grad_loaded * b_float[None, :, :], axis=2)
        grad_b = grad_b + jnp.einsum("hjn,hj->jn", grad_loaded, loading, precision=highest)
        tail_term = grad_loading * loading
        grad_cum = grad_cum - tail_term
        grad_last = jnp.sum(tail_term, axis=1) + grad_decay * carry_decay
        grad_step = grad_step + grad_loading * tail_weight
        grad_weighted = jnp.einsum(
            "hip,hnp->hin", grad_y, state_c, preferred_element_type=jnp.float32
        )
        grad_head = jnp.sum(grad_weighted * c_float[None, :, :], axis=2)
        grad_c = grad_c + jnp.einsum("hin,hi->in", grad_weighted, head_weight, precision=highest)
        grad_cum = grad_cum + grad_head * head_weight
        grad_cum = grad_cum.at[:, SPAN - 1].add(grad_last)
        grad_log = jnp.einsum("ij,hi->hj", lower_tri, grad_cum, precision=highest)
        return (grad_inner, grad_b, grad_c, grad_step, grad_log)

    back_items = per_span + (
        grad_spans,
        grad_local_states.astype(jnp.bfloat16),
        state_low,
        grad_carry_decay,
    )
    grad_inner_s, grad_b_s, grad_c_s, grad_step_s, grad_log_s = lax.map(backward_span, back_items)
    grad_inner = (
        grad_inner_s.transpose(0, 2, 1, 3).reshape(tokens_here, inner_here)
        + grad_mixed.astype(jnp.float32) * skip_rep
    )
    grad_log_decay = grad_log_s.transpose(0, 2, 1).reshape(tokens_here, heads_here)
    grad_step_total = (
        grad_step_s.transpose(0, 2, 1).reshape(tokens_here, heads_here) - grad_log_decay * rates
    )
    grad_a_log = jnp.sum(grad_log_decay * log_decay, axis=0)
    grad_step_pre = grad_step_total * jax.nn.sigmoid(step_pre)
    grad_dt_bias = jnp.sum(grad_step_pre, axis=0)
    grad_step_raw = grad_step_pre.astype(jnp.bfloat16)
    grad_bc = lax.psum(
        jnp.concatenate(
            [grad_b_s.reshape(tokens_here, STATE), grad_c_s.reshape(tokens_here, STATE)], axis=1
        ),
        "head",
    )
    grad_conv = jnp.concatenate([grad_inner, grad_bc], axis=1) * silu_slope(conv_out)
    grad_conv_bias = jnp.sum(grad_conv, axis=0)
    grad_conv_weight = jnp.stack(
        [
            jnp.sum(grad_conv * padded[offset : offset + tokens_here] * tap_masks[offset], axis=0)
            for offset in range(CONV)
        ]
    )
    grad_padded = jnp.zeros(padded.shape, jnp.float32)
    for offset in range(CONV):
        grad_padded = grad_padded + jnp.pad(
            conv_weight[offset] * grad_conv * tap_masks[offset],
            ((offset, CONV - 1 - offset), (0, 0)),
        )
    returned = passed_along(grad_padded[: CONV - 1], "seq", -1)
    grad_conv_in = (
        grad_padded[CONV - 1 :] + jnp.pad(returned, ((tokens_here - (CONV - 1), 0), (0, 0)))
    ).astype(jnp.bfloat16)
    grad_x_pre = grad_conv_in[:, :inner_here]
    grad_bc_pre = grad_conv_in[:, inner_here:]
    contract_rows = (((0,), (0,)), ((), ()))
    contract_cols = (((1,), (1,)), ((), ()))
    grad_w_z = lax.dot_general(
        gathered, grad_gate_pre, contract_rows, preferred_element_type=jnp.float32
    )
    grad_w_x = lax.dot_general(
        gathered, grad_x_pre, contract_rows, preferred_element_type=jnp.float32
    )
    grad_w_dt = lax.dot_general(
        gathered, grad_step_raw, contract_rows, preferred_element_type=jnp.float32
    )
    grad_w_bc = lax.dot_general(
        normed, grad_bc_pre, contract_rows, preferred_element_type=jnp.float32
    )
    partial_back = lax.dot_general(
        grad_gate_pre, w_z, contract_cols, preferred_element_type=jnp.float32
    )
    partial_back = partial_back + lax.dot_general(
        grad_x_pre, w_x, contract_cols, preferred_element_type=jnp.float32
    )
    partial_back = partial_back + lax.dot_general(
        grad_step_raw, w_dt, contract_cols, preferred_element_type=jnp.float32
    )
    grad_normed = lax.psum_scatter(partial_back, "head", scatter_dimension=1, tiled=True)
    grad_normed = grad_normed + lax.dot_general(
        grad_bc_pre, w_bc, contract_cols, preferred_element_type=jnp.float32
    )
    grad_scaled_in = grad_normed * norm_gain
    grad_norm_gain = jnp.sum(grad_normed * inputs * scale_in[:, None], axis=0)
    norm_inner = lax.psum(jnp.sum(grad_scaled_in * inputs, axis=1), "head")
    grad_in = (
        cotangent.astype(jnp.float32)
        + scale_in[:, None] * grad_scaled_in
        - inputs * (scale_in**3 * norm_inner / D)[:, None]
    )
    summed = lax.psum(
        (
            grad_norm_gain,
            grad_w_z,
            grad_w_x,
            grad_w_bc,
            grad_w_dt,
            grad_conv_weight[:, :inner_here],
            grad_conv_bias[:inner_here],
            grad_conv_weight[:, inner_here:],
            grad_conv_bias[inner_here:],
            grad_dt_bias,
            grad_a_log,
            grad_d_skip,
            grad_gate_gain,
            grad_w_out,
        ),
        "seq",
    )
    return (
        layer_out,
        grad_in,
        summed[0],
        summed[1],
        summed[2],
        summed[3],
        summed[4],
        summed[5],
        summed[6],
        summed[7],
        summed[8],
        summed[9],
        summed[10],
        summed[11],
        summed[12],
        summed[13],
    )


BF = jnp.bfloat16
F32 = jnp.float32
MESH = pl.DeviceIdType.MESH
ROWS = 512
BLOCK = 384
CHANNELS = 768
WIDE = 1024
HALO = 16
SEQ = 8
LINE = 4
ALONG = "seq"
ACROSS = "head"
NN = (((1,), (0,)), ((), ()))
NT = (((1,), (1,)), ((), ()))
TN = (((0,), (0,)), ((), ()))


def mul(a, b, dims=NN):
    return lax.dot_general(a, b, dims, preferred_element_type=F32)


def cut(start, size, mult):
    return pl.ds(pl.multiple_of(start, mult), size)


def parts(v, n):
    out = []
    for _ in range(n):
        p = v.astype(BF)
        out.append(p)
        v = v - p.astype(F32)
    return out


def along_line(z, ends, middles):
    k = jnp.where(lax.rem(z, 3) == 0, ends, middles)
    return jnp.where(z >= 2, 3 - k, k)


def lanes_sum(v):
    total = v[:, 0:128]
    for i in range(1, v.shape[1] // 128):
        total = total + v[:, 128 * i : 128 * i + 128]
    return total


def rows_sum(v):
    return jnp.sum(v.reshape(v.shape[0] // 8, 8, v.shape[1]), axis=0)


def wide_of(v, n):
    return jnp.concatenate([v] * n, axis=1)


def to_row(part):
    return jnp.sum(part.T, axis=0, keepdims=True)


def to_col(row):
    return jnp.broadcast_to(row, (128, row.shape[1])).T


def loop(n, body):
    def run(i, carry):
        body(i)
        return carry

    lax.fori_loop(0, n, run, 0)


def remote(src, dst, send, recv, peer):
    return pltpu.make_async_remote_copy(
        src_ref=src, dst_ref=dst, send_sem=send, recv_sem=recv, device_id=peer, device_id_type=MESH
    )


class Total:
    def __init__(self, whole, bufs, send, recv, freed, base, me):
        self.w = whole
        self.freed, self.slot = freed, 3 * (base // 10)
        self.r0, self.ra, self.rb, self.qa, self.qb = bufs
        self.send, self.recv, self.base = send, recv, base
        self.c, self.x, self.y, self.s = me
        self.rows, self.cols = whole.shape
        self.live, self.left = {}, set()

    def peer(self, bit):
        return {ALONG: self.s + bit - 2 * bit * {1: self.c, 2: self.x, 4: self.y}[bit]}

    def free(self, k, n, bit):
        self.sent(k)
        pl.semaphore_signal(
            self.freed.at[self.slot + n], inc=1, device_id=self.peer(bit), device_id_type=MESH
        )

    def copy(self, k, src, dst, bit):
        d = remote(src, dst, self.send.at[self.base + k], self.recv.at[self.base + k], self.peer(bit))
        d.start()
        self.live[k] = d
        self.left.add(k)

    def wait(self, k):
        self.live[k].wait_recv()

    def sent(self, k):
        self.left.remove(k)
        self.live[k].wait_send()

    def add(self, start, got, rows, col, cols, step):
        def body(i):
            at = (cut(start + i * step, step, 16), pl.ds(col, cols))
            new = self.w[at].astype(F32) + got[cut(i * step, step, 16), :].astype(F32)
            self.w[at] = new.astype(self.w.dtype)

        loop(rows // step, body)

    def s0(self):
        h = self.rows // 2
        self.copy(0, self.w.at[cut((1 - self.c) * h, h, 16)], self.r0, 1)

    def s1(self):
        h, q, m = self.rows // 2, self.rows // 4, self.cols // 2
        base = self.c * h
        self.free(0, 0, 1)
        self.wait(0)
        self.add(base, self.r0, h, 0, self.cols, 32)
        self.copy(1, self.w.at[cut(base + (1 - self.x) * q, q, 16), pl.ds(0, m)], self.ra, 2)
        self.copy(2, self.w.at[cut(base + (1 - self.y) * q, q, 16), pl.ds(m, m)], self.rb, 4)

    def s2(self):
        h, q, e, m = self.rows // 2, self.rows // 4, self.rows // 8, self.cols // 2
        ba = self.c * h + self.x * q
        bb = self.c * h + self.y * q
        self.wait(1)
        self.add(ba, self.ra, q, 0, m, 32)
        self.sent(2)
        self.copy(3, self.w.at[cut(ba + (1 - self.y) * e, e, 16), pl.ds(0, m)], self.qa, 4)
        self.wait(2)
        self.add(bb, self.rb, q, m, m, 32)
        self.sent(1)
        self.copy(4, self.w.at[cut(bb + (1 - self.x) * e, e, 16), pl.ds(m, m)], self.qb, 2)

    def s3(self):
        h, q, e, m = self.rows // 2, self.rows // 4, self.rows // 8, self.cols // 2
        ba = self.c * h + self.x * q + self.y * e
        bb = self.c * h + self.y * q + self.x * e
        self.free(3, 1, 4)
        self.free(4, 2, 2)
        self.wait(3)
        self.add(ba, self.qa, e, 0, m, 16)
        pl.semaphore_wait(self.freed.at[self.slot + 1], 1)
        p = self.w.at[cut(ba, e, 16), pl.ds(0, m)]
        self.copy(5, p, p, 4)
        self.wait(4)
        self.add(bb, self.qb, e, m, m, 16)
        pl.semaphore_wait(self.freed.at[self.slot + 2], 1)
        p = self.w.at[cut(bb, e, 16), pl.ds(m, m)]
        self.copy(6, p, p, 2)

    def s4(self):
        h, q, m = self.rows // 2, self.rows // 4, self.cols // 2
        self.wait(5)
        p = self.w.at[cut(self.c * h + self.x * q, q, 16), pl.ds(0, m)]
        self.copy(7, p, p, 2)
        self.wait(6)
        p = self.w.at[cut(self.c * h + self.y * q, q, 16), pl.ds(m, m)]
        self.copy(8, p, p, 4)

    def s5(self):
        h = self.rows // 2
        self.wait(7)
        self.wait(8)
        pl.semaphore_wait(self.freed.at[self.slot], 1)
        p = self.w.at[cut(self.c * h, h, 16)]
        self.copy(9, p, p, 1)

    def s6(self):
        self.wait(9)
        for k in sorted(self.left):
            self.sent(k)


def total_bufs(rows, cols, kind):
    sizes = [(2, 1), (4, 2), (4, 2), (8, 2), (8, 2)]
    return [pltpu.VMEM((rows // a, cols // b), kind) for a, b in sizes]


class Refs:
    def __init__(self, named):
        self.__dict__.update(named)


def layer_kernel(named, sum_bufs):
    g = Refs(named)
    g.ggn = g.acc.at[:, pl.ds(0, CHANNELS)]
    g.z = g.ggn
    g.gn = g.xg.at[:, pl.ds(0, CHANNELS)]
    g.gz = g.xg.at[:, pl.ds(CHANNELS, CHANNELS)]
    g.gconv = g.slope
    g.gx = g.gm
    g.own_in = g.acc.at[:, pl.ds(0, BLOCK)]
    g.own = g.gated.at[:, pl.ds(0, BLOCK)]
    g.gb = g.gated.at[:, pl.ds(BLOCK, 128)]
    g.gc = g.gated.at[:, pl.ds(BLOCK + 128, 128)]
    s = lax.axis_index(ALONG)
    z = lax.axis_index(ACROSS)
    me = (lax.rem(s, 2), lax.rem(s // 2, 2), s // 4, s)
    zpeers = [{ACROSS: lax.rem(z + d, LINE)} for d in range(1, LINE)]
    speers = [{ALONG: lax.rem(s + d, SEQ)} for d in range(1, SEQ)]

    loads = []
    for i, (src, dst) in enumerate(
        [(g.x_hbm, g.x), (g.w_x, g.wx), (g.w_z, g.wz), (g.cot_hbm, g.cotg.at[:, cut(z * BLOCK, BLOCK, 128)]), (g.w_out, g.wo)]
    ):
        d = pltpu.make_async_copy(src, dst, g.load_sem.at[i])
        d.start()
        loads.append(d)

    g.params[...] = jnp.zeros(g.params.shape, F32)
    vectors = (g.norm_gain, g.conv_x_b, g.conv_bc_b, g.dt_bias, g.a_log, g.d_skip, g.gate_gain)
    for i, v in enumerate(vectors):
        for n in range(v.shape[0]):
            g.params[i : i + 1, 128 * n : 128 * n + v.shape[1]] = v[n : n + 1, :]

    sem = pltpu.get_barrier_semaphore()
    for p in zpeers + speers:
        pl.semaphore_signal(sem, inc=1, device_id=p, device_id_type=MESH)
    pl.semaphore_wait(sem, len(zpeers) + len(speers))

    pending = []

    def send(src, dst, sems, i, peer):
        d = remote(src, dst, sems[0].at[i], sems[1].at[i], peer)
        d.start()
        pending.append(d)
        return d

    loads[0].wait()
    loads[3].wait()
    gain = g.params[0:1, 0:BLOCK]
    xv = g.x[...].astype(F32)
    g.ssq[z] = to_row(lanes_sum(xv * xv))
    g.gains[z] = gain
    core, chip = me[0], s // 2
    partner = {ALONG: s + 1 - 2 * core}
    chips = [{ALONG: lax.rem(s + 2 * d, SEQ)} for d in range(1, 4)]
    piece = cut(48 * (4 * core + chip), 48, 16)
    own = cut(z * BLOCK, BLOCK, 128)
    g.wbc[z, piece, :] = g.w_bc[piece, :]
    small = []
    for i, p in enumerate(zpeers):
        small.append(send(g.ssq.at[z], g.ssq.at[z], g.small, i, p))
        small.append(send(g.gains.at[z], g.gains.at[z], g.small, 3 + i, p))
        small.append(send(g.w_bc.at[piece], g.wbc.at[z, piece], g.small, 6 + i, p))
    middle = lax.rem(z, 3) != 0
    near = [along_line(z, a, b) for a, b in ((1, 2), (2, 0), (3, 3))]

    def block_copy(src, whole, base, slot, k, to):
        cols = cut(k * BLOCK, BLOCK, 128)
        return remote(src, whole.at[:, cols], g.gather_s.at[base + slot], g.gather_r.at[base + k], {ACROSS: to})

    def gather(src, whole, base):
        for j in range(2):
            pending.append(block_copy(src, whole, base, j, z, near[j]))
            pending[-1].start()
        third = block_copy(src, whole, base, 2, z, near[2])

        @pl.when(jnp.logical_not(middle))
        def _():
            third.start()

        return third

    def gathered(src, whole, base, j):
        block_copy(src, whole, base, 0, near[j], z).wait_recv()

    def relay(whole, base):
        part = whole.at[:, cut(near[0] * BLOCK, BLOCK, 128)]

        @pl.when(middle)
        def _():
            block_copy(part, whole, base, 2, near[0], near[1]).start()

    x_own = [block_copy(g.x, g.xg, 0, j, z, near[j]) for j in range(2)]
    x_on = [block_copy(g.xg.at[:, cut(near[j] * BLOCK, BLOCK, 128)], g.xg, 0, 2 + j, near[j], near[1 - j % 2]) for j in range(2)]
    x_on.append(block_copy(g.xg.at[:, cut(near[2] * BLOCK, BLOCK, 128)], g.xg, 0, 4, near[2], near[1]))
    x_own[0].start()

    @pl.when(middle)
    def _():
        x_own[1].start()


    g.wd[...] = jnp.zeros(g.wd.shape, BF)
    g.wd[0:12, :] = g.w_dt[...]
    g.taps[...] = jnp.zeros(g.taps.shape, F32)
    g.taps[0:4, 0:CHANNELS] = g.conv_x_w[...]
    g.taps[0:4, CHANNELS:WIDE] = g.conv_bc_w[...]
    g.taps[4:5, 0:CHANNELS] = g.params[1:2, :]
    g.taps[4:5, CHANNELS:WIDE] = g.params[2:3, 0:256]
    expand_row = lax.broadcasted_iota(jnp.int32, (256, CHANNELS), 0)
    expand_col = lax.broadcasted_iota(jnp.int32, (256, CHANNELS), 1)
    g.spread[...] = jnp.where((expand_col >> 6) == (expand_row & 127), 1.0, 0.0).astype(BF)
    starts = [jnp.int32(0)]
    for k in range(7):
        starts.append(starts[-1] + g.lengths[k])

    def segment(pos):
        total = jnp.full(pos.shape, -1, jnp.int32)
        for k in range(8):
            total = total + jnp.where(pos >= starts[k], 1, 0)
        return total.astype(F32)

    g.segc[...] = segment(
        lax.broadcasted_iota(jnp.int32, (ROWS + HALO, 128), 0) + (s * ROWS - HALO)
    )
    g.segr[...] = segment(lax.broadcasted_iota(jnp.int32, (8, ROWS), 1) + s * ROWS)
    tri_i = lax.broadcasted_iota(jnp.int32, (SPAN, SPAN), 0)
    tri_j = lax.broadcasted_iota(jnp.int32, (SPAN, SPAN), 1)
    g.tri[...] = jnp.where(tri_i >= tri_j, 1.0, 0.0).astype(BF)
    lane = lax.broadcasted_iota(jnp.int32, (1, 128), 1)
    left = lane < 64

    def spread(v):
        hi, lo = parts(v, 2)
        return mul(jnp.concatenate([hi, lo], axis=1), g.spread[...])

    def head_sum(v):
        hi, lo = parts(v, 2)
        e = g.spread[0:128, :]
        return mul(hi, e, NT) + mul(lo, e, NT)

    g.skipe[...] = spread(jnp.broadcast_to(g.params[5:6, 0:128], (8, 128)))
    rates = jnp.exp(g.params[4:5, 0:128])

    for d in small:
        d.wait_recv()
    wide = [
        send(g.wbc.at[:, piece], g.wbc.at[:, piece], g.wide, i, p) for i, p in enumerate(chips)
    ]
    total = g.ssq[0] + g.ssq[1] + g.ssq[2] + g.ssq[3]
    g.xscale[...] = to_col(lax.rsqrt(total / D + epsilon))

    def normalise(k, src):
        gk = g.gains[k]
        cols = cut(k * BLOCK, BLOCK, 128)

        def body(i):
            at = cut(i * 64, 64, 16)
            v = src(at, cols).astype(F32)
            g.xn[at, cols] = (v * wide_of(g.xscale[at, :], 3) * gk).astype(BF)

        loop(ROWS // 64, body)

    def project(k, w, cols, base, first, width=256):
        at = cut(k * BLOCK, BLOCK, 128)

        def body(n):
            p = mul(g.xn[:, at], w[cut(k * BLOCK, BLOCK, 16), cut(n * width, width, 128)])
            dst = cut(base + n * width, width, 128)
            if first:
                g.acc[:, dst] = p
            else:
                g.acc[:, dst] += p

        loop(cols // width, body)

    def project_dt(k, first):
        at = cut(k * BLOCK, BLOCK, 128)
        p = mul(g.xn[:, at], g.wd[:, at], NT)
        if first:
            g.acc[:, WIDE + CHANNELS :] = p
        else:
            g.acc[:, WIDE + CHANNELS :] += p

    normalise(z, lambda at, cols: g.x[at, :])
    loads[1].wait()
    loads[2].wait()
    project(z, g.wx, CHANNELS, 0, True)
    project(z, g.wz, CHANNELS, WIDE, True)
    project_dt(z, True)
    for i, k in enumerate(near):
        if i != 1:
            gathered(g.x, g.xg, 0, i)
        else:
            @pl.when(jnp.logical_not(middle))
            def _():
                gathered(g.x, g.xg, 0, 1)

        if i == 2:
            @pl.when(middle)
            def _():
                x_on[2].start()

        if i == 0:
            @pl.when(middle)
            def _():
                x_on[0].start()
                gathered(g.x, g.xg, 0, 1)
                x_on[1].start()

            for d in wide:
                d.wait_recv()
            share = g.wbc.at[:, cut(192 * core, 192, 16)]
            wide = [send(share, share, g.wide, 3, partner)]
        if i == 2:
            pending.append(gather(g.cotg.at[:, own], g.cotg, 5))
        normalise(k, lambda at, cols: g.xg[at, cols])
        project(k, g.wx, CHANNELS, 0, False)
        if i < 2:
            project(k, g.wz, CHANNELS, WIDE, False)
            project_dt(k, False)
    for d in wide:
        d.wait_recv()
    g.acc[:, CHANNELS:WIDE] = sum(
        mul(g.xn[:, BLOCK * k : BLOCK * k + BLOCK], g.wbc[k]) for k in range(LINE)
    )

    g.edge[...] = g.acc[ROWS - HALO : ROWS, 0:WIDE].astype(BF)
    edge = remote(g.edge, g.halo, g.edge_sem.at[0], g.edge_sem.at[1], {ALONG: s + 1})

    @pl.when(s < SEQ - 1)
    def _():
        edge.start()

    @pl.when(s == 0)
    def _():
        g.halo[...] = jnp.zeros(g.halo.shape, BF)

    def put(i):
        g.cf[cut(HALO + i * 64, 64, 8), :] = (
            g.acc[cut(i * 64, 64, 8), 0:WIDE].astype(BF).astype(F32)
        )

    loop(ROWS // 64, put)
    project(near[2], g.wz, CHANNELS, WIDE, False)
    project_dt(near[2], False)

    step_pre = g.acc[:, WIDE + CHANNELS :] + g.params[3:4, 0:128]
    g.step[...] = jnp.where(lane < 12, jax.nn.softplus(step_pre), 0.0)
    for q in range(2):
        rows = pl.ds(q * SPAN, SPAN)
        log_decay = -rates * g.step[rows, :]
        cum = sum(mul(g.tri[...], p) for p in parts(log_decay, 3))
        g.cum[rows, :] = cum
        g.cumt[q] = cum.T[0:16, :]
        last = cum[SPAN - 1 : SPAN, :]
        seg = g.segc[pl.ds(HALO + q * SPAN, SPAN), :]
        seg_last = g.segc[HALO + q * SPAN + SPAN - 1 : HALO + q * SPAN + SPAN, :]
        seg_prev = g.segc[HALO + q * SPAN - 1 : HALO + q * SPAN, :]
        tail = jnp.where(seg == seg_last, jnp.exp(last - cum), 0.0)
        load = tail * g.step[rows, :]
        lead = jnp.where(seg == seg_prev, jnp.exp(cum), 0.0)
        g.tail[rows, :] = tail
        g.load[rows, :] = load
        g.lead[rows, :] = lead
        g.loadt[q] = load.T[0:16, :]
        g.leadt[q] = lead.T[0:16, :]
        g.stept[q] = g.step[rows, :].T[0:16, :]
        carry = jnp.where(seg_last == seg_prev, jnp.exp(last), 0.0)
        g.carry[q] = jnp.broadcast_to(carry, (8, 128))
        g.carrye[q] = spread(jnp.broadcast_to(carry, (8, 128)))
    g.decay[0] = g.carrye[0] * g.carrye[1]

    def taps_of(first, cols):
        v = g.cf[cut(first + 8, 72, 8), cols]
        sv = g.segc[cut(first + 8, 72, 8), :]
        width = v.shape[1] // 128
        out = []
        for k in range(3):
            same = pltpu.roll(sv, 67 - k, 0)[0:64] == sv[8:72]
            out.append(jnp.where(wide_of(same, width), pltpu.roll(v, 67 - k, 0)[0:64], 0.0))
        out.append(v[8:72])
        return out

    def convolve(i):
        first = i * 64
        at = cut(first, 64, 16)
        for n in range(4):
            cols = pl.ds(n * 256, 256)
            v = jnp.broadcast_to(g.taps[4:5, cols], (64, 256))
            for k, t in enumerate(taps_of(first, cols)):
                v = v + g.taps[k : k + 1, cols] * t
            sig = jax.nn.sigmoid(v)
            act = (v * sig).astype(BF)
            g.slope[at, cols] = sig * (1.0 + v * (1.0 - sig))
            if n < 3:
                g.inner[at, cols] = act
            else:
                g.b[at, :] = act[:, 0:128]
                g.c[at, :] = act[:, 128:256]

    loop(ROWS // 64 - 1, lambda i: convolve(i + 1))

    @pl.when(s > 0)
    def _():
        edge.wait_recv()

    g.cf[0:HALO, :] = g.halo[...].astype(F32)
    convolve(0)

    g.bt[...] = g.b[...].astype(F32).T
    g.ct[...] = g.c[...].astype(F32).T

    def outer(maps, weights, vals):
        def body(t):
            q, p = t // 6, lax.rem(t, 6)
            at = cut(p * 128, 128, 128)
            v = vals[cut(q * SPAN, SPAN, 256), at]
            m = maps[:, cut(q * SPAN, SPAN, 256)]
            o = [mul((m * weights[q, pl.ds(2 * p + e, 1), :]).astype(BF), v) for e in range(2)]
            g.local[q, :, at] = jnp.where(left, o[0], o[1])

        loop(12, body)

    outer(g.bt, g.loadt, g.inner)
    c0, c1 = g.carrye[0][0:1], g.carrye[1][0:1]
    half, rest = cut(core * BLOCK, BLOCK, 128), cut((1 - core) * BLOCK, BLOCK, 128)
    later = []

    class Chain:
        def __init__(self, mine, other, joined, got, result, base, way):
            self.mine, self.other, self.joined, self.got, self.result = mine, other, joined, got, result
            self.base, self.way = base, way
            self.near = self.link(joined, got.at[0], 1, way)
            self.far = self.link(joined, got.at[1], 2, 2 * way)

        def link(self, src, dst, i, hop):
            to = {ALONG: s + 2 * hop}
            return remote(src, dst, g.st_send.at[self.base + i], g.st_recv.at[self.base + i], to)

        def share(self):
            self.first = send(self.mine, self.other, (g.st_send, g.st_recv), self.base, partner)

        def join(self):
            self.first.wait_recv()
            own, other = self.mine[:, half], self.other[:, half]
            even, odd = jnp.where(core == 0, own, other), jnp.where(core == 0, other, own)
            if self.way > 0:
                self.joined[...] = odd_decay() * even + odd
            else:
                self.joined[...] = even + even_decay() * odd
            for d, hop in ((self.near, 1), (self.far, 2)):
                pass_on(d, hop * self.way)
            for i, hop in ((0, 1), (1, 2)):
                outside = chip - hop * self.way

                @pl.when((outside < 0) | (outside > 3))
                def _():
                    self.got[i] = jnp.zeros((STATE, BLOCK), F32)

        def meet(self, decay):
            for d, hop in ((self.near, 1), (self.far, 2)):
                arrive(d, hop * self.way)
            self.result[:, half] = self.got[0] + decay * self.got[1]
            p = self.result.at[:, half]
            self.last = send(p, p, (g.st_send, g.st_recv), self.base + 3, partner)

        def end(self):
            self.last.wait_recv()

    def pass_on(d, hop):
        inside = (chip + hop >= 0) & (chip + hop <= 3)

        @pl.when(inside)
        def _():
            d.start()

        later.append((inside, d))

    def arrive(d, hop):
        @pl.when((chip - hop >= 0) & (chip - hop <= 3))
        def _():
            d.wait_recv()

    def odd_decay():
        return jnp.where(core == 0, g.decay[1, 0:1, half], g.decay[0, 0:1, half])

    def even_decay():
        return jnp.where(core == 0, g.decay[0, 0:1, half], g.decay[1, 0:1, half])

    g.mine[...] = c1 * g.local[0] + g.local[1]
    ahead = Chain(g.mine, g.other, g.joined, g.got, g.chain, 0, 1)
    ahead.share()
    dec = send(g.decay.at[0], g.decay.at[1], (g.st_send, g.st_recv), 8, partner)
    both_up = remote(g.both, g.boths.at[0], g.st_send.at[9], g.st_recv.at[9], {ALONG: s + 2})
    both_down = remote(g.both, g.boths.at[1], g.st_send.at[10], g.st_recv.at[10], {ALONG: s - 2})

    def head_cols(ref, rows, p):
        moved = pltpu.roll(ref[rows, :], lax.rem(128 - 2 * p, 128), 1)
        return moved[:, 0:1], moved[:, 1:2]

    def inside(q, first, count):
        rows = cut(q * SPAN, SPAN, 256)
        seg = g.segc[cut(HALO + q * SPAN, SPAN, 16), 0:1]
        segr = g.segr[0:1, cut(q * SPAN, SPAN, 256)]
        scores = mul(g.c[rows, :], g.b[rows, :], NT)
        g.scores[...] = jnp.where((tri_i >= tri_j) & (seg == segr), scores, 0.0)

        def pair(t):
            p = first + t
            cols = head_cols(g.cum, rows, p)
            at = cut(p * 128, 128, 128)
            outs = []
            for e in range(2):
                row = g.cumt[q, pl.ds(2 * p + e, 1), :]
                step = g.stept[q, pl.ds(2 * p + e, 1), :]
                fall = jnp.exp(jnp.minimum(cols[e] - row, 0.0))
                outs.append(mul((g.scores[...] * fall * step).astype(BF), g.inner[rows, at]))
            g.out[rows, at] = jnp.where(left, outs[0], outs[1])

        loop(count, pair)

    inside(0, 0, 3)
    dec.wait_recv()
    g.both[...] = g.decay[0, :, half] * g.decay[1, :, half]
    ahead.join()
    pass_on(both_up, 1)
    pass_on(both_down, -1)
    for i, hop in ((0, 1), (1, -1)):
        @pl.when((chip - hop < 0) | (chip - hop > 3))
        def _():
            g.boths[i] = jnp.zeros((8, BLOCK), F32)

    inside(0, 3, 3)
    gathered(g.cotg.at[:, own], g.cotg, 5, 0)
    relay(g.cotg, 5)
    inside(1, 0, 6)

    arrive(both_up, 1)
    loads[4].wait()
    gate_gain = g.params[6:7, :]

    def down(k, first):
        at = cut(k * BLOCK, BLOCK, 128)

        def body(n):
            cols = cut(n * 256, 256, 256)
            p = mul(g.cotg[:, at], g.wo[cols, at], NT)
            if first:
                g.ggn[:, cols] = p
            else:
                g.ggn[:, cols] += p

        loop(3, body)

    down(z, True)
    down(near[0], False)
    ahead.meet(g.boths[0, 0:1, :])

    def act(i):
        at = cut(i * 64, 64, 16)
        pre = g.acc[at, gate_cols]
        g.gated[at, :] = pre * jax.nn.sigmoid(pre)

    gate_cols = pl.ds(WIDE, CHANNELS)
    loop(ROWS // 64, act)
    ahead.end()
    from_chips = g.chain[...]
    incoming = jnp.where(core == 0, from_chips, g.other[...] + g.decay[1, 0:1] * from_chips)
    g.sin[0] = incoming
    g.sin[1] = g.local[0] + c0 * incoming
    for q in range(2):
        g.slow[q] = g.sin[q].astype(BF)

    def outside(t):
        q, p = t // 6, lax.rem(t, 6)
        rows, at = cut(q * SPAN, SPAN, 256), cut(p * 128, 128, 128)
        cols = head_cols(g.lead, rows, p)
        cv = g.c[rows, :].astype(F32)
        o = [mul((cv * cols[e]).astype(BF), g.slow[q, :, at]) for e in range(2)]
        g.out[rows, at] += jnp.where(left, o[0], o[1])

    loop(12, outside)

    skip = g.skipe[0:1]

    def gate(i):
        at = cut(i * 64, 64, 16)
        mixed = g.out[at, :] + g.inner[at, :].astype(F32) * skip
        gated = mixed * g.gated[at, :]
        g.gated[at, :] = gated
        g.part[0, at, :] = lanes_sum(gated * gated)

    loop(ROWS // 64, gate)
    g.stats[z, 0:1, :] = to_row(g.part[0])

    for i in (1, 2):
        gathered(g.cotg.at[:, own], g.cotg, 5, i)
        down(near[i], False)

    def inner_part(i):
        at = cut(i * 64, 64, 16)
        g.part[1, at, :] = lanes_sum(g.ggn[at, :] * gate_gain * g.gated[at, :])

    loop(ROWS // 64, inner_part)
    g.stats[z, 1:2, :] = to_row(g.part[1])
    stat = [send(g.stats.at[z], g.stats.at[z], g.stat, i, p) for i, p in enumerate(zpeers)]
    dests = [along_line(z, a, b) for a, b in ((2, 3), (3, 0), (1, 2))]

    class Scatter:
        def __init__(self, sent, got, via, base):
            self.sent, self.got, self.via, self.base = sent, got, via, base

        def copy(self, j, dst, i, to):
            return remote(self.sent[j], dst, g.block_s.at[self.base + j], g.block_r.at[self.base + i], {ACROSS: to})

        def direct(self, j):
            slot = lax.rem(z - dests[j] + 7, 4)
            return self.copy(j, self.got.at[slot], slot, dests[j])

        def block(self, j, value):
            v = value
            if j == 2:
                @pl.when(middle)
                def _():
                    self.copy(0, self.via, 3, z).wait_recv()

                v = v + self.via[...].astype(F32)
            self.sent[j][...] = v.astype(BF)
            if j == 0:
                @pl.when(middle)
                def _():
                    self.direct(0).start()

                @pl.when(jnp.logical_not(middle))
                def _():
                    self.copy(0, self.via, 3, dests[2]).start()
            else:
                self.direct(j).start()

        def arrived(self):
            for i in (0, 2):
                self.copy(0, self.got.at[i], i, z).wait_recv()

            @pl.when(jnp.logical_not(middle))
            def _():
                self.copy(0, self.got.at[1], 1, z).wait_recv()

        def left(self):
            for j in range(3):
                self.copy(j, self.via, 3, z).wait_send()

    blocks = [pl.ds(0, BLOCK), pl.ds(BLOCK, BLOCK)]
    out_blocks = Scatter([g.sblk.at[j] for j in range(3)], g.rblk, g.via, 0)
    in_blocks = Scatter(
        [g.gn.at[:, blocks[0]], g.gn.at[:, blocks[1]], g.inner.at[:, blocks[0]]], g.rblk2, g.via2, 4
    )

    @pl.when(middle)
    def _():
        g.rblk[1] = jnp.zeros((ROWS, BLOCK), BF)
        g.rblk2[1] = jnp.zeros((ROWS, BLOCK), BF)

    @pl.when(jnp.logical_not(middle))
    def _():
        g.via[...] = jnp.zeros((ROWS, BLOCK), BF)
        g.via2[...] = jnp.zeros((ROWS, BLOCK), BF)

    def out_block(k):
        return mul(g.gn[...], g.wo[:, cut(k * BLOCK, BLOCK, 128)])

    for d in stat:
        d.wait_recv()
    sums = g.stats[0] + g.stats[1] + g.stats[2] + g.stats[3]
    gscale = lax.rsqrt(sums[0:1] / INNER + epsilon)
    g.part[0] = to_col(gscale)
    g.part[1] = to_col(gscale * gscale * gscale * sums[1:2] / INNER)
    @pl.when(middle)
    def _():
        for d in x_on:
            d.wait_send()

    g.vacc[...] = jnp.zeros(g.vacc.shape, F32)
    g.pack[...] = jnp.zeros(g.pack.shape, F32)
    g.bcv[z] = jnp.zeros((8, 256), F32)

    def ungate(i):
        at = cut(i * 64, 64, 16)
        a = wide_of(g.part[0, at, :], 6)
        pre = g.acc[at, gate_cols]
        vals = g.inner[at, :].astype(F32)
        mixed = g.out[at, :] + vals * skip
        gated, ggn = g.gated[at, :], g.ggn[at, :]
        g.gn[at, :] = (gated * a * gate_gain).astype(BF)
        gg = a * (ggn * gate_gain) - gated * wide_of(g.part[1, at, :], 6)
        sig = jax.nn.sigmoid(pre)
        gm = (gg * (pre * sig)).astype(BF)
        g.gm[at, :] = gm
        g.gz[at, :] = (gg * mixed * (sig * (1.0 + pre * (1.0 - sig)))).astype(BF)
        g.vacc[0] += rows_sum(ggn * gated * a)
        g.vacc[1] += rows_sum(gm.astype(F32) * vals)

    loop(ROWS // 64, ungate)
    out_blocks.block(0, out_block(dests[0]))
    out_blocks.block(1, out_block(dests[1]))

    outer(g.ct, g.leadt, g.gm)
    g.mine_b[...] = g.local[0] + c0 * g.local[1]
    behind = Chain(g.mine_b, g.other_b, g.joined_b, g.got_b, g.chain_b, 4, -1)
    behind.share()

    t_out, t_z, t_xa, t_xb = [
        Total(ref, sum_bufs[5 * i : 5 * i + 5], g.tot_send, g.tot_recv, g.freed, 10 * i, me)
        for i, ref in enumerate((g.p_out, g.p_z, g.p_xa, g.p_xb))
    ]

    def grad_out(n):
        at = cut(n * 256, 256, 256)
        g.p_out[at, :] = mul(g.gn[:, at], g.cotg[...], TN).astype(BF)

    loop(3, grad_out)
    behind.join()
    t_out.s0()

    def grad_z(n):
        at = cut(n * 256, 256, 256)
        g.p_z[at, :] = mul(g.xn[:, at], g.gz[...], TN).astype(BF)

    loop(6, grad_z)
    t_z.s0()
    t_out.s1()

    t_z.s1()
    g.own[...] = mul(g.gn[...], g.wo[:, own])

    def inside_back(q, first, count):
        rows = cut(q * SPAN, SPAN, 256)
        seg = g.segc[cut(HALO + q * SPAN, SPAN, 16), 0:1]
        segr = g.segr[0:1, cut(q * SPAN, SPAN, 256)]
        mask = (tri_i <= tri_j) & (seg == segr)
        if first == 0:
            g.scores[...] = jnp.where(mask, mul(g.b[rows, :], g.c[rows, :], NT), 0.0)
            g.gscores[...] = jnp.zeros((SPAN, SPAN), F32)

        def pair(t):
            p = first + t
            cols = head_cols(g.cum, rows, p)
            at = cut(p * 128, 128, 128)
            steps = head_cols(g.step, rows, p)
            gm = g.gm[rows, at]
            outs = []
            for e in range(2):
                row = g.cumt[q, pl.ds(2 * p + e, 1), :]
                fall = jnp.exp(jnp.minimum(row - cols[e], 0.0)) * steps[e]
                outs.append(mul((g.scores[...] * fall).astype(BF), gm))
                keep = left if e == 0 else jnp.logical_not(left)
                vals = jnp.where(keep, g.inner[rows, at].astype(F32), 0.0).astype(BF)
                g.gscores[...] += mul(vals, gm, NT) * fall
            g.z[rows, at] = jnp.where(left, outs[0], outs[1])

        loop(count, pair)
        if first + count < 6:
            return
        gs = jnp.where(mask, g.gscores[...], 0.0)
        hi, lo = parts(gs, 2)
        g.gb[rows, :] = mul(hi, g.c[rows, :]) + mul(lo, g.c[rows, :])
        g.gc[rows, :] = mul(hi, g.b[rows, :], TN) + mul(lo, g.b[rows, :], TN)

    inside_back(1, 0, 6)
    arrive(both_down, -1)
    behind.meet(g.boths[1, 0:1, :])
    inside_back(0, 0, 3)
    inside_back(0, 3, 3)

    behind.end()
    from_chips = g.chain_b[...]
    beyond = jnp.where(core == 1, from_chips, g.other_b[...] + g.decay[1, 0:1] * from_chips)
    g.gloc[1] = beyond
    g.gloc[0] = g.local[1] + c1 * beyond
    ends = []
    for q in range(2):
        rows = pl.ds(q * SPAN, SPAN)
        glow = g.gloc[q].astype(BF)
        vals = g.inner[rows, :].astype(F32)
        gm = g.gm[rows, :].astype(F32)
        loade = spread(g.load[rows, :])
        bg = mul(g.b[rows, :], glow)
        zed = g.z[rows, :]
        carry_sum = jnp.sum(g.gloc[q] * g.sin[q], axis=0, keepdims=True)
        grad_carry = head_sum(jnp.broadcast_to(carry_sum, (8, CHANNELS)))[0:1]
        t1 = head_sum(gm * g.out[rows, :])
        q1 = head_sum(vals * zed)
        q2 = head_sum(vals * bg)
        step, load = g.step[rows, :], g.load[rows, :]
        tail_term = q2 * load
        gcum = t1 - q1 - tail_term
        end = jnp.sum(tail_term, axis=0, keepdims=True) + grad_carry * g.carry[q][0:1]
        is_last = lax.broadcasted_iota(jnp.int32, (SPAN, 128), 0) == SPAN - 1
        gcum = gcum + jnp.where(is_last, end, 0.0)
        glog = sum(mul(g.tri[...], p, TN) for p in parts(gcum, 3))
        gstep = jnp.where(step > 1e-30, q1 / jnp.maximum(step, 1e-30), 0.0) + q2 * g.tail[rows, :]
        gpre = (gstep - rates * glog) * jax.nn.sigmoid(
            g.acc[rows, WIDE + CHANNELS :] + g.params[3:4, 0:128]
        )
        g.gsr[rows, :] = gpre.astype(BF)
        ends.append((rows_sum(gpre), rows_sum(glog * (-rates * step))))
        g.z[rows, :] = zed + loade * bg + skip * gm
        g.gb[rows, :] += sum(mul(p, glow, NT) for p in parts(vals * loade, 2))
        g.gc[rows, :] += sum(mul(p, g.slow[q], NT) for p in parts(gm * spread(g.lead[rows, :]), 2))
        if q == 0:
            t_out.s2()
            out_blocks.block(2, out_block(dests[2]))
    g.pack[16:24, 0:128] = jnp.broadcast_to(
        jnp.sum(ends[0][0] + ends[1][0], axis=0, keepdims=True), (8, 128)
    )
    g.pack[16:24, 128:256] = jnp.broadcast_to(
        jnp.sum(ends[0][1] + ends[1][1], axis=0, keepdims=True), (8, 128)
    )
    def grads_of(at, n):
        cols = pl.ds(n * 256, 256)
        if n < 3:
            v = g.z[at, cols]
        else:
            v = jnp.concatenate([g.gb[at, :], g.gc[at, :]], axis=1)
        return v * g.slope[at, cols]

    def slopes(i):
        at = cut(i * 64, 64, 16)
        for n in range(4):
            g.gconv[cut(i * 64, 64, 8), pl.ds(n * 256, 256)] = grads_of(at, n)

    g.gconv[ROWS : ROWS + 16, :] = jnp.zeros((16, WIDE), F32)
    loop(ROWS // 64, slopes)

    v = g.gconv[0:8, :]
    sv = g.segc[HALO - 8 : HALO + 8, :]
    back_rows = jnp.zeros((8, WIDE), F32)
    for k in range(3):
        shift = 3 - k
        full = jnp.concatenate([jnp.zeros((8, WIDE), F32), v], axis=0)
        src = pltpu.roll(full, 16 - shift, 0)[0:8]
        same = pltpu.roll(sv, 16 - shift, 0)[0:8] == sv[0:8]
        back_rows = back_rows + jnp.where(wide_of(same, 8), g.taps[k : k + 1, :] * src, 0.0)
    g.ret_out[...] = back_rows
    ret = remote(g.ret_out, g.ret_in, g.edge_sem.at[2], g.edge_sem.at[3], {ALONG: s - 1})

    @pl.when(s > 0)
    def _():
        ret.start()

    @pl.when(s == SEQ - 1)
    def _():
        g.ret_in[...] = jnp.zeros((8, WIDE), F32)

    g.wacc[...] = jnp.zeros(g.wacc.shape, F32)
    t_z.s2()

    def convolve_back(i):
        first = i * 64
        at = cut(first, 64, 16)
        sv = g.segc[cut(first + HALO, 64, 8), :]
        ahead = jnp.where(i < ROWS // 64 - 1, 1.0, 0.0)
        for n in range(4):
            cols = pl.ds(n * 256, 256)
            v = g.gconv[cut(first, 72, 8), cols]
            here = v[0:64]
            total = g.taps[3:4, cols] * here
            nxt = g.segc[cut(jnp.minimum(first + HALO + 64, ROWS + HALO - 8), 8, 8), :]
            sfull = jnp.concatenate([sv, nxt], axis=0)
            for k in range(3):
                shift = 3 - k
                same = pltpu.roll(sfull, 72 - shift, 0)[0:64] == sv
                src = pltpu.roll(v, 72 - shift, 0)[0:64]
                total = total + jnp.where(wide_of(same, 2), g.taps[k : k + 1, cols] * src, 0.0)
            if n < 3:
                g.gx[at, cols] = total.astype(BF)
            else:
                for k, v in enumerate(parts(total, 2)):
                    g.gbc[k, at, :] = v

            @pl.when(i == ROWS // 64 - 1)
            def _():
                g.tail_rows[:, cols] = total[48:64]

            for k, t in enumerate(taps_of(first, cols)):
                g.wacc[k, :, cols] += rows_sum(here * t)
            g.wacc[4, :, cols] += rows_sum(here)

    loop(ROWS // 64, convolve_back)
    t_out.s3()

    @pl.when(s < SEQ - 1)
    def _():
        ret.wait_recv()

    last_rows = g.tail_rows[...] + jnp.concatenate([jnp.zeros((8, WIDE), F32), g.ret_in[...]], axis=0)
    g.gx[ROWS - 16 : ROWS, :] = last_rows[:, 0:CHANNELS].astype(BF)
    for k, v in enumerate(parts(last_rows[:, CHANNELS:WIDE], 2)):
        g.gbc[k, ROWS - 16 : ROWS, :] = v

    def bc_block(at):
        return sum(mul(g.xn[:, at], g.gbc[k], TN) for k in range(2))

    for k in range(5):
        row = jnp.sum(g.wacc[k], axis=0, keepdims=True)
        g.pack[k : k + 1, :] = row[:, 0:CHANNELS]
        g.bcv[z, k : k + 1, :] = row[:, CHANNELS:WIDE]
    bcv = [send(g.bcv.at[z], g.bcv.at[z], g.bcvsem, i, p) for i, p in enumerate(zpeers)]
    bcs = []
    bc_parts = [g.acc.at[pl.ds(0, BLOCK), pl.ds(WIDE + 256 * i, 256)] for i in range(3)]
    bc_parts.append(g.acc.at[pl.ds(0, BLOCK), pl.ds(BLOCK, 256)])
    mine, other = cut(core * 192, 192, 16), cut((1 - core) * 192, 192, 16)
    halves = []
    for i in range(LINE):
        bc_parts[i][...] = bc_block(cut(lax.rem(z + 1 + i, LINE) * BLOCK, BLOCK, 128))
        halves.append(send(bc_parts[i].at[other], g.hbc.at[i], g.bcsem, 3 + i, partner))

    def grad_x(ref, first):
        def body(n):
            at = cut(n * 256, 256, 256)
            ref[at, :] = mul(g.xn[:, cut(first + n * 256, 256, 256)], g.gx[...], TN).astype(BF)

        loop(3, body)

    t_z.s3()
    grad_x(g.p_xa, 0)
    t_xa.s0()
    grad_x(g.p_xb, CHANNELS)
    t_xb.s0()
    for d in halves:
        d.wait_recv()
    g.bcsum[...] = bc_parts[3][mine, :] + g.hbc[3]
    for i, p in enumerate(zpeers):
        g.tbc[i] = (bc_parts[i][mine, :] + g.hbc[i]).astype(BF)
        bcs.append(send(g.tbc.at[i], g.rbc.at[i], g.bcsem, i, p))

    def back_block(k):
        at = cut(k * BLOCK, BLOCK, 16)
        v = mul(g.gx[...], g.wx[at, :], NT) + mul(g.gz[...], g.wz[at, :], NT)
        return v + mul(g.gsr[...], g.wd[:, cut(k * BLOCK, BLOCK, 128)]) + mul(g.gbc[0], g.wbc[k], NT) + mul(g.gbc[1], g.wbc[k], NT)

    in_blocks.block(0, back_block(dests[0]))
    t_xa.s1()
    t_xb.s1()
    t_out.s4()
    in_blocks.block(1, back_block(dests[1]))
    g.own_in[...] = back_block(z)
    t_xa.s2()
    t_z.s4()
    t_xb.s2()

    for d in bcs + bcv:
        d.wait_recv()
    g.pack[8:16, 0:256] = g.bcv[0] + g.bcv[1] + g.bcv[2] + g.bcv[3]
    g.pack[5:6, :] = jnp.sum(g.vacc[0], axis=0, keepdims=True)
    skips = head_sum(jnp.broadcast_to(jnp.sum(g.vacc[1], axis=0, keepdims=True), (8, CHANNELS)))
    g.pack[16:24, 256:384] = skips
    bc = g.bcsum[...]
    for i in range(3):
        bc = bc + g.rbc[i].astype(F32)
    g.q_out[0:192, :] = bc.astype(BF)
    for n in range(6):
        cols = pl.ds(256 * n, 256)
        g.few[16 * n : 16 * n + 16, :] = mul(g.gsr[...], g.xn[:, cols], TN)[0:16]
    for n in range(3):
        g.few[96 + 24 * n : 120 + 24 * n, :] = g.pack[:, 256 * n : 256 * n + 256]
    g.few[168:192, :] = jnp.zeros((24, 256), F32)
    few = send(g.few, g.few_in, g.restsem, 0, partner)
    in_blocks.block(2, back_block(dests[2]))
    t_xa.s3()
    few.wait_recv()
    few_half = cut(96 * core, 96, 8)
    g.q_out[192:288, :] = (g.few[few_half, :] + g.few_in[few_half, :]).astype(BF)
    across_x = send(g.q_out, g.q_in.at[0], g.restsem, 1, {ALONG: s + 2 - 4 * me[1]})
    t_xb.s3()
    t_xa.s4()
    across_x.wait_recv()
    g.q_mid[...] = (g.q_out[...].astype(F32) + g.q_in[0].astype(F32)).astype(BF)
    across_y = send(g.q_mid, g.q_in.at[1], g.restsem, 2, {ALONG: s + 4 - 8 * me[2]})
    t_xb.s4()
    t_out.s5()
    out_blocks.arrived()
    out_sum = g.own[...]
    for i in range(3):
        out_sum = out_sum + g.rblk[i].astype(F32)
    g.layer_out[...] = (g.x[...].astype(F32) + out_sum).astype(BF)

    in_blocks.arrived()
    g.nacc[...] = jnp.zeros(g.nacc.shape, F32)

    def finish(i):
        at = cut(i * 64, 64, 16)
        v = g.own_in[at, :]
        for k in range(3):
            v = v + g.rblk2[k, at, :].astype(F32)
        g.own_in[at, :] = v
        x = g.x[at, :].astype(F32)
        g.part[0, at, :] = lanes_sum(v * gain * x)
        g.nacc[...] += rows_sum(v * x * wide_of(g.xscale[at, :], 3))

    loop(ROWS // 64, finish)
    g.nstat[z] = to_row(g.part[0])
    nst = [send(g.nstat.at[z], g.nstat.at[z], g.nsem, i, p) for i, p in enumerate(zpeers)]
    g.ngain[0] = jnp.sum(g.nacc[...], axis=0, keepdims=True)
    ngs = [send(g.ngain.at[0], g.ngain.at[1 + i], g.nsem, 3 + i, p) for i, p in enumerate(speers)]
    t_z.s5()
    t_xa.s5()
    t_xb.s5()
    across_y.wait_recv()
    g.rest[core] = g.q_mid[...].astype(F32) + g.q_in[1].astype(F32)
    q_last = send(g.rest.at[core], g.rest.at[core], g.restsem, 3, partner)
    t_out.s6()
    store = [pltpu.make_async_copy(g.p_out, g.grad_out, g.load_sem.at[5])]
    store[0].start()
    t_z.s6()
    store.append(pltpu.make_async_copy(g.p_z, g.grad_z, g.load_sem.at[6]))
    store[1].start()
    for d in nst:
        d.wait_recv()
    rows = g.nstat[0] + g.nstat[1] + g.nstat[2] + g.nstat[3]
    g.part[0] = to_col(rows / D)

    def last(i):
        at = cut(i * 64, 64, 16)
        sc = wide_of(g.xscale[at, :], 3)
        x = g.x[at, :].astype(F32)
        g.grad_in[at, :] = (
            g.cotg[at, own].astype(F32)
            + sc * (g.own_in[at, :] * gain)
            - x * (sc * sc * sc * wide_of(g.part[0, at, :], 3))
        )

    loop(ROWS // 64, last)
    for d in ngs:
        d.wait_recv()
    total = g.ngain[0]
    for i in range(7):
        total = total + g.ngain[1 + i]
    g.grad_gain[...] = jnp.broadcast_to(total, (8, BLOCK))
    q_last.wait_recv()
    for i, (t, ref) in enumerate(((t_xa, g.p_xa), (t_xb, g.p_xb))):
        t.s6()
        rows_of = pl.ds(CHANNELS * i, CHANNELS)
        store.append(pltpu.make_async_copy(ref, g.grad_x.at[rows_of], g.load_sem.at[7 + i]))
        store[-1].start()
    for d in pending:
        d.wait_send()

    @pl.when(s < SEQ - 1)
    def _():
        edge.wait_send()

    @pl.when(s > 0)
    def _():
        ret.wait_send()

    x_own[0].wait_send()

    @pl.when(middle)
    def _():
        x_own[1].wait_send()

    for inside_it, d in later:
        @pl.when(inside_it)
        def _():
            d.wait_send()

    out_blocks.left()
    in_blocks.left()
    for d in store:
        d.wait()


def unpack_kernel(
    layer_hbm, in_hbm, out_low, z_low, x_low, rest, gain_sum,
    layer_out, grad_in, gain, w_z, w_x, w_bc, w_dt, conv_x_w, conv_x_b, conv_bc_w, conv_bc_b, dt_bias, a_log, d_skip, gate_gain, w_out,
    low_a, low_b, low_c, full_a, full_b, full_c, keep_a, keep_b, in_sem, out_sem,
):
    steps = 6
    mats = [(out_low, low_a, full_a, w_out), (z_low, low_b, full_b, w_z), (x_low, low_c, full_c, w_x)]
    loads, stores = [], []
    for m, (src, low, _, _) in enumerate(mats):
        n = low.shape[0] // steps
        for i in range(steps):
            at = pl.ds(i * n, n)
            loads.append(pltpu.make_async_copy(src.at[at], low.at[at], in_sem.at[steps * m + i]))
    for i, (src, dst) in enumerate([(layer_hbm, keep_a), (in_hbm, keep_b)]):
        loads.append(pltpu.make_async_copy(src, dst, in_sem.at[18 + i]))
    for d in loads:
        d.start()
    for n in range(3):
        gain[n : n + 1, :] = gain_sum[0:1, 128 * n : 128 * n + 128]
    w_bc[0:192, :] = rest[0, 0:192, :]
    w_bc[192:BLOCK, :] = rest[1, 0:192, :]
    for n in range(6):
        w_dt[:, 256 * n : 256 * n + 256] = rest[0, 192 + 16 * n : 204 + 16 * n, :]
    for n in range(3):
        at, base = pl.ds(256 * n, 256), 192 + 24 * n
        conv_x_w[:, at] = rest[1, base : base + 4, :]
        for e in range(2):
            lanes, to = pl.ds(128 * e, 128), pl.ds(2 * n + e, 1)
            conv_x_b[to, :] = rest[1, base + 4 : base + 5, lanes]
            gate_gain[to, :] = rest[1, base + 5 : base + 6, lanes]
    conv_bc_w[...] = rest[1, 200:204, :]
    for e in range(2):
        conv_bc_b[e : e + 1, :] = rest[1, 204:205, 128 * e : 128 * e + 128]
    dt_bias[...] = rest[1, 208:209, 0:12]
    a_log[...] = rest[1, 208:209, 128:140]
    d_skip[...] = rest[1, 232:233, 0:12]
    for m, (_, low, full, dst) in enumerate(mats):
        n = low.shape[0] // steps
        for i in range(steps):
            loads[steps * m + i].wait()
            at = pl.ds(i * n, n)
            full[at, :] = low[at, :].astype(F32)
            stores.append(pltpu.make_async_copy(full.at[at], dst.at[at], out_sem.at[steps * m + i]))
            stores[-1].start()
    for i, (src, dst) in enumerate([(keep_a, layer_out), (keep_b, grad_in)]):
        loads[18 + i].wait()
        stores.append(pltpu.make_async_copy(src, dst, out_sem.at[18 + i]))
        stores[-1].start()
    for d in stores:
        d.wait()


def fast_layer(
    hidden_in, seq_lengths, norm_gain, w_z, w_x, w_bc, w_dt, conv_x_w, conv_x_b, conv_bc_w,
    conv_bc_b, dt_bias, a_log, d_skip, gate_gain, w_out, cotangent,
):
    row = lambda v: v.reshape(-1, min(128, v.shape[0]))
    vm = pl.BlockSpec(memory_space=pltpu.VMEM)
    hbm = pl.BlockSpec(memory_space=pltpu.HBM)
    sm = pl.BlockSpec(memory_space=pltpu.SMEM)
    ins = dict(
        x_hbm=(hidden_in, hbm), cot_hbm=(cotangent, hbm), w_x=(w_x, hbm), w_z=(w_z, hbm), w_out=(w_out, hbm),
        lengths=(seq_lengths, sm), norm_gain=(row(norm_gain), vm), conv_x_b=(row(conv_x_b), vm),
        conv_bc_b=(row(conv_bc_b), vm), dt_bias=(row(dt_bias), vm), a_log=(row(a_log), vm), d_skip=(row(d_skip), vm),
        gate_gain=(row(gate_gain), vm), w_bc=(w_bc, vm), w_dt=(w_dt.T, vm),
        conv_x_w=(conv_x_w, vm), conv_bc_w=(conv_bc_w, vm),
    )
    outs = dict(
        layer_out=((ROWS, BLOCK), BF, vm),
        grad_in=((ROWS, BLOCK), F32, vm),
        grad_out=((CHANNELS, D), BF, hbm),
        grad_z=((D, CHANNELS), BF, hbm),
        grad_x=((D, CHANNELS), BF, hbm),
        rest=((2, 288, 256), F32, vm),
        grad_gain=((8, BLOCK), F32, vm),
    )
    V = pltpu.VMEM
    S = pltpu.SemaphoreType.DMA
    scr = dict(
        x=V((ROWS, BLOCK), BF),
        wx=V((D, CHANNELS), BF),
        wz=V((D, CHANNELS), BF),
        wo=V((CHANNELS, D), BF),
        xg=V((ROWS, D), BF),
        xn=V((ROWS, D), BF),
        cotg=V((ROWS, D), BF),
        ssq=V((LINE, 1, ROWS), F32),
        gains=V((LINE, 1, BLOCK), F32),
        wbc=V((LINE, BLOCK, 256), BF),
        wd=V((128, D), BF),
        params=V((8, CHANNELS), F32),
        taps=V((8, WIDE), F32),
        spread=V((256, CHANNELS), BF),
        segc=V((ROWS + HALO, 128), F32),
        segr=V((8, ROWS), F32),
        tri=V((SPAN, SPAN), BF),
        skipe=V((8, CHANNELS), F32),
        xscale=V((ROWS, 128), F32),
        acc=V((ROWS, WIDE + CHANNELS + 128), F32),
        edge=V((HALO, WIDE), BF),
        halo=V((HALO, WIDE), BF),
        cf=V((ROWS + HALO, WIDE), F32),
        step=V((ROWS, 128), F32),
        cum=V((ROWS, 128), F32),
        cumt=V((2, 16, SPAN), F32),
        tail=V((ROWS, 128), F32),
        load=V((ROWS, 128), F32),
        lead=V((ROWS, 128), F32),
        carry=V((2, 8, 128), F32),
        carrye=V((2, 8, CHANNELS), F32),
        decay=V((2, 8, CHANNELS), F32),
        slope=V((ROWS + 16, WIDE), F32),
        inner=V((ROWS, CHANNELS), BF),
        b=V((ROWS, 128), BF),
        c=V((ROWS, 128), BF),
        bt=V((STATE, ROWS), F32),
        ct=V((STATE, ROWS), F32),
        loadt=V((2, 16, SPAN), F32),
        leadt=V((2, 16, SPAN), F32),
        stept=V((2, 16, SPAN), F32),
        local=V((2, STATE, CHANNELS), F32),
        mine=V((STATE, CHANNELS), F32),
        other=V((STATE, CHANNELS), F32),
        joined=V((STATE, BLOCK), F32),
        got=V((2, STATE, BLOCK), F32),
        chain=V((STATE, CHANNELS), F32),
        mine_b=V((STATE, CHANNELS), F32),
        other_b=V((STATE, CHANNELS), F32),
        joined_b=V((STATE, BLOCK), F32),
        got_b=V((2, STATE, BLOCK), F32),
        chain_b=V((STATE, CHANNELS), F32),
        both=V((8, BLOCK), F32),
        boths=V((2, 8, BLOCK), F32),
        scores=V((SPAN, SPAN), F32),
        gscores=V((SPAN, SPAN), F32),
        out=V((ROWS, CHANNELS), F32),
        sin=V((2, STATE, CHANNELS), F32),
        slow=V((2, STATE, CHANNELS), BF),
        gated=V((ROWS, CHANNELS), F32),
        part=V((2, ROWS, 128), F32),
        stats=V((LINE, 2, ROWS), F32),
        vacc=V((2, 8, CHANNELS), F32),
        gm=V((ROWS, CHANNELS), BF),
        gloc=V((2, STATE, CHANNELS), F32),
        sblk=V((3, ROWS, BLOCK), BF),
        rblk=V((3, ROWS, BLOCK), BF),
        rblk2=V((3, ROWS, BLOCK), BF),
        gsr=V((ROWS, 128), BF),
        pack=V((24, CHANNELS), F32),
        ret_out=V((8, WIDE), F32),
        ret_in=V((8, WIDE), F32),
        wacc=V((5, 8, WIDE), F32),
        gbc=V((2, ROWS, 256), BF),
        tail_rows=V((16, WIDE), F32),
        hbc=V((LINE, 192, 256), F32),
        tbc=V((3, 192, 256), BF),
        rbc=V((3, 192, 256), BF),
        via=V((ROWS, BLOCK), BF),
        via2=V((ROWS, BLOCK), BF),
        bcv=V((LINE, 8, 256), F32),
        nacc=V((8, BLOCK), F32),
        nstat=V((LINE, 1, ROWS), F32),
        ngain=V((8, 1, BLOCK), F32),
        p_out=V((CHANNELS, D), BF),
        p_z=V((D, CHANNELS), BF),
        p_xa=V((CHANNELS, CHANNELS), BF),
        p_xb=V((CHANNELS, CHANNELS), BF),
        bcsum=V((192, 256), F32),
        few=V((192, 256), F32),
        few_in=V((192, 256), F32),
        q_out=V((288, 256), BF),
        q_mid=V((288, 256), BF),
        q_in=V((2, 288, 256), BF),
        load_sem=S((9,)),
        edge_sem=S((4,)),
        gather_s=S((8,)),
        gather_r=S((9,)),
        block_s=S((8,)),
        block_r=S((8,)),
        st_send=S((11,)),
        st_recv=S((11,)),
        tot_send=S((40,)),
        tot_recv=S((40,)),
        freed=pltpu.SemaphoreType.REGULAR((12,)),
    )
    pairs = dict(
        small=9,
        wide=4,
        stat=3,
        bcsem=7,
        restsem=4,
        bcvsem=3,
        nsem=10,
    )
    sums = [(CHANNELS, D, BF), (D, CHANNELS, BF), (CHANNELS, CHANNELS, BF), (CHANNELS, CHANNELS, BF)]
    bufs = [b for spec in sums for b in total_bufs(*spec)]
    sems = [S((k,)) for k in pairs.values() for _ in range(2)]
    names = [*ins, *outs, *scr]

    def kernel(*refs):
        n, m = len(names), len(names) + len(bufs)
        d = dict(zip(names, refs[:n]))
        rest = refs[m:]
        for i, name in enumerate(pairs):
            d[name] = (rest[2 * i], rest[2 * i + 1])
        layer_kernel(d, refs[n:m])

    res = pl.pallas_call(
        kernel,
        out_shape=[jax.ShapeDtypeStruct(sh, dt) for sh, dt, _ in outs.values()],
        in_specs=[sp for _, sp in ins.values()],
        out_specs=[sp for _, _, sp in outs.values()],
        scratch_shapes=[*scr.values(), *bufs, *sems],
        compiler_params=pltpu.CompilerParams(collective_id=0, has_side_effects=True, vmem_limit_bytes=66 * 2**20 - 2**21),
        name="layer",
    )(*[a for a, _ in ins.values()])
    layer_out, grad_in, grad_out, grad_z, grad_x, rest, grad_gain = res
    shapes = dict(
        layer_out=((ROWS, BLOCK), BF, hbm), grad_in=((ROWS, BLOCK), F32, hbm), gain=((3, 128), F32, vm), w_z=((D, CHANNELS), F32, hbm),
        w_x=((D, CHANNELS), F32, hbm), w_bc=((BLOCK, 256), F32, vm), w_dt=((12, D), F32, vm), conv_x_w=((4, CHANNELS), F32, vm),
        conv_x_b=((6, 128), F32, vm), conv_bc_w=((4, 256), F32, vm), conv_bc_b=((2, 128), F32, vm), dt_bias=((1, 12), F32, vm),
        a_log=((1, 12), F32, vm), d_skip=((1, 12), F32, vm), gate_gain=((6, 128), F32, vm), w_out=((CHANNELS, D), F32, hbm),
    )
    final = pl.pallas_call(
        unpack_kernel,
        out_shape=[jax.ShapeDtypeStruct(sh, dt) for sh, dt, _ in shapes.values()],
        in_specs=[hbm] * 5 + [vm] * 2,
        out_specs=[sp for _, _, sp in shapes.values()],
        scratch_shapes=[
            V((CHANNELS, D), BF), V((D, CHANNELS), BF), V((D, CHANNELS), BF),
            V((CHANNELS, D), F32), V((D, CHANNELS), F32), V((D, CHANNELS), F32),
            V((ROWS, BLOCK), BF), V((ROWS, BLOCK), F32), S((20,)), S((20,)),
        ],
        compiler_params=pltpu.CompilerParams(vmem_limit_bytes=63 * 2**20),
    )(layer_out, grad_in, grad_out, grad_z, grad_x, rest, grad_gain)
    flat = [v.reshape(v.size) if v.shape[1] <= 128 else v for v in final]
    flat[6] = flat[6].T
    return tuple(flat)


def solution(mesh):
    placed = (
        P("seq", "head"),
        P(),
        P("head"),
        P(None, "head"),
        P(None, "head"),
        P("head", None),
        P(None, "head"),
        P(None, "head"),
        P("head"),
        P(),
        P(),
        P("head"),
        P("head"),
        P("head"),
        P("head"),
        P("head", None),
        P("seq", "head"),
    )
    fits = mesh.shape["seq"] == SEQ and mesh.shape["head"] == LINE
    return jax.shard_map(
        fast_layer if fits else on_device,
        mesh=mesh,
        in_specs=placed,
        out_specs=(
            P("seq", "head"),
            P("seq", "head"),
            P("head"),
            P(None, "head"),
            P(None, "head"),
            P("head", None),
            P(None, "head"),
            P(None, "head"),
            P("head"),
            P(),
            P(),
            P("head"),
            P("head"),
            P("head"),
            P("head"),
            P("head", None),
        ),
        check_vma=False,
    )
```

```python
import jax
import jax.numpy as jnp
from jax import lax
from jax.experimental import pallas as pl
from jax.experimental.pallas import tpu as pltpu
from jax.sharding import PartitionSpec as P

D = 1536
HEAD_DIM = 64
STATE = 128
CONV = 4
SPAN = 256
INNER = 3072


epsilon = 1e-05
highest = lax.Precision.HIGHEST


def prefix(part, axis, combine, identity, reverse):
    count = lax.axis_size(axis)
    place = lax.axis_index(axis)
    ahead = count - 1 - place if reverse else place
    gathered = jax.tree.map(lambda a: lax.all_gather(a, axis), part)
    state = jax.tree.map(lambda a, e: jnp.zeros_like(a) + jnp.asarray(e, a.dtype), part, identity)

    def one(hop, state):
        source = count - 1 - hop if reverse else hop
        return combine(
            state, jax.tree.map(lambda a: lax.dynamic_index_in_dim(a, source, 0, False), gathered)
        )

    return lax.fori_loop(0, ahead, one, state)


def passed_along(block, axis, distance):
    devices = range(lax.axis_size(axis))
    route = [(i - distance, i) for i in devices if i - distance in devices]
    return lax.ppermute(block, axis, route)


def segment_of(positions, starts):
    return jnp.sum((positions[:, None] >= starts[None, :]).astype(jnp.int32), axis=1) - 1


def silu_slope(values):
    sigmoid_val = jax.nn.sigmoid(values)
    return sigmoid_val * (1.0 + values * (1.0 - sigmoid_val))


def chain_join(earlier, later):
    return (earlier[0] * later[0], earlier[1] * later[0][:, None, None] + later[1])


def state_prefix(decay, summary, backwards):
    identity = (jnp.ones_like(decay), jnp.zeros_like(summary))
    result = prefix((decay, summary), "seq", chain_join, identity, backwards)
    return result[1]


def span_terms(span_item, lower_tri):
    inner_c, b_rows, c_rows, step_c, cumul_c, seg_rows, seg_prev = span_item
    same_seq = ((seg_rows[:, None] == seg_rows[None, :]) & (lower_tri > 0.5))[None, :, :]
    spread = cumul_c[:, :, None] - cumul_c[:, None, :]
    decay_mat = jnp.where(same_seq, jnp.exp(jnp.where(same_seq, spread, 0.0)), 0.0)
    scores = lax.dot_general(
        c_rows, b_rows, (((1,), (1,)), ((), ())), preferred_element_type=jnp.float32
    )
    mixing = scores[None, :, :] * decay_mat * step_c[:, None, :]
    last_cum = cumul_c[:, SPAN - 1]
    tail_weight = (
        jnp.exp(last_cum[:, None] - cumul_c)
        * (seg_rows == seg_rows[SPAN - 1]).astype(jnp.float32)[None, :]
    )
    head_weight = jnp.exp(cumul_c) * (seg_rows == seg_prev).astype(jnp.float32)[None, :]
    carry_decay = jnp.exp(last_cum) * (seg_rows[SPAN - 1] == seg_prev).astype(jnp.float32)
    return (decay_mat, scores, mixing, tail_weight, head_weight, carry_decay)


def on_device(
    hidden_in,
    seq_lengths,
    norm_gain,
    w_z,
    w_x,
    w_bc,
    w_dt,
    conv_x_w,
    conv_x_b,
    conv_bc_w,
    conv_bc_b,
    dt_bias,
    a_log,
    d_skip,
    gate_gain,
    w_out,
    cotangent,
):
    tokens_here = hidden_in.shape[0]
    heads_here = dt_bias.shape[0]
    inner_here = w_z.shape[1]
    spans = tokens_here // SPAN
    first_pos = lax.axis_index("seq") * tokens_here
    starts = jnp.cumsum(seq_lengths) - seq_lengths
    segment = segment_of(first_pos + jnp.arange(tokens_here, dtype=jnp.int32), starts)
    edge_segment = segment_of(
        first_pos - (CONV - 1) + jnp.arange(CONV - 1, dtype=jnp.int32), starts
    )
    span_prev = segment_of(first_pos - 1 + jnp.arange(spans, dtype=jnp.int32) * SPAN, starts)
    row_ids = jnp.arange(SPAN)
    lower_tri = (row_ids[:, None] >= row_ids[None, :]).astype(jnp.float32)
    inputs = hidden_in.astype(jnp.float32)
    squares = lax.psum(jnp.sum(inputs * inputs, axis=1), "head")
    scale_in = lax.rsqrt(squares / D + epsilon)
    normed = (inputs * scale_in[:, None] * norm_gain).astype(jnp.bfloat16)
    gathered, bc_weight = (
        lax.all_gather(normed, "head", axis=1, tiled=True),
        lax.all_gather(w_bc, "head", axis=0, tiled=True),
    )
    gate_pre = jnp.dot(gathered, w_z, preferred_element_type=jnp.float32)
    x_part = jnp.dot(gathered, w_x, preferred_element_type=jnp.float32)
    bc_part = jnp.dot(gathered, bc_weight, preferred_element_type=jnp.float32)
    conv_in = jnp.concatenate([x_part, bc_part], axis=1).astype(jnp.bfloat16)
    step_raw = jnp.dot(gathered, w_dt, preferred_element_type=jnp.float32)
    edge_rows = passed_along(conv_in[tokens_here - (CONV - 1) :], "seq", 1)
    padded = jnp.concatenate([edge_rows, conv_in], axis=0).astype(jnp.float32)
    seg_padded = jnp.concatenate([edge_segment, segment])
    conv_weight = jnp.concatenate([conv_x_w, conv_bc_w], axis=1)
    conv_bias = jnp.concatenate([conv_x_b, conv_bc_b])
    tap_masks = [
        (seg_padded[offset : offset + tokens_here] == segment).astype(jnp.float32)[:, None]
        for offset in range(CONV)
    ]
    conv_out = jnp.zeros(conv_in.shape, jnp.float32) + conv_bias[None, :]
    for offset in range(CONV):
        conv_out = (
            conv_out
            + conv_weight[offset] * padded[offset : offset + tokens_here] * tap_masks[offset]
        )
    activated = jax.nn.silu(conv_out)
    inner_vals = activated[:, :inner_here].astype(jnp.bfloat16)
    b_vals = activated[:, inner_here : inner_here + STATE].astype(jnp.bfloat16)
    c_vals = activated[:, inner_here + STATE :].astype(jnp.bfloat16)
    step_pre = step_raw + dt_bias
    step_size = jax.nn.softplus(step_pre)
    rates = jnp.exp(a_log)
    log_decay = -rates * step_size
    decay_heads = log_decay.reshape(spans, SPAN, heads_here).transpose(0, 2, 1)
    step_heads = step_size.reshape(spans, SPAN, heads_here).transpose(0, 2, 1)
    cumul = jnp.einsum("ij,chj->chi", lower_tri, decay_heads, precision=highest)
    inner_spans = inner_vals.reshape(spans, SPAN, heads_here, HEAD_DIM).transpose(0, 2, 1, 3)
    c_spans = c_vals.reshape(spans, SPAN, STATE)
    per_span = (
        inner_spans,
        b_vals.reshape(spans, SPAN, STATE),
        c_spans,
        step_heads,
        cumul,
        segment.reshape(spans, SPAN),
        span_prev,
    )

    def forward_span(span_item):
        decay_mat, scores, mixing, tail_weight, head_weight, carry_decay = span_terms(
            span_item, lower_tri
        )
        inner_c = span_item[0]
        y_inside = jnp.einsum(
            "hij,hjp->hip", mixing.astype(jnp.bfloat16), inner_c, preferred_element_type=jnp.float32
        )
        loaded = (
            span_item[1].astype(jnp.float32)[None, :, :] * (tail_weight * span_item[3])[:, :, None]
        ).astype(jnp.bfloat16)
        local_state = jnp.einsum(
            "hjn,hjp->hnp", loaded, inner_c, preferred_element_type=jnp.float32
        )
        return (y_inside, local_state, carry_decay, head_weight)

    y_inside, local_states, carry_decay, head_weight = lax.map(forward_span, per_span)

    def advance(state_carry, span_item):
        running, factor = state_carry
        local_c, decay_c = span_item
        return ((decay_c[:, None, None] * running + local_c, decay_c * factor), (running, factor))

    zero_state = jnp.zeros((heads_here, STATE, HEAD_DIM), jnp.float32)
    unit_decay = jnp.ones((heads_here,), jnp.float32)
    (device_state, device_decay), (local_in, local_factor) = lax.scan(
        advance, (zero_state, unit_decay), (local_states, carry_decay)
    )
    incoming = state_prefix(device_decay, device_state, False)
    state_in = local_in + local_factor[:, :, None, None] * incoming
    state_low = state_in.astype(jnp.bfloat16)
    c_weighted = (c_spans.astype(jnp.float32)[:, None, :, :] * head_weight[:, :, :, None]).astype(
        jnp.bfloat16
    )
    y_outside = jnp.einsum(
        "chin,chnp->chip", c_weighted, state_low, preferred_element_type=jnp.float32
    )
    skip_rep = jnp.repeat(d_skip, HEAD_DIM)
    mixed_out = (y_inside + y_outside).transpose(0, 2, 1, 3).reshape(
        tokens_here, inner_here
    ) + inner_vals.astype(jnp.float32) * skip_rep
    gate_act = jax.nn.silu(gate_pre)
    gated = mixed_out * gate_act
    gate_squares = lax.psum(jnp.sum(gated * gated, axis=1), "head")
    scale_gate = lax.rsqrt(gate_squares / INNER + epsilon)
    gate_normed = (gated * scale_gate[:, None] * gate_gain).astype(jnp.bfloat16)
    partial_value = jnp.dot(gate_normed, w_out, preferred_element_type=jnp.float32)
    mixed_sum = lax.psum_scatter(partial_value, "head", scatter_dimension=1, tiled=True)
    layer_out = (inputs + mixed_sum).astype(jnp.bfloat16)
    grad_full = lax.all_gather(cotangent, "head", axis=1, tiled=True)
    grad_gate_normed = lax.dot_general(
        grad_full, w_out, (((1,), (1,)), ((), ())), preferred_element_type=jnp.float32
    )
    grad_w_out = lax.dot_general(
        gate_normed, grad_full, (((0,), (0,)), ((), ())), preferred_element_type=jnp.float32
    )
    grad_gate_gain = jnp.sum(grad_gate_normed * gated * scale_gate[:, None], axis=0)
    grad_scaled = grad_gate_normed * gate_gain
    gate_inner = lax.psum(jnp.sum(grad_scaled * gated, axis=1), "head")
    grad_gated = (
        scale_gate[:, None] * grad_scaled - gated * (scale_gate**3 * gate_inner / INNER)[:, None]
    )
    grad_mixed = (grad_gated * gate_act).astype(jnp.bfloat16)
    grad_gate_pre = (grad_gated * mixed_out * silu_slope(gate_pre)).astype(jnp.bfloat16)
    grad_d_skip = jnp.sum(
        (grad_mixed.astype(jnp.float32) * inner_vals.astype(jnp.float32)).reshape(
            tokens_here, heads_here, HEAD_DIM
        ),
        axis=(0, 2),
    )
    grad_spans = grad_mixed.reshape(spans, SPAN, heads_here, HEAD_DIM).transpose(0, 2, 1, 3)
    from_inter = jnp.einsum(
        "chin,chip->chnp", c_weighted, grad_spans, preferred_element_type=jnp.float32
    )

    def retreat(state_carry, span_item):
        running, factor = state_carry
        local_c, decay_c = span_item
        current = local_c + decay_c[:, None, None] * running
        product = decay_c * factor
        return ((current, product), (current, product))

    (device_grad, device_reach), (local_grad, local_reach) = lax.scan(
        retreat, (zero_state, unit_decay), (from_inter, carry_decay), reverse=True
    )
    beyond = state_prefix(device_reach, device_grad, True)
    grad_state_in = local_grad + local_reach[:, :, None, None] * beyond
    grad_local_states = jnp.concatenate([grad_state_in[1:], beyond[None]], axis=0)
    grad_carry_decay = jnp.sum(grad_local_states * state_in, axis=(2, 3))

    def backward_span(span_item):
        span_base = span_item[:7]
        inner_c, b_rows, c_rows, step_c = (span_base[0], span_base[1], span_base[2], span_base[3])
        grad_y, grad_state, state_c, grad_decay = (
            span_item[7],
            span_item[8],
            span_item[9],
            span_item[10],
        )
        decay_mat, scores, mixing, tail_weight, head_weight, carry_decay = span_terms(
            span_base, lower_tri
        )
        grad_mixing = jnp.einsum(
            "hip,hjp->hij", grad_y, inner_c, preferred_element_type=jnp.float32
        )
        grad_inner = jnp.einsum(
            "hij,hip->hjp", mixing.astype(jnp.bfloat16), grad_y, preferred_element_type=jnp.float32
        )
        related = grad_mixing * mixing
        grad_cum = jnp.sum(related, axis=2) - jnp.sum(related, axis=1)
        grad_scores = jnp.sum(grad_mixing * decay_mat * step_c[:, None, :], axis=0)
        grad_step = jnp.sum(grad_mixing * decay_mat * scores[None, :, :], axis=1)
        b_float = b_rows.astype(jnp.float32)
        c_float = c_rows.astype(jnp.float32)
        grad_c = jnp.dot(grad_scores, b_float, precision=highest)
        grad_b = lax.dot_general(grad_scores, c_float, (((0,), (0,)), ((), ())), precision=highest)
        loading = tail_weight * step_c
        loaded = (b_float[None, :, :] * loading[:, :, None]).astype(jnp.bfloat16)
        grad_loaded = jnp.einsum(
            "hjp,hnp->hjn", inner_c, grad_state, preferred_element_type=jnp.float32
        )
        grad_inner = grad_inner + jnp.einsum(
            "hjn,hnp->hjp", loaded, grad_state, preferred_element_type=jnp.float32
        )
        grad_loading = jnp.sum(grad_loaded * b_float[None, :, :], axis=2)
        grad_b = grad_b + jnp.einsum("hjn,hj->jn", grad_loaded, loading, precision=highest)
        tail_term = grad_loading * loading
        grad_cum = grad_cum - tail_term
        grad_last = jnp.sum(tail_term, axis=1) + grad_decay * carry_decay
        grad_step = grad_step + grad_loading * tail_weight
        grad_weighted = jnp.einsum(
            "hip,hnp->hin", grad_y, state_c, preferred_element_type=jnp.float32
        )
        grad_head = jnp.sum(grad_weighted * c_float[None, :, :], axis=2)
        grad_c = grad_c + jnp.einsum("hin,hi->in", grad_weighted, head_weight, precision=highest)
        grad_cum = grad_cum + grad_head * head_weight
        grad_cum = grad_cum.at[:, SPAN - 1].add(grad_last)
        grad_log = jnp.einsum("ij,hi->hj", lower_tri, grad_cum, precision=highest)
        return (grad_inner, grad_b, grad_c, grad_step, grad_log)

    back_items = per_span + (
        grad_spans,
        grad_local_states.astype(jnp.bfloat16),
        state_low,
        grad_carry_decay,
    )
    grad_inner_s, grad_b_s, grad_c_s, grad_step_s, grad_log_s = lax.map(backward_span, back_items)
    grad_inner = (
        grad_inner_s.transpose(0, 2, 1, 3).reshape(tokens_here, inner_here)
        + grad_mixed.astype(jnp.float32) * skip_rep
    )
    grad_log_decay = grad_log_s.transpose(0, 2, 1).reshape(tokens_here, heads_here)
    grad_step_total = (
        grad_step_s.transpose(0, 2, 1).reshape(tokens_here, heads_here) - grad_log_decay * rates
    )
    grad_a_log = jnp.sum(grad_log_decay * log_decay, axis=0)
    grad_step_pre = grad_step_total * jax.nn.sigmoid(step_pre)
    grad_dt_bias = jnp.sum(grad_step_pre, axis=0)
    grad_step_raw = grad_step_pre.astype(jnp.bfloat16)
    grad_bc = lax.psum(
        jnp.concatenate(
            [grad_b_s.reshape(tokens_here, STATE), grad_c_s.reshape(tokens_here, STATE)], axis=1
        ),
        "head",
    )
    grad_conv = jnp.concatenate([grad_inner, grad_bc], axis=1) * silu_slope(conv_out)
    grad_conv_bias = jnp.sum(grad_conv, axis=0)
    grad_conv_weight = jnp.stack(
        [
            jnp.sum(grad_conv * padded[offset : offset + tokens_here] * tap_masks[offset], axis=0)
            for offset in range(CONV)
        ]
    )
    grad_padded = jnp.zeros(padded.shape, jnp.float32)
    for offset in range(CONV):
        grad_padded = grad_padded + jnp.pad(
            conv_weight[offset] * grad_conv * tap_masks[offset],
            ((offset, CONV - 1 - offset), (0, 0)),
        )
    returned = passed_along(grad_padded[: CONV - 1], "seq", -1)
    grad_conv_in = (
        grad_padded[CONV - 1 :] + jnp.pad(returned, ((tokens_here - (CONV - 1), 0), (0, 0)))
    ).astype(jnp.bfloat16)
    grad_x_pre = grad_conv_in[:, :inner_here]
    grad_bc_pre = grad_conv_in[:, inner_here:]
    contract_rows = (((0,), (0,)), ((), ()))
    contract_cols = (((1,), (1,)), ((), ()))
    grad_w_z = lax.dot_general(
        gathered, grad_gate_pre, contract_rows, preferred_element_type=jnp.float32
    )
    grad_w_x = lax.dot_general(
        gathered, grad_x_pre, contract_rows, preferred_element_type=jnp.float32
    )
    grad_w_dt = lax.dot_general(
        gathered, grad_step_raw, contract_rows, preferred_element_type=jnp.float32
    )
    grad_w_bc = lax.dot_general(
        normed, grad_bc_pre, contract_rows, preferred_element_type=jnp.float32
    )
    partial_back = lax.dot_general(
        grad_gate_pre, w_z, contract_cols, preferred_element_type=jnp.float32
    )
    partial_back = partial_back + lax.dot_general(
        grad_x_pre, w_x, contract_cols, preferred_element_type=jnp.float32
    )
    partial_back = partial_back + lax.dot_general(
        grad_step_raw, w_dt, contract_cols, preferred_element_type=jnp.float32
    )
    grad_normed = lax.psum_scatter(partial_back, "head", scatter_dimension=1, tiled=True)
    grad_normed = grad_normed + lax.dot_general(
        grad_bc_pre, w_bc, contract_cols, preferred_element_type=jnp.float32
    )
    grad_scaled_in = grad_normed * norm_gain
    grad_norm_gain = jnp.sum(grad_normed * inputs * scale_in[:, None], axis=0)
    norm_inner = lax.psum(jnp.sum(grad_scaled_in * inputs, axis=1), "head")
    grad_in = (
        cotangent.astype(jnp.float32)
        + scale_in[:, None] * grad_scaled_in
        - inputs * (scale_in**3 * norm_inner / D)[:, None]
    )
    summed = lax.psum(
        (
            grad_norm_gain,
            grad_w_z,
            grad_w_x,
            grad_w_bc,
            grad_w_dt,
            grad_conv_weight[:, :inner_here],
            grad_conv_bias[:inner_here],
            grad_conv_weight[:, inner_here:],
            grad_conv_bias[inner_here:],
            grad_dt_bias,
            grad_a_log,
            grad_d_skip,
            grad_gate_gain,
            grad_w_out,
        ),
        "seq",
    )
    return (
        layer_out,
        grad_in,
        summed[0],
        summed[1],
        summed[2],
        summed[3],
        summed[4],
        summed[5],
        summed[6],
        summed[7],
        summed[8],
        summed[9],
        summed[10],
        summed[11],
        summed[12],
        summed[13],
    )


BF = jnp.bfloat16
F32 = jnp.float32
MESH = pl.DeviceIdType.MESH
ROWS = 512
BLOCK = 384
CHANNELS = 768
WIDE = 1024
HALO = 16
SEQ = 8
LINE = 4
ALONG = "seq"
ACROSS = "head"
NN = (((1,), (0,)), ((), ()))
NT = (((1,), (1,)), ((), ()))
TN = (((0,), (0,)), ((), ()))


def mul(a, b, dims=NN):
    return lax.dot_general(a, b, dims, preferred_element_type=F32)


def cut(start, size, mult):
    return pl.ds(pl.multiple_of(start, mult), size)


def parts(v, n):
    out = []
    for _ in range(n):
        p = v.astype(BF)
        out.append(p)
        v = v - p.astype(F32)
    return out


def along_line(z, ends, middles):
    k = jnp.where(lax.rem(z, 3) == 0, ends, middles)
    return jnp.where(z >= 2, 3 - k, k)


def lanes_sum(v):
    total = v[:, 0:128]
    for i in range(1, v.shape[1] // 128):
        total = total + v[:, 128 * i : 128 * i + 128]
    return total


def rows_sum(v):
    return jnp.sum(v.reshape(v.shape[0] // 8, 8, v.shape[1]), axis=0)


def wide_of(v, n):
    return jnp.concatenate([v] * n, axis=1)


def to_row(part):
    return jnp.sum(part.T, axis=0, keepdims=True)


def to_col(row):
    return jnp.broadcast_to(row, (128, row.shape[1])).T


def loop(n, body):
    def run(i, carry):
        body(i)
        return carry

    lax.fori_loop(0, n, run, 0)


def remote(src, dst, send, recv, peer):
    return pltpu.make_async_remote_copy(
        src_ref=src, dst_ref=dst, send_sem=send, recv_sem=recv, device_id=peer, device_id_type=MESH
    )


class Total:
    def __init__(self, whole, bufs, send, recv, freed, base, me):
        self.w = whole
        self.freed, self.slot = freed, 3 * (base // 10)
        self.r0, self.ra, self.rb, self.qa, self.qb = bufs
        self.send, self.recv, self.base = send, recv, base
        self.c, self.x, self.y, self.s = me
        self.rows, self.cols = whole.shape
        self.live, self.left = {}, set()

    def peer(self, bit):
        return {ALONG: self.s + bit - 2 * bit * {1: self.c, 2: self.x, 4: self.y}[bit]}

    def free(self, k, n, bit):
        self.sent(k)
        pl.semaphore_signal(
            self.freed.at[self.slot + n], inc=1, device_id=self.peer(bit), device_id_type=MESH
        )

    def copy(self, k, src, dst, bit):
        d = remote(src, dst, self.send.at[self.base + k], self.recv.at[self.base + k], self.peer(bit))
        d.start()
        self.live[k] = d
        self.left.add(k)

    def wait(self, k):
        self.live[k].wait_recv()

    def sent(self, k):
        self.left.remove(k)
        self.live[k].wait_send()

    def add(self, start, got, rows, col, cols, step):
        def body(i):
            at = (cut(start + i * step, step, 16), pl.ds(col, cols))
            new = self.w[at].astype(F32) + got[cut(i * step, step, 16), :].astype(F32)
            self.w[at] = new.astype(self.w.dtype)

        loop(rows // step, body)

    def s0(self):
        h = self.rows // 2
        self.copy(0, self.w.at[cut((1 - self.c) * h, h, 16)], self.r0, 1)

    def s1(self):
        h, q, m = self.rows // 2, self.rows // 4, self.cols // 2
        base = self.c * h
        self.free(0, 0, 1)
        self.wait(0)
        self.add(base, self.r0, h, 0, self.cols, 32)
        self.copy(1, self.w.at[cut(base + (1 - self.x) * q, q, 16), pl.ds(0, m)], self.ra, 2)
        self.copy(2, self.w.at[cut(base + (1 - self.y) * q, q, 16), pl.ds(m, m)], self.rb, 4)

    def s2(self):
        h, q, e, m = self.rows // 2, self.rows // 4, self.rows // 8, self.cols // 2
        ba = self.c * h + self.x * q
        bb = self.c * h + self.y * q
        self.wait(1)
        self.add(ba, self.ra, q, 0, m, 32)
        self.sent(2)
        self.copy(3, self.w.at[cut(ba + (1 - self.y) * e, e, 16), pl.ds(0, m)], self.qa, 4)
        self.wait(2)
        self.add(bb, self.rb, q, m, m, 32)
        self.sent(1)
        self.copy(4, self.w.at[cut(bb + (1 - self.x) * e, e, 16), pl.ds(m, m)], self.qb, 2)

    def s3(self):
        h, q, e, m = self.rows // 2, self.rows // 4, self.rows // 8, self.cols // 2
        ba = self.c * h + self.x * q + self.y * e
        bb = self.c * h + self.y * q + self.x * e
        self.free(3, 1, 4)
        self.free(4, 2, 2)
        self.wait(3)
        self.add(ba, self.qa, e, 0, m, 16)
        pl.semaphore_wait(self.freed.at[self.slot + 1], 1)
        p = self.w.at[cut(ba, e, 16), pl.ds(0, m)]
        self.copy(5, p, p, 4)
        self.wait(4)
        self.add(bb, self.qb, e, m, m, 16)
        pl.semaphore_wait(self.freed.at[self.slot + 2], 1)
        p = self.w.at[cut(bb, e, 16), pl.ds(m, m)]
        self.copy(6, p, p, 2)

    def s4(self):
        h, q, m = self.rows // 2, self.rows // 4, self.cols // 2
        self.wait(5)
        p = self.w.at[cut(self.c * h + self.x * q, q, 16), pl.ds(0, m)]
        self.copy(7, p, p, 2)
        self.wait(6)
        p = self.w.at[cut(self.c * h + self.y * q, q, 16), pl.ds(m, m)]
        self.copy(8, p, p, 4)

    def s5(self):
        h = self.rows // 2
        self.wait(7)
        self.wait(8)
        pl.semaphore_wait(self.freed.at[self.slot], 1)
        p = self.w.at[cut(self.c * h, h, 16)]
        self.copy(9, p, p, 1)

    def s6(self):
        self.wait(9)
        for k in sorted(self.left):
            self.sent(k)


def total_bufs(rows, cols, kind):
    sizes = [(2, 1), (4, 2), (4, 2), (8, 2), (8, 2)]
    return [pltpu.VMEM((rows // a, cols // b), kind) for a, b in sizes]


class Refs:
    def __init__(self, named):
        self.__dict__.update(named)


def layer_kernel(named, sum_bufs):
    g = Refs(named)
    g.ggn = g.acc.at[:, pl.ds(0, CHANNELS)]
    g.z = g.ggn
    g.gn = g.xg.at[:, pl.ds(0, CHANNELS)]
    g.gz = g.xg.at[:, pl.ds(CHANNELS, CHANNELS)]
    g.gconv = g.slope
    g.gx = g.gm
    g.own_in = g.acc.at[:, pl.ds(0, BLOCK)]
    g.own = g.gated.at[:, pl.ds(0, BLOCK)]
    g.gb = g.gated.at[:, pl.ds(BLOCK, 128)]
    g.gc = g.gated.at[:, pl.ds(BLOCK + 128, 128)]
    s = lax.axis_index(ALONG)
    z = lax.axis_index(ACROSS)
    me = (lax.rem(s, 2), lax.rem(s // 2, 2), s // 4, s)
    zpeers = [{ACROSS: lax.rem(z + d, LINE)} for d in range(1, LINE)]
    speers = [{ALONG: lax.rem(s + d, SEQ)} for d in range(1, SEQ)]

    loads = []
    for i, (src, dst) in enumerate(
        [(g.x_hbm, g.x), (g.w_x, g.wx), (g.w_z, g.wz), (g.cot_hbm, g.cotg.at[:, cut(z * BLOCK, BLOCK, 128)]), (g.w_out, g.wo)]
    ):
        d = pltpu.make_async_copy(src, dst, g.load_sem.at[i])
        d.start()
        loads.append(d)

    g.params[...] = jnp.zeros(g.params.shape, F32)
    vectors = (g.norm_gain, g.conv_x_b, g.conv_bc_b, g.dt_bias, g.a_log, g.d_skip, g.gate_gain)
    for i, v in enumerate(vectors):
        for n in range(v.shape[0]):
            g.params[i : i + 1, 128 * n : 128 * n + v.shape[1]] = v[n : n + 1, :]

    sem = pltpu.get_barrier_semaphore()
    for p in zpeers + speers:
        pl.semaphore_signal(sem, inc=1, device_id=p, device_id_type=MESH)
    pl.semaphore_wait(sem, len(zpeers) + len(speers))

    pending = []

    def send(src, dst, sems, i, peer):
        d = remote(src, dst, sems[0].at[i], sems[1].at[i], peer)
        d.start()
        pending.append(d)
        return d

    loads[0].wait()
    loads[3].wait()
    gain = g.params[0:1, 0:BLOCK]
    xv = g.x[...].astype(F32)
    g.ssq[z] = to_row(lanes_sum(xv * xv))
    g.gains[z] = gain
    core, chip = me[0], s // 2
    partner = {ALONG: s + 1 - 2 * core}
    chips = [{ALONG: lax.rem(s + 2 * d, SEQ)} for d in range(1, 4)]
    piece = cut(48 * (4 * core + chip), 48, 16)
    own = cut(z * BLOCK, BLOCK, 128)
    g.wbc[z, piece, :] = g.w_bc[piece, :]
    small = []
    for i, p in enumerate(zpeers):
        small.append(send(g.ssq.at[z], g.ssq.at[z], g.small, i, p))
        small.append(send(g.gains.at[z], g.gains.at[z], g.small, 3 + i, p))
        small.append(send(g.w_bc.at[piece], g.wbc.at[z, piece], g.small, 6 + i, p))
    middle = lax.rem(z, 3) != 0
    near = [along_line(z, a, b) for a, b in ((1, 2), (2, 0), (3, 3))]

    def block_copy(src, whole, base, slot, k, to):
        cols = cut(k * BLOCK, BLOCK, 128)
        return remote(src, whole.at[:, cols], g.gather_s.at[base + slot], g.gather_r.at[base + k], {ACROSS: to})

    def gather(src, whole, base):
        for j in range(2):
            pending.append(block_copy(src, whole, base, j, z, near[j]))
            pending[-1].start()
        third = block_copy(src, whole, base, 2, z, near[2])

        @pl.when(jnp.logical_not(middle))
        def _():
            third.start()

        return third

    def gathered(src, whole, base, j):
        block_copy(src, whole, base, 0, near[j], z).wait_recv()

    def relay(whole, base):
        part = whole.at[:, cut(near[0] * BLOCK, BLOCK, 128)]

        @pl.when(middle)
        def _():
            block_copy(part, whole, base, 2, near[0], near[1]).start()

    x_own = [block_copy(g.x, g.xg, 0, j, z, near[j]) for j in range(2)]
    x_on = [block_copy(g.xg.at[:, cut(near[j] * BLOCK, BLOCK, 128)], g.xg, 0, 2 + j, near[j], near[1 - j % 2]) for j in range(2)]
    x_on.append(block_copy(g.xg.at[:, cut(near[2] * BLOCK, BLOCK, 128)], g.xg, 0, 4, near[2], near[1]))
    x_own[0].start()

    @pl.when(middle)
    def _():
        x_own[1].start()


    g.wd[...] = jnp.zeros(g.wd.shape, BF)
    g.wd[0:12, :] = g.w_dt[...]
    g.taps[...] = jnp.zeros(g.taps.shape, F32)
    g.taps[0:4, 0:CHANNELS] = g.conv_x_w[...]
    g.taps[0:4, CHANNELS:WIDE] = g.conv_bc_w[...]
    g.taps[4:5, 0:CHANNELS] = g.params[1:2, :]
    g.taps[4:5, CHANNELS:WIDE] = g.params[2:3, 0:256]
    expand_row = lax.broadcasted_iota(jnp.int32, (256, CHANNELS), 0)
    expand_col = lax.broadcasted_iota(jnp.int32, (256, CHANNELS), 1)
    g.spread[...] = jnp.where((expand_col >> 6) == (expand_row & 127), 1.0, 0.0).astype(BF)
    starts = [jnp.int32(0)]
    for k in range(7):
        starts.append(starts[-1] + g.lengths[k])

    def segment(pos):
        total = jnp.full(pos.shape, -1, jnp.int32)
        for k in range(8):
            total = total + jnp.where(pos >= starts[k], 1, 0)
        return total.astype(F32)

    g.segc[...] = segment(
        lax.broadcasted_iota(jnp.int32, (ROWS + HALO, 128), 0) + (s * ROWS - HALO)
    )
    g.segr[...] = segment(lax.broadcasted_iota(jnp.int32, (8, ROWS), 1) + s * ROWS)
    tri_i = lax.broadcasted_iota(jnp.int32, (SPAN, SPAN), 0)
    tri_j = lax.broadcasted_iota(jnp.int32, (SPAN, SPAN), 1)
    g.tri[...] = jnp.where(tri_i >= tri_j, 1.0, 0.0).astype(BF)
    lane = lax.broadcasted_iota(jnp.int32, (1, 128), 1)
    left = lane < 64

    def spread(v):
        hi, lo = parts(v, 2)
        return mul(jnp.concatenate([hi, lo], axis=1), g.spread[...])

    def head_sum(v):
        hi, lo = parts(v, 2)
        e = g.spread[0:128, :]
        return mul(hi, e, NT) + mul(lo, e, NT)

    g.skipe[...] = spread(jnp.broadcast_to(g.params[5:6, 0:128], (8, 128)))
    rates = jnp.exp(g.params[4:5, 0:128])

    for d in small:
        d.wait_recv()
    wide = [
        send(g.wbc.at[:, piece], g.wbc.at[:, piece], g.wide, i, p) for i, p in enumerate(chips)
    ]
    total = g.ssq[0] + g.ssq[1] + g.ssq[2] + g.ssq[3]
    g.xscale[...] = to_col(lax.rsqrt(total / D + epsilon))

    def normalise(k, src):
        gk = g.gains[k]
        cols = cut(k * BLOCK, BLOCK, 128)

        def body(i):
            at = cut(i * 64, 64, 16)
            v = src(at, cols).astype(F32)
            g.xn[at, cols] = (v * wide_of(g.xscale[at, :], 3) * gk).astype(BF)

        loop(ROWS // 64, body)

    def project(k, w, cols, base, first, width=256):
        at = cut(k * BLOCK, BLOCK, 128)

        def body(n):
            p = mul(g.xn[:, at], w[cut(k * BLOCK, BLOCK, 16), cut(n * width, width, 128)])
            dst = cut(base + n * width, width, 128)
            if first:
                g.acc[:, dst] = p
            else:
                g.acc[:, dst] += p

        loop(cols // width, body)

    def project_dt(k, first):
        at = cut(k * BLOCK, BLOCK, 128)
        p = mul(g.xn[:, at], g.wd[:, at], NT)
        if first:
            g.acc[:, WIDE + CHANNELS :] = p
        else:
            g.acc[:, WIDE + CHANNELS :] += p

    normalise(z, lambda at, cols: g.x[at, :])
    loads[1].wait()
    loads[2].wait()
    project(z, g.wx, CHANNELS, 0, True)
    project(z, g.wz, CHANNELS, WIDE, True)
    project_dt(z, True)
    for i, k in enumerate(near):
        if i != 1:
            gathered(g.x, g.xg, 0, i)
        else:
            @pl.when(jnp.logical_not(middle))
            def _():
                gathered(g.x, g.xg, 0, 1)

        if i == 2:
            @pl.when(middle)
            def _():
                x_on[2].start()

        if i == 0:
            @pl.when(middle)
            def _():
                x_on[0].start()
                gathered(g.x, g.xg, 0, 1)
                x_on[1].start()

            for d in wide:
                d.wait_recv()
            share = g.wbc.at[:, cut(192 * core, 192, 16)]
            wide = [send(share, share, g.wide, 3, partner)]
        if i == 2:
            pending.append(gather(g.cotg.at[:, own], g.cotg, 5))
        normalise(k, lambda at, cols: g.xg[at, cols])
        project(k, g.wx, CHANNELS, 0, False)
        if i < 2:
            project(k, g.wz, CHANNELS, WIDE, False)
            project_dt(k, False)
    for d in wide:
        d.wait_recv()
    g.acc[:, CHANNELS:WIDE] = sum(
        mul(g.xn[:, BLOCK * k : BLOCK * k + BLOCK], g.wbc[k]) for k in range(LINE)
    )

    g.edge[...] = g.acc[ROWS - HALO : ROWS, 0:WIDE].astype(BF)
    edge = remote(g.edge, g.halo, g.edge_sem.at[0], g.edge_sem.at[1], {ALONG: s + 1})

    @pl.when(s < SEQ - 1)
    def _():
        edge.start()

    @pl.when(s == 0)
    def _():
        g.halo[...] = jnp.zeros(g.halo.shape, BF)

    def put(i):
        g.cf[cut(HALO + i * 64, 64, 8), :] = (
            g.acc[cut(i * 64, 64, 8), 0:WIDE].astype(BF).astype(F32)
        )

    loop(ROWS // 64, put)
    project(near[2], g.wz, CHANNELS, WIDE, False)
    project_dt(near[2], False)

    step_pre = g.acc[:, WIDE + CHANNELS :] + g.params[3:4, 0:128]
    g.step[...] = jnp.where(lane < 12, jax.nn.softplus(step_pre), 0.0)
    for q in range(2):
        rows = pl.ds(q * SPAN, SPAN)
        log_decay = -rates * g.step[rows, :]
        cum = sum(mul(g.tri[...], p) for p in parts(log_decay, 3))
        g.cum[rows, :] = cum
        g.cumt[q] = cum.T[0:16, :]
        last = cum[SPAN - 1 : SPAN, :]
        seg = g.segc[pl.ds(HALO + q * SPAN, SPAN), :]
        seg_last = g.segc[HALO + q * SPAN + SPAN - 1 : HALO + q * SPAN + SPAN, :]
        seg_prev = g.segc[HALO + q * SPAN - 1 : HALO + q * SPAN, :]
        tail = jnp.where(seg == seg_last, jnp.exp(last - cum), 0.0)
        load = tail * g.step[rows, :]
        lead = jnp.where(seg == seg_prev, jnp.exp(cum), 0.0)
        g.tail[rows, :] = tail
        g.load[rows, :] = load
        g.lead[rows, :] = lead
        g.loadt[q] = load.T[0:16, :]
        g.leadt[q] = lead.T[0:16, :]
        g.stept[q] = g.step[rows, :].T[0:16, :]
        carry = jnp.where(seg_last == seg_prev, jnp.exp(last), 0.0)
        g.carry[q] = jnp.broadcast_to(carry, (8, 128))
        g.carrye[q] = spread(jnp.broadcast_to(carry, (8, 128)))
    g.decay[0] = g.carrye[0] * g.carrye[1]

    def taps_of(first, cols):
        v = g.cf[cut(first + 8, 72, 8), cols]
        sv = g.segc[cut(first + 8, 72, 8), :]
        width = v.shape[1] // 128
        out = []
        for k in range(3):
            same = pltpu.roll(sv, 67 - k, 0)[0:64] == sv[8:72]
            out.append(jnp.where(wide_of(same, width), pltpu.roll(v, 67 - k, 0)[0:64], 0.0))
        out.append(v[8:72])
        return out

    def convolve(i):
        first = i * 64
        at = cut(first, 64, 16)
        for n in range(4):
            cols = pl.ds(n * 256, 256)
            v = jnp.broadcast_to(g.taps[4:5, cols], (64, 256))
            for k, t in enumerate(taps_of(first, cols)):
                v = v + g.taps[k : k + 1, cols] * t
            sig = jax.nn.sigmoid(v)
            act = (v * sig).astype(BF)
            g.slope[at, cols] = sig * (1.0 + v * (1.0 - sig))
            if n < 3:
                g.inner[at, cols] = act
            else:
                g.b[at, :] = act[:, 0:128]
                g.c[at, :] = act[:, 128:256]

    loop(ROWS // 64 - 1, lambda i: convolve(i + 1))

    @pl.when(s > 0)
    def _():
        edge.wait_recv()

    g.cf[0:HALO, :] = g.halo[...].astype(F32)
    convolve(0)

    g.bt[...] = g.b[...].astype(F32).T
    g.ct[...] = g.c[...].astype(F32).T

    def outer(maps, weights, vals):
        def body(t):
            q, p = t // 6, lax.rem(t, 6)
            at = cut(p * 128, 128, 128)
            v = vals[cut(q * SPAN, SPAN, 256), at]
            m = maps[:, cut(q * SPAN, SPAN, 256)]
            o = [mul((m * weights[q, pl.ds(2 * p + e, 1), :]).astype(BF), v) for e in range(2)]
            g.local[q, :, at] = jnp.where(left, o[0], o[1])

        loop(12, body)

    outer(g.bt, g.loadt, g.inner)
    c0, c1 = g.carrye[0][0:1], g.carrye[1][0:1]
    half, rest = cut(core * BLOCK, BLOCK, 128), cut((1 - core) * BLOCK, BLOCK, 128)
    later = []

    class Chain:
        def __init__(self, mine, other, joined, got, result, base, way):
            self.mine, self.other, self.joined, self.got, self.result = mine, other, joined, got, result
            self.base, self.way = base, way
            self.near = self.link(joined, got.at[0], 1, way)
            self.far = self.link(joined, got.at[1], 2, 2 * way)

        def link(self, src, dst, i, hop):
            to = {ALONG: s + 2 * hop}
            return remote(src, dst, g.st_send.at[self.base + i], g.st_recv.at[self.base + i], to)

        def share(self):
            self.first = send(self.mine, self.other, (g.st_send, g.st_recv), self.base, partner)

        def join(self):
            self.first.wait_recv()
            own, other = self.mine[:, half], self.other[:, half]
            even, odd = jnp.where(core == 0, own, other), jnp.where(core == 0, other, own)
            if self.way > 0:
                self.joined[...] = odd_decay() * even + odd
            else:
                self.joined[...] = even + even_decay() * odd
            for d, hop in ((self.near, 1), (self.far, 2)):
                pass_on(d, hop * self.way)
            for i, hop in ((0, 1), (1, 2)):
                outside = chip - hop * self.way

                @pl.when((outside < 0) | (outside > 3))
                def _():
                    self.got[i] = jnp.zeros((STATE, BLOCK), F32)

        def meet(self, decay):
            for d, hop in ((self.near, 1), (self.far, 2)):
                arrive(d, hop * self.way)
            self.result[:, half] = self.got[0] + decay * self.got[1]
            p = self.result.at[:, half]
            self.last = send(p, p, (g.st_send, g.st_recv), self.base + 3, partner)

        def end(self):
            self.last.wait_recv()

    def pass_on(d, hop):
        inside = (chip + hop >= 0) & (chip + hop <= 3)

        @pl.when(inside)
        def _():
            d.start()

        later.append((inside, d))

    def arrive(d, hop):
        @pl.when((chip - hop >= 0) & (chip - hop <= 3))
        def _():
            d.wait_recv()

    def odd_decay():
        return jnp.where(core == 0, g.decay[1, 0:1, half], g.decay[0, 0:1, half])

    def even_decay():
        return jnp.where(core == 0, g.decay[0, 0:1, half], g.decay[1, 0:1, half])

    g.mine[...] = c1 * g.local[0] + g.local[1]
    ahead = Chain(g.mine, g.other, g.joined, g.got, g.chain, 0, 1)
    ahead.share()
    dec = send(g.decay.at[0], g.decay.at[1], (g.st_send, g.st_recv), 8, partner)
    both_up = remote(g.both, g.boths.at[0], g.st_send.at[9], g.st_recv.at[9], {ALONG: s + 2})
    both_down = remote(g.both, g.boths.at[1], g.st_send.at[10], g.st_recv.at[10], {ALONG: s - 2})

    def head_cols(ref, rows, p):
        moved = pltpu.roll(ref[rows, :], lax.rem(128 - 2 * p, 128), 1)
        return moved[:, 0:1], moved[:, 1:2]

    def inside(q, first, count):
        rows = cut(q * SPAN, SPAN, 256)
        seg = g.segc[cut(HALO + q * SPAN, SPAN, 16), 0:1]
        segr = g.segr[0:1, cut(q * SPAN, SPAN, 256)]
        scores = mul(g.c[rows, :], g.b[rows, :], NT)
        g.scores[...] = jnp.where((tri_i >= tri_j) & (seg == segr), scores, 0.0)

        def pair(t):
            p = first + t
            cols = head_cols(g.cum, rows, p)
            at = cut(p * 128, 128, 128)
            outs = []
            for e in range(2):
                row = g.cumt[q, pl.ds(2 * p + e, 1), :]
                step = g.stept[q, pl.ds(2 * p + e, 1), :]
                fall = jnp.exp(jnp.minimum(cols[e] - row, 0.0))
                outs.append(mul((g.scores[...] * fall * step).astype(BF), g.inner[rows, at]))
            g.out[rows, at] = jnp.where(left, outs[0], outs[1])

        loop(count, pair)

    inside(0, 0, 3)
    dec.wait_recv()
    g.both[...] = g.decay[0, :, half] * g.decay[1, :, half]
    ahead.join()
    pass_on(both_up, 1)
    pass_on(both_down, -1)
    for i, hop in ((0, 1), (1, -1)):
        @pl.when((chip - hop < 0) | (chip - hop > 3))
        def _():
            g.boths[i] = jnp.zeros((8, BLOCK), F32)

    inside(0, 3, 3)
    gathered(g.cotg.at[:, own], g.cotg, 5, 0)
    relay(g.cotg, 5)
    inside(1, 0, 6)

    arrive(both_up, 1)
    loads[4].wait()
    gate_gain = g.params[6:7, :]

    def down(k, first):
        at = cut(k * BLOCK, BLOCK, 128)

        def body(n):
            cols = cut(n * 256, 256, 256)
            p = mul(g.cotg[:, at], g.wo[cols, at], NT)
            if first:
                g.ggn[:, cols] = p
            else:
                g.ggn[:, cols] += p

        loop(3, body)

    down(z, True)
    down(near[0], False)
    ahead.meet(g.boths[0, 0:1, :])

    def act(i):
        at = cut(i * 64, 64, 16)
        pre = g.acc[at, gate_cols]
        g.gated[at, :] = pre * jax.nn.sigmoid(pre)

    gate_cols = pl.ds(WIDE, CHANNELS)
    loop(ROWS // 64, act)
    ahead.end()
    from_chips = g.chain[...]
    incoming = jnp.where(core == 0, from_chips, g.other[...] + g.decay[1, 0:1] * from_chips)
    g.sin[0] = incoming
    g.sin[1] = g.local[0] + c0 * incoming
    for q in range(2):
        g.slow[q] = g.sin[q].astype(BF)

    def outside(t):
        q, p = t // 6, lax.rem(t, 6)
        rows, at = cut(q * SPAN, SPAN, 256), cut(p * 128, 128, 128)
        cols = head_cols(g.lead, rows, p)
        cv = g.c[rows, :].astype(F32)
        o = [mul((cv * cols[e]).astype(BF), g.slow[q, :, at]) for e in range(2)]
        g.out[rows, at] += jnp.where(left, o[0], o[1])

    loop(12, outside)

    skip = g.skipe[0:1]

    def gate(i):
        at = cut(i * 64, 64, 16)
        mixed = g.out[at, :] + g.inner[at, :].astype(F32) * skip
        gated = mixed * g.gated[at, :]
        g.gated[at, :] = gated
        g.part[0, at, :] = lanes_sum(gated * gated)

    loop(ROWS // 64, gate)
    g.sqs[z] = to_row(g.part[0])
    squares = [send(g.sqs.at[z], g.sqs.at[z], g.sqsem, i, p) for i, p in enumerate(zpeers)]

    for i in (1, 2):
        gathered(g.cotg.at[:, own], g.cotg, 5, i)
        down(near[i], False)

    def inner_part(i):
        at = cut(i * 64, 64, 16)
        g.part[1, at, :] = lanes_sum(g.ggn[at, :] * gate_gain * g.gated[at, :])

    loop(ROWS // 64, inner_part)
    g.stats[z] = to_row(g.part[1])
    stat = [send(g.stats.at[z], g.stats.at[z], g.stat, i, p) for i, p in enumerate(zpeers)]
    dests = [along_line(z, a, b) for a, b in ((2, 3), (3, 0), (1, 2))]

    class Scatter:
        def __init__(self, sent, got, via, base):
            self.sent, self.got, self.via, self.base = sent, got, via, base

        def copy(self, j, dst, i, to):
            return remote(self.sent[j], dst, g.block_s.at[self.base + j], g.block_r.at[self.base + i], {ACROSS: to})

        def direct(self, j):
            slot = lax.rem(z - dests[j] + 7, 4)
            return self.copy(j, self.got.at[slot], slot, dests[j])

        def block(self, j, value):
            v = value
            if j == 2:
                @pl.when(middle)
                def _():
                    self.copy(0, self.via, 3, z).wait_recv()

                v = v + self.via[...].astype(F32)
            self.sent[j][...] = v.astype(BF)
            if j == 0:
                @pl.when(middle)
                def _():
                    self.direct(0).start()

                @pl.when(jnp.logical_not(middle))
                def _():
                    self.copy(0, self.via, 3, dests[2]).start()
            else:
                self.direct(j).start()

        def arrived(self):
            for i in (0, 2):
                self.copy(0, self.got.at[i], i, z).wait_recv()

            @pl.when(jnp.logical_not(middle))
            def _():
                self.copy(0, self.got.at[1], 1, z).wait_recv()

        def left(self):
            for j in range(3):
                self.copy(j, self.via, 3, z).wait_send()

    blocks = [pl.ds(0, BLOCK), pl.ds(BLOCK, BLOCK)]
    out_blocks = Scatter([g.sblk.at[j] for j in range(3)], g.rblk, g.via, 0)
    in_blocks = Scatter(
        [g.gn.at[:, blocks[0]], g.gn.at[:, blocks[1]], g.inner.at[:, blocks[0]]], g.rblk2, g.via2, 4
    )

    @pl.when(middle)
    def _():
        g.rblk[1] = jnp.zeros((ROWS, BLOCK), BF)
        g.rblk2[1] = jnp.zeros((ROWS, BLOCK), BF)

    @pl.when(jnp.logical_not(middle))
    def _():
        g.via[...] = jnp.zeros((ROWS, BLOCK), BF)
        g.via2[...] = jnp.zeros((ROWS, BLOCK), BF)

    def out_block(k):
        return mul(g.gn[...], g.wo[:, cut(k * BLOCK, BLOCK, 128)])

    for d in squares:
        d.wait_recv()
    gscale = lax.rsqrt((g.sqs[0] + g.sqs[1] + g.sqs[2] + g.sqs[3]) / INNER + epsilon)
    g.part[0] = to_col(gscale)

    @pl.when(middle)
    def _():
        for d in x_on:
            d.wait_send()

    def norm_gate(i):
        at = cut(i * 64, 64, 16)
        g.gn[at, :] = (g.gated[at, :] * wide_of(g.part[0, at, :], 6) * gate_gain).astype(BF)

    loop(ROWS // 64, norm_gate)
    out_blocks.block(0, out_block(dests[0]))
    out_blocks.block(1, out_block(dests[1]))
    t_out, t_z, t_xa, t_xb = [
        Total(ref, sum_bufs[5 * i : 5 * i + 5], g.tot_send, g.tot_recv, g.freed, 10 * i, me)
        for i, ref in enumerate((g.p_out, g.p_z, g.p_xa, g.p_xb))
    ]

    def grad_out(n):
        at = cut(n * 256, 256, 256)
        g.p_out[at, :] = mul(g.gn[:, at], g.cotg[...], TN).astype(BF)

    loop(3, grad_out)
    t_out.s0()

    for d in stat:
        d.wait_recv()
    sums = g.stats[0] + g.stats[1] + g.stats[2] + g.stats[3]
    g.part[1] = to_col(gscale * gscale * gscale * sums / INNER)
    g.vacc[...] = jnp.zeros(g.vacc.shape, F32)
    g.pack[...] = jnp.zeros(g.pack.shape, F32)
    g.bcv[z] = jnp.zeros((8, 256), F32)

    def ungate(i):
        at = cut(i * 64, 64, 16)
        a = wide_of(g.part[0, at, :], 6)
        pre = g.acc[at, gate_cols]
        vals = g.inner[at, :].astype(F32)
        mixed = g.out[at, :] + vals * skip
        gated, ggn = g.gated[at, :], g.ggn[at, :]
        gg = a * (ggn * gate_gain) - gated * wide_of(g.part[1, at, :], 6)
        sig = jax.nn.sigmoid(pre)
        gm = (gg * (pre * sig)).astype(BF)
        g.gm[at, :] = gm
        g.gz[at, :] = (gg * mixed * (sig * (1.0 + pre * (1.0 - sig)))).astype(BF)
        g.vacc[0] += rows_sum(ggn * gated * a)
        g.vacc[1] += rows_sum(gm.astype(F32) * vals)

    loop(ROWS // 64, ungate)
    t_out.s1()

    outer(g.ct, g.leadt, g.gm)
    g.mine_b[...] = g.local[0] + c0 * g.local[1]
    behind = Chain(g.mine_b, g.other_b, g.joined_b, g.got_b, g.chain_b, 4, -1)
    behind.share()

    def grad_z(n):
        at = cut(n * 256, 256, 256)
        g.p_z[at, :] = mul(g.xn[:, at], g.gz[...], TN).astype(BF)

    loop(6, grad_z)
    behind.join()
    t_z.s0()
    g.own[...] = mul(g.gn[...], g.wo[:, own])

    def inside_back(q, first, count):
        rows = cut(q * SPAN, SPAN, 256)
        seg = g.segc[cut(HALO + q * SPAN, SPAN, 16), 0:1]
        segr = g.segr[0:1, cut(q * SPAN, SPAN, 256)]
        mask = (tri_i <= tri_j) & (seg == segr)
        if first == 0:
            g.scores[...] = jnp.where(mask, mul(g.b[rows, :], g.c[rows, :], NT), 0.0)
            g.gscores[...] = jnp.zeros((SPAN, SPAN), F32)

        def pair(t):
            p = first + t
            cols = head_cols(g.cum, rows, p)
            at = cut(p * 128, 128, 128)
            steps = head_cols(g.step, rows, p)
            gm = g.gm[rows, at]
            outs = []
            for e in range(2):
                row = g.cumt[q, pl.ds(2 * p + e, 1), :]
                fall = jnp.exp(jnp.minimum(row - cols[e], 0.0)) * steps[e]
                outs.append(mul((g.scores[...] * fall).astype(BF), gm))
                keep = left if e == 0 else jnp.logical_not(left)
                vals = jnp.where(keep, g.inner[rows, at].astype(F32), 0.0).astype(BF)
                g.gscores[...] += mul(vals, gm, NT) * fall
            g.z[rows, at] = jnp.where(left, outs[0], outs[1])

        loop(count, pair)
        if first + count < 6:
            return
        gs = jnp.where(mask, g.gscores[...], 0.0)
        hi, lo = parts(gs, 2)
        g.gb[rows, :] = mul(hi, g.c[rows, :]) + mul(lo, g.c[rows, :])
        g.gc[rows, :] = mul(hi, g.b[rows, :], TN) + mul(lo, g.b[rows, :], TN)

    inside_back(1, 0, 3)
    t_z.s1()
    inside_back(1, 3, 3)
    inside_back(0, 0, 6)
    arrive(both_down, -1)
    behind.meet(g.boths[1, 0:1, :])
    out_blocks.block(2, out_block(dests[2]))
    t_out.s2()

    behind.end()
    from_chips = g.chain_b[...]
    beyond = jnp.where(core == 1, from_chips, g.other_b[...] + g.decay[1, 0:1] * from_chips)
    g.gloc[1] = beyond
    g.gloc[0] = g.local[1] + c1 * beyond
    ends = []
    for q in range(2):
        rows = pl.ds(q * SPAN, SPAN)
        glow = g.gloc[q].astype(BF)
        vals = g.inner[rows, :].astype(F32)
        gm = g.gm[rows, :].astype(F32)
        loade = spread(g.load[rows, :])
        bg = mul(g.b[rows, :], glow)
        zed = g.z[rows, :]
        carry_sum = jnp.sum(g.gloc[q] * g.sin[q], axis=0, keepdims=True)
        grad_carry = head_sum(jnp.broadcast_to(carry_sum, (8, CHANNELS)))[0:1]
        t1 = head_sum(gm * g.out[rows, :])
        q1 = head_sum(vals * zed)
        q2 = head_sum(vals * bg)
        step, load = g.step[rows, :], g.load[rows, :]
        tail_term = q2 * load
        gcum = t1 - q1 - tail_term
        end = jnp.sum(tail_term, axis=0, keepdims=True) + grad_carry * g.carry[q][0:1]
        is_last = lax.broadcasted_iota(jnp.int32, (SPAN, 128), 0) == SPAN - 1
        gcum = gcum + jnp.where(is_last, end, 0.0)
        glog = sum(mul(g.tri[...], p, TN) for p in parts(gcum, 3))
        gstep = jnp.where(step > 1e-30, q1 / jnp.maximum(step, 1e-30), 0.0) + q2 * g.tail[rows, :]
        gpre = (gstep - rates * glog) * jax.nn.sigmoid(
            g.acc[rows, WIDE + CHANNELS :] + g.params[3:4, 0:128]
        )
        g.gsr[rows, :] = gpre.astype(BF)
        ends.append((rows_sum(gpre), rows_sum(glog * (-rates * step))))
        g.z[rows, :] = zed + loade * bg + skip * gm
        g.gb[rows, :] += sum(mul(p, glow, NT) for p in parts(vals * loade, 2))
        g.gc[rows, :] += sum(mul(p, g.slow[q], NT) for p in parts(gm * spread(g.lead[rows, :]), 2))
    g.pack[16:24, 0:128] = jnp.broadcast_to(
        jnp.sum(ends[0][0] + ends[1][0], axis=0, keepdims=True), (8, 128)
    )
    g.pack[16:24, 128:256] = jnp.broadcast_to(
        jnp.sum(ends[0][1] + ends[1][1], axis=0, keepdims=True), (8, 128)
    )
    def grads_of(at, n):
        cols = pl.ds(n * 256, 256)
        if n < 3:
            v = g.z[at, cols]
        else:
            v = jnp.concatenate([g.gb[at, :], g.gc[at, :]], axis=1)
        return v * g.slope[at, cols]

    def slopes(i):
        at = cut(i * 64, 64, 16)
        for n in range(4):
            g.gconv[cut(i * 64, 64, 8), pl.ds(n * 256, 256)] = grads_of(at, n)

    g.gconv[ROWS : ROWS + 16, :] = jnp.zeros((16, WIDE), F32)
    loop(ROWS // 64, slopes)

    v = g.gconv[0:8, :]
    sv = g.segc[HALO - 8 : HALO + 8, :]
    back_rows = jnp.zeros((8, WIDE), F32)
    for k in range(3):
        shift = 3 - k
        full = jnp.concatenate([jnp.zeros((8, WIDE), F32), v], axis=0)
        src = pltpu.roll(full, 16 - shift, 0)[0:8]
        same = pltpu.roll(sv, 16 - shift, 0)[0:8] == sv[0:8]
        back_rows = back_rows + jnp.where(wide_of(same, 8), g.taps[k : k + 1, :] * src, 0.0)
    g.ret_out[...] = back_rows
    ret = remote(g.ret_out, g.ret_in, g.edge_sem.at[2], g.edge_sem.at[3], {ALONG: s - 1})

    @pl.when(s > 0)
    def _():
        ret.start()

    @pl.when(s == SEQ - 1)
    def _():
        g.ret_in[...] = jnp.zeros((8, WIDE), F32)

    g.wacc[...] = jnp.zeros(g.wacc.shape, F32)

    def convolve_back(i):
        first = i * 64
        at = cut(first, 64, 16)
        sv = g.segc[cut(first + HALO, 64, 8), :]
        ahead = jnp.where(i < ROWS // 64 - 1, 1.0, 0.0)
        for n in range(4):
            cols = pl.ds(n * 256, 256)
            v = g.gconv[cut(first, 72, 8), cols]
            here = v[0:64]
            total = g.taps[3:4, cols] * here
            nxt = g.segc[cut(jnp.minimum(first + HALO + 64, ROWS + HALO - 8), 8, 8), :]
            sfull = jnp.concatenate([sv, nxt], axis=0)
            for k in range(3):
                shift = 3 - k
                same = pltpu.roll(sfull, 72 - shift, 0)[0:64] == sv
                src = pltpu.roll(v, 72 - shift, 0)[0:64]
                total = total + jnp.where(wide_of(same, 2), g.taps[k : k + 1, cols] * src, 0.0)
            if n < 3:
                g.gx[at, cols] = total.astype(BF)
            else:
                for k, v in enumerate(parts(total, 2)):
                    g.gbc[k, at, :] = v

            @pl.when(i == ROWS // 64 - 1)
            def _():
                g.tail_rows[:, cols] = total[48:64]

            for k, t in enumerate(taps_of(first, cols)):
                g.wacc[k, :, cols] += rows_sum(here * t)
            g.wacc[4, :, cols] += rows_sum(here)

    loop(ROWS // 64, convolve_back)
    t_z.s2()

    @pl.when(s < SEQ - 1)
    def _():
        ret.wait_recv()

    last_rows = g.tail_rows[...] + jnp.concatenate([jnp.zeros((8, WIDE), F32), g.ret_in[...]], axis=0)
    g.gx[ROWS - 16 : ROWS, :] = last_rows[:, 0:CHANNELS].astype(BF)
    for k, v in enumerate(parts(last_rows[:, CHANNELS:WIDE], 2)):
        g.gbc[k, ROWS - 16 : ROWS, :] = v

    def bc_block(at):
        both = mul(g.xn[:, at], jnp.concatenate([g.gbc[0], g.gbc[1]], axis=1), TN)
        return both[:, 0:256] + both[:, 256:512]

    for k in range(5):
        row = jnp.sum(g.wacc[k], axis=0, keepdims=True)
        g.pack[k : k + 1, :] = row[:, 0:CHANNELS]
        g.bcv[z, k : k + 1, :] = row[:, CHANNELS:WIDE]
    bcv = [send(g.bcv.at[z], g.bcv.at[z], g.bcvsem, i, p) for i, p in enumerate(zpeers)]
    def grad_x(ref, first):
        def body(n):
            at = cut(n * 256, 256, 256)
            ref[at, :] = mul(g.xn[:, cut(first + n * 256, 256, 256)], g.gx[...], TN).astype(BF)

        loop(3, body)

    grad_x(g.p_xa, 0)
    t_xa.s0()
    grad_x(g.p_xb, CHANNELS)
    t_xb.s0()
    t_out.s3()
    bcs = []
    bc_parts = [g.acc.at[pl.ds(0, BLOCK), pl.ds(WIDE + 256 * i, 256)] for i in range(3)]
    bc_parts.append(g.acc.at[pl.ds(0, BLOCK), pl.ds(BLOCK, 256)])
    mine, other = cut(core * 192, 192, 16), cut((1 - core) * 192, 192, 16)
    halves = []
    for i in range(LINE):
        bc_parts[i][...] = bc_block(cut(lax.rem(z + 1 + i, LINE) * BLOCK, BLOCK, 128))
        halves.append(send(bc_parts[i].at[other], g.hbc.at[i], g.bcsem, 3 + i, partner))
    t_xa.s1()
    t_xb.s1()
    for d in halves:
        d.wait_recv()
    g.bcsum[...] = bc_parts[3][mine, :] + g.hbc[3]
    for i, p in enumerate(zpeers):
        g.tbc[i] = (bc_parts[i][mine, :] + g.hbc[i]).astype(BF)
        bcs.append(send(g.tbc.at[i], g.rbc.at[i], g.bcsem, i, p))

    def back_block(k):
        at = cut(k * BLOCK, BLOCK, 16)
        v = mul(g.gx[...], g.wx[at, :], NT) + mul(g.gz[...], g.wz[at, :], NT)
        return v + mul(g.gsr[...], g.wd[:, cut(k * BLOCK, BLOCK, 128)]) + mul(g.gbc[0], g.wbc[k], NT) + mul(g.gbc[1], g.wbc[k], NT)

    in_blocks.block(0, back_block(dests[0]))
    t_z.s3()
    in_blocks.block(1, back_block(dests[1]))
    t_out.s4()
    g.own_in[...] = back_block(z)
    t_xa.s2()
    t_xb.s2()
    t_z.s4()

    for d in bcs + bcv:
        d.wait_recv()
    g.pack[8:16, 0:256] = g.bcv[0] + g.bcv[1] + g.bcv[2] + g.bcv[3]
    g.pack[5:6, :] = jnp.sum(g.vacc[0], axis=0, keepdims=True)
    skips = head_sum(jnp.broadcast_to(jnp.sum(g.vacc[1], axis=0, keepdims=True), (8, CHANNELS)))
    g.pack[16:24, 256:384] = skips
    bc = g.bcsum[...]
    for i in range(3):
        bc = bc + g.rbc[i].astype(F32)
    g.q_out[0:192, :] = bc.astype(BF)
    for n in range(6):
        cols = pl.ds(256 * n, 256)
        g.few[16 * n : 16 * n + 16, :] = mul(g.gsr[...], g.xn[:, cols], TN)[0:16]
    for n in range(3):
        g.few[96 + 24 * n : 120 + 24 * n, :] = g.pack[:, 256 * n : 256 * n + 256]
    g.few[168:192, :] = jnp.zeros((24, 256), F32)
    few = send(g.few, g.few_in, g.restsem, 0, partner)
    in_blocks.block(2, back_block(dests[2]))
    t_xa.s3()
    few.wait_recv()
    few_half = cut(96 * core, 96, 8)
    g.q_out[192:288, :] = (g.few[few_half, :] + g.few_in[few_half, :]).astype(BF)
    across_x = send(g.q_out, g.q_in.at[0], g.restsem, 1, {ALONG: s + 2 - 4 * me[1]})
    t_xb.s3()
    t_xa.s4()
    across_x.wait_recv()
    g.q_mid[...] = (g.q_out[...].astype(F32) + g.q_in[0].astype(F32)).astype(BF)
    across_y = send(g.q_mid, g.q_in.at[1], g.restsem, 2, {ALONG: s + 4 - 8 * me[2]})
    t_xb.s4()
    t_out.s5()
    out_blocks.arrived()
    out_sum = g.own[...]
    for i in range(3):
        out_sum = out_sum + g.rblk[i].astype(F32)
    g.layer_out[...] = (g.x[...].astype(F32) + out_sum).astype(BF)

    in_blocks.arrived()
    g.nacc[...] = jnp.zeros(g.nacc.shape, F32)

    def finish(i):
        at = cut(i * 64, 64, 16)
        v = g.own_in[at, :]
        for k in range(3):
            v = v + g.rblk2[k, at, :].astype(F32)
        g.own_in[at, :] = v
        x = g.x[at, :].astype(F32)
        g.part[0, at, :] = lanes_sum(v * gain * x)
        g.nacc[...] += rows_sum(v * x * wide_of(g.xscale[at, :], 3))

    loop(ROWS // 64, finish)
    g.nstat[z] = to_row(g.part[0])
    nst = [send(g.nstat.at[z], g.nstat.at[z], g.nsem, i, p) for i, p in enumerate(zpeers)]
    g.ngain[0] = jnp.sum(g.nacc[...], axis=0, keepdims=True)
    ngs = [send(g.ngain.at[0], g.ngain.at[1 + i], g.nsem, 3 + i, p) for i, p in enumerate(speers)]
    t_z.s5()
    t_xa.s5()
    t_xb.s5()
    across_y.wait_recv()
    g.rest[core] = g.q_mid[...].astype(F32) + g.q_in[1].astype(F32)
    q_last = send(g.rest.at[core], g.rest.at[core], g.restsem, 3, partner)
    t_out.s6()
    store = [pltpu.make_async_copy(g.p_out, g.grad_out, g.load_sem.at[5])]
    store[0].start()
    t_z.s6()
    store.append(pltpu.make_async_copy(g.p_z, g.grad_z, g.load_sem.at[6]))
    store[1].start()
    for d in nst:
        d.wait_recv()
    rows = g.nstat[0] + g.nstat[1] + g.nstat[2] + g.nstat[3]
    g.part[0] = to_col(rows / D)

    def last(i):
        at = cut(i * 64, 64, 16)
        sc = wide_of(g.xscale[at, :], 3)
        x = g.x[at, :].astype(F32)
        g.grad_in[at, :] = (
            g.cotg[at, own].astype(F32)
            + sc * (g.own_in[at, :] * gain)
            - x * (sc * sc * sc * wide_of(g.part[0, at, :], 3))
        )

    loop(ROWS // 64, last)
    for d in ngs:
        d.wait_recv()
    total = g.ngain[0]
    for i in range(7):
        total = total + g.ngain[1 + i]
    g.grad_gain[...] = jnp.broadcast_to(total, (8, BLOCK))
    q_last.wait_recv()
    for i, (t, ref) in enumerate(((t_xa, g.p_xa), (t_xb, g.p_xb))):
        t.s6()
        rows_of = pl.ds(CHANNELS * i, CHANNELS)
        store.append(pltpu.make_async_copy(ref, g.grad_x.at[rows_of], g.load_sem.at[7 + i]))
        store[-1].start()
    for d in pending:
        d.wait_send()

    @pl.when(s < SEQ - 1)
    def _():
        edge.wait_send()

    @pl.when(s > 0)
    def _():
        ret.wait_send()

    x_own[0].wait_send()

    @pl.when(middle)
    def _():
        x_own[1].wait_send()

    for inside_it, d in later:
        @pl.when(inside_it)
        def _():
            d.wait_send()

    out_blocks.left()
    in_blocks.left()
    for d in store:
        d.wait()


def unpack_kernel(
    layer_hbm, in_hbm, out_low, z_low, x_low, rest_hbm, gain_sum,
    layer_out, grad_in, gain, w_z, w_x, w_bc, w_dt, conv_x_w, conv_x_b, conv_bc_w, conv_bc_b, dt_bias, a_log, d_skip, gate_gain, w_out,
    low_a, low_b, low_c, full_a, full_b, full_c, keep_a, keep_b, rest, bc_rows, in_sem, out_sem,
):
    steps = 6
    mats = [(out_low, low_a, full_a, w_out), (z_low, low_b, full_b, w_z), (x_low, low_c, full_c, w_x)]
    loads, stores = [], []
    for m, (src, low, _, _) in enumerate(mats):
        n = low.shape[0] // steps
        for i in range(steps):
            at = pl.ds(i * n, n)
            loads.append(pltpu.make_async_copy(src.at[at], low.at[at], in_sem.at[steps * m + i]))
    for i, (src, dst) in enumerate([(layer_hbm, keep_a), (in_hbm, keep_b), (rest_hbm, rest)]):
        loads.append(pltpu.make_async_copy(src, dst, in_sem.at[18 + i]))
    for d in loads:
        d.start()
    for m, (_, low, full, dst) in enumerate(mats):
        n = low.shape[0] // steps
        for i in range(steps):
            loads[steps * m + i].wait()
            at = pl.ds(i * n, n)
            full[at, :] = low[at, :].astype(F32)
            stores.append(pltpu.make_async_copy(full.at[at], dst.at[at], out_sem.at[steps * m + i]))
            stores[-1].start()
    for i, (src, dst) in enumerate([(keep_a, layer_out), (keep_b, grad_in)]):
        loads[18 + i].wait()
        stores.append(pltpu.make_async_copy(src, dst, out_sem.at[18 + i]))
        stores[-1].start()
    loads[20].wait()
    for n in range(3):
        gain[n : n + 1, :] = gain_sum[0:1, 128 * n : 128 * n + 128]
    bc_rows[0:192, :] = rest[0, 0:192, :]
    bc_rows[192:BLOCK, :] = rest[1, 0:192, :]
    stores.append(pltpu.make_async_copy(bc_rows, w_bc, out_sem.at[20]))
    stores[-1].start()
    for n in range(6):
        w_dt[:, 256 * n : 256 * n + 256] = rest[0, 192 + 16 * n : 204 + 16 * n, :]
    for n in range(3):
        at, base = pl.ds(256 * n, 256), 192 + 24 * n
        conv_x_w[:, at] = rest[1, base : base + 4, :]
        for e in range(2):
            lanes, to = pl.ds(128 * e, 128), pl.ds(2 * n + e, 1)
            conv_x_b[to, :] = rest[1, base + 4 : base + 5, lanes]
            gate_gain[to, :] = rest[1, base + 5 : base + 6, lanes]
    conv_bc_w[...] = rest[1, 200:204, :]
    for e in range(2):
        conv_bc_b[e : e + 1, :] = rest[1, 204:205, 128 * e : 128 * e + 128]
    dt_bias[...] = rest[1, 208:209, 0:12]
    a_log[...] = rest[1, 208:209, 128:140]
    d_skip[...] = rest[1, 232:233, 0:12]
    for d in stores:
        d.wait()


def fast_layer(
    hidden_in, seq_lengths, norm_gain, w_z, w_x, w_bc, w_dt, conv_x_w, conv_x_b, conv_bc_w,
    conv_bc_b, dt_bias, a_log, d_skip, gate_gain, w_out, cotangent,
):
    row = lambda v: v.reshape(-1, min(128, v.shape[0]))
    vm = pl.BlockSpec(memory_space=pltpu.VMEM)
    hbm = pl.BlockSpec(memory_space=pltpu.HBM)
    sm = pl.BlockSpec(memory_space=pltpu.SMEM)
    ins = dict(
        x_hbm=(hidden_in, hbm), cot_hbm=(cotangent, hbm), w_x=(w_x, hbm), w_z=(w_z, hbm), w_out=(w_out, hbm),
        lengths=(seq_lengths, sm), norm_gain=(row(norm_gain), vm), conv_x_b=(row(conv_x_b), vm),
        conv_bc_b=(row(conv_bc_b), vm), dt_bias=(row(dt_bias), vm), a_log=(row(a_log), vm), d_skip=(row(d_skip), vm),
        gate_gain=(row(gate_gain), vm), w_bc=(w_bc, vm), w_dt=(w_dt.T, vm),
        conv_x_w=(conv_x_w, vm), conv_bc_w=(conv_bc_w, vm),
    )
    outs = dict(
        layer_out=((ROWS, BLOCK), BF, vm),
        grad_in=((ROWS, BLOCK), F32, vm),
        grad_out=((CHANNELS, D), BF, hbm),
        grad_z=((D, CHANNELS), BF, hbm),
        grad_x=((D, CHANNELS), BF, hbm),
        rest=((2, 288, 256), F32, vm),
        grad_gain=((8, BLOCK), F32, vm),
    )
    V = pltpu.VMEM
    S = pltpu.SemaphoreType.DMA
    scr = dict(
        x=V((ROWS, BLOCK), BF),
        wx=V((D, CHANNELS), BF),
        wz=V((D, CHANNELS), BF),
        wo=V((CHANNELS, D), BF),
        xg=V((ROWS, D), BF),
        xn=V((ROWS, D), BF),
        cotg=V((ROWS, D), BF),
        ssq=V((LINE, 1, ROWS), F32),
        gains=V((LINE, 1, BLOCK), F32),
        wbc=V((LINE, BLOCK, 256), BF),
        wd=V((128, D), BF),
        params=V((8, CHANNELS), F32),
        taps=V((8, WIDE), F32),
        spread=V((256, CHANNELS), BF),
        segc=V((ROWS + HALO, 128), F32),
        segr=V((8, ROWS), F32),
        tri=V((SPAN, SPAN), BF),
        skipe=V((8, CHANNELS), F32),
        xscale=V((ROWS, 128), F32),
        acc=V((ROWS, WIDE + CHANNELS + 128), F32),
        edge=V((HALO, WIDE), BF),
        halo=V((HALO, WIDE), BF),
        cf=V((ROWS + HALO, WIDE), F32),
        step=V((ROWS, 128), F32),
        cum=V((ROWS, 128), F32),
        cumt=V((2, 16, SPAN), F32),
        tail=V((ROWS, 128), F32),
        load=V((ROWS, 128), F32),
        lead=V((ROWS, 128), F32),
        carry=V((2, 8, 128), F32),
        carrye=V((2, 8, CHANNELS), F32),
        decay=V((2, 8, CHANNELS), F32),
        slope=V((ROWS + 16, WIDE), F32),
        inner=V((ROWS, CHANNELS), BF),
        b=V((ROWS, 128), BF),
        c=V((ROWS, 128), BF),
        bt=V((STATE, ROWS), F32),
        ct=V((STATE, ROWS), F32),
        loadt=V((2, 16, SPAN), F32),
        leadt=V((2, 16, SPAN), F32),
        stept=V((2, 16, SPAN), F32),
        local=V((2, STATE, CHANNELS), F32),
        mine=V((STATE, CHANNELS), F32),
        other=V((STATE, CHANNELS), F32),
        joined=V((STATE, BLOCK), F32),
        got=V((2, STATE, BLOCK), F32),
        chain=V((STATE, CHANNELS), F32),
        mine_b=V((STATE, CHANNELS), F32),
        other_b=V((STATE, CHANNELS), F32),
        joined_b=V((STATE, BLOCK), F32),
        got_b=V((2, STATE, BLOCK), F32),
        chain_b=V((STATE, CHANNELS), F32),
        both=V((8, BLOCK), F32),
        boths=V((2, 8, BLOCK), F32),
        scores=V((SPAN, SPAN), F32),
        gscores=V((SPAN, SPAN), F32),
        out=V((ROWS, CHANNELS), F32),
        sin=V((2, STATE, CHANNELS), F32),
        slow=V((2, STATE, CHANNELS), BF),
        gated=V((ROWS, CHANNELS), F32),
        part=V((2, ROWS, 128), F32),
        stats=V((LINE, 1, ROWS), F32),
        sqs=V((LINE, 1, ROWS), F32),
        vacc=V((2, 8, CHANNELS), F32),
        gm=V((ROWS, CHANNELS), BF),
        gloc=V((2, STATE, CHANNELS), F32),
        sblk=V((3, ROWS, BLOCK), BF),
        rblk=V((3, ROWS, BLOCK), BF),
        rblk2=V((3, ROWS, BLOCK), BF),
        gsr=V((ROWS, 128), BF),
        pack=V((24, CHANNELS), F32),
        ret_out=V((8, WIDE), F32),
        ret_in=V((8, WIDE), F32),
        wacc=V((5, 8, WIDE), F32),
        gbc=V((2, ROWS, 256), BF),
        tail_rows=V((16, WIDE), F32),
        hbc=V((LINE, 192, 256), F32),
        tbc=V((3, 192, 256), BF),
        rbc=V((3, 192, 256), BF),
        via=V((ROWS, BLOCK), BF),
        via2=V((ROWS, BLOCK), BF),
        bcv=V((LINE, 8, 256), F32),
        nacc=V((8, BLOCK), F32),
        nstat=V((LINE, 1, ROWS), F32),
        ngain=V((8, 1, BLOCK), F32),
        p_out=V((CHANNELS, D), BF),
        p_z=V((D, CHANNELS), BF),
        p_xa=V((CHANNELS, CHANNELS), BF),
        p_xb=V((CHANNELS, CHANNELS), BF),
        bcsum=V((192, 256), F32),
        few=V((192, 256), F32),
        few_in=V((192, 256), F32),
        q_out=V((288, 256), BF),
        q_mid=V((288, 256), BF),
        q_in=V((2, 288, 256), BF),
        load_sem=S((9,)),
        edge_sem=S((4,)),
        gather_s=S((8,)),
        gather_r=S((9,)),
        block_s=S((8,)),
        block_r=S((8,)),
        st_send=S((11,)),
        st_recv=S((11,)),
        tot_send=S((40,)),
        tot_recv=S((40,)),
        freed=pltpu.SemaphoreType.REGULAR((12,)),
    )
    pairs = dict(
        small=9,
        wide=4,
        stat=3,
        sqsem=3,
        bcsem=7,
        restsem=4,
        bcvsem=3,
        nsem=10,
    )
    sums = [(CHANNELS, D, BF), (D, CHANNELS, BF), (CHANNELS, CHANNELS, BF), (CHANNELS, CHANNELS, BF)]
    bufs = [b for spec in sums for b in total_bufs(*spec)]
    sems = [S((k,)) for k in pairs.values() for _ in range(2)]
    names = [*ins, *outs, *scr]

    def kernel(*refs):
        n, m = len(names), len(names) + len(bufs)
        d = dict(zip(names, refs[:n]))
        rest = refs[m:]
        for i, name in enumerate(pairs):
            d[name] = (rest[2 * i], rest[2 * i + 1])
        layer_kernel(d, refs[n:m])

    res = pl.pallas_call(
        kernel,
        out_shape=[jax.ShapeDtypeStruct(sh, dt) for sh, dt, _ in outs.values()],
        in_specs=[sp for _, sp in ins.values()],
        out_specs=[sp for _, _, sp in outs.values()],
        scratch_shapes=[*scr.values(), *bufs, *sems],
        compiler_params=pltpu.CompilerParams(collective_id=0, has_side_effects=True, vmem_limit_bytes=66 * 2**20 - 2**21),
        name="layer",
    )(*[a for a, _ in ins.values()])
    layer_out, grad_in, grad_out, grad_z, grad_x, rest, grad_gain = res
    shapes = dict(
        layer_out=((ROWS, BLOCK), BF, hbm), grad_in=((ROWS, BLOCK), F32, hbm), gain=((3, 128), F32, vm), w_z=((D, CHANNELS), F32, hbm),
        w_x=((D, CHANNELS), F32, hbm), w_bc=((BLOCK, 256), F32, hbm), w_dt=((12, D), F32, vm), conv_x_w=((4, CHANNELS), F32, vm),
        conv_x_b=((6, 128), F32, vm), conv_bc_w=((4, 256), F32, vm), conv_bc_b=((2, 128), F32, vm), dt_bias=((1, 12), F32, vm),
        a_log=((1, 12), F32, vm), d_skip=((1, 12), F32, vm), gate_gain=((6, 128), F32, vm), w_out=((CHANNELS, D), F32, hbm),
    )
    final = pl.pallas_call(
        unpack_kernel,
        out_shape=[jax.ShapeDtypeStruct(sh, dt) for sh, dt, _ in shapes.values()],
        in_specs=[hbm] * 6 + [vm],
        out_specs=[sp for _, _, sp in shapes.values()],
        scratch_shapes=[
            V((CHANNELS, D), BF), V((D, CHANNELS), BF), V((D, CHANNELS), BF),
            V((CHANNELS, D), F32), V((D, CHANNELS), F32), V((D, CHANNELS), F32),
            V((ROWS, BLOCK), BF), V((ROWS, BLOCK), F32), V((2, 288, 256), F32), V((BLOCK, 256), F32), S((21,)), S((21,)),
        ],
        compiler_params=pltpu.CompilerParams(vmem_limit_bytes=63 * 2**20),
    )(layer_out, grad_in, grad_out, grad_z, grad_x, rest, grad_gain)
    flat = [v.reshape(v.size) if v.shape[1] <= 128 else v for v in final]
    flat[6] = flat[6].T
    return tuple(flat)


def solution(mesh):
    placed = (
        P("seq", "head"),
        P(),
        P("head"),
        P(None, "head"),
        P(None, "head"),
        P("head", None),
        P(None, "head"),
        P(None, "head"),
        P("head"),
        P(),
        P(),
        P("head"),
        P("head"),
        P("head"),
        P("head"),
        P("head", None),
        P("seq", "head"),
    )
    fits = mesh.shape["seq"] == SEQ and mesh.shape["head"] == LINE
    return jax.shard_map(
        fast_layer if fits else on_device,
        mesh=mesh,
        in_specs=placed,
        out_specs=(
            P("seq", "head"),
            P("seq", "head"),
            P("head"),
            P(None, "head"),
            P(None, "head"),
            P("head", None),
            P(None, "head"),
            P(None, "head"),
            P("head"),
            P(),
            P(),
            P("head"),
            P("head"),
            P("head"),
            P("head"),
            P("head", None),
        ),
        check_vma=False,
    )
```

```python
import jax
import jax.numpy as jnp
from jax import lax
from jax.experimental import pallas as pl
from jax.experimental.pallas import tpu as pltpu
from jax.sharding import PartitionSpec as P

D = 1536
HEAD_DIM = 64
STATE = 128
CONV = 4
SPAN = 256
INNER = 3072


epsilon = 1e-05
highest = lax.Precision.HIGHEST


def prefix(part, axis, combine, identity, reverse):
    count = lax.axis_size(axis)
    place = lax.axis_index(axis)
    ahead = count - 1 - place if reverse else place
    gathered = jax.tree.map(lambda a: lax.all_gather(a, axis), part)
    state = jax.tree.map(lambda a, e: jnp.zeros_like(a) + jnp.asarray(e, a.dtype), part, identity)

    def one(hop, state):
        source = count - 1 - hop if reverse else hop
        return combine(
            state, jax.tree.map(lambda a: lax.dynamic_index_in_dim(a, source, 0, False), gathered)
        )

    return lax.fori_loop(0, ahead, one, state)


def passed_along(block, axis, distance):
    devices = range(lax.axis_size(axis))
    route = [(i - distance, i) for i in devices if i - distance in devices]
    return lax.ppermute(block, axis, route)


def segment_of(positions, starts):
    return jnp.sum((positions[:, None] >= starts[None, :]).astype(jnp.int32), axis=1) - 1


def silu_slope(values):
    sigmoid_val = jax.nn.sigmoid(values)
    return sigmoid_val * (1.0 + values * (1.0 - sigmoid_val))


def chain_join(earlier, later):
    return (earlier[0] * later[0], earlier[1] * later[0][:, None, None] + later[1])


def state_prefix(decay, summary, backwards):
    identity = (jnp.ones_like(decay), jnp.zeros_like(summary))
    result = prefix((decay, summary), "seq", chain_join, identity, backwards)
    return result[1]


def span_terms(span_item, lower_tri):
    inner_c, b_rows, c_rows, step_c, cumul_c, seg_rows, seg_prev = span_item
    same_seq = ((seg_rows[:, None] == seg_rows[None, :]) & (lower_tri > 0.5))[None, :, :]
    spread = cumul_c[:, :, None] - cumul_c[:, None, :]
    decay_mat = jnp.where(same_seq, jnp.exp(jnp.where(same_seq, spread, 0.0)), 0.0)
    scores = lax.dot_general(
        c_rows, b_rows, (((1,), (1,)), ((), ())), preferred_element_type=jnp.float32
    )
    mixing = scores[None, :, :] * decay_mat * step_c[:, None, :]
    last_cum = cumul_c[:, SPAN - 1]
    tail_weight = (
        jnp.exp(last_cum[:, None] - cumul_c)
        * (seg_rows == seg_rows[SPAN - 1]).astype(jnp.float32)[None, :]
    )
    head_weight = jnp.exp(cumul_c) * (seg_rows == seg_prev).astype(jnp.float32)[None, :]
    carry_decay = jnp.exp(last_cum) * (seg_rows[SPAN - 1] == seg_prev).astype(jnp.float32)
    return (decay_mat, scores, mixing, tail_weight, head_weight, carry_decay)


def on_device(
    hidden_in,
    seq_lengths,
    norm_gain,
    w_z,
    w_x,
    w_bc,
    w_dt,
    conv_x_w,
    conv_x_b,
    conv_bc_w,
    conv_bc_b,
    dt_bias,
    a_log,
    d_skip,
    gate_gain,
    w_out,
    cotangent,
):
    tokens_here = hidden_in.shape[0]
    heads_here = dt_bias.shape[0]
    inner_here = w_z.shape[1]
    spans = tokens_here // SPAN
    first_pos = lax.axis_index("seq") * tokens_here
    starts = jnp.cumsum(seq_lengths) - seq_lengths
    segment = segment_of(first_pos + jnp.arange(tokens_here, dtype=jnp.int32), starts)
    edge_segment = segment_of(
        first_pos - (CONV - 1) + jnp.arange(CONV - 1, dtype=jnp.int32), starts
    )
    span_prev = segment_of(first_pos - 1 + jnp.arange(spans, dtype=jnp.int32) * SPAN, starts)
    row_ids = jnp.arange(SPAN)
    lower_tri = (row_ids[:, None] >= row_ids[None, :]).astype(jnp.float32)
    inputs = hidden_in.astype(jnp.float32)
    squares = lax.psum(jnp.sum(inputs * inputs, axis=1), "head")
    scale_in = lax.rsqrt(squares / D + epsilon)
    normed = (inputs * scale_in[:, None] * norm_gain).astype(jnp.bfloat16)
    gathered, bc_weight = (
        lax.all_gather(normed, "head", axis=1, tiled=True),
        lax.all_gather(w_bc, "head", axis=0, tiled=True),
    )
    gate_pre = jnp.dot(gathered, w_z, preferred_element_type=jnp.float32)
    x_part = jnp.dot(gathered, w_x, preferred_element_type=jnp.float32)
    bc_part = jnp.dot(gathered, bc_weight, preferred_element_type=jnp.float32)
    conv_in = jnp.concatenate([x_part, bc_part], axis=1).astype(jnp.bfloat16)
    step_raw = jnp.dot(gathered, w_dt, preferred_element_type=jnp.float32)
    edge_rows = passed_along(conv_in[tokens_here - (CONV - 1) :], "seq", 1)
    padded = jnp.concatenate([edge_rows, conv_in], axis=0).astype(jnp.float32)
    seg_padded = jnp.concatenate([edge_segment, segment])
    conv_weight = jnp.concatenate([conv_x_w, conv_bc_w], axis=1)
    conv_bias = jnp.concatenate([conv_x_b, conv_bc_b])
    tap_masks = [
        (seg_padded[offset : offset + tokens_here] == segment).astype(jnp.float32)[:, None]
        for offset in range(CONV)
    ]
    conv_out = jnp.zeros(conv_in.shape, jnp.float32) + conv_bias[None, :]
    for offset in range(CONV):
        conv_out = (
            conv_out
            + conv_weight[offset] * padded[offset : offset + tokens_here] * tap_masks[offset]
        )
    activated = jax.nn.silu(conv_out)
    inner_vals = activated[:, :inner_here].astype(jnp.bfloat16)
    b_vals = activated[:, inner_here : inner_here + STATE].astype(jnp.bfloat16)
    c_vals = activated[:, inner_here + STATE :].astype(jnp.bfloat16)
    step_pre = step_raw + dt_bias
    step_size = jax.nn.softplus(step_pre)
    rates = jnp.exp(a_log)
    log_decay = -rates * step_size
    decay_heads = log_decay.reshape(spans, SPAN, heads_here).transpose(0, 2, 1)
    step_heads = step_size.reshape(spans, SPAN, heads_here).transpose(0, 2, 1)
    cumul = jnp.einsum("ij,chj->chi", lower_tri, decay_heads, precision=highest)
    inner_spans = inner_vals.reshape(spans, SPAN, heads_here, HEAD_DIM).transpose(0, 2, 1, 3)
    c_spans = c_vals.reshape(spans, SPAN, STATE)
    per_span = (
        inner_spans,
        b_vals.reshape(spans, SPAN, STATE),
        c_spans,
        step_heads,
        cumul,
        segment.reshape(spans, SPAN),
        span_prev,
    )

    def forward_span(span_item):
        decay_mat, scores, mixing, tail_weight, head_weight, carry_decay = span_terms(
            span_item, lower_tri
        )
        inner_c = span_item[0]
        y_inside = jnp.einsum(
            "hij,hjp->hip", mixing.astype(jnp.bfloat16), inner_c, preferred_element_type=jnp.float32
        )
        loaded = (
            span_item[1].astype(jnp.float32)[None, :, :] * (tail_weight * span_item[3])[:, :, None]
        ).astype(jnp.bfloat16)
        local_state = jnp.einsum(
            "hjn,hjp->hnp", loaded, inner_c, preferred_element_type=jnp.float32
        )
        return (y_inside, local_state, carry_decay, head_weight)

    y_inside, local_states, carry_decay, head_weight = lax.map(forward_span, per_span)

    def advance(state_carry, span_item):
        running, factor = state_carry
        local_c, decay_c = span_item
        return ((decay_c[:, None, None] * running + local_c, decay_c * factor), (running, factor))

    zero_state = jnp.zeros((heads_here, STATE, HEAD_DIM), jnp.float32)
    unit_decay = jnp.ones((heads_here,), jnp.float32)
    (device_state, device_decay), (local_in, local_factor) = lax.scan(
        advance, (zero_state, unit_decay), (local_states, carry_decay)
    )
    incoming = state_prefix(device_decay, device_state, False)
    state_in = local_in + local_factor[:, :, None, None] * incoming
    state_low = state_in.astype(jnp.bfloat16)
    c_weighted = (c_spans.astype(jnp.float32)[:, None, :, :] * head_weight[:, :, :, None]).astype(
        jnp.bfloat16
    )
    y_outside = jnp.einsum(
        "chin,chnp->chip", c_weighted, state_low, preferred_element_type=jnp.float32
    )
    skip_rep = jnp.repeat(d_skip, HEAD_DIM)
    mixed_out = (y_inside + y_outside).transpose(0, 2, 1, 3).reshape(
        tokens_here, inner_here
    ) + inner_vals.astype(jnp.float32) * skip_rep
    gate_act = jax.nn.silu(gate_pre)
    gated = mixed_out * gate_act
    gate_squares = lax.psum(jnp.sum(gated * gated, axis=1), "head")
    scale_gate = lax.rsqrt(gate_squares / INNER + epsilon)
    gate_normed = (gated * scale_gate[:, None] * gate_gain).astype(jnp.bfloat16)
    partial_value = jnp.dot(gate_normed, w_out, preferred_element_type=jnp.float32)
    mixed_sum = lax.psum_scatter(partial_value, "head", scatter_dimension=1, tiled=True)
    layer_out = (inputs + mixed_sum).astype(jnp.bfloat16)
    grad_full = lax.all_gather(cotangent, "head", axis=1, tiled=True)
    grad_gate_normed = lax.dot_general(
        grad_full, w_out, (((1,), (1,)), ((), ())), preferred_element_type=jnp.float32
    )
    grad_w_out = lax.dot_general(
        gate_normed, grad_full, (((0,), (0,)), ((), ())), preferred_element_type=jnp.float32
    )
    grad_gate_gain = jnp.sum(grad_gate_normed * gated * scale_gate[:, None], axis=0)
    grad_scaled = grad_gate_normed * gate_gain
    gate_inner = lax.psum(jnp.sum(grad_scaled * gated, axis=1), "head")
    grad_gated = (
        scale_gate[:, None] * grad_scaled - gated * (scale_gate**3 * gate_inner / INNER)[:, None]
    )
    grad_mixed = (grad_gated * gate_act).astype(jnp.bfloat16)
    grad_gate_pre = (grad_gated * mixed_out * silu_slope(gate_pre)).astype(jnp.bfloat16)
    grad_d_skip = jnp.sum(
        (grad_mixed.astype(jnp.float32) * inner_vals.astype(jnp.float32)).reshape(
            tokens_here, heads_here, HEAD_DIM
        ),
        axis=(0, 2),
    )
    grad_spans = grad_mixed.reshape(spans, SPAN, heads_here, HEAD_DIM).transpose(0, 2, 1, 3)
    from_inter = jnp.einsum(
        "chin,chip->chnp", c_weighted, grad_spans, preferred_element_type=jnp.float32
    )

    def retreat(state_carry, span_item):
        running, factor = state_carry
        local_c, decay_c = span_item
        current = local_c + decay_c[:, None, None] * running
        product = decay_c * factor
        return ((current, product), (current, product))

    (device_grad, device_reach), (local_grad, local_reach) = lax.scan(
        retreat, (zero_state, unit_decay), (from_inter, carry_decay), reverse=True
    )
    beyond = state_prefix(device_reach, device_grad, True)
    grad_state_in = local_grad + local_reach[:, :, None, None] * beyond
    grad_local_states = jnp.concatenate([grad_state_in[1:], beyond[None]], axis=0)
    grad_carry_decay = jnp.sum(grad_local_states * state_in, axis=(2, 3))

    def backward_span(span_item):
        span_base = span_item[:7]
        inner_c, b_rows, c_rows, step_c = (span_base[0], span_base[1], span_base[2], span_base[3])
        grad_y, grad_state, state_c, grad_decay = (
            span_item[7],
            span_item[8],
            span_item[9],
            span_item[10],
        )
        decay_mat, scores, mixing, tail_weight, head_weight, carry_decay = span_terms(
            span_base, lower_tri
        )
        grad_mixing = jnp.einsum(
            "hip,hjp->hij", grad_y, inner_c, preferred_element_type=jnp.float32
        )
        grad_inner = jnp.einsum(
            "hij,hip->hjp", mixing.astype(jnp.bfloat16), grad_y, preferred_element_type=jnp.float32
        )
        related = grad_mixing * mixing
        grad_cum = jnp.sum(related, axis=2) - jnp.sum(related, axis=1)
        grad_scores = jnp.sum(grad_mixing * decay_mat * step_c[:, None, :], axis=0)
        grad_step = jnp.sum(grad_mixing * decay_mat * scores[None, :, :], axis=1)
        b_float = b_rows.astype(jnp.float32)
        c_float = c_rows.astype(jnp.float32)
        grad_c = jnp.dot(grad_scores, b_float, precision=highest)
        grad_b = lax.dot_general(grad_scores, c_float, (((0,), (0,)), ((), ())), precision=highest)
        loading = tail_weight * step_c
        loaded = (b_float[None, :, :] * loading[:, :, None]).astype(jnp.bfloat16)
        grad_loaded = jnp.einsum(
            "hjp,hnp->hjn", inner_c, grad_state, preferred_element_type=jnp.float32
        )
        grad_inner = grad_inner + jnp.einsum(
            "hjn,hnp->hjp", loaded, grad_state, preferred_element_type=jnp.float32
        )
        grad_loading = jnp.sum(grad_loaded * b_float[None, :, :], axis=2)
        grad_b = grad_b + jnp.einsum("hjn,hj->jn", grad_loaded, loading, precision=highest)
        tail_term = grad_loading * loading
        grad_cum = grad_cum - tail_term
        grad_last = jnp.sum(tail_term, axis=1) + grad_decay * carry_decay
        grad_step = grad_step + grad_loading * tail_weight
        grad_weighted = jnp.einsum(
            "hip,hnp->hin", grad_y, state_c, preferred_element_type=jnp.float32
        )
        grad_head = jnp.sum(grad_weighted * c_float[None, :, :], axis=2)
        grad_c = grad_c + jnp.einsum("hin,hi->in", grad_weighted, head_weight, precision=highest)
        grad_cum = grad_cum + grad_head * head_weight
        grad_cum = grad_cum.at[:, SPAN - 1].add(grad_last)
        grad_log = jnp.einsum("ij,hi->hj", lower_tri, grad_cum, precision=highest)
        return (grad_inner, grad_b, grad_c, grad_step, grad_log)

    back_items = per_span + (
        grad_spans,
        grad_local_states.astype(jnp.bfloat16),
        state_low,
        grad_carry_decay,
    )
    grad_inner_s, grad_b_s, grad_c_s, grad_step_s, grad_log_s = lax.map(backward_span, back_items)
    grad_inner = (
        grad_inner_s.transpose(0, 2, 1, 3).reshape(tokens_here, inner_here)
        + grad_mixed.astype(jnp.float32) * skip_rep
    )
    grad_log_decay = grad_log_s.transpose(0, 2, 1).reshape(tokens_here, heads_here)
    grad_step_total = (
        grad_step_s.transpose(0, 2, 1).reshape(tokens_here, heads_here) - grad_log_decay * rates
    )
    grad_a_log = jnp.sum(grad_log_decay * log_decay, axis=0)
    grad_step_pre = grad_step_total * jax.nn.sigmoid(step_pre)
    grad_dt_bias = jnp.sum(grad_step_pre, axis=0)
    grad_step_raw = grad_step_pre.astype(jnp.bfloat16)
    grad_bc = lax.psum(
        jnp.concatenate(
            [grad_b_s.reshape(tokens_here, STATE), grad_c_s.reshape(tokens_here, STATE)], axis=1
        ),
        "head",
    )
    grad_conv = jnp.concatenate([grad_inner, grad_bc], axis=1) * silu_slope(conv_out)
    grad_conv_bias = jnp.sum(grad_conv, axis=0)
    grad_conv_weight = jnp.stack(
        [
            jnp.sum(grad_conv * padded[offset : offset + tokens_here] * tap_masks[offset], axis=0)
            for offset in range(CONV)
        ]
    )
    grad_padded = jnp.zeros(padded.shape, jnp.float32)
    for offset in range(CONV):
        grad_padded = grad_padded + jnp.pad(
            conv_weight[offset] * grad_conv * tap_masks[offset],
            ((offset, CONV - 1 - offset), (0, 0)),
        )
    returned = passed_along(grad_padded[: CONV - 1], "seq", -1)
    grad_conv_in = (
        grad_padded[CONV - 1 :] + jnp.pad(returned, ((tokens_here - (CONV - 1), 0), (0, 0)))
    ).astype(jnp.bfloat16)
    grad_x_pre = grad_conv_in[:, :inner_here]
    grad_bc_pre = grad_conv_in[:, inner_here:]
    contract_rows = (((0,), (0,)), ((), ()))
    contract_cols = (((1,), (1,)), ((), ()))
    grad_w_z = lax.dot_general(
        gathered, grad_gate_pre, contract_rows, preferred_element_type=jnp.float32
    )
    grad_w_x = lax.dot_general(
        gathered, grad_x_pre, contract_rows, preferred_element_type=jnp.float32
    )
    grad_w_dt = lax.dot_general(
        gathered, grad_step_raw, contract_rows, preferred_element_type=jnp.float32
    )
    grad_w_bc = lax.dot_general(
        normed, grad_bc_pre, contract_rows, preferred_element_type=jnp.float32
    )
    partial_back = lax.dot_general(
        grad_gate_pre, w_z, contract_cols, preferred_element_type=jnp.float32
    )
    partial_back = partial_back + lax.dot_general(
        grad_x_pre, w_x, contract_cols, preferred_element_type=jnp.float32
    )
    partial_back = partial_back + lax.dot_general(
        grad_step_raw, w_dt, contract_cols, preferred_element_type=jnp.float32
    )
    grad_normed = lax.psum_scatter(partial_back, "head", scatter_dimension=1, tiled=True)
    grad_normed = grad_normed + lax.dot_general(
        grad_bc_pre, w_bc, contract_cols, preferred_element_type=jnp.float32
    )
    grad_scaled_in = grad_normed * norm_gain
    grad_norm_gain = jnp.sum(grad_normed * inputs * scale_in[:, None], axis=0)
    norm_inner = lax.psum(jnp.sum(grad_scaled_in * inputs, axis=1), "head")
    grad_in = (
        cotangent.astype(jnp.float32)
        + scale_in[:, None] * grad_scaled_in
        - inputs * (scale_in**3 * norm_inner / D)[:, None]
    )
    summed = lax.psum(
        (
            grad_norm_gain,
            grad_w_z,
            grad_w_x,
            grad_w_bc,
            grad_w_dt,
            grad_conv_weight[:, :inner_here],
            grad_conv_bias[:inner_here],
            grad_conv_weight[:, inner_here:],
            grad_conv_bias[inner_here:],
            grad_dt_bias,
            grad_a_log,
            grad_d_skip,
            grad_gate_gain,
            grad_w_out,
        ),
        "seq",
    )
    return (
        layer_out,
        grad_in,
        summed[0],
        summed[1],
        summed[2],
        summed[3],
        summed[4],
        summed[5],
        summed[6],
        summed[7],
        summed[8],
        summed[9],
        summed[10],
        summed[11],
        summed[12],
        summed[13],
    )


BF = jnp.bfloat16
F32 = jnp.float32
MESH = pl.DeviceIdType.MESH
ROWS = 512
BLOCK = 384
CHANNELS = 768
WIDE = 1024
HALO = 16
SEQ = 8
LINE = 4
ALONG = "seq"
ACROSS = "head"
NN = (((1,), (0,)), ((), ()))
NT = (((1,), (1,)), ((), ()))
TN = (((0,), (0,)), ((), ()))


def mul(a, b, dims=NN):
    return lax.dot_general(a, b, dims, preferred_element_type=F32)


def cut(start, size, mult):
    return pl.ds(pl.multiple_of(start, mult), size)


def parts(v, n):
    out = []
    for _ in range(n):
        p = v.astype(BF)
        out.append(p)
        v = v - p.astype(F32)
    return out


def along_line(z, ends, middles):
    k = jnp.where(lax.rem(z, 3) == 0, ends, middles)
    return jnp.where(z >= 2, 3 - k, k)


def lanes_sum(v):
    total = v[:, 0:128]
    for i in range(1, v.shape[1] // 128):
        total = total + v[:, 128 * i : 128 * i + 128]
    return total


def rows_sum(v):
    return jnp.sum(v.reshape(v.shape[0] // 8, 8, v.shape[1]), axis=0)


def wide_of(v, n):
    return jnp.concatenate([v] * n, axis=1)


def to_row(part):
    return jnp.sum(part.T, axis=0, keepdims=True)


def to_col(row):
    return jnp.broadcast_to(row, (128, row.shape[1])).T


def loop(n, body):
    def run(i, carry):
        body(i)
        return carry

    lax.fori_loop(0, n, run, 0)


def remote(src, dst, send, recv, peer):
    return pltpu.make_async_remote_copy(
        src_ref=src, dst_ref=dst, send_sem=send, recv_sem=recv, device_id=peer, device_id_type=MESH
    )


class Total:
    def __init__(self, whole, bufs, send, recv, freed, base, me):
        self.w = whole
        self.freed, self.slot = freed, 3 * (base // 10)
        self.r0, self.ra, self.rb, self.qa, self.qb = bufs
        self.send, self.recv, self.base = send, recv, base
        self.c, self.x, self.y, self.s = me
        self.rows, self.cols = whole.shape
        self.live, self.left = {}, set()

    def peer(self, bit):
        return {ALONG: self.s + bit - 2 * bit * {1: self.c, 2: self.x, 4: self.y}[bit]}

    def free(self, k, n, bit):
        self.sent(k)
        pl.semaphore_signal(
            self.freed.at[self.slot + n], inc=1, device_id=self.peer(bit), device_id_type=MESH
        )

    def copy(self, k, src, dst, bit):
        d = remote(src, dst, self.send.at[self.base + k], self.recv.at[self.base + k], self.peer(bit))
        d.start()
        self.live[k] = d
        self.left.add(k)

    def wait(self, k):
        self.live[k].wait_recv()

    def sent(self, k):
        self.left.remove(k)
        self.live[k].wait_send()

    def add(self, start, got, rows, col, cols, step):
        def body(i):
            at = (cut(start + i * step, step, 16), pl.ds(col, cols))
            new = self.w[at].astype(F32) + got[cut(i * step, step, 16), :].astype(F32)
            self.w[at] = new.astype(self.w.dtype)

        loop(rows // step, body)

    def s0(self):
        h = self.rows // 2
        self.copy(0, self.w.at[cut((1 - self.c) * h, h, 16)], self.r0, 1)

    def s1(self):
        h, q, m = self.rows // 2, self.rows // 4, self.cols // 2
        base = self.c * h
        self.free(0, 0, 1)
        self.wait(0)
        self.add(base, self.r0, h, 0, self.cols, 32)
        self.copy(1, self.w.at[cut(base + (1 - self.x) * q, q, 16), pl.ds(0, m)], self.ra, 2)
        self.copy(2, self.w.at[cut(base + (1 - self.y) * q, q, 16), pl.ds(m, m)], self.rb, 4)

    def s2(self):
        h, q, e, m = self.rows // 2, self.rows // 4, self.rows // 8, self.cols // 2
        ba = self.c * h + self.x * q
        bb = self.c * h + self.y * q
        self.wait(1)
        self.add(ba, self.ra, q, 0, m, 32)
        self.sent(2)
        self.copy(3, self.w.at[cut(ba + (1 - self.y) * e, e, 16), pl.ds(0, m)], self.qa, 4)
        self.wait(2)
        self.add(bb, self.rb, q, m, m, 32)
        self.sent(1)
        self.copy(4, self.w.at[cut(bb + (1 - self.x) * e, e, 16), pl.ds(m, m)], self.qb, 2)

    def s3(self):
        h, q, e, m = self.rows // 2, self.rows // 4, self.rows // 8, self.cols // 2
        ba = self.c * h + self.x * q + self.y * e
        bb = self.c * h + self.y * q + self.x * e
        self.free(3, 1, 4)
        self.free(4, 2, 2)
        self.wait(3)
        self.add(ba, self.qa, e, 0, m, 16)
        pl.semaphore_wait(self.freed.at[self.slot + 1], 1)
        p = self.w.at[cut(ba, e, 16), pl.ds(0, m)]
        self.copy(5, p, p, 4)
        self.wait(4)
        self.add(bb, self.qb, e, m, m, 16)
        pl.semaphore_wait(self.freed.at[self.slot + 2], 1)
        p = self.w.at[cut(bb, e, 16), pl.ds(m, m)]
        self.copy(6, p, p, 2)

    def s4(self):
        h, q, m = self.rows // 2, self.rows // 4, self.cols // 2
        self.wait(5)
        p = self.w.at[cut(self.c * h + self.x * q, q, 16), pl.ds(0, m)]
        self.copy(7, p, p, 2)
        self.wait(6)
        p = self.w.at[cut(self.c * h + self.y * q, q, 16), pl.ds(m, m)]
        self.copy(8, p, p, 4)

    def s5(self):
        h = self.rows // 2
        self.wait(7)
        self.wait(8)
        pl.semaphore_wait(self.freed.at[self.slot], 1)
        p = self.w.at[cut(self.c * h, h, 16)]
        self.copy(9, p, p, 1)

    def s6(self):
        self.wait(9)
        for k in sorted(self.left):
            self.sent(k)


def total_bufs(rows, cols, kind):
    sizes = [(2, 1), (4, 2), (4, 2), (8, 2), (8, 2)]
    return [pltpu.VMEM((rows // a, cols // b), kind) for a, b in sizes]


class Refs:
    def __init__(self, named):
        self.__dict__.update(named)


def layer_kernel(named, sum_bufs):
    g = Refs(named)
    g.ggn = g.acc.at[:, pl.ds(0, CHANNELS)]
    g.z = g.ggn
    g.gn = g.xg.at[:, pl.ds(0, CHANNELS)]
    g.gz = g.xg.at[:, pl.ds(CHANNELS, CHANNELS)]
    g.gconv = g.slope
    g.gx = g.gm
    g.own_in = g.acc.at[:, pl.ds(0, BLOCK)]
    g.own = g.gated.at[:, pl.ds(0, BLOCK)]
    g.gb = g.gated.at[:, pl.ds(BLOCK, 128)]
    g.gc = g.gated.at[:, pl.ds(BLOCK + 128, 128)]
    s = lax.axis_index(ALONG)
    z = lax.axis_index(ACROSS)
    me = (lax.rem(s, 2), lax.rem(s // 2, 2), s // 4, s)
    zpeers = [{ACROSS: lax.rem(z + d, LINE)} for d in range(1, LINE)]
    speers = [{ALONG: lax.rem(s + d, SEQ)} for d in range(1, SEQ)]

    loads = []
    for i, (src, dst) in enumerate(
        [(g.x_hbm, g.x), (g.w_x, g.wx), (g.w_z, g.wz), (g.cot_hbm, g.cotg.at[:, cut(z * BLOCK, BLOCK, 128)]), (g.w_out, g.wo)]
    ):
        d = pltpu.make_async_copy(src, dst, g.load_sem.at[i])
        d.start()
        loads.append(d)

    g.params[...] = jnp.zeros(g.params.shape, F32)
    vectors = (g.norm_gain, g.conv_x_b, g.conv_bc_b, g.dt_bias, g.a_log, g.d_skip, g.gate_gain)
    for i, v in enumerate(vectors):
        for n in range(v.shape[0]):
            g.params[i : i + 1, 128 * n : 128 * n + v.shape[1]] = v[n : n + 1, :]

    sem = pltpu.get_barrier_semaphore()
    for p in zpeers + speers:
        pl.semaphore_signal(sem, inc=1, device_id=p, device_id_type=MESH)
    pl.semaphore_wait(sem, len(zpeers) + len(speers))

    pending = []

    def send(src, dst, sems, i, peer):
        d = remote(src, dst, sems[0].at[i], sems[1].at[i], peer)
        d.start()
        pending.append(d)
        return d

    loads[0].wait()
    loads[3].wait()
    gain = g.params[0:1, 0:BLOCK]
    xv = g.x[...].astype(F32)
    g.ssq[z] = to_row(lanes_sum(xv * xv))
    g.gains[z] = gain
    core, chip = me[0], s // 2
    partner = {ALONG: s + 1 - 2 * core}
    chips = [{ALONG: lax.rem(s + 2 * d, SEQ)} for d in range(1, 4)]
    piece = cut(48 * (4 * core + chip), 48, 16)
    own = cut(z * BLOCK, BLOCK, 128)
    g.wbc[z, piece, :] = g.w_bc[piece, :]
    small = []
    for i, p in enumerate(zpeers):
        small.append(send(g.ssq.at[z], g.ssq.at[z], g.small, i, p))
        small.append(send(g.gains.at[z], g.gains.at[z], g.small, 3 + i, p))
        small.append(send(g.w_bc.at[piece], g.wbc.at[z, piece], g.small, 6 + i, p))
    middle = lax.rem(z, 3) != 0
    near = [along_line(z, a, b) for a, b in ((1, 2), (2, 0), (3, 3))]

    def block_copy(src, whole, base, slot, k, to):
        cols = cut(k * BLOCK, BLOCK, 128)
        return remote(src, whole.at[:, cols], g.gather_s.at[base + slot], g.gather_r.at[base + k], {ACROSS: to})

    def gather(src, whole, base):
        for j in range(2):
            pending.append(block_copy(src, whole, base, j, z, near[j]))
            pending[-1].start()
        third = block_copy(src, whole, base, 2, z, near[2])

        @pl.when(jnp.logical_not(middle))
        def _():
            third.start()

        return third

    def gathered(src, whole, base, j):
        block_copy(src, whole, base, 0, near[j], z).wait_recv()

    def relay(whole, base):
        part = whole.at[:, cut(near[0] * BLOCK, BLOCK, 128)]

        @pl.when(middle)
        def _():
            block_copy(part, whole, base, 2, near[0], near[1]).start()

    x_own = [block_copy(g.x, g.xg, 0, j, z, near[j]) for j in range(2)]
    x_on = [block_copy(g.xg.at[:, cut(near[j] * BLOCK, BLOCK, 128)], g.xg, 0, 2 + j, near[j], near[1 - j % 2]) for j in range(2)]
    x_on.append(block_copy(g.xg.at[:, cut(near[2] * BLOCK, BLOCK, 128)], g.xg, 0, 4, near[2], near[1]))
    x_own[0].start()

    @pl.when(middle)
    def _():
        x_own[1].start()


    g.wd[...] = jnp.zeros(g.wd.shape, BF)
    g.wd[0:12, :] = g.w_dt[...]
    g.taps[...] = jnp.zeros(g.taps.shape, F32)
    g.taps[0:4, 0:CHANNELS] = g.conv_x_w[...]
    g.taps[0:4, CHANNELS:WIDE] = g.conv_bc_w[...]
    g.taps[4:5, 0:CHANNELS] = g.params[1:2, :]
    g.taps[4:5, CHANNELS:WIDE] = g.params[2:3, 0:256]
    expand_row = lax.broadcasted_iota(jnp.int32, (256, CHANNELS), 0)
    expand_col = lax.broadcasted_iota(jnp.int32, (256, CHANNELS), 1)
    g.spread[...] = jnp.where((expand_col >> 6) == (expand_row & 127), 1.0, 0.0).astype(BF)
    starts = [jnp.int32(0)]
    for k in range(7):
        starts.append(starts[-1] + g.lengths[k])

    def segment(pos):
        total = jnp.full(pos.shape, -1, jnp.int32)
        for k in range(8):
            total = total + jnp.where(pos >= starts[k], 1, 0)
        return total.astype(F32)

    g.segc[...] = segment(
        lax.broadcasted_iota(jnp.int32, (ROWS + HALO, 128), 0) + (s * ROWS - HALO)
    )
    g.segr[...] = segment(lax.broadcasted_iota(jnp.int32, (8, ROWS), 1) + s * ROWS)
    tri_i = lax.broadcasted_iota(jnp.int32, (SPAN, SPAN), 0)
    tri_j = lax.broadcasted_iota(jnp.int32, (SPAN, SPAN), 1)
    g.tri[...] = jnp.where(tri_i >= tri_j, 1.0, 0.0).astype(BF)
    lane = lax.broadcasted_iota(jnp.int32, (1, 128), 1)
    left = lane < 64

    def spread(v):
        hi, lo = parts(v, 2)
        return mul(jnp.concatenate([hi, lo], axis=1), g.spread[...])

    def head_sum(v):
        hi, lo = parts(v, 2)
        e = g.spread[0:128, :]
        return mul(hi, e, NT) + mul(lo, e, NT)

    g.skipe[...] = spread(jnp.broadcast_to(g.params[5:6, 0:128], (8, 128)))
    rates = jnp.exp(g.params[4:5, 0:128])

    for d in small:
        d.wait_recv()
    wide = [
        send(g.wbc.at[:, piece], g.wbc.at[:, piece], g.wide, i, p) for i, p in enumerate(chips)
    ]
    total = g.ssq[0] + g.ssq[1] + g.ssq[2] + g.ssq[3]
    g.xscale[...] = to_col(lax.rsqrt(total / D + epsilon))

    def normalise(k, src):
        gk = g.gains[k]
        cols = cut(k * BLOCK, BLOCK, 128)

        def body(i):
            at = cut(i * 64, 64, 16)
            v = src(at, cols).astype(F32)
            g.xn[at, cols] = (v * wide_of(g.xscale[at, :], 3) * gk).astype(BF)

        loop(ROWS // 64, body)

    def project(k, w, cols, base, first, width=256):
        at = cut(k * BLOCK, BLOCK, 128)

        def body(n):
            p = mul(g.xn[:, at], w[cut(k * BLOCK, BLOCK, 16), cut(n * width, width, 128)])
            dst = cut(base + n * width, width, 128)
            if first:
                g.acc[:, dst] = p
            else:
                g.acc[:, dst] += p

        loop(cols // width, body)

    def project_dt(k, first):
        at = cut(k * BLOCK, BLOCK, 128)
        p = mul(g.xn[:, at], g.wd[:, at], NT)
        if first:
            g.acc[:, WIDE + CHANNELS :] = p
        else:
            g.acc[:, WIDE + CHANNELS :] += p

    normalise(z, lambda at, cols: g.x[at, :])
    loads[1].wait()
    loads[2].wait()
    project(z, g.wx, CHANNELS, 0, True)
    project(z, g.wz, CHANNELS, WIDE, True)
    project_dt(z, True)
    for i, k in enumerate(near):
        if i != 1:
            gathered(g.x, g.xg, 0, i)
        else:
            @pl.when(jnp.logical_not(middle))
            def _():
                gathered(g.x, g.xg, 0, 1)

        if i == 2:
            @pl.when(middle)
            def _():
                x_on[2].start()

        if i == 0:
            @pl.when(middle)
            def _():
                x_on[0].start()
                gathered(g.x, g.xg, 0, 1)
                x_on[1].start()

            for d in wide:
                d.wait_recv()
            share = g.wbc.at[:, cut(192 * core, 192, 16)]
            wide = [send(share, share, g.wide, 3, partner)]
        if i == 2:
            pending.append(gather(g.cotg.at[:, own], g.cotg, 5))
        normalise(k, lambda at, cols: g.xg[at, cols])
        project(k, g.wx, CHANNELS, 0, False)
        if i < 2:
            project(k, g.wz, CHANNELS, WIDE, False)
            project_dt(k, False)
    for d in wide:
        d.wait_recv()
    g.acc[:, CHANNELS:WIDE] = sum(
        mul(g.xn[:, BLOCK * k : BLOCK * k + BLOCK], g.wbc[k]) for k in range(LINE)
    )

    g.edge[...] = g.acc[ROWS - HALO : ROWS, 0:WIDE].astype(BF)
    edge = remote(g.edge, g.halo, g.edge_sem.at[0], g.edge_sem.at[1], {ALONG: s + 1})

    @pl.when(s < SEQ - 1)
    def _():
        edge.start()

    @pl.when(s == 0)
    def _():
        g.halo[...] = jnp.zeros(g.halo.shape, BF)

    def put(i):
        g.cf[cut(HALO + i * 64, 64, 8), :] = (
            g.acc[cut(i * 64, 64, 8), 0:WIDE].astype(BF).astype(F32)
        )

    loop(ROWS // 64, put)
    project(near[2], g.wz, CHANNELS, WIDE, False)
    project_dt(near[2], False)

    step_pre = g.acc[:, WIDE + CHANNELS :] + g.params[3:4, 0:128]
    g.step[...] = jnp.where(lane < 12, jax.nn.softplus(step_pre), 0.0)
    for q in range(2):
        rows = pl.ds(q * SPAN, SPAN)
        log_decay = -rates * g.step[rows, :]
        cum = sum(mul(g.tri[...], p) for p in parts(log_decay, 3))
        g.cum[rows, :] = cum
        g.cumt[q] = cum.T[0:16, :]
        last = cum[SPAN - 1 : SPAN, :]
        seg = g.segc[pl.ds(HALO + q * SPAN, SPAN), :]
        seg_last = g.segc[HALO + q * SPAN + SPAN - 1 : HALO + q * SPAN + SPAN, :]
        seg_prev = g.segc[HALO + q * SPAN - 1 : HALO + q * SPAN, :]
        tail = jnp.where(seg == seg_last, jnp.exp(last - cum), 0.0)
        load = tail * g.step[rows, :]
        lead = jnp.where(seg == seg_prev, jnp.exp(cum), 0.0)
        g.tail[rows, :] = tail
        g.load[rows, :] = load
        g.lead[rows, :] = lead
        g.loadt[q] = load.T[0:16, :]
        g.leadt[q] = lead.T[0:16, :]
        g.stept[q] = g.step[rows, :].T[0:16, :]
        carry = jnp.where(seg_last == seg_prev, jnp.exp(last), 0.0)
        g.carry[q] = jnp.broadcast_to(carry, (8, 128))
        g.carrye[q] = spread(jnp.broadcast_to(carry, (8, 128)))
    g.decay[0] = g.carrye[0] * g.carrye[1]

    def taps_of(first, cols):
        v = g.cf[cut(first + 8, 72, 8), cols]
        sv = g.segc[cut(first + 8, 72, 8), :]
        width = v.shape[1] // 128
        out = []
        for k in range(3):
            same = pltpu.roll(sv, 67 - k, 0)[0:64] == sv[8:72]
            out.append(jnp.where(wide_of(same, width), pltpu.roll(v, 67 - k, 0)[0:64], 0.0))
        out.append(v[8:72])
        return out

    def convolve(i):
        first = i * 64
        at = cut(first, 64, 16)
        for n in range(4):
            cols = pl.ds(n * 256, 256)
            v = jnp.broadcast_to(g.taps[4:5, cols], (64, 256))
            for k, t in enumerate(taps_of(first, cols)):
                v = v + g.taps[k : k + 1, cols] * t
            sig = jax.nn.sigmoid(v)
            act = (v * sig).astype(BF)
            g.slope[at, cols] = sig * (1.0 + v * (1.0 - sig))
            if n < 3:
                g.inner[at, cols] = act
            else:
                g.b[at, :] = act[:, 0:128]
                g.c[at, :] = act[:, 128:256]

    loop(ROWS // 64 - 1, lambda i: convolve(i + 1))

    @pl.when(s > 0)
    def _():
        edge.wait_recv()

    g.cf[0:HALO, :] = g.halo[...].astype(F32)
    convolve(0)

    g.bt[...] = g.b[...].astype(F32).T
    g.ct[...] = g.c[...].astype(F32).T

    def outer(maps, weights, vals):
        def body(t):
            q, p = t // 6, lax.rem(t, 6)
            at = cut(p * 128, 128, 128)
            v = vals[cut(q * SPAN, SPAN, 256), at]
            m = maps[:, cut(q * SPAN, SPAN, 256)]
            o = [mul((m * weights[q, pl.ds(2 * p + e, 1), :]).astype(BF), v) for e in range(2)]
            g.local[q, :, at] = jnp.where(left, o[0], o[1])

        loop(12, body)

    outer(g.bt, g.loadt, g.inner)
    c0, c1 = g.carrye[0][0:1], g.carrye[1][0:1]
    half, rest = cut(core * BLOCK, BLOCK, 128), cut((1 - core) * BLOCK, BLOCK, 128)
    later = []

    class Chain:
        def __init__(self, mine, other, joined, far, got, result, base, way):
            self.mine, self.other, self.joined, self.got, self.result = mine, other, joined, got, result
            self.base, self.way = base, way
            self.near = self.link(joined, got, 1, way)
            self.far_from, self.far_to = far
            self.far = self.link(self.far_from, self.far_to, 2, 2 * way)

        def link(self, src, dst, i, hop):
            to = {ALONG: s + 2 * hop}
            return remote(src, dst, g.st_send.at[self.base + i], g.st_recv.at[self.base + i], to)

        def share(self):
            self.first = send(self.mine, self.other, (g.st_send, g.st_recv), self.base, partner)

        def join(self):
            self.first.wait_recv()
            own, other = self.mine[:, half], self.other[:, half]
            even, odd = jnp.where(core == 0, own, other), jnp.where(core == 0, other, own)
            if self.way > 0:
                self.joined[...] = odd_decay() * even + odd
            else:
                self.joined[...] = even + even_decay() * odd
            if self.far_from is not self.joined:
                self.far_from[...] = self.joined[...].astype(BF)
            for d, hop in ((self.near, 1), (self.far, 2)):
                pass_on(d, hop * self.way)
            for to, hop in ((self.got, 1), (self.far_to, 2)):
                outside = chip - hop * self.way

                @pl.when((outside < 0) | (outside > 3))
                def _():
                    to[...] = jnp.zeros((STATE, BLOCK), to.dtype)

        def meet(self, decay):
            for d, hop in ((self.near, 1), (self.far, 2)):
                arrive(d, hop * self.way)
            self.result[:, half] = self.got[...] + decay * self.far_to[...].astype(F32)
            p = self.result.at[:, half]
            self.last = send(p, p, (g.st_send, g.st_recv), self.base + 3, partner)

        def end(self):
            self.last.wait_recv()

    def pass_on(d, hop):
        inside = (chip + hop >= 0) & (chip + hop <= 3)

        @pl.when(inside)
        def _():
            d.start()

        later.append((inside, d))

    def arrive(d, hop):
        @pl.when((chip - hop >= 0) & (chip - hop <= 3))
        def _():
            d.wait_recv()

    def odd_decay():
        return jnp.where(core == 0, g.decay[1, 0:1, half], g.decay[0, 0:1, half])

    def even_decay():
        return jnp.where(core == 0, g.decay[0, 0:1, half], g.decay[1, 0:1, half])

    g.mine[...] = c1 * g.local[0] + g.local[1]
    ahead = Chain(g.mine, g.other, g.joined, (g.joined, g.got.at[1]), g.got.at[0], g.chain, 0, 1)
    ahead.share()
    dec = send(g.decay.at[0], g.decay.at[1], (g.st_send, g.st_recv), 8, partner)
    both_up = remote(g.both, g.boths.at[0], g.st_send.at[9], g.st_recv.at[9], {ALONG: s + 2})
    both_down = remote(g.both, g.boths.at[1], g.st_send.at[10], g.st_recv.at[10], {ALONG: s - 2})

    def head_cols(ref, rows, p):
        moved = pltpu.roll(ref[rows, :], lax.rem(128 - 2 * p, 128), 1)
        return moved[:, 0:1], moved[:, 1:2]

    def inside(q, first, count):
        rows = cut(q * SPAN, SPAN, 256)
        seg = g.segc[cut(HALO + q * SPAN, SPAN, 16), 0:1]
        segr = g.segr[0:1, cut(q * SPAN, SPAN, 256)]
        scores = mul(g.c[rows, :], g.b[rows, :], NT)
        g.scores[...] = jnp.where((tri_i >= tri_j) & (seg == segr), scores, 0.0)

        def pair(t):
            p = first + t
            cols = head_cols(g.cum, rows, p)
            at = cut(p * 128, 128, 128)
            outs = []
            for e in range(2):
                row = g.cumt[q, pl.ds(2 * p + e, 1), :]
                step = g.stept[q, pl.ds(2 * p + e, 1), :]
                fall = jnp.exp(jnp.minimum(cols[e] - row, 0.0))
                outs.append(mul((g.scores[...] * fall * step).astype(BF), g.inner[rows, at]))
            g.out[rows, at] = jnp.where(left, outs[0], outs[1])

        loop(count, pair)

    inside(0, 0, 3)
    dec.wait_recv()
    g.both[...] = g.decay[0, :, half] * g.decay[1, :, half]
    ahead.join()
    pass_on(both_up, 1)
    pass_on(both_down, -1)
    for i, hop in ((0, 1), (1, -1)):
        @pl.when((chip - hop < 0) | (chip - hop > 3))
        def _():
            g.boths[i] = jnp.zeros((8, BLOCK), F32)

    inside(0, 3, 3)
    gathered(g.cotg.at[:, own], g.cotg, 5, 0)
    relay(g.cotg, 5)
    inside(1, 0, 6)

    arrive(both_up, 1)
    loads[4].wait()
    gate_gain = g.params[6:7, :]

    def down(k, first):
        at = cut(k * BLOCK, BLOCK, 128)

        def body(n):
            cols = cut(n * 256, 256, 256)
            p = mul(g.cotg[:, at], g.wo[cols, at], NT)
            if first:
                g.ggn[:, cols] = p
            else:
                g.ggn[:, cols] += p

        loop(3, body)

    down(z, True)
    down(near[0], False)
    ahead.meet(g.boths[0, 0:1, :])

    def act(i):
        at = cut(i * 64, 64, 16)
        pre = g.acc[at, gate_cols]
        g.gated[at, :] = pre * jax.nn.sigmoid(pre)

    gate_cols = pl.ds(WIDE, CHANNELS)
    loop(ROWS // 64, act)
    ahead.end()
    from_chips = g.chain[...]
    incoming = jnp.where(core == 0, from_chips, g.other[...] + g.decay[1, 0:1] * from_chips)
    g.sin[0] = incoming
    g.sin[1] = g.local[0] + c0 * incoming
    for q in range(2):
        g.slow[q] = g.sin[q].astype(BF)

    def outside(t):
        q, p = t // 6, lax.rem(t, 6)
        rows, at = cut(q * SPAN, SPAN, 256), cut(p * 128, 128, 128)
        cols = head_cols(g.lead, rows, p)
        cv = g.c[rows, :].astype(F32)
        o = [mul((cv * cols[e]).astype(BF), g.slow[q, :, at]) for e in range(2)]
        g.out[rows, at] += jnp.where(left, o[0], o[1])

    loop(12, outside)

    skip = g.skipe[0:1]

    def gate(i):
        at = cut(i * 64, 64, 16)
        mixed = g.out[at, :] + g.inner[at, :].astype(F32) * skip
        gated = mixed * g.gated[at, :]
        g.gated[at, :] = gated
        g.part[0, at, :] = lanes_sum(gated * gated)

    loop(ROWS // 64, gate)
    g.sqs[z] = to_row(g.part[0])
    squares = [send(g.sqs.at[z], g.sqs.at[z], g.sqsem, i, p) for i, p in enumerate(zpeers)]

    for i in (1, 2):
        gathered(g.cotg.at[:, own], g.cotg, 5, i)
        down(near[i], False)

    def inner_part(i):
        at = cut(i * 64, 64, 16)
        g.part[1, at, :] = lanes_sum(g.ggn[at, :] * gate_gain * g.gated[at, :])

    loop(ROWS // 64, inner_part)
    g.stats[z] = to_row(g.part[1])
    stat = [send(g.stats.at[z], g.stats.at[z], g.stat, i, p) for i, p in enumerate(zpeers)]
    dests = [along_line(z, a, b) for a, b in ((2, 3), (3, 0), (1, 2))]

    class Scatter:
        def __init__(self, sent, got, via, base):
            self.sent, self.got, self.via, self.base = sent, got, via, base

        def copy(self, j, dst, i, to):
            return remote(self.sent[j], dst, g.block_s.at[self.base + j], g.block_r.at[self.base + i], {ACROSS: to})

        def direct(self, j):
            slot = lax.rem(z - dests[j] + 7, 4)
            return self.copy(j, self.got.at[slot], slot, dests[j])

        def block(self, j, value):
            v = value
            if j == 2:
                @pl.when(middle)
                def _():
                    self.copy(0, self.via, 3, z).wait_recv()

                v = v + self.via[...].astype(F32)
            self.sent[j][...] = v.astype(BF)
            if j == 0:
                @pl.when(middle)
                def _():
                    self.direct(0).start()

                @pl.when(jnp.logical_not(middle))
                def _():
                    self.copy(0, self.via, 3, dests[2]).start()
            else:
                self.direct(j).start()

        def arrived(self):
            for i in (0, 2):
                self.copy(0, self.got.at[i], i, z).wait_recv()

            @pl.when(jnp.logical_not(middle))
            def _():
                self.copy(0, self.got.at[1], 1, z).wait_recv()

        def left(self):
            for j in range(3):
                self.copy(j, self.via, 3, z).wait_send()

    blocks = [pl.ds(0, BLOCK), pl.ds(BLOCK, BLOCK)]
    out_blocks = Scatter([g.sblk.at[j] for j in range(3)], g.rblk, g.via, 0)
    in_blocks = Scatter(
        [g.gn.at[:, blocks[0]], g.gn.at[:, blocks[1]], g.inner.at[:, blocks[0]]], g.rblk2, g.via2, 4
    )

    @pl.when(middle)
    def _():
        g.rblk[1] = jnp.zeros((ROWS, BLOCK), BF)
        g.rblk2[1] = jnp.zeros((ROWS, BLOCK), BF)

    @pl.when(jnp.logical_not(middle))
    def _():
        g.via[...] = jnp.zeros((ROWS, BLOCK), BF)
        g.via2[...] = jnp.zeros((ROWS, BLOCK), BF)

    def out_block(k):
        return mul(g.gn[...], g.wo[:, cut(k * BLOCK, BLOCK, 128)])

    for d in squares:
        d.wait_recv()
    gscale = lax.rsqrt((g.sqs[0] + g.sqs[1] + g.sqs[2] + g.sqs[3]) / INNER + epsilon)
    g.part[0] = to_col(gscale)

    @pl.when(middle)
    def _():
        for d in x_on:
            d.wait_send()

    def norm_gate(i):
        at = cut(i * 64, 64, 16)
        g.gn[at, :] = (g.gated[at, :] * wide_of(g.part[0, at, :], 6) * gate_gain).astype(BF)

    loop(ROWS // 64, norm_gate)
    out_blocks.block(0, out_block(dests[0]))
    out_blocks.block(1, out_block(dests[1]))
    t_out, t_z, t_xa, t_xb = [
        Total(ref, sum_bufs[5 * i : 5 * i + 5], g.tot_send, g.tot_recv, g.freed, 10 * i, me)
        for i, ref in enumerate((g.p_out, g.p_z, g.p_xa, g.p_xb))
    ]

    def grad_out(n):
        at = cut(n * 256, 256, 256)
        g.p_out[at, :] = mul(g.gn[:, at], g.cotg[...], TN).astype(BF)

    loop(3, grad_out)
    t_out.s0()

    for d in stat:
        d.wait_recv()
    sums = g.stats[0] + g.stats[1] + g.stats[2] + g.stats[3]
    g.part[1] = to_col(gscale * gscale * gscale * sums / INNER)
    g.vacc[...] = jnp.zeros(g.vacc.shape, F32)
    g.pack[...] = jnp.zeros(g.pack.shape, F32)
    g.bcv[z] = jnp.zeros((8, 256), F32)

    def ungate(i):
        at = cut(i * 64, 64, 16)
        a = wide_of(g.part[0, at, :], 6)
        pre = g.acc[at, gate_cols]
        vals = g.inner[at, :].astype(F32)
        mixed = g.out[at, :] + vals * skip
        gated, ggn = g.gated[at, :], g.ggn[at, :]
        gg = a * (ggn * gate_gain) - gated * wide_of(g.part[1, at, :], 6)
        sig = jax.nn.sigmoid(pre)
        gm = (gg * (pre * sig)).astype(BF)
        g.gm[at, :] = gm
        g.gz[at, :] = (gg * mixed * (sig * (1.0 + pre * (1.0 - sig)))).astype(BF)
        g.vacc[0] += rows_sum(ggn * gated * a)
        g.vacc[1] += rows_sum(gm.astype(F32) * vals)

    loop(ROWS // 64, ungate)
    t_out.s1()

    outer(g.ct, g.leadt, g.gm)
    g.mine_b[...] = g.local[0] + c0 * g.local[1]
    behind = Chain(g.mine_b, g.other_b, g.joined_b, (g.low_b, g.far_b), g.got_b, g.chain_b, 4, -1)
    behind.share()

    def grad_z(n):
        at = cut(n * 256, 256, 256)
        g.p_z[at, :] = mul(g.xn[:, at], g.gz[...], TN).astype(BF)

    loop(6, grad_z)
    behind.join()
    t_z.s0()
    g.own[...] = mul(g.gn[...], g.wo[:, own])

    def inside_back(q, first, count):
        rows = cut(q * SPAN, SPAN, 256)
        seg = g.segc[cut(HALO + q * SPAN, SPAN, 16), 0:1]
        segr = g.segr[0:1, cut(q * SPAN, SPAN, 256)]
        mask = (tri_i <= tri_j) & (seg == segr)
        if first == 0:
            g.scores[...] = jnp.where(mask, mul(g.b[rows, :], g.c[rows, :], NT), 0.0)
            g.gscores[...] = jnp.zeros((SPAN, SPAN), F32)

        def pair(t):
            p = first + t
            cols = head_cols(g.cum, rows, p)
            at = cut(p * 128, 128, 128)
            steps = head_cols(g.step, rows, p)
            gm = g.gm[rows, at]
            outs = []
            for e in range(2):
                row = g.cumt[q, pl.ds(2 * p + e, 1), :]
                fall = jnp.exp(jnp.minimum(row - cols[e], 0.0)) * steps[e]
                outs.append(mul((g.scores[...] * fall).astype(BF), gm))
                keep = left if e == 0 else jnp.logical_not(left)
                vals = jnp.where(keep, g.inner[rows, at].astype(F32), 0.0).astype(BF)
                g.gscores[...] += mul(vals, gm, NT) * fall
            g.z[rows, at] = jnp.where(left, outs[0], outs[1])

        loop(count, pair)
        if first + count < 6:
            return
        gs = jnp.where(mask, g.gscores[...], 0.0)
        hi, lo = parts(gs, 2)
        g.gb[rows, :] = mul(hi, g.c[rows, :]) + mul(lo, g.c[rows, :])
        g.gc[rows, :] = mul(hi, g.b[rows, :], TN) + mul(lo, g.b[rows, :], TN)

    inside_back(1, 0, 6)
    inside_back(0, 0, 6)
    t_z.s1()
    arrive(both_down, -1)
    behind.meet(g.boths[1, 0:1, :])
    out_blocks.block(2, out_block(dests[2]))
    t_out.s2()

    behind.end()
    from_chips = g.chain_b[...]
    beyond = jnp.where(core == 1, from_chips, g.other_b[...] + g.decay[1, 0:1] * from_chips)
    g.gloc[1] = beyond
    g.gloc[0] = g.local[1] + c1 * beyond
    ends = []
    for q in range(2):
        rows = pl.ds(q * SPAN, SPAN)
        glow = g.gloc[q].astype(BF)
        vals = g.inner[rows, :].astype(F32)
        gm = g.gm[rows, :].astype(F32)
        loade = spread(g.load[rows, :])
        bg = mul(g.b[rows, :], glow)
        zed = g.z[rows, :]
        carry_sum = jnp.sum(g.gloc[q] * g.sin[q], axis=0, keepdims=True)
        grad_carry = head_sum(jnp.broadcast_to(carry_sum, (8, CHANNELS)))[0:1]
        t1 = head_sum(gm * g.out[rows, :])
        q1 = head_sum(vals * zed)
        q2 = head_sum(vals * bg)
        step, load = g.step[rows, :], g.load[rows, :]
        tail_term = q2 * load
        gcum = t1 - q1 - tail_term
        end = jnp.sum(tail_term, axis=0, keepdims=True) + grad_carry * g.carry[q][0:1]
        is_last = lax.broadcasted_iota(jnp.int32, (SPAN, 128), 0) == SPAN - 1
        gcum = gcum + jnp.where(is_last, end, 0.0)
        glog = sum(mul(g.tri[...], p, TN) for p in parts(gcum, 3))
        gstep = jnp.where(step > 1e-30, q1 / jnp.maximum(step, 1e-30), 0.0) + q2 * g.tail[rows, :]
        gpre = (gstep - rates * glog) * jax.nn.sigmoid(
            g.acc[rows, WIDE + CHANNELS :] + g.params[3:4, 0:128]
        )
        g.gsr[rows, :] = gpre.astype(BF)
        ends.append((rows_sum(gpre), rows_sum(glog * (-rates * step))))
        g.z[rows, :] = zed + loade * bg + skip * gm
        g.gb[rows, :] += sum(mul(p, glow, NT) for p in parts(vals * loade, 2))
        g.gc[rows, :] += sum(mul(p, g.slow[q], NT) for p in parts(gm * spread(g.lead[rows, :]), 2))
    g.pack[16:24, 0:128] = jnp.broadcast_to(
        jnp.sum(ends[0][0] + ends[1][0], axis=0, keepdims=True), (8, 128)
    )
    g.pack[16:24, 128:256] = jnp.broadcast_to(
        jnp.sum(ends[0][1] + ends[1][1], axis=0, keepdims=True), (8, 128)
    )
    def grads_of(at, n):
        cols = pl.ds(n * 256, 256)
        if n < 3:
            v = g.z[at, cols]
        else:
            v = jnp.concatenate([g.gb[at, :], g.gc[at, :]], axis=1)
        return v * g.slope[at, cols]

    def slopes(i):
        at = cut(i * 64, 64, 16)
        for n in range(4):
            g.gconv[cut(i * 64, 64, 8), pl.ds(n * 256, 256)] = grads_of(at, n)

    g.gconv[ROWS : ROWS + 16, :] = jnp.zeros((16, WIDE), F32)
    loop(ROWS // 64, slopes)

    v = g.gconv[0:8, :]
    sv = g.segc[HALO - 8 : HALO + 8, :]
    back_rows = jnp.zeros((8, WIDE), F32)
    for k in range(3):
        shift = 3 - k
        full = jnp.concatenate([jnp.zeros((8, WIDE), F32), v], axis=0)
        src = pltpu.roll(full, 16 - shift, 0)[0:8]
        same = pltpu.roll(sv, 16 - shift, 0)[0:8] == sv[0:8]
        back_rows = back_rows + jnp.where(wide_of(same, 8), g.taps[k : k + 1, :] * src, 0.0)
    g.ret_out[...] = back_rows
    ret = remote(g.ret_out, g.ret_in, g.edge_sem.at[2], g.edge_sem.at[3], {ALONG: s - 1})

    @pl.when(s > 0)
    def _():
        ret.start()

    @pl.when(s == SEQ - 1)
    def _():
        g.ret_in[...] = jnp.zeros((8, WIDE), F32)

    g.wacc[...] = jnp.zeros(g.wacc.shape, F32)

    def convolve_back(i):
        first = i * 64
        at = cut(first, 64, 16)
        sv = g.segc[cut(first + HALO, 64, 8), :]
        ahead = jnp.where(i < ROWS // 64 - 1, 1.0, 0.0)
        for n in range(4):
            cols = pl.ds(n * 256, 256)
            v = g.gconv[cut(first, 72, 8), cols]
            here = v[0:64]
            total = g.taps[3:4, cols] * here
            nxt = g.segc[cut(jnp.minimum(first + HALO + 64, ROWS + HALO - 8), 8, 8), :]
            sfull = jnp.concatenate([sv, nxt], axis=0)
            for k in range(3):
                shift = 3 - k
                same = pltpu.roll(sfull, 72 - shift, 0)[0:64] == sv
                src = pltpu.roll(v, 72 - shift, 0)[0:64]
                total = total + jnp.where(wide_of(same, 2), g.taps[k : k + 1, cols] * src, 0.0)
            if n < 3:
                g.gx[at, cols] = total.astype(BF)
            else:
                for k, v in enumerate(parts(total, 2)):
                    g.gbc[k, at, :] = v

            @pl.when(i == ROWS // 64 - 1)
            def _():
                g.tail_rows[:, cols] = total[48:64]

            for k, t in enumerate(taps_of(first, cols)):
                g.wacc[k, :, cols] += rows_sum(here * t)
            g.wacc[4, :, cols] += rows_sum(here)

    loop(ROWS // 64, convolve_back)
    t_z.s2()

    @pl.when(s < SEQ - 1)
    def _():
        ret.wait_recv()

    last_rows = g.tail_rows[...] + jnp.concatenate([jnp.zeros((8, WIDE), F32), g.ret_in[...]], axis=0)
    g.gx[ROWS - 16 : ROWS, :] = last_rows[:, 0:CHANNELS].astype(BF)
    for k, v in enumerate(parts(last_rows[:, CHANNELS:WIDE], 2)):
        g.gbc[k, ROWS - 16 : ROWS, :] = v

    def bc_block(at):
        both = mul(g.xn[:, at], jnp.concatenate([g.gbc[0], g.gbc[1]], axis=1), TN)
        return both[:, 0:256] + both[:, 256:512]

    for k in range(5):
        row = jnp.sum(g.wacc[k], axis=0, keepdims=True)
        g.pack[k : k + 1, :] = row[:, 0:CHANNELS]
        g.bcv[z, k : k + 1, :] = row[:, CHANNELS:WIDE]
    bcv = [send(g.bcv.at[z], g.bcv.at[z], g.bcvsem, i, p) for i, p in enumerate(zpeers)]
    def grad_x(ref, first):
        def body(n):
            at = cut(n * 256, 256, 256)
            ref[at, :] = mul(g.xn[:, cut(first + n * 256, 256, 256)], g.gx[...], TN).astype(BF)

        loop(3, body)

    grad_x(g.p_xa, 0)
    t_xa.s0()
    grad_x(g.p_xb, CHANNELS)
    t_xb.s0()
    t_out.s3()
    bcs = []
    bc_parts = [g.acc.at[pl.ds(0, BLOCK), pl.ds(WIDE + 256 * i, 256)] for i in range(3)]
    bc_parts.append(g.acc.at[pl.ds(0, BLOCK), pl.ds(BLOCK, 256)])
    mine, other = cut(core * 192, 192, 16), cut((1 - core) * 192, 192, 16)
    halves = []
    for i in range(LINE):
        bc_parts[i][...] = bc_block(cut(lax.rem(z + 1 + i, LINE) * BLOCK, BLOCK, 128))
        halves.append(send(bc_parts[i].at[other], g.hbc.at[i], g.bcsem, 3 + i, partner))
    t_xa.s1()
    t_xb.s1()
    for d in halves:
        d.wait_recv()
    g.bcsum[...] = bc_parts[3][mine, :] + g.hbc[3]
    for i, p in enumerate(zpeers):
        g.tbc[i] = (bc_parts[i][mine, :] + g.hbc[i]).astype(BF)
        bcs.append(send(g.tbc.at[i], g.rbc.at[i], g.bcsem, i, p))

    def back_block(k):
        at = cut(k * BLOCK, BLOCK, 16)
        v = mul(g.gx[...], g.wx[at, :], NT) + mul(g.gz[...], g.wz[at, :], NT)
        return v + mul(g.gsr[...], g.wd[:, cut(k * BLOCK, BLOCK, 128)]) + mul(g.gbc[0], g.wbc[k], NT) + mul(g.gbc[1], g.wbc[k], NT)

    in_blocks.block(0, back_block(dests[0]))
    t_z.s3()
    in_blocks.block(1, back_block(dests[1]))
    t_out.s4()
    g.own_in[...] = back_block(z)
    t_xa.s2()
    t_xb.s2()
    t_z.s4()

    for d in bcs + bcv:
        d.wait_recv()
    g.pack[8:16, 0:256] = g.bcv[0] + g.bcv[1] + g.bcv[2] + g.bcv[3]
    g.pack[5:6, :] = jnp.sum(g.vacc[0], axis=0, keepdims=True)
    skips = head_sum(jnp.broadcast_to(jnp.sum(g.vacc[1], axis=0, keepdims=True), (8, CHANNELS)))
    g.pack[16:24, 256:384] = skips
    bc = g.bcsum[...]
    for i in range(3):
        bc = bc + g.rbc[i].astype(F32)
    g.q_out[0:192, :] = bc.astype(BF)
    for n in range(6):
        cols = pl.ds(256 * n, 256)
        g.few[16 * n : 16 * n + 16, :] = mul(g.gsr[...], g.xn[:, cols], TN)[0:16]
    for n in range(3):
        g.few[96 + 24 * n : 120 + 24 * n, :] = g.pack[:, 256 * n : 256 * n + 256]
    g.few[168:192, :] = jnp.zeros((24, 256), F32)
    few = send(g.few, g.few_in, g.restsem, 0, partner)
    in_blocks.block(2, back_block(dests[2]))
    t_xa.s3()
    few.wait_recv()
    few_half = cut(96 * core, 96, 8)
    g.q_out[192:288, :] = (g.few[few_half, :] + g.few_in[few_half, :]).astype(BF)
    across_x = send(g.q_out, g.q_in.at[0], g.restsem, 1, {ALONG: s + 2 - 4 * me[1]})
    t_xb.s3()
    t_xa.s4()
    across_x.wait_recv()
    g.q_mid[...] = (g.q_out[...].astype(F32) + g.q_in[0].astype(F32)).astype(BF)
    across_y = send(g.q_mid, g.q_in.at[1], g.restsem, 2, {ALONG: s + 4 - 8 * me[2]})
    t_xb.s4()
    t_out.s5()
    out_blocks.arrived()
    out_sum = g.own[...]
    for i in range(3):
        out_sum = out_sum + g.rblk[i].astype(F32)
    g.layer_out[...] = (g.x[...].astype(F32) + out_sum).astype(BF)

    in_blocks.arrived()
    g.nacc[...] = jnp.zeros(g.nacc.shape, F32)

    def finish(i):
        at = cut(i * 64, 64, 16)
        v = g.own_in[at, :]
        for k in range(3):
            v = v + g.rblk2[k, at, :].astype(F32)
        g.own_in[at, :] = v
        x = g.x[at, :].astype(F32)
        g.part[0, at, :] = lanes_sum(v * gain * x)
        g.nacc[...] += rows_sum(v * x * wide_of(g.xscale[at, :], 3))

    loop(ROWS // 64, finish)
    g.nstat[z] = to_row(g.part[0])
    nst = [send(g.nstat.at[z], g.nstat.at[z], g.nsem, i, p) for i, p in enumerate(zpeers)]
    g.ngain[0] = jnp.sum(g.nacc[...], axis=0, keepdims=True)
    ngs = [send(g.ngain.at[0], g.ngain.at[1 + i], g.nsem, 3 + i, p) for i, p in enumerate(speers)]
    t_z.s5()
    t_xa.s5()
    t_xb.s5()
    across_y.wait_recv()
    g.rest[core] = g.q_mid[...].astype(F32) + g.q_in[1].astype(F32)
    q_last = send(g.rest.at[core], g.rest.at[core], g.restsem, 3, partner)
    t_out.s6()
    store = [pltpu.make_async_copy(g.p_out, g.grad_out, g.load_sem.at[5])]
    store[0].start()
    t_z.s6()
    store.append(pltpu.make_async_copy(g.p_z, g.grad_z, g.load_sem.at[6]))
    store[1].start()
    for d in nst:
        d.wait_recv()
    rows = g.nstat[0] + g.nstat[1] + g.nstat[2] + g.nstat[3]
    g.part[0] = to_col(rows / D)

    def last(i):
        at = cut(i * 64, 64, 16)
        sc = wide_of(g.xscale[at, :], 3)
        x = g.x[at, :].astype(F32)
        g.grad_in[at, :] = (
            g.cotg[at, own].astype(F32)
            + sc * (g.own_in[at, :] * gain)
            - x * (sc * sc * sc * wide_of(g.part[0, at, :], 3))
        )

    loop(ROWS // 64, last)
    for d in ngs:
        d.wait_recv()
    total = g.ngain[0]
    for i in range(7):
        total = total + g.ngain[1 + i]
    g.grad_gain[...] = jnp.broadcast_to(total, (8, BLOCK))
    q_last.wait_recv()
    for i, (t, ref) in enumerate(((t_xa, g.p_xa), (t_xb, g.p_xb))):
        t.s6()
        rows_of = pl.ds(CHANNELS * i, CHANNELS)
        store.append(pltpu.make_async_copy(ref, g.grad_x.at[rows_of], g.load_sem.at[7 + i]))
        store[-1].start()
    for d in pending:
        d.wait_send()

    @pl.when(s < SEQ - 1)
    def _():
        edge.wait_send()

    @pl.when(s > 0)
    def _():
        ret.wait_send()

    x_own[0].wait_send()

    @pl.when(middle)
    def _():
        x_own[1].wait_send()

    for inside_it, d in later:
        @pl.when(inside_it)
        def _():
            d.wait_send()

    out_blocks.left()
    in_blocks.left()
    for d in store:
        d.wait()


def unpack_kernel(
    layer_hbm, in_hbm, out_low, z_low, x_low, rest_hbm, gain_sum,
    layer_out, grad_in, gain, w_z, w_x, w_bc, w_dt, conv_x_w, conv_x_b, conv_bc_w, conv_bc_b, dt_bias, a_log, d_skip, gate_gain, w_out,
    low_a, low_b, low_c, full_a, full_b, full_c, keep_a, keep_b, rest, bc_rows, in_sem, out_sem,
):
    steps = 3
    mats = [(out_low, low_a, full_a, w_out), (z_low, low_b, full_b, w_z), (x_low, low_c, full_c, w_x)]
    loads, stores = [], []
    for m, (src, low, _, _) in enumerate(mats):
        n = low.shape[0] // steps
        for i in range(steps):
            at = pl.ds(i * n, n)
            loads.append(pltpu.make_async_copy(src.at[at], low.at[at], in_sem.at[steps * m + i]))
    for i, (src, dst) in enumerate([(layer_hbm, keep_a), (in_hbm, keep_b), (rest_hbm, rest)]):
        loads.append(pltpu.make_async_copy(src, dst, in_sem.at[9 + i]))
    for d in loads:
        d.start()
    for m, (_, low, full, dst) in enumerate(mats):
        n = low.shape[0] // steps
        for i in range(steps):
            loads[steps * m + i].wait()
            at = pl.ds(i * n, n)
            full[at, :] = low[at, :].astype(F32)
            stores.append(pltpu.make_async_copy(full.at[at], dst.at[at], out_sem.at[steps * m + i]))
            stores[-1].start()
    for i, (src, dst) in enumerate([(keep_a, layer_out), (keep_b, grad_in)]):
        loads[9 + i].wait()
        stores.append(pltpu.make_async_copy(src, dst, out_sem.at[9 + i]))
        stores[-1].start()
    loads[11].wait()
    for n in range(3):
        gain[n : n + 1, :] = gain_sum[0:1, 128 * n : 128 * n + 128]
    bc_rows[0:192, :] = rest[0, 0:192, :]
    bc_rows[192:BLOCK, :] = rest[1, 0:192, :]
    stores.append(pltpu.make_async_copy(bc_rows, w_bc, out_sem.at[11]))
    stores[-1].start()
    for n in range(6):
        w_dt[:, 256 * n : 256 * n + 256] = rest[0, 192 + 16 * n : 204 + 16 * n, :]
    for n in range(3):
        at, base = pl.ds(256 * n, 256), 192 + 24 * n
        conv_x_w[:, at] = rest[1, base : base + 4, :]
        for e in range(2):
            lanes, to = pl.ds(128 * e, 128), pl.ds(2 * n + e, 1)
            conv_x_b[to, :] = rest[1, base + 4 : base + 5, lanes]
            gate_gain[to, :] = rest[1, base + 5 : base + 6, lanes]
    conv_bc_w[...] = rest[1, 200:204, :]
    for e in range(2):
        conv_bc_b[e : e + 1, :] = rest[1, 204:205, 128 * e : 128 * e + 128]
    dt_bias[...] = rest[1, 208:209, 0:12]
    a_log[...] = rest[1, 208:209, 128:140]
    d_skip[...] = rest[1, 232:233, 0:12]
    for d in stores:
        d.wait()


def fast_layer(
    hidden_in, seq_lengths, norm_gain, w_z, w_x, w_bc, w_dt, conv_x_w, conv_x_b, conv_bc_w,
    conv_bc_b, dt_bias, a_log, d_skip, gate_gain, w_out, cotangent,
):
    row = lambda v: v.reshape(-1, min(128, v.shape[0]))
    vm = pl.BlockSpec(memory_space=pltpu.VMEM)
    hbm = pl.BlockSpec(memory_space=pltpu.HBM)
    sm = pl.BlockSpec(memory_space=pltpu.SMEM)
    ins = dict(
        x_hbm=(hidden_in, hbm), cot_hbm=(cotangent, hbm), w_x=(w_x, hbm), w_z=(w_z, hbm), w_out=(w_out, hbm),
        lengths=(seq_lengths, sm), norm_gain=(row(norm_gain), vm), conv_x_b=(row(conv_x_b), vm),
        conv_bc_b=(row(conv_bc_b), vm), dt_bias=(row(dt_bias), vm), a_log=(row(a_log), vm), d_skip=(row(d_skip), vm),
        gate_gain=(row(gate_gain), vm), w_bc=(w_bc, vm), w_dt=(w_dt.T, vm),
        conv_x_w=(conv_x_w, vm), conv_bc_w=(conv_bc_w, vm),
    )
    outs = dict(
        layer_out=((ROWS, BLOCK), BF, vm),
        grad_in=((ROWS, BLOCK), F32, vm),
        grad_out=((CHANNELS, D), BF, hbm),
        grad_z=((D, CHANNELS), BF, hbm),
        grad_x=((D, CHANNELS), BF, hbm),
        rest=((2, 288, 256), F32, vm),
        grad_gain=((8, BLOCK), F32, vm),
    )
    V = pltpu.VMEM
    S = pltpu.SemaphoreType.DMA
    scr = dict(
        x=V((ROWS, BLOCK), BF),
        wx=V((D, CHANNELS), BF),
        wz=V((D, CHANNELS), BF),
        wo=V((CHANNELS, D), BF),
        xg=V((ROWS, D), BF),
        xn=V((ROWS, D), BF),
        cotg=V((ROWS, D), BF),
        ssq=V((LINE, 1, ROWS), F32),
        gains=V((LINE, 1, BLOCK), F32),
        wbc=V((LINE, BLOCK, 256), BF),
        wd=V((128, D), BF),
        params=V((8, CHANNELS), F32),
        taps=V((8, WIDE), F32),
        spread=V((256, CHANNELS), BF),
        segc=V((ROWS + HALO, 128), F32),
        segr=V((8, ROWS), F32),
        tri=V((SPAN, SPAN), BF),
        skipe=V((8, CHANNELS), F32),
        xscale=V((ROWS, 128), F32),
        acc=V((ROWS, WIDE + CHANNELS + 128), F32),
        edge=V((HALO, WIDE), BF),
        halo=V((HALO, WIDE), BF),
        cf=V((ROWS + HALO, WIDE), F32),
        step=V((ROWS, 128), F32),
        cum=V((ROWS, 128), F32),
        cumt=V((2, 16, SPAN), F32),
        tail=V((ROWS, 128), F32),
        load=V((ROWS, 128), F32),
        lead=V((ROWS, 128), F32),
        carry=V((2, 8, 128), F32),
        carrye=V((2, 8, CHANNELS), F32),
        decay=V((2, 8, CHANNELS), F32),
        slope=V((ROWS + 16, WIDE), F32),
        inner=V((ROWS, CHANNELS), BF),
        b=V((ROWS, 128), BF),
        c=V((ROWS, 128), BF),
        bt=V((STATE, ROWS), F32),
        ct=V((STATE, ROWS), F32),
        loadt=V((2, 16, SPAN), F32),
        leadt=V((2, 16, SPAN), F32),
        stept=V((2, 16, SPAN), F32),
        local=V((2, STATE, CHANNELS), F32),
        mine=V((STATE, CHANNELS), F32),
        other=V((STATE, CHANNELS), F32),
        joined=V((STATE, BLOCK), F32),
        got=V((2, STATE, BLOCK), F32),
        chain=V((STATE, CHANNELS), F32),
        mine_b=V((STATE, CHANNELS), F32),
        other_b=V((STATE, CHANNELS), F32),
        joined_b=V((STATE, BLOCK), F32),
        got_b=V((STATE, BLOCK), F32),
        low_b=V((STATE, BLOCK), BF),
        far_b=V((STATE, BLOCK), BF),
        chain_b=V((STATE, CHANNELS), F32),
        both=V((8, BLOCK), F32),
        boths=V((2, 8, BLOCK), F32),
        scores=V((SPAN, SPAN), F32),
        gscores=V((SPAN, SPAN), F32),
        out=V((ROWS, CHANNELS), F32),
        sin=V((2, STATE, CHANNELS), F32),
        slow=V((2, STATE, CHANNELS), BF),
        gated=V((ROWS, CHANNELS), F32),
        part=V((2, ROWS, 128), F32),
        stats=V((LINE, 1, ROWS), F32),
        sqs=V((LINE, 1, ROWS), F32),
        vacc=V((2, 8, CHANNELS), F32),
        gm=V((ROWS, CHANNELS), BF),
        gloc=V((2, STATE, CHANNELS), F32),
        sblk=V((3, ROWS, BLOCK), BF),
        rblk=V((3, ROWS, BLOCK), BF),
        rblk2=V((3, ROWS, BLOCK), BF),
        gsr=V((ROWS, 128), BF),
        pack=V((24, CHANNELS), F32),
        ret_out=V((8, WIDE), F32),
        ret_in=V((8, WIDE), F32),
        wacc=V((5, 8, WIDE), F32),
        gbc=V((2, ROWS, 256), BF),
        tail_rows=V((16, WIDE), F32),
        hbc=V((LINE, 192, 256), F32),
        tbc=V((3, 192, 256), BF),
        rbc=V((3, 192, 256), BF),
        via=V((ROWS, BLOCK), BF),
        via2=V((ROWS, BLOCK), BF),
        bcv=V((LINE, 8, 256), F32),
        nacc=V((8, BLOCK), F32),
        nstat=V((LINE, 1, ROWS), F32),
        ngain=V((8, 1, BLOCK), F32),
        p_out=V((CHANNELS, D), BF),
        p_z=V((D, CHANNELS), BF),
        p_xa=V((CHANNELS, CHANNELS), BF),
        p_xb=V((CHANNELS, CHANNELS), BF),
        bcsum=V((192, 256), F32),
        few=V((192, 256), F32),
        few_in=V((192, 256), F32),
        q_out=V((288, 256), BF),
        q_mid=V((288, 256), BF),
        q_in=V((2, 288, 256), BF),
        load_sem=S((9,)),
        edge_sem=S((4,)),
        gather_s=S((8,)),
        gather_r=S((9,)),
        block_s=S((8,)),
        block_r=S((8,)),
        st_send=S((11,)),
        st_recv=S((11,)),
        tot_send=S((40,)),
        tot_recv=S((40,)),
        freed=pltpu.SemaphoreType.REGULAR((12,)),
    )
    pairs = dict(
        small=9,
        wide=4,
        stat=3,
        sqsem=3,
        bcsem=7,
        restsem=4,
        bcvsem=3,
        nsem=10,
    )
    sums = [(CHANNELS, D, BF), (D, CHANNELS, BF), (CHANNELS, CHANNELS, BF), (CHANNELS, CHANNELS, BF)]
    bufs = [b for spec in sums for b in total_bufs(*spec)]
    sems = [S((k,)) for k in pairs.values() for _ in range(2)]
    names = [*ins, *outs, *scr]

    def kernel(*refs):
        n, m = len(names), len(names) + len(bufs)
        d = dict(zip(names, refs[:n]))
        rest = refs[m:]
        for i, name in enumerate(pairs):
            d[name] = (rest[2 * i], rest[2 * i + 1])
        layer_kernel(d, refs[n:m])

    res = pl.pallas_call(
        kernel,
        out_shape=[jax.ShapeDtypeStruct(sh, dt) for sh, dt, _ in outs.values()],
        in_specs=[sp for _, sp in ins.values()],
        out_specs=[sp for _, _, sp in outs.values()],
        scratch_shapes=[*scr.values(), *bufs, *sems],
        compiler_params=pltpu.CompilerParams(collective_id=0, has_side_effects=True, vmem_limit_bytes=66 * 2**20 - 2**21),
        name="layer",
    )(*[a for a, _ in ins.values()])
    layer_out, grad_in, grad_out, grad_z, grad_x, rest, grad_gain = res
    shapes = dict(
        layer_out=((ROWS, BLOCK), BF, hbm), grad_in=((ROWS, BLOCK), F32, hbm), gain=((3, 128), F32, vm), w_z=((D, CHANNELS), F32, hbm),
        w_x=((D, CHANNELS), F32, hbm), w_bc=((BLOCK, 256), F32, hbm), w_dt=((12, D), F32, vm), conv_x_w=((4, CHANNELS), F32, vm),
        conv_x_b=((6, 128), F32, vm), conv_bc_w=((4, 256), F32, vm), conv_bc_b=((2, 128), F32, vm), dt_bias=((1, 12), F32, vm),
        a_log=((1, 12), F32, vm), d_skip=((1, 12), F32, vm), gate_gain=((6, 128), F32, vm), w_out=((CHANNELS, D), F32, hbm),
    )
    final = pl.pallas_call(
        unpack_kernel,
        out_shape=[jax.ShapeDtypeStruct(sh, dt) for sh, dt, _ in shapes.values()],
        in_specs=[hbm] * 6 + [vm],
        out_specs=[sp for _, _, sp in shapes.values()],
        scratch_shapes=[
            V((CHANNELS, D), BF), V((D, CHANNELS), BF), V((D, CHANNELS), BF),
            V((CHANNELS, D), F32), V((D, CHANNELS), F32), V((D, CHANNELS), F32),
            V((ROWS, BLOCK), BF), V((ROWS, BLOCK), F32), V((2, 288, 256), F32), V((BLOCK, 256), F32), S((12,)), S((12,)),
        ],
        compiler_params=pltpu.CompilerParams(vmem_limit_bytes=63 * 2**20),
    )(layer_out, grad_in, grad_out, grad_z, grad_x, rest, grad_gain)
    flat = [v.reshape(v.size) if v.shape[1] <= 128 else v for v in final]
    flat[6] = flat[6].T
    return tuple(flat)


def solution(mesh):
    placed = (
        P("seq", "head"),
        P(),
        P("head"),
        P(None, "head"),
        P(None, "head"),
        P("head", None),
        P(None, "head"),
        P(None, "head"),
        P("head"),
        P(),
        P(),
        P("head"),
        P("head"),
        P("head"),
        P("head"),
        P("head", None),
        P("seq", "head"),
    )
    fits = mesh.shape["seq"] == SEQ and mesh.shape["head"] == LINE
    return jax.shard_map(
        fast_layer if fits else on_device,
        mesh=mesh,
        in_specs=placed,
        out_specs=(
            P("seq", "head"),
            P("seq", "head"),
            P("head"),
            P(None, "head"),
            P(None, "head"),
            P("head", None),
            P(None, "head"),
            P(None, "head"),
            P("head"),
            P(),
            P(),
            P("head"),
            P("head"),
            P("head"),
            P("head"),
            P("head", None),
        ),
        check_vma=False,
    )
```
